32 devices in a mesh: rep: 4 (over x, y), dp: 8 (over z, core).
Axes of the slice: x: 2, y: 2, z: 4, core: 2. Of those that a mesh axis runs over, the one named last changes fastest.
Arguments:
- x: bfloat16 [32, 1024, 896], P(('rep', 'dp')), parts along dimension 0
- dy: bfloat16 [32, 1024, 896], P(('rep', 'dp')), parts along dimension 0
- wq: bfloat16 [2, 896, 1024], replicated
- wk: bfloat16 [2, 896, 512], replicated
- wv: bfloat16 [2, 896, 512], replicated
- wo: bfloat16 [2, 1024, 896], replicated
- w_gate: bfloat16 [2, 896, 3584], replicated
- w_up: bfloat16 [2, 896, 3584], replicated
- w_down: bfloat16 [2, 3584, 896], replicated
- m_wq: float32 [2, 896, 1024], P(None, 'dp')
- m_wk: float32 [2, 896, 512], P(None, 'dp')
- m_wv: float32 [2, 896, 512], P(None, 'dp')
- m_wo: float32 [2, 1024, 896], P(None, 'dp')
- m_w_gate: float32 [2, 896, 3584], P(None, 'dp')
- m_w_up: float32 [2, 896, 3584], P(None, 'dp')
- m_w_down: float32 [2, 3584, 896], P(None, 'dp')
- v_wq: float32 [2, 896, 1024], P(None, 'dp')
- v_wk: float32 [2, 896, 512], P(None, 'dp')
- v_wv: float32 [2, 896, 512], P(None, 'dp')
- v_wo: float32 [2, 1024, 896], P(None, 'dp')
- v_w_gate: float32 [2, 896, 3584], P(None, 'dp')
- v_w_up: float32 [2, 896, 3584], P(None, 'dp')
- v_w_down: float32 [2, 3584, 896], P(None, 'dp')
Outputs:
- output 1: bfloat16 [8, 896, 1024], P('rep'), parts along dimension 0
- output 2: bfloat16 [8, 896, 512], P('rep'), parts along dimension 0
- output 3: bfloat16 [8, 896, 512], P('rep'), parts along dimension 0
- output 4: bfloat16 [8, 1024, 896], P('rep'), parts along dimension 0
- output 5: bfloat16 [8, 896, 3584], P('rep'), parts along dimension 0
- output 6: bfloat16 [8, 896, 3584], P('rep'), parts along dimension 0
- output 7: bfloat16 [8, 3584, 896], P('rep'), parts along dimension 0
- output 8: float32 [8, 896, 1024], P('rep', 'dp'), parts along dimension 0
- output 9: float32 [8, 896, 512], P('rep', 'dp'), parts along dimension 0
- output 10: float32 [8, 896, 512], P('rep', 'dp'), parts along dimension 0
- output 11: float32 [8, 1024, 896], P('rep', 'dp'), parts along dimension 0
- output 12: float32 [8, 896, 3584], P('rep', 'dp'), parts along dimension 0
- output 13: float32 [8, 896, 3584], P('rep', 'dp'), parts along dimension 0
- output 14: float32 [8, 3584, 896], P('rep', 'dp'), parts along dimension 0
- output 15: float32 [8, 896, 1024], P('rep', 'dp'), parts along dimension 0
- output 16: float32 [8, 896, 512], P('rep', 'dp'), parts along dimension 0
- output 17: float32 [8, 896, 512], P('rep', 'dp'), parts along dimension 0
- output 18: float32 [8, 1024, 896], P('rep', 'dp'), parts along dimension 0
- output 19: float32 [8, 896, 3584], P('rep', 'dp'), parts along dimension 0
- output 20: float32 [8, 896, 3584], P('rep', 'dp'), parts along dimension 0
- output 21: float32 [8, 3584, 896], P('rep', 'dp'), parts along dimension 0
There are 4 independent parts. The reference program is written for one: setup_inputs(seed, part) draws one part's arguments, and reference() takes and returns one part's arrays. A program takes and returns all parts, laid end to end along the dimension named above; an argument that names none is the same for every part.
All inputs are finite; a program needn't handle non-finite values.
Results may differ from the reference program's by a relative error of at most 0.024.
Values are sent between devices in bfloat16 or wider.
A program may use at most 2 GiB of HBM per device.

```python
import jax
import jax.numpy as jnp
from jax import lax

SEQUENCES = 8
TOKENS = 1024
D = 896
HEADS = 4
KV_HEADS = 2
HEAD = 256
FF = 3584
LAYERS = 2
THETA = 10000
NAMES = ("wq", "wk", "wv", "wo", "w_gate", "w_up", "w_down")
SHAPES = {
    "wq": (LAYERS, D, HEADS * HEAD),
    "wk": (LAYERS, D, KV_HEADS * HEAD),
    "wv": (LAYERS, D, KV_HEADS * HEAD),
    "wo": (LAYERS, HEADS * HEAD, D),
    "w_gate": (LAYERS, D, FF),
    "w_up": (LAYERS, D, FF),
    "w_down": (LAYERS, FF, D),
}


def bump(key, n, height):
    away = (jnp.arange(n, dtype=jnp.int32) - jax.random.randint(key, (), 0, n, jnp.int32)) % n
    return jnp.where(away < n // 8, height, 1.0)


def together(key, own, strength):
    shared = jax.random.normal(key, own.shape[1:], jnp.float32)
    return (own + strength * shared) * lax.rsqrt(1 + strength * strength)


def setup_inputs(seed: int = 0, part: int = 0) -> dict:
    kx, kdy, ka, kb, kz, kf, kh, kl, *keys = jax.random.split(jax.random.key(seed), 8 + 3 * len(NAMES))
    kx, kdy, ka, kb = (jax.random.fold_in(k, part) for k in (kx, kdy, ka, kb))
    kw, km, kv = (keys[i::3] for i in range(3))
    shape = (SEQUENCES, TOKENS, D)
    much_x, much_dy = jax.random.uniform(kz, (2,), jnp.float32, 0.0, 1.0)
    loud = 2.0 ** jax.random.uniform(jax.random.fold_in(kz, 1), (), jnp.float32, -1.0, 2.0)
    layers = 2.0 ** jax.random.uniform(kl, (LAYERS, 1, 1), jnp.float32, -1.0, 1.0)
    times = {"wq": 1.0, "wk": 1.0, "wv": 2.0, "wo": layers, "w_gate": 1.0, "w_up": bump(kh, FF, 4.0), "w_down": layers}
    x = together(ka, jax.random.normal(kx, shape, jnp.float32), much_x) * bump(kf, D, 4.0)
    dy = together(kb, jax.random.normal(kdy, shape, jnp.float32), much_dy)
    drawn = {"x": x.astype(jnp.bfloat16), "dy": (loud * dy * (SEQUENCES * TOKENS) ** -0.5).astype(jnp.bfloat16)}
    for key, name in zip(kw, NAMES, strict=True):
        drawn[name] = (jax.random.normal(key, SHAPES[name], jnp.float32) * SHAPES[name][1] ** -0.5 * times[name]).astype(jnp.bfloat16)
    for key, name in zip(km, NAMES, strict=True):
        drawn[f"m_{name}"] = 0.1 * jax.random.normal(key, SHAPES[name], jnp.float32)
    for key, name in zip(kv, NAMES, strict=True):
        drawn[f"v_{name}"] = loud * loud * jax.random.uniform(key, SHAPES[name], jnp.float32, 0.2, 0.6)
    return drawn


def matmul(a, w):
    return jnp.dot(a, w, preferred_element_type=jnp.float32).astype(jnp.bfloat16)


def normed(h):
    wide = h.astype(jnp.float32)
    scale = lax.rsqrt(jnp.mean(wide**2, -1, keepdims=True) + 1e-6)
    return (wide * scale).astype(jnp.bfloat16)


def turned(t, theta):
    half = t.shape[-1] // 2
    angle = jnp.arange(t.shape[0], dtype=jnp.float32)[:, None] * theta ** (-jnp.arange(half, dtype=jnp.float32) / half)
    cos, sin = jnp.cos(angle)[:, None], jnp.sin(angle)[:, None]
    a, b = t[..., :half].astype(jnp.float32), t[..., half:].astype(jnp.float32)
    return jnp.concatenate([a * cos - b * sin, b * cos + a * sin], -1).astype(jnp.bfloat16)


def seen_by(q, k, v):
    tokens, kv = q.shape[0], k.shape[1]
    q = q.reshape(tokens, kv, -1, q.shape[-1])
    scores = jnp.einsum("tgsd,ugd->gstu", q.astype(jnp.float32), k.astype(jnp.float32)) * q.shape[-1] ** -0.5
    place = jnp.arange(tokens)
    weights = jax.nn.softmax(jnp.where(place[:, None] >= place, scores, -jnp.inf), -1).astype(jnp.bfloat16)
    return jnp.einsum("gstu,ugd->tgsd", weights.astype(jnp.float32), v.astype(jnp.float32)).astype(jnp.bfloat16).reshape(tokens, -1)


def layer(h, w):
    a = normed(h)
    q, k = (turned(matmul(a, w[name]).reshape(h.shape[0], -1, HEAD), THETA) for name in ("wq", "wk"))
    h = h + matmul(seen_by(q, k, matmul(a, w["wv"]).reshape(h.shape[0], -1, HEAD)), w["wo"])
    b = normed(h)
    gate = jnp.dot(b, w["w_gate"], preferred_element_type=jnp.float32)
    up = jnp.dot(b, w["w_up"], preferred_element_type=jnp.float32)
    return h + matmul((jax.nn.silu(gate) * up).astype(jnp.bfloat16), w["w_down"])


def adamw(w, m, v, g):
    m = 0.9 * m + 0.1 * g
    v = 0.95 * v + 0.05 * g * g
    step = m * lax.rsqrt(v + 1e-8) + 0.1 * w
    return (w - 0.02 * step).astype(jnp.bfloat16), m, v


def stack(weights, h):
    return lax.scan(lambda h, w: (layer(h, w), None), h, weights)[0]


def reference(x, dy, wq, wk, wv, wo, w_gate, w_up, w_down, m_wq, m_wk, m_wv, m_wo, m_w_gate, m_w_up, m_w_down, v_wq, v_wk, v_wv, v_wo, v_w_gate, v_w_up, v_w_down):
    weights = dict(zip(NAMES, (wq, wk, wv, wo, w_gate, w_up, w_down), strict=True))

    def take(so_far, sequence):
        h, by_y = sequence
        _, back = jax.vjp(stack, weights, h)
        by_weights, by_h = back(by_y)
        return jax.tree.map(lambda total, term: total + term.astype(jnp.float32), so_far, by_weights), by_h

    none_yet = {name: jnp.zeros(w.shape, jnp.float32) for name, w in weights.items()}
    by_weights, by_x = lax.scan(take, none_yet, (x, dy))
    gradients = [by_weights[name].astype(jnp.bfloat16).astype(jnp.float32) for name in NAMES]
    first = (m_wq, m_wk, m_wv, m_wo, m_w_gate, m_w_up, m_w_down)
    second = (v_wq, v_wk, v_wv, v_wo, v_w_gate, v_w_up, v_w_down)
    new = [adamw(weights[name].astype(jnp.float32), m, v, g) for name, m, v, g in zip(NAMES, first, second, gradients, strict=True)]
    return tuple(one[which] for which in range(3) for one in new)
```

```python
import functools

import jax
import jax.numpy as jnp
from jax import lax
from jax.experimental import pallas as pl
from jax.experimental.pallas import tpu as pltpu
from jax.sharding import PartitionSpec as P

LOG2E = 1.4426950408889634
HIDDEN = -2e30
VMEM = 56 * 2**20
F32, BF16 = jnp.float32, jnp.bfloat16
MESH = pl.DeviceIdType.MESH
T, D, FF, HEADS, KV, HEAD = 1024, 896, 3584, 4, 2, 256
THETA = 10000
NAMES = ("wq", "wk", "wv", "wo", "w_gate", "w_up", "w_down")
ROWS = 256
TF = 512


def dot(a, b):
    return jnp.dot(a, b, preferred_element_type=F32)


def dot_t(a, b):
    return lax.dot_general(a, b, (((1,), (1,)), ((), ())), preferred_element_type=F32)


def _scale(wide):
    return lax.rsqrt(jnp.mean(wide * wide, -1, keepdims=True) + 1e-6)


def _norm_back(h, by):
    s = _scale(h)
    return by * s - h * (s * s * s * jnp.mean(by * h, -1, keepdims=True))


E = HEAD**-0.5 * LOG2E
GROUP = HEADS // KV
PIECES = T // ROWS


def _piece(i):
    return slice(ROWS * i, ROWS * (i + 1))


def _side(ref, i):
    return jnp.concatenate([ref[n, _piece(i), :] for n in range(GROUP)], axis=0)


def _line(ref, i):
    return jnp.concatenate([ref[0, n : n + 1, _piece(i)] for n in range(GROUP)], axis=1)


def _visible():
    shape = (ROWS, GROUP * ROWS)
    return lax.broadcasted_iota(jnp.int32, shape, 0) <= lax.rem(lax.broadcasted_iota(jnp.int32, shape, 1), ROWS)


def _attend(q_ref, k_ref, v_ref, o_ref, ot_ref, lse_ref):
    seen = _visible()
    turned = v_ref[0].T
    for i in range(PIECES):
        q = _side(q_ref, i)
        scores = [dot_t(k_ref[0, _piece(j), :], q) for j in range(i + 1)]
        scores[i] = jnp.where(seen, scores[i], HIDDEN)
        top = functools.reduce(jnp.maximum, [s.max(axis=0, keepdims=True) for s in scores])
        total, mix = 0.0, 0.0
        for j, s in enumerate(scores):
            p = jnp.exp2((s - top) * E)
            total = total + p.sum(axis=0, keepdims=True)
            mix = mix + dot(turned[:, _piece(j)], p.astype(BF16))
        out = (mix * (1.0 / total)).astype(BF16)
        lse = top * E + jnp.log(total) * LOG2E
        for n in range(GROUP):
            ot_ref[HEAD * n : HEAD * (n + 1), _piece(i)] = out[:, _piece(n)]
            o_ref[n, _piece(i), :] = out[:, _piece(n)].T
            lse_ref[0, n : n + 1, _piece(i)] = lse[:, _piece(n)]


def _attend_back(q_ref, k_ref, v_ref, do_ref, lse_ref, delta_ref, dq_ref, dk_ref, dv_ref, dk_s, dv_s):
    seen = _visible()
    turned = k_ref[0].T
    for i in range(PIECES):
        q, do, lse, delta = _side(q_ref, i), _side(do_ref, i), _line(lse_ref, i), _line(delta_ref, i)
        dq = 0.0
        for j in range(i + 1):
            at = _piece(j)
            p = jnp.exp2(dot_t(k_ref[0, at, :], q) * E - lse)
            if j == i:
                p = jnp.where(seen, p, 0.0)
            ds = (p * (dot_t(v_ref[0, at, :], do) - delta)).astype(BF16)
            by_v, by_k = dot(p.astype(BF16), do), dot(ds, q)
            dv_s[at, :] = by_v if j == i else dv_s[at, :] + by_v
            dk_s[at, :] = by_k if j == i else dk_s[at, :] + by_k
            dq = dq + dot(turned[:, at], ds)
        dq = (dq * HEAD**-0.5).astype(BF16)
        for n in range(GROUP):
            dq_ref[n, _piece(i), :] = dq[:, _piece(n)].T
    dk_ref[0] = (dk_s[...] * HEAD**-0.5).astype(BF16)
    dv_ref[0] = dv_s[...].astype(BF16)


QUERIES, KEYS, LINES = (pl.BlockSpec(shape, lambda i: (i, 0, 0)) for shape in ((GROUP, T, HEAD), (1, T, HEAD), (1, GROUP, T)))


def attend(q, k, v):
    return pl.pallas_call(
        _attend,
        grid=(KV,),
        in_specs=[QUERIES, KEYS, KEYS],
        out_specs=[QUERIES, pl.BlockSpec((GROUP * HEAD, T), lambda i: (i, 0)), LINES],
        out_shape=[jax.ShapeDtypeStruct(q.shape, BF16), jax.ShapeDtypeStruct((HEADS * HEAD, T), BF16), jax.ShapeDtypeStruct((KV, GROUP, T), F32)],
        compiler_params=pltpu.CompilerParams(vmem_limit_bytes=VMEM),
        name="attend",
    )(q, k, v)


def attend_back(q, k, v, do, lse, delta):
    return pl.pallas_call(
        _attend_back,
        grid=(KV,),
        in_specs=[QUERIES, KEYS, KEYS, QUERIES, LINES, LINES],
        out_specs=[QUERIES, KEYS, KEYS],
        out_shape=[jax.ShapeDtypeStruct(t.shape, BF16) for t in (q, k, v)],
        scratch_shapes=[pltpu.VMEM((T, HEAD), F32), pltpu.VMEM((T, HEAD), F32)],
        compiler_params=pltpu.CompilerParams(vmem_limit_bytes=VMEM),
        name="attend_back",
    )(q, k, v, do, lse, delta)


def _before(h_ref, wq_ref, wk_ref, wv_ref, cos_ref, sin_ref, q_ref, k_ref, v_ref, at_ref):
    wide = h_ref[...].astype(F32)
    a = (wide * _scale(wide)).astype(BF16)
    at_ref[...] = a.T
    cos, sin = cos_ref[...], sin_ref[...]
    half = HEAD // 2
    for out, w, heads, turn in ((q_ref, wq_ref, HEADS, True), (k_ref, wk_ref, KV, True), (v_ref, wv_ref, KV, False)):
        t = dot(a, w[0]).astype(BF16)
        for i in range(heads):
            part = t[:, HEAD * i : HEAD * (i + 1)]
            if turn:
                x, y = part[:, :half].astype(F32), part[:, half:].astype(F32)
                part = jnp.concatenate([x * cos - y * sin, y * cos + x * sin], -1).astype(BF16)
            out[i] = part


def _whole(shape, layer=None):
    if layer is None:
        return pl.BlockSpec(shape, lambda j: (0,) * len(shape))
    return pl.BlockSpec((1, *shape), lambda j: (layer,) + (0,) * len(shape))


def before(h, wq, wk, wv, cos, sin, layer):
    heads = lambda n: pl.BlockSpec((n, ROWS, HEAD), lambda j: (0, j, 0))
    tokens = lambda n: pl.BlockSpec((ROWS, n), lambda j: (j, 0))
    return pl.pallas_call(
        _before,
        grid=(T // ROWS,),
        in_specs=[tokens(D), _whole((D, HEADS * HEAD), layer), _whole((D, KV * HEAD), layer), _whole((D, KV * HEAD), layer), tokens(HEAD // 2), tokens(HEAD // 2)],
        out_specs=[heads(HEADS), heads(KV), heads(KV), pl.BlockSpec((D, ROWS), lambda j: (0, j))],
        out_shape=[jax.ShapeDtypeStruct(s, BF16) for s in ((HEADS, T, HEAD), (KV, T, HEAD), (KV, T, HEAD), (D, T))],
        compiler_params=pltpu.CompilerParams(vmem_limit_bytes=VMEM),
        name="before",
    )(h, wq, wk, wv, cos, sin)


def _after(*refs, chain):
    dq_ref, dk_ref, dv_ref, cos_ref, sin_ref = refs[:5]
    d_ref = refs[-2] if chain else refs[-1]
    cos, sin = cos_ref[...], sin_ref[...]
    half = HEAD // 2
    at = 0
    for ref, heads, turn in ((dq_ref, HEADS, True), (dk_ref, KV, True), (dv_ref, KV, False)):
        for i in range(heads):
            part = ref[i]
            if turn:
                x, y = part[:, :half].astype(F32), part[:, half:].astype(F32)
                part = jnp.concatenate([x * cos + y * sin, y * cos - x * sin], -1).astype(BF16)
            d_ref[:, at : at + HEAD] = part
            at += HEAD
    if chain:
        wq_ref, wk_ref, wv_ref, h_ref, by_ref = refs[5:10]
        n, m = HEADS * HEAD, KV * HEAD
        by = dot_t(d_ref[:, :n], wq_ref[0]) + dot_t(d_ref[:, n : n + m], wk_ref[0]) + dot_t(d_ref[:, n + m :], wv_ref[0])
        by = by.astype(BF16).astype(F32)
        inner = _norm_back(h_ref[...].astype(F32), by).astype(BF16)
        refs[-1][...] = (by_ref[...].astype(F32) + inner.astype(F32)).astype(BF16)


def after(dq, dk, dv, cos, sin, extra, layer):
    heads = lambda n: pl.BlockSpec((n, ROWS, HEAD), lambda j: (0, j, 0))
    tokens = lambda n: pl.BlockSpec((ROWS, n), lambda j: (j, 0))
    wide = (HEADS + 2 * KV) * HEAD
    specs = [heads(HEADS), heads(KV), heads(KV), tokens(HEAD // 2), tokens(HEAD // 2)]
    outs = [(tokens(wide), (T, wide))]
    if extra:
        specs += [_whole((D, HEADS * HEAD), layer), _whole((D, KV * HEAD), layer), _whole((D, KV * HEAD), layer), tokens(D), tokens(D)]
        outs += [(tokens(D), (T, D))]
    return pl.pallas_call(
        functools.partial(_after, chain=bool(extra)),
        grid=(T // ROWS,),
        in_specs=specs,
        out_specs=[o[0] for o in outs],
        out_shape=[jax.ShapeDtypeStruct(o[1], BF16) for o in outs],
        compiler_params=pltpu.CompilerParams(vmem_limit_bytes=VMEM),
        name="after",
    )(dq, dk, dv, cos, sin, *extra)


def _mlp(*refs, names, forward, backward):
    r = dict(zip(names, refs, strict=True))
    j = pl.program_id(0)
    h1 = r["h1"]

    def blocks(body):
        lax.fori_loop(0, T // ROWS, lambda i, _: body(pl.ds(pl.multiple_of(ROWS * i, ROWS), ROWS)), None)

    def enter(rows):
        r["acc_s"][rows, :] = jnp.zeros((ROWS, D), F32)
        if forward:
            total = sum(dot(r["o"][n, rows, :], r["wo"][0, HEAD * n : HEAD * (n + 1), :]) for n in range(HEADS))
            h1[rows, :] = (r["h"][rows, :].astype(F32) + total.astype(BF16).astype(F32)).astype(BF16)
            wide = h1[rows, :].astype(F32)
            b = (wide * _scale(wide)).astype(BF16)
            r["b_s"][rows, :] = b
            r["bt"][:, rows] = b.T

    def middle(rows):
        if forward:
            gate, up = dot(r["b_s"][rows, :], r["wg"][0]), dot(r["b_s"][rows, :], r["wu"][0])
        else:
            gate, up = r["gate"][rows, :], r["up"][rows, :]
        sig = 1.0 / (1.0 + jnp.exp(-gate))
        silu = gate * sig
        hidden = (silu * up).astype(BF16)
        if not backward:
            r["gate"][rows, :] = gate
            r["up"][rows, :] = up
            r["acc_s"][rows, :] += dot(hidden, r["wd"][0])
        else:
            by = dot_t(r["dy"][rows, :], r["wd"][0]).astype(BF16).astype(F32)
            d_up = (by * silu).astype(BF16)
            d_gate = (by * up * (sig * (1.0 + gate * (1.0 - sig)))).astype(BF16)
            r["hidt"][:, rows] = hidden.T
            r["dup"][rows, :] = d_up
            r["dgate"][rows, :] = d_gate
            r["acc_s"][rows, :] += dot_t(d_gate, r["wg"][0]) + dot_t(d_up, r["wu"][0])

    def leave(rows):
        total = r["acc_s"][rows, :].astype(BF16).astype(F32)
        if not backward:
            r["h2"][rows, :] = (h1[rows, :].astype(F32) + total).astype(BF16)
            return
        inner = _norm_back(h1[rows, :].astype(F32), total).astype(BF16)
        d1 = (r["dy"][rows, :].astype(F32) + inner.astype(F32)).astype(BF16)
        r["d1"][rows, :] = d1
        for n in range(HEADS):
            do = dot_t(d1, r["wo"][0, HEAD * n : HEAD * (n + 1), :]).astype(BF16)
            r["do"][n, rows, :] = do
            both = do.astype(F32) * r["o"][n, rows, :].astype(F32)
            r["delta"][n // GROUP, n % GROUP : n % GROUP + 1, rows] = both.T.sum(0, keepdims=True)

    @pl.when(j == 0)
    def _():
        blocks(enter)

    blocks(middle)

    @pl.when(j == pl.num_programs(0) - 1)
    def _():
        blocks(leave)


def mlp(values, layer, forward, backward):
    columns = pl.BlockSpec((T, TF), lambda j: (0, j))
    tokens, heads = _whole((T, D)), _whole((HEADS, T, HEAD))
    known = {
        "o": heads, "h": tokens, "h1": tokens, "dy": tokens, "gate": columns, "up": columns,
        "wo": _whole((HEADS * HEAD, D), layer),
        "wg": pl.BlockSpec((1, D, TF), lambda j: (layer, 0, j)),
        "wu": pl.BlockSpec((1, D, TF), lambda j: (layer, 0, j)),
        "wd": pl.BlockSpec((1, TF, D), lambda j: (layer, j, 0)),
    }
    outs, scratch = {}, {"acc_s": pltpu.VMEM((T, D), F32)}
    if forward:
        outs |= {"bt": (_whole((D, T)), (D, T), BF16)}
        scratch |= {"b_s": pltpu.VMEM((T, D), BF16)}
        if backward:
            scratch |= {"h1": pltpu.VMEM((T, D), BF16)}
        else:
            outs |= {"h1": (tokens, (T, D), BF16), "h2": (tokens, (T, D), BF16), "gate": (columns, (T, FF), F32), "up": (columns, (T, FF), F32)}
    if backward:
        outs |= {"hidt": (pl.BlockSpec((TF, T), lambda j: (j, 0)), (FF, T), BF16), "dgate": (columns, (T, FF), BF16), "dup": (columns, (T, FF), BF16),
                 "d1": (tokens, (T, D), BF16), "do": (heads, (HEADS, T, HEAD), BF16), "delta": (_whole((KV, GROUP, T)), (KV, GROUP, T), F32)}
    names = (*values, *outs, *scratch)
    got = pl.pallas_call(
        functools.partial(_mlp, names=names, forward=forward, backward=backward),
        grid=(FF // TF,),
        in_specs=[known[name] for name in values],
        out_specs=[o[0] for o in outs.values()],
        out_shape=[jax.ShapeDtypeStruct(o[1], o[2]) for o in outs.values()],
        scratch_shapes=list(scratch.values()),
        compiler_params=pltpu.CompilerParams(vmem_limit_bytes=VMEM),
        name="mlp",
    )(*values.values())
    return dict(zip(outs, got, strict=True))


LANES = 128
BLOCK = 448
SLOTS = 4
SUMS = 5
KINDS = {"P": (112, 512), "Q": (64, 896)}
PLAN = (("w_down", 7, "Q"), ("w_gate", 7, "P"), ("w_up", 7, "P"), ("wo", 2, "Q"), ("wq", 2, "P"), ("wk", 1, "P"), ("wv", 1, "P"))
FIRST = {name: sum(p[1] for p in PLAN[:i]) for i, (name, _, _) in enumerate(PLAN)}
PER_LAYER = sum(p[1] for p in PLAN)
CHUNKS = 2 * PER_LAYER
TICKS = CHUNKS + 11
ACTS = ("hidt", "bt", "ot", "at", "dy", "dgate", "dup", "d1", "dqkv")
CHIPS = 4


def _update(*refs):
    acts = [dict(zip(ACTS, refs[n * len(ACTS) : (n + 1) * len(ACTS)])) for n in range(2)]
    rest = refs[2 * len(ACTS) :]
    w_in, m_in, v_in = (dict(zip(NAMES, rest[i : i + 7])) for i in (0, 7, 14))
    wp, gp = rest[21:23]
    (ab, db, chip, ps, pr, su, ru, sd, rd, wn, gn, mb, vb, wb,
     ab_sem, db_sem, opt_sem, out_sem, ps_s, ps_r, su_s, su_r, sd_s, sd_r, am_s, am_r, au_s, au_r, ad_s, ad_r, free_m, free_u, free_d) = rest[23:]
    rep, me = lax.axis_index("rep"), lax.axis_index("dp")
    z, core = me // 2, me % 2
    mate, above, below = me + 1 - 2 * core, me + 2, me - 2
    has_above, has_below = z < CHIPS - 1, z > 0
    mine = core

    def remote(src, dst, send, recv, to):
        return pltpu.make_async_remote_copy(src_ref=src, dst_ref=dst, send_sem=send, recv_sem=recv, device_id=(rep, to), device_id_type=MESH)

    def tell(sem, to):
        pl.semaphore_signal(sem, inc=1, device_id=(rep, to), device_id_type=MESH)

    def ok(k):
        return (k >= 0) & (k < CHUNKS)


    def load_operands(k, buf, half):
        a = acts[half]
        for first, count, kind, left, right in (
            (0, 7, "Q", "hidt", "dy"), (7, 7, "P", "bt", "dgate"), (14, 7, "P", "bt", "dup"), (21, 2, "Q", "ot", "d1"), (23, 4, "P", "at", "dqkv"),
        ):
            low = half * PER_LAYER + first
            rows, cols = KINDS[kind]
            whole = a[left].shape[0] // 8

            @pl.when((k >= low) & (k < low + count))
            def _():
                j = k - low
                for e in range(8):
                    owner = 2 * (e % 4) + (1 - core if e < 4 else core)
                    at = pl.multiple_of(whole * owner + (rows * j if kind == "Q" else 0), 16)
                    pltpu.make_async_copy(a[left].at[pl.ds(at, rows), :], ab.at[buf, pl.ds(rows * e, rows), :], ab_sem.at[buf]).start()
                if kind == "Q":
                    pltpu.make_async_copy(a[right], db.at[buf], db_sem.at[buf]).start()
                else:
                    there = a[right].at[:, pl.ds(pl.multiple_of(cols * j, cols), cols)]
                    pltpu.make_async_copy(there, db.at[buf, :, pl.ds(0, cols)], db_sem.at[buf]).start()

    def wait_operands(buf, kind):
        rows, cols = KINDS[kind]
        pltpu.make_async_copy(acts[0]["hidt"].at[pl.ds(0, 8 * rows), :], ab.at[buf, pl.ds(0, 8 * rows), :], ab_sem.at[buf]).wait()
        pltpu.make_async_copy(acts[0]["dgate"].at[:, pl.ds(0, cols)], db.at[buf, :, pl.ds(0, cols)], db_sem.at[buf]).wait()

    def optimizer_copies(k, buf, do):
        half = k // PER_LAYER
        layer, r = 1 - half, k % PER_LAYER
        for name, count, kind in PLAN:
            rows, cols = KINDS[kind]

            @pl.when((r >= FIRST[name]) & (r < FIRST[name] + count))
            def _():
                j = r - FIRST[name]
                whole = w_in[name].shape[1] // 8
                down = pl.multiple_of(rows * j if kind == "Q" else 0 * j, 16)
                right = pl.ds(0, cols) if kind == "Q" else pl.ds(pl.multiple_of(cols * j, cols), cols)
                for n, (ref, at, to) in enumerate(((m_in[name], down, mb), (v_in[name], down, vb), (w_in[name], pl.multiple_of(whole * me + down, 16), wb))):
                    do(pltpu.make_async_copy(ref.at[layer, pl.ds(at, rows), right], to.at[buf, pl.ds(0, rows), pl.ds(0, cols)], opt_sem.at[buf, n]))


    barrier = pltpu.get_barrier_semaphore()
    load_operands(0, 0, 0)
    tell(barrier, mate)

    @pl.when(has_above)
    def _():
        tell(barrier, above)

    @pl.when(has_below)
    def _():
        tell(barrier, below)

    @pl.when(has_above & has_below)
    def _():
        pl.semaphore_wait(barrier, 3)

    @pl.when(jnp.logical_not(has_above & has_below))
    def _():
        pl.semaphore_wait(barrier, 2)

    def tick(t, _):
        slot, prev, late = t % SLOTS, (t + SLOTS - 1) % SLOTS, (t + 1) % SLOTS
        two = t % 2


        @pl.when(t >= 3)
        def _():
            pl.semaphore_wait(free_m, 1)

            @pl.when(has_above)
            def _():
                pl.semaphore_wait(free_u, 1)

            @pl.when(has_below)
            def _():
                pl.semaphore_wait(free_d, 1)

            @pl.when(ok(t - 3))
            def _():
                for s in range(CHIPS):
                    remote(ps.at[late, s], pr.at[late, s], ps_s.at[late, s], ps_r.at[late, s], mate).wait_send()

            @pl.when(ok(t - 3 - 1 - z))
            def _():
                for s in range(1, CHIPS):
                    @pl.when(s > z)
                    def _():
                        remote(su.at[late, s], ru.at[late, s], su_s.at[late, s], su_r.at[late, s], mate).wait_send()

            @pl.when(ok(t - 3 - 1 - (CHIPS - 1 - z)))
            def _():
                for s in range(CHIPS - 1):
                    @pl.when(s < z)
                    def _():
                        remote(sd.at[late, s], rd.at[late, s], sd_s.at[late, s], sd_r.at[late, s], mate).wait_send()

            def gone(s, _):
                @pl.when(ok(t - 3 - 4 - jnp.abs(z - s)))
                def _():
                    there = wp.at[0, 0]
                    remote(there, there, am_s.at[late, s], am_r.at[late, s], mate).wait_send()

                    @pl.when((s <= z) & has_above)
                    def _():
                        remote(there, there, au_s.at[late, s], au_r.at[late, s], mate).wait_send()

                    @pl.when((s >= z) & has_below)
                    def _():
                        remote(there, there, ad_s.at[late, s], ad_r.at[late, s], mate).wait_send()

            lax.fori_loop(0, CHIPS, gone, None)

            @pl.when(ok(t - 3 - 4))
            def _():
                pltpu.make_async_copy(wn.at[late], wp.at[0, 0], out_sem.at[late, 0]).wait()
                pltpu.make_async_copy(gn.at[late], gp.at[0], out_sem.at[late, 1]).wait()


        for half in range(2):
            load_operands(t + 1, 1 - two, half)

        @pl.when(ok(t - 3))
        def _():
            optimizer_copies(t - 3, 1 - two, lambda copy: copy.start())


        def pass_on(s, k, from_above):
            got, send, here, there, there_r, to = (rd, sd, sd_s, rd, sd_r, below) if from_above else (ru, su, su_s, ru, su_r, above)
            remote(send.at[prev, s], got.at[prev, s], here.at[prev, s], there_r.at[prev, s], mate).wait_recv()
            value = chip[k % SUMS, s] + got[prev, s].astype(F32)
            chip[k % SUMS, s] = value
            send[slot, s] = value.astype(BF16)

            @pl.when((s < z) if from_above else (s > z))
            def _():
                remote(send.at[slot, s], there.at[slot, s], here.at[slot, s], there_r.at[slot, s], to).start()

        up_k, down_k = t - 1 - z, t - 1 - (CHIPS - 1 - z)
        for i in range(CHIPS - 1):
            @pl.when(has_below & ok(up_k) & (CHIPS - 1 - i >= z))
            def _():
                pass_on(CHIPS - 1 - i, up_k, False)

            @pl.when(has_above & ok(down_k) & (i <= z))
            def _():
                pass_on(i, down_k, True)


        @pl.when(ok(t - 4))
        def _():
            k = t - 4
            optimizer_copies(k, two, lambda copy: copy.wait())
            r = k % PER_LAYER
            is_q = (r < FIRST["w_gate"]) | ((r >= FIRST["wo"]) & (r < FIRST["wq"]))
            for kind, test in (("Q", is_q), ("P", jnp.logical_not(is_q))):
                rows, cols = KINDS[kind]

                @pl.when(test)
                def _():
                    for j in range(cols // LANES):
                        at, over = slice(rows * j, rows * (j + 1)), slice(LANES * j, LANES * (j + 1))
                        low = chip[k % SUMS, z, at, :].astype(BF16)
                        g = low.astype(F32)
                        m = 0.9 * mb[two, :rows, over] + 0.1 * g
                        v = 0.95 * vb[two, :rows, over] + 0.05 * g * g
                        w = wb[two, :rows, over].astype(F32)
                        wn[slot, at, :] = (w - 0.02 * (m * lax.rsqrt(v + 1e-8) + 0.1 * w)).astype(BF16)
                        gn[slot, at, :] = low

            pltpu.make_async_copy(wn.at[slot], wp.at[k, me], out_sem.at[slot, 0]).start()
            pltpu.make_async_copy(gn.at[slot], gp.at[k], out_sem.at[slot, 1]).start()


        def spread(s, _):
            k = t - 4 - jnp.abs(z - s)

            @pl.when(ok(k))
            def _():
                there = wp.at[k, 2 * s + core]

                @pl.when(s < z)
                def _():
                    remote(there, there, au_s.at[prev, s], au_r.at[prev, s], mate).wait_recv()

                @pl.when(s > z)
                def _():
                    remote(there, there, ad_s.at[prev, s], ad_r.at[prev, s], mate).wait_recv()

                def sends(source):
                    @pl.when((s <= z) & has_above)
                    def _():
                        remote(source, there, au_s.at[slot, s], au_r.at[slot, s], above).start()

                    @pl.when((s >= z) & has_below)
                    def _():
                        remote(source, there, ad_s.at[slot, s], ad_r.at[slot, s], below).start()

                    remote(source, there, am_s.at[slot, s], am_r.at[slot, s], mate).start()

                @pl.when(s == z)
                def _():
                    sends(wn.at[slot])

                @pl.when(s != z)
                def _():
                    sends(there)

        lax.fori_loop(0, CHIPS, spread, None)


        @pl.when(ok(t - 1))
        def _():
            for s in (3, 0, 2, 1):
                remote(ps.at[prev, s], pr.at[prev, s], ps_s.at[prev, s], ps_r.at[prev, s], mate).wait_recv()
                value = chip[(t - 1) % SUMS, s] + pr[prev, s].astype(F32)
                chip[(t - 1) % SUMS, s] = value
                if s > 0:
                    @pl.when(z == 0)
                    def _():
                        su[slot, s] = value.astype(BF16)
                        remote(su.at[slot, s], ru.at[slot, s], su_s.at[slot, s], su_r.at[slot, s], above).start()
                if s < CHIPS - 1:
                    @pl.when(z == CHIPS - 1)
                    def _():
                        sd[slot, s] = value.astype(BF16)
                        remote(sd.at[slot, s], rd.at[slot, s], sd_s.at[slot, s], sd_r.at[slot, s], below).start()


        @pl.when(ok(t))
        def _():
            r = t % PER_LAYER
            is_q = (r < FIRST["w_gate"]) | ((r >= FIRST["wo"]) & (r < FIRST["wq"]))
            for kind, test in (("Q", is_q), ("P", jnp.logical_not(is_q))):
                rows, cols = KINDS[kind]

                @pl.when(test)
                def _():
                    wait_operands(two, kind)
                    for own in range(2):
                        got = dot(ab[two, 4 * rows * own : 4 * rows * (own + 1), :], db[two, :, :cols])
                        for s in range(CHIPS):
                            for j in range(cols // LANES):
                                piece = got[rows * s : rows * (s + 1), LANES * j : LANES * (j + 1)]
                                if own:
                                    chip[t % SUMS, s, rows * j : rows * (j + 1), :] = piece
                                else:
                                    ps[slot, s, rows * j : rows * (j + 1), :] = piece.astype(BF16)
                        if not own:
                            for s in (3, 0, 2, 1):
                                remote(ps.at[slot, s], pr.at[slot, s], ps_s.at[slot, s], ps_r.at[slot, s], mate).start()


        def arrived(s, _):
            @pl.when(ok(t - 5 - jnp.abs(z - s)))
            def _():
                there = wp.at[0, 0]
                remote(there, there, am_s.at[prev, s], am_r.at[prev, s], mate).wait_recv()

        lax.fori_loop(0, CHIPS, arrived, None)

        @pl.when(t < TICKS - 3)
        def _():
            tell(free_m, mate)

            @pl.when(has_above)
            def _():
                tell(free_d, above)

            @pl.when(has_below)
            def _():
                tell(free_u, below)

    lax.fori_loop(0, TICKS, tick, None)


def update(acts, w, m, v):
    vm, sem = pltpu.VMEM, pltpu.SemaphoreType
    block = (BLOCK, LANES)
    four = lambda: sem.DMA((SLOTS, CHIPS))
    scratch = [
        vm((2, T, T), BF16), vm((2, T, D), BF16), vm((SUMS, CHIPS, *block), F32),
        *(vm((SLOTS, CHIPS, *block), BF16) for _ in range(6)),
        vm((SLOTS, *block), BF16), vm((SLOTS, *block), BF16),
        vm((2, 112, D), F32), vm((2, 112, D), F32), vm((2, 112, D), BF16),
        sem.DMA((2,)), sem.DMA((2,)), sem.DMA((2, 3)), sem.DMA((SLOTS, 2)),
        *(four() for _ in range(12)),
        sem.REGULAR, sem.REGULAR, sem.REGULAR,
    ]
    given = [a[name] for a in acts for name in ACTS] + [*w, *m, *v]
    return pl.pallas_call(
        _update,
        in_specs=[pl.BlockSpec(memory_space=pl.ANY)] * len(given),
        out_specs=[pl.BlockSpec(memory_space=pl.ANY)] * 2,
        out_shape=[jax.ShapeDtypeStruct((CHUNKS, 8, *block), BF16), jax.ShapeDtypeStruct((CHUNKS, *block), BF16)],
        scratch_shapes=scratch,
        compiler_params=pltpu.CompilerParams(collective_id=0, has_side_effects=True, vmem_limit_bytes=60 * 2**20),
        cost_estimate=pl.CostEstimate(flops=2 * T * 24772608, bytes_accessed=400 * 2**20, transcendentals=0),
        name="update",
    )(*given)


def _unpack(wp_ref, gp_ref, m_ref, v_ref, w_out, m_out, v_out, *, kind):
    rows, cols = KINDS[kind]
    for j in range(cols // LANES):
        at, over = slice(rows * j, rows * (j + 1)), slice(LANES * j, LANES * (j + 1))
        for n in range(8):
            if kind == "P":
                w_out[0, rows * n : rows * (n + 1), over] = wp_ref[0, n, at, :]
            else:
                w_out[0, n, :, over] = wp_ref[0, n, at, :]
        g = gp_ref[0, at, :].astype(F32)
        m_out[0, :, over] = 0.9 * m_ref[0, :, over] + 0.1 * g
        v_out[0, :, over] = 0.95 * v_ref[0, :, over] + 0.05 * g * g


def unpack(name, wp, gp, m, v):
    count, kind = next(p[1:] for p in PLAN if p[0] == name)
    rows, cols = KINDS[kind]
    chunk = lambda layer, j: (1 - layer) * PER_LAYER + FIRST[name] + j
    _, height, width = m.shape
    if kind == "P":
        own = pl.BlockSpec((1, rows, cols), lambda layer, j: (layer, 0, j))
        full, shape = pl.BlockSpec((1, 8 * rows, cols), lambda layer, j: (layer, 0, j)), (2, 8 * height, width)
    else:
        own = pl.BlockSpec((1, rows, cols), lambda layer, j: (layer, j, 0))
        full, shape = pl.BlockSpec((1, 8, rows, cols), lambda layer, j: (layer, 0, j, 0)), (2, 8, height, width)
    w, m, v = pl.pallas_call(
        functools.partial(_unpack, kind=kind),
        grid=(2, count),
        in_specs=[pl.BlockSpec((1, 8, BLOCK, LANES), lambda layer, j: (chunk(layer, j), 0, 0, 0)), pl.BlockSpec((1, BLOCK, LANES), lambda layer, j: (chunk(layer, j), 0, 0)), own, own],
        out_specs=[full, own, own],
        out_shape=[jax.ShapeDtypeStruct(shape, BF16), jax.ShapeDtypeStruct(m.shape, F32), jax.ShapeDtypeStruct(v.shape, F32)],
        compiler_params=pltpu.CompilerParams(vmem_limit_bytes=VMEM),
        name="unpack",
    )(wp, gp, m, v)
    return w.reshape(2, 8 * height, width), m, v


def solution(mesh):
    def step(x, dy, *arrays):
        w, m, v = (dict(zip(NAMES, arrays[i : i + 7], strict=True)) for i in (0, 7, 14))
        half = HEAD // 2
        angle = jnp.arange(T, dtype=F32)[:, None] * THETA ** (-jnp.arange(half, dtype=F32) / half)
        cos, sin = jnp.cos(angle), jnp.sin(angle)
        kinds = {"wo": w["wo"], "wg": w["w_gate"], "wu": w["w_up"], "wd": w["w_down"]}

        def attention_of(h, layer):
            q, k, v, at = before(h, w["wq"], w["wk"], w["wv"], cos, sin, layer)
            out, ot, lse = attend(q, k, v)
            return {"qkv": (q, k, v), "o": out, "ot": ot, "at": at, "lse": lse}

        def attention_back(kept, by, extra, layer):
            return after(*attend_back(*kept["qkv"], by["do"], kept["lse"], by["delta"]), cos, sin, extra, layer)

        h0, y_by = x[0], dy[0]
        a0 = attention_of(h0, 0)
        f0 = mlp({"o": a0["o"], "h": h0, **kinds}, 0, True, False)
        h2 = f0["h2"]
        a1 = attention_of(h2, 1)
        b1 = mlp({"o": a1["o"], "h": h2, "dy": y_by, **kinds}, 1, True, True)
        dqkv1, by1 = attention_back(a1, b1, (w["wq"], w["wk"], w["wv"], h2, b1["d1"]), 1)
        b0 = mlp({"o": a0["o"], "h1": f0["h1"], "gate": f0["gate"], "up": f0["up"], "dy": by1, **kinds}, 0, False, True)
        (dqkv0,) = attention_back(a0, b0, (), 0)
        acts = [a1 | b1 | {"dy": y_by, "dqkv": dqkv1}, a0 | f0 | b0 | {"dy": by1, "dqkv": dqkv0}]
        wp, gp = update(acts, w.values(), m.values(), v.values())
        new = [unpack(name, wp, gp, m[name], v[name]) for name in NAMES]
        return tuple(one[which] for which in range(3) for one in new)

    states, all_of, cut = P(("rep", "dp"), None, None), P(None, None, None), P(None, "dp", None)
    return jax.shard_map(
        step,
        mesh=mesh,
        in_specs=(states, states) + (all_of,) * 7 + (cut,) * 14,
        out_specs=(P("rep", None, None),) * 7 + (P("rep", "dp", None),) * 14,
        check_vma=False,
    )
```

```python
import functools

import jax
import jax.numpy as jnp
from jax import lax
from jax.experimental import pallas as pl
from jax.experimental.pallas import tpu as pltpu
from jax.sharding import PartitionSpec as P

LOG2E = 1.4426950408889634
HIDDEN = -2e30
VMEM = 56 * 2**20
F32, BF16 = jnp.float32, jnp.bfloat16
MESH = pl.DeviceIdType.MESH
T, D, FF, HEADS, KV, HEAD = 1024, 896, 3584, 4, 2, 256
THETA = 10000
NAMES = ("wq", "wk", "wv", "wo", "w_gate", "w_up", "w_down")
ROWS = 256
TF = 512
PIECES = T // ROWS


def loop(count, body):
    lax.fori_loop(0, count, lambda i, _: body(i), None)


def dot(a, b):
    return jnp.dot(a, b, preferred_element_type=F32)


def dot_t(a, b):
    return lax.dot_general(a, b, (((1,), (1,)), ((), ())), preferred_element_type=F32)


def _scale(wide):
    return lax.rsqrt(jnp.mean(wide * wide, -1, keepdims=True) + 1e-6)


def _norm_back(h, by):
    s = _scale(h)
    return by * s - h * (s * s * s * jnp.mean(by * h, -1, keepdims=True))


E = HEAD**-0.5 * LOG2E
GROUP = HEADS // KV


def _piece(i):
    return slice(ROWS * i, ROWS * (i + 1))


def _side(ref, i):
    return jnp.concatenate([ref[n, _piece(i), :] for n in range(GROUP)], axis=0)


def _visible():
    shape = (ROWS, GROUP * ROWS)
    return lax.broadcasted_iota(jnp.int32, shape, 0) <= lax.rem(lax.broadcasted_iota(jnp.int32, shape, 1), ROWS)


def _attend(q_ref, k_ref, v_ref, o_ref, ot_ref, lse_ref):
    seen = _visible()
    turned = v_ref[0].T
    for i in range(PIECES):
        q = _side(q_ref, i)
        scores = [dot_t(k_ref[0, _piece(j), :], q) for j in range(i + 1)]
        scores[i] = jnp.where(seen, scores[i], HIDDEN)
        top = functools.reduce(jnp.maximum, [s.max(axis=0, keepdims=True) for s in scores])
        total, mix = 0.0, 0.0
        for j, s in enumerate(scores):
            p = jnp.exp2((s - top) * E)
            total = total + p.sum(axis=0, keepdims=True)
            mix = mix + dot(turned[:, _piece(j)], p.astype(BF16))
        out = (mix * (1.0 / total)).astype(BF16)
        lse = top * E + jnp.log(total) * LOG2E
        for n in range(GROUP):
            ot_ref[HEAD * n : HEAD * (n + 1), _piece(i)] = out[:, _piece(n)]
            o_ref[n, _piece(i), :] = out[:, _piece(n)].T
            lse_ref[0, n : n + 1, _piece(i)] = lse[:, _piece(n)]


QUERIES, KEYS, LINES = (pl.BlockSpec(shape, lambda i: (i, 0, 0)) for shape in ((GROUP, T, HEAD), (1, T, HEAD), (1, GROUP, T)))


def attend(q, k, v):
    return pl.pallas_call(
        _attend,
        grid=(KV,),
        in_specs=[QUERIES, KEYS, KEYS],
        out_specs=[QUERIES, pl.BlockSpec((GROUP * HEAD, T), lambda i: (i, 0)), LINES],
        out_shape=[jax.ShapeDtypeStruct(q.shape, BF16), jax.ShapeDtypeStruct((HEADS * HEAD, T), BF16), jax.ShapeDtypeStruct((KV, GROUP, T), F32)],
        compiler_params=pltpu.CompilerParams(vmem_limit_bytes=VMEM),
        name="attend",
    )(q, k, v)


def _before(h_ref, wq_ref, wk_ref, wv_ref, cos_ref, sin_ref, q_ref, k_ref, v_ref, at_ref):
    wide = h_ref[...].astype(F32)
    a = (wide * _scale(wide)).astype(BF16)
    at_ref[...] = a.T
    cos, sin = cos_ref[...], sin_ref[...]
    for out, w, heads, turn in ((q_ref, wq_ref, HEADS, True), (k_ref, wk_ref, KV, True), (v_ref, wv_ref, KV, False)):
        t = dot(a, w[0]).astype(BF16)
        for i in range(heads):
            part = t[:, HEAD * i : HEAD * (i + 1)]
            if turn:
                x, y = part[:, :HALF].astype(F32), part[:, HALF:].astype(F32)
                part = jnp.concatenate([x * cos - y * sin, y * cos + x * sin], -1).astype(BF16)
            out[i] = part


def _whole(shape, layer=None):
    if layer is None:
        return pl.BlockSpec(shape, lambda j: (0,) * len(shape))
    return pl.BlockSpec((1, *shape), lambda j: (layer,) + (0,) * len(shape))


def before(h, wq, wk, wv, cos, sin, layer):
    heads = lambda n: pl.BlockSpec((n, ROWS, HEAD), lambda j: (0, j, 0))
    tokens = lambda n: pl.BlockSpec((ROWS, n), lambda j: (j, 0))
    return pl.pallas_call(
        _before,
        grid=(T // ROWS,),
        in_specs=[tokens(D), _whole((D, HEADS * HEAD), layer), _whole((D, KV * HEAD), layer), _whole((D, KV * HEAD), layer), tokens(HALF), tokens(HALF)],
        out_specs=[heads(HEADS), heads(KV), heads(KV), pl.BlockSpec((D, ROWS), lambda j: (0, j))],
        out_shape=[jax.ShapeDtypeStruct(s, BF16) for s in ((HEADS, T, HEAD), (KV, T, HEAD), (KV, T, HEAD), (D, T))],
        compiler_params=pltpu.CompilerParams(vmem_limit_bytes=VMEM),
        name="before",
    )(h, wq, wk, wv, cos, sin)


def _enter(o_ref, h_ref, wo_ref, h1_ref, b_ref, bt_ref, rows):
    total = sum(dot(o_ref[n, rows, :], wo_ref[0, HEAD * n : HEAD * (n + 1), :]) for n in range(HEADS))
    h1 = (h_ref[rows, :].astype(F32) + total.astype(BF16).astype(F32)).astype(BF16)
    wide = h1.astype(F32)
    b = (wide * _scale(wide)).astype(BF16)
    h1_ref[rows, :] = h1
    b_ref[rows, :] = b
    bt_ref[:, rows] = b.T


def _project(*refs):
    _enter(*refs, slice(0, ROWS))


def project(o, h, wo, layer):
    tokens = pl.BlockSpec((ROWS, D), lambda j: (j, 0))
    return pl.pallas_call(
        _project,
        grid=(T // ROWS,),
        in_specs=[pl.BlockSpec((HEADS, ROWS, HEAD), lambda j: (0, j, 0)), tokens, _whole((HEADS * HEAD, D), layer)],
        out_specs=[tokens, tokens, pl.BlockSpec((D, ROWS), lambda j: (0, j))],
        out_shape=[jax.ShapeDtypeStruct(shape, BF16) for shape in ((T, D), (T, D), (D, T))],
        compiler_params=pltpu.CompilerParams(vmem_limit_bytes=VMEM),
        name="project",
    )(o, h, wo)


def _mlp(o_ref, h_ref, wo_ref, wg_ref, wu_ref, wd_ref, h1_ref, b_ref, bt_ref, h2_ref, acc_s):
    j = pl.program_id(0)

    def blocks(body):
        loop(PIECES, lambda i: body(pl.ds(pl.multiple_of(ROWS * i, ROWS), ROWS)))

    def enter(rows):
        acc_s[rows, :] = jnp.zeros((ROWS, D), F32)
        _enter(o_ref, h_ref, wo_ref, h1_ref, b_ref, bt_ref, rows)

    def middle(rows):
        gate, up = dot(b_ref[rows, :], wg_ref[0]), dot(b_ref[rows, :], wu_ref[0])
        hidden = (gate * (1.0 / (1.0 + jnp.exp(-gate))) * up).astype(BF16)
        acc_s[rows, :] += dot(hidden, wd_ref[0])

    def leave(rows):
        h2_ref[rows, :] = (h1_ref[rows, :].astype(F32) + acc_s[rows, :].astype(BF16).astype(F32)).astype(BF16)

    @pl.when(j == 0)
    def _():
        blocks(enter)

    blocks(middle)

    @pl.when(j == pl.num_programs(0) - 1)
    def _():
        blocks(leave)


def mlp(o, h, wo, wg, wu, wd, layer):
    tokens = _whole((T, D))
    columns = pl.BlockSpec((1, D, TF), lambda j: (layer, 0, j))
    return pl.pallas_call(
        _mlp,
        grid=(FF // TF,),
        in_specs=[_whole((HEADS, T, HEAD)), tokens, _whole((HEADS * HEAD, D), layer), columns, columns, pl.BlockSpec((1, TF, D), lambda j: (layer, j, 0))],
        out_specs=[tokens, tokens, _whole((D, T)), tokens],
        out_shape=[jax.ShapeDtypeStruct(shape, BF16) for shape in ((T, D), (T, D), (D, T), (T, D))],
        scratch_shapes=[pltpu.VMEM((T, D), F32)],
        compiler_params=pltpu.CompilerParams(vmem_limit_bytes=VMEM),
        name="mlp",
    )(o, h, wo, wg, wu, wd)


LANES = 128
BLOCK = 448
SLOTS = 4
SUMS = 5
EARLY = 2
LAG = 22
P_BLOCK, Q_BLOCK = (112, 512), (64, 896)
TILES = FF // TF
DOWN_AT, WO_AT, QKV_AT, PER_LAYER = 14, 21, 23, 27
CHUNKS = 2 * PER_LAYER
TICKS = CHUNKS + 11 + EARLY
CHIPS = 4
HALF, T_HALF = HEAD // 2, T // 2
N_Q, N_K = HEADS * HEAD, KV * HEAD
LEAVE, HEADS_AT, AFTER = 13, 14, 17


def _is_q(r):
    return (r >= DOWN_AT) & (r < QKV_AT)


def _place(k):
    layer, r = 1 - k // PER_LAYER, k % PER_LAYER
    double, single = (r % 2) * DOWN_AT + layer * TILES + r // 2, 2 * DOWN_AT + layer * TILES + r - DOWN_AT
    return jnp.where(r < DOWN_AT, double, jnp.where(r < WO_AT, single, 3 * DOWN_AT + layer * (PER_LAYER - WO_AT) + r - WO_AT))


def _owners(layer, r):
    mlp_chunk = r < DOWN_AT
    return (
        ("w_gate", mlp_chunk & (r % 2 == 0), r // 2), ("w_up", mlp_chunk & (r % 2 == 1), r // 2),
        ("w_down", (r >= DOWN_AT) & (r < WO_AT), r - DOWN_AT), ("wo", (r >= WO_AT) & (r < QKV_AT), r - WO_AT),
        ("wq", (r >= QKV_AT) & (r < QKV_AT + 2), r - QKV_AT), ("wk", r == QKV_AT + 2, 0 * r), ("wv", r == QKV_AT + 3, 0 * r),
    )


LAYER_INPUTS = ("o", "ot", "at", "bt", "b", "h1", "q", "k", "v", "lse")
INPUTS = ("dy", "h", "cos", "sin")
OUTPUTS = ("wp", "gp", "hidt", "dgate", "dup", "d1", "dqkv", "by1")
SCRATCH = ("ab", "db", "chip", "ps", "pr", "su", "ru", "sd", "rd", "wn", "gn", "mb", "vb", "wb", "x1", "x2", "oo", "wg", "wu", "wd", "acc", "dg", "du", "ht",
           "qq", "kk", "vv", "dq", "cosb", "sinb", "lseb", "delta",
           "ab_sem", "db_sem", "opt_sem", "out_sem", "tile_sem", "x_sem", "o_sem", "qkv_sem", "lse_sem", "write_sem",
           "ps_s", "ps_r", "su_s", "su_r", "sd_s", "sd_r", "am_s", "am_r", "au_s", "au_r", "ad_s", "ad_r", "free_m", "free_u", "free_d")


def _update(*refs):
    n_layer = len(LAYER_INPUTS)
    acts = [dict(zip(LAYER_INPUTS, refs[n * n_layer : (n + 1) * n_layer])) for n in range(2)]
    refs = refs[2 * n_layer :]
    w_in, m_in, v_in = (dict(zip(NAMES, refs[i : i + 7])) for i in (0, 7, 14))
    r_ = dict(zip((*INPUTS, *OUTPUTS, *SCRATCH), refs[21:], strict=True))
    (ab, db, chip, ps, pr, su, ru, sd, rd, wn, gn, mb, vb, wb, x1, x2, oo, wg, wu, wd, acc, dg, du, ht, qq, kk, vv, dq, cosb, sinb, lseb, delta,
     ab_sem, db_sem, opt_sem, out_sem, tile_sem, x_sem, o_sem, qkv_sem, lse_sem, write_sem,
     ps_s, ps_r, su_s, su_r, sd_s, sd_r, am_s, am_r, au_s, au_r, ad_s, ad_r, free_m, free_u, free_d) = (r_[name] for name in SCRATCH)
    wp, gp = r_["wp"], r_["gp"]
    rep, me = lax.axis_index("rep"), lax.axis_index("dp")
    z, core = me // 2, me % 2
    mate, above, below = me + 1 - 2 * core, me + 2, me - 2
    has_above, has_below = z < CHIPS - 1, z > 0

    def remote(src, dst, send, recv, to):
        return pltpu.make_async_remote_copy(src_ref=src, dst_ref=dst, send_sem=send, recv_sem=recv, device_id=(rep, to), device_id_type=MESH)

    def tell(sem, to):
        pl.semaphore_signal(sem, inc=1, device_id=(rep, to), device_id_type=MESH)

    def local(src, dst, sem):
        return pltpu.make_async_copy(src, dst, sem)

    def ok(k):
        return (k >= 0) & (k < CHUNKS)

    def tokens(start, count):
        return pl.ds(pl.multiple_of(start, ROWS), count)


    def tile_copies(half, j, buf):
        layer, over = 1 - half, pl.ds(pl.multiple_of(TF * j, TF), TF)
        return [
            local(w_in["w_gate"].at[layer, :, over], wg.at[buf], tile_sem.at[buf, 0]),
            local(w_in["w_up"].at[layer, :, over], wu.at[buf], tile_sem.at[buf, 1]),
            local(w_in["w_down"].at[layer, over, :], wd.at[buf], tile_sem.at[buf, 2]),
        ]

    def wo_copies(half):
        return [local(w_in["wo"].at[1 - half, pl.ds(TF * n, TF), :], wd.at[n], tile_sem.at[n, 2]) for n in range(2)]

    def qkv_weight_copies():
        return [
            local(w_in["wq"].at[1, :, pl.ds(0, TF)], wg.at[0], tile_sem.at[0, 0]), local(w_in["wq"].at[1, :, pl.ds(TF, TF)], wg.at[1], tile_sem.at[1, 0]),
            local(w_in["wk"].at[1], wu.at[0], tile_sem.at[0, 1]), local(w_in["wv"].at[1], wu.at[1], tile_sem.at[1, 1]),
        ]

    def head_copies(a, head):
        return [
            local(a["q"].at[pl.ds(GROUP * head, GROUP)], qq, qkv_sem.at[0]), local(a["k"].at[head], kk, qkv_sem.at[1]),
            local(a["v"].at[head], vv, qkv_sem.at[2]),
        ]

    def unit_of(n):
        half = (n >= AFTER + 2 + EARLY).astype(jnp.int32)
        return half, n - EARLY - LAG * half

    def start(copies):
        for copy in copies:
            copy.start()

    def wait(copies):
        for copy in copies:
            copy.wait()

    def writes(half, tau):
        u = tau + EARLY
        j, first = u // 2, tokens(T_HALF * (u % 2), T_HALF)
        over = pl.ds(pl.multiple_of(TF * j, TF), TF)
        part = tokens(T_HALF * (tau - AFTER), T_HALF)
        after_at = (tau >= AFTER) & (tau < AFTER + 2)
        return (
            ((u >= 0) & (u < 2 * TILES), lambda: [
                local(dg, r_["dgate"].at[half, first, over], write_sem.at[0]), local(du, r_["dup"].at[half, first, over], write_sem.at[1]),
                local(ht, r_["hidt"].at[half, over, first], write_sem.at[2])]),
            (tau == LEAVE, lambda: [local(x1, r_["d1"].at[half], write_sem.at[0])]),
            (after_at, lambda: [local(dq.at[part, :], r_["dqkv"].at[half, part, :], write_sem.at[0])]),
            (after_at & (half == 0), lambda: [local(x1.at[part, :], r_["by1"].at[part, :], write_sem.at[1])]),
        )

    def for_layer(half, test, body):
        for n in range(2):
            pl.when(test & (half == n))(functools.partial(body, acts[n]))

    def fetch(n):
        half, tau = unit_of(n)
        u = tau + EARLY

        @pl.when((tau == -EARLY - 1) & (half == 1))
        def _():
            start(tile_copies(half, 0, 0))
            start([local(acts[1]["b"], x2, x_sem.at[1])])

        @pl.when((u >= 0) & (u % 2 == 0) & (u < 2 * TILES - 2))
        def _():
            start(tile_copies(half, u // 2 + 1, (u // 2 + 1) % 2))

        @pl.when(tau == LEAVE - 1)
        def _():
            start(wo_copies(half))

        for_layer(half, tau == LEAVE - 1, lambda a: start([local(a["h1"], x2, x_sem.at[1]), local(a["o"], oo, o_sem)]))
        for_layer(half, tau == LEAVE, lambda a: start([*head_copies(a, 0), local(a["lse"], lseb, lse_sem)]))
        for_layer(half, tau == HEADS_AT + 1, lambda a: start(head_copies(a, 1)))

        @pl.when((tau == LEAVE - 1) & (half == 0))
        def _():
            start(qkv_weight_copies())

        @pl.when((tau == HEADS_AT) & (half == 0))
        def _():
            start([local(r_["h"], x2, x_sem.at[1])])

    def mlp_unit(u, buf):
        def rows_of(i):
            rows, out = tokens(T_HALF * (u % 2) + ROWS * i, ROWS), tokens(ROWS * i, ROWS)
            gate, up = dot(x2[rows, :], wg[buf]), dot(x2[rows, :], wu[buf])
            sig = 1.0 / (1.0 + jnp.exp(-gate))
            silu = gate * sig
            by = dot_t(x1[rows, :], wd[buf]).astype(BF16).astype(F32)
            d_up = (by * silu).astype(BF16)
            d_gate = (by * up * (sig * (1.0 + gate * (1.0 - sig)))).astype(BF16)
            ht[:, out] = (silu * up).astype(BF16).T
            du[out, :] = d_up
            dg[out, :] = d_gate
            acc[rows, :] += dot_t(d_gate, wg[buf]) + dot_t(d_up, wu[buf])

        loop(PIECES // 2, rows_of)

    def leave_unit(i):
        rows = tokens(ROWS * i, ROWS)
        inner = _norm_back(x2[rows, :].astype(F32), acc[rows, :].astype(BF16).astype(F32)).astype(BF16)
        d1 = (x1[rows, :].astype(F32) + inner.astype(F32)).astype(BF16)
        x1[rows, :] = d1
        for n in range(HEADS):
            low = HEAD * (n % 2)
            do = dot_t(d1, wd[n // 2, low : low + HEAD, :]).astype(BF16)
            both = do.astype(F32) * oo[n, rows, :].astype(F32)
            oo[n, rows, :] = do
            delta[n // GROUP, n % GROUP : n % GROUP + 1, rows] = both.T.sum(0, keepdims=True)

    def turn_back(part, rows):
        cos, sin = cosb[rows, :], sinb[rows, :]
        x, y = part[:, :HALF].astype(F32), part[:, HALF:].astype(F32)
        return jnp.concatenate([x * cos + y * sin, y * cos - x * sin], -1).astype(BF16)

    def head_unit(head):
        seen = _visible()
        turned = kk[...].T
        line = lambda ref, i: jnp.concatenate([ref[head, n : n + 1, _piece(i)] for n in range(GROUP)], axis=1)
        column = lambda at: pl.ds(pl.multiple_of(at, HEAD), HEAD)
        dk_at, dv_at = slice(0, HEAD), slice(HEAD, 2 * HEAD)
        for i in range(PIECES):
            q, lse, dl = _side(qq, i), line(lseb, i), line(delta, i)
            do = jnp.concatenate([oo[GROUP * head + n, _piece(i), :] for n in range(GROUP)], axis=0)
            by_q = 0.0
            for j in range(i + 1):
                at = _piece(j)
                p = jnp.exp2(dot_t(kk[at, :], q) * E - lse)
                if j == i:
                    p = jnp.where(seen, p, 0.0)
                ds = (p * (dot_t(vv[at, :], do) - dl)).astype(BF16)
                by_v, by_k = dot(p.astype(BF16), do), dot(ds, q)
                acc[at, dv_at] = by_v if j == i else acc[at, dv_at] + by_v
                acc[at, dk_at] = by_k if j == i else acc[at, dk_at] + by_k
                by_q = by_q + dot(turned[:, at], ds)
            by_q = (by_q * HEAD**-0.5).astype(BF16)
            for n in range(GROUP):
                dq[_piece(i), column(HEAD * (GROUP * head + n))] = turn_back(by_q[:, _piece(n)].T, _piece(i))
        for i in range(PIECES):
            dq[_piece(i), column(N_Q + HEAD * head)] = turn_back((acc[_piece(i), dk_at] * HEAD**-0.5).astype(BF16), _piece(i))
            dq[_piece(i), column(N_Q + N_K + HEAD * head)] = acc[_piece(i), dv_at].astype(BF16)

    def after_unit(rows):
        by = sum(dot_t(dq[rows, TF * n : TF * (n + 1)], (wg, wu)[n // 2][n % 2]) for n in range(4)).astype(BF16).astype(F32)
        inner = _norm_back(x2[rows, :].astype(F32), by).astype(BF16)
        x1[rows, :] = (x1[rows, :].astype(F32) + inner.astype(F32)).astype(BF16)

    def work(n):
        half, tau = unit_of(n)
        u = tau + EARLY

        @pl.when((u >= 0) & (u < 2 * TILES))
        def _():
            buf = u // 2 % 2

            @pl.when(u % 2 == 0)
            def _():
                wait(tile_copies(half, u // 2, buf))

            @pl.when(u == 0)
            def _():
                wait([local(acts[0]["b"], x2, x_sem.at[1])])
                acc[...] = jnp.zeros((T, D), F32)

            mlp_unit(u, buf)

        @pl.when(tau == LEAVE)
        def _():
            wait([local(acts[0]["h1"], x2, x_sem.at[1]), local(acts[0]["o"], oo, o_sem), *wo_copies(half)])
            loop(PIECES, leave_unit)

        @pl.when((tau == HEADS_AT) | (tau == HEADS_AT + 2))
        def _():
            @pl.when(tau == HEADS_AT)
            def _():
                wait([local(acts[0]["lse"], lseb, lse_sem)])

            wait(head_copies(acts[0], 0))
            head_unit((tau - HEADS_AT) // 2)

        @pl.when((tau >= AFTER) & (tau < AFTER + 2) & (half == 0))
        def _():
            @pl.when(tau == AFTER)
            def _():
                wait([local(r_["h"], x2, x_sem.at[1]), *qkv_weight_copies()])

            loop(PIECES // 2, lambda i: after_unit(tokens(T_HALF * (tau - AFTER) + ROWS * i, ROWS)))

        for test, copies in writes(half, tau):
            pl.when(test)(lambda: start(copies()))


    def load_operands(k):
        half, r = k // PER_LAYER, k % PER_LAYER

        def from_rows(ref, block, down):
            rows, whole = block[0], ref.shape[0] // 8
            for e in range(8):
                owner = 2 * (e % 4) + (1 - core if e < 4 else core)
                at = pl.multiple_of(whole * owner + down, 16)
                local(ref.at[pl.ds(at, rows), :], ab.at[pl.ds(rows * e, rows), :], ab_sem).start()

        def from_columns(ref, j):
            local(ref.at[:, pl.ds(pl.multiple_of(TF * j, TF), TF)], db.at[:, pl.ds(0, TF)], db_sem).start()

        for_layer(half, r < DOWN_AT, lambda a: from_rows(a["bt"], P_BLOCK, 0))
        for_layer(half, r >= QKV_AT, lambda a: from_rows(a["at"], P_BLOCK, 0))
        for_layer(half, (r >= WO_AT) & (r < QKV_AT), lambda a: from_rows(a["ot"], Q_BLOCK, Q_BLOCK[0] * (r - WO_AT)))

        @pl.when((r < DOWN_AT) & (r % 2 == 0))
        def _():
            from_columns(r_["dgate"].at[half], r // 2)

        @pl.when((r < DOWN_AT) & (r % 2 == 1))
        def _():
            from_columns(r_["dup"].at[half], r // 2)

        @pl.when((r >= DOWN_AT) & (r < WO_AT))
        def _():
            from_rows(r_["hidt"].at[half], Q_BLOCK, Q_BLOCK[0] * (r - DOWN_AT))

            @pl.when(half == 0)
            def _():
                local(r_["dy"], db, db_sem).start()

            @pl.when(half == 1)
            def _():
                local(r_["by1"], db, db_sem).start()

        @pl.when((r >= WO_AT) & (r < QKV_AT))
        def _():
            local(r_["d1"].at[half], db, db_sem).start()

        @pl.when(r >= QKV_AT)
        def _():
            from_columns(r_["dqkv"].at[half], r - QKV_AT)

    def wait_operands(block):
        rows, cols = block
        local(r_["hidt"].at[0, pl.ds(0, 8 * rows), :], ab.at[pl.ds(0, 8 * rows), :], ab_sem).wait()
        local(r_["dgate"].at[0, :, pl.ds(0, cols)], db.at[:, pl.ds(0, cols)], db_sem).wait()

    def optimizer_copies(k, buf, do):
        layer, r = 1 - k // PER_LAYER, k % PER_LAYER
        for name, test, j in _owners(layer, r):
            rows, cols = block = Q_BLOCK if name in ("w_down", "wo") else P_BLOCK

            @pl.when(test)
            def _():
                whole = w_in[name].shape[1] // 8
                down = pl.multiple_of(rows * j if block == Q_BLOCK else 0 * j, 16)
                right = pl.ds(0, cols) if block == Q_BLOCK else pl.ds(pl.multiple_of(cols * j, cols), cols)
                for n, (ref, at, to) in enumerate(((m_in[name], down, mb), (v_in[name], down, vb), (w_in[name], pl.multiple_of(whole * me + down, 16), wb))):
                    do(local(ref.at[layer, pl.ds(at, rows), right], to.at[buf, pl.ds(0, rows), pl.ds(0, cols)], opt_sem.at[buf, n]))


    barrier = pltpu.get_barrier_semaphore()
    first = [local(r_["dy"], x1, x_sem.at[0]), local(r_["cos"], cosb, o_sem), local(r_["sin"], sinb, lse_sem)]
    start([*tile_copies(0, 0, 0), local(acts[0]["b"], x2, x_sem.at[1]), *first])
    tell(barrier, mate)

    @pl.when(has_above)
    def _():
        tell(barrier, above)

    @pl.when(has_below)
    def _():
        tell(barrier, below)

    @pl.when(has_above & has_below)
    def _():
        pl.semaphore_wait(barrier, 3)

    @pl.when(jnp.logical_not(has_above & has_below))
    def _():
        pl.semaphore_wait(barrier, 2)

    wait(first)

    def tick(n):
        t = n - EARLY
        slot, prev, late = n % SLOTS, (n + SLOTS - 1) % SLOTS, (n + 1) % SLOTS
        two = n % 2


        @pl.when(n >= 3)
        def _():
            pl.semaphore_wait(free_m, 1)

            @pl.when(has_above)
            def _():
                pl.semaphore_wait(free_u, 1)

            @pl.when(has_below)
            def _():
                pl.semaphore_wait(free_d, 1)

            @pl.when(ok(t - 3))
            def _():
                for s in range(CHIPS):
                    remote(ps.at[late, s], pr.at[late, s], ps_s.at[late, s], ps_r.at[late, s], mate).wait_send()

            @pl.when(ok(t - 4 - z))
            def _():
                for s in range(1, CHIPS):
                    @pl.when(s > z)
                    def _():
                        remote(su.at[late, s], ru.at[late, s], su_s.at[late, s], su_r.at[late, s], mate).wait_send()

            @pl.when(ok(t - 4 - (CHIPS - 1 - z)))
            def _():
                for s in range(CHIPS - 1):
                    @pl.when(s < z)
                    def _():
                        remote(sd.at[late, s], rd.at[late, s], sd_s.at[late, s], sd_r.at[late, s], mate).wait_send()

            def gone(s):
                @pl.when(ok(t - 7 - jnp.abs(z - s)))
                def _():
                    there = wp.at[0, 0]
                    remote(there, there, am_s.at[late, s], am_r.at[late, s], mate).wait_send()

                    @pl.when((s <= z) & has_above)
                    def _():
                        remote(there, there, au_s.at[late, s], au_r.at[late, s], mate).wait_send()

                    @pl.when((s >= z) & has_below)
                    def _():
                        remote(there, there, ad_s.at[late, s], ad_r.at[late, s], mate).wait_send()

            loop(CHIPS, gone)

            @pl.when(ok(t - 7))
            def _():
                local(wn.at[late], wp.at[0, 0], out_sem.at[late, 0]).wait()
                local(gn.at[late], gp.at[0], out_sem.at[late, 1]).wait()


        for test, copies in writes(*unit_of(n - 1)):
            pl.when(test & (n > 0))(lambda: wait(copies()))
        fetch(n)

        @pl.when(ok(t))
        def _():
            load_operands(t)

        @pl.when(ok(t - 3))
        def _():
            optimizer_copies(t - 3, 1 - two, lambda copy: copy.start())


        def pass_on(s, k, from_above):
            got, send, here, there, to = (rd, sd, sd_s, sd_r, below) if from_above else (ru, su, su_s, su_r, above)
            remote(send.at[prev, s], got.at[prev, s], here.at[prev, s], there.at[prev, s], mate).wait_recv()
            value = chip[k % SUMS, s] + got[prev, s].astype(F32)
            chip[k % SUMS, s] = value
            send[slot, s] = value.astype(BF16)

            @pl.when((s < z) if from_above else (s > z))
            def _():
                remote(send.at[slot, s], got.at[slot, s], here.at[slot, s], there.at[slot, s], to).start()

        up_k, down_k = t - 1 - z, t - 1 - (CHIPS - 1 - z)
        for i in range(CHIPS - 1):
            @pl.when(has_below & ok(up_k) & (CHIPS - 1 - i >= z))
            def _():
                pass_on(CHIPS - 1 - i, up_k, False)

            @pl.when(has_above & ok(down_k) & (i <= z))
            def _():
                pass_on(i, down_k, True)


        @pl.when(ok(t - 4))
        def _():
            k = t - 4
            optimizer_copies(k, two, lambda copy: copy.wait())
            is_q = _is_q(k % PER_LAYER)
            for (rows, cols), test in ((Q_BLOCK, is_q), (P_BLOCK, jnp.logical_not(is_q))):
                @pl.when(test)
                def _():
                    for j in range(cols // LANES):
                        at, over = slice(rows * j, rows * (j + 1)), slice(LANES * j, LANES * (j + 1))
                        low = chip[k % SUMS, z, at, :].astype(BF16)
                        m, v = _moments(mb[two, :rows, over], vb[two, :rows, over], low.astype(F32))
                        w = wb[two, :rows, over].astype(F32)
                        wn[slot, at, :] = (w - 0.02 * (m * lax.rsqrt(v + 1e-8) + 0.1 * w)).astype(BF16)
                        gn[slot, at, :] = low

            at = _place(k)
            local(wn.at[slot], wp.at[at, me], out_sem.at[slot, 0]).start()
            local(gn.at[slot], gp.at[at], out_sem.at[slot, 1]).start()


        def sends(s, source, there):
            @pl.when((s <= z) & has_above)
            def _():
                remote(source, there, au_s.at[slot, s], au_r.at[slot, s], above).start()

            @pl.when((s >= z) & has_below)
            def _():
                remote(source, there, ad_s.at[slot, s], ad_r.at[slot, s], below).start()

            remote(source, there, am_s.at[slot, s], am_r.at[slot, s], mate).start()

        @pl.when(ok(t - 4))
        def _():
            sends(z, wn.at[slot], wp.at[_place(t - 4), me])

        work(n)

        def spread(s):
            k = t - 4 - jnp.abs(z - s)

            @pl.when(ok(k) & (s != z))
            def _():
                there = wp.at[_place(k), 2 * s + core]

                @pl.when(s < z)
                def _():
                    remote(there, there, au_s.at[prev, s], au_r.at[prev, s], mate).wait_recv()

                @pl.when(s > z)
                def _():
                    remote(there, there, ad_s.at[prev, s], ad_r.at[prev, s], mate).wait_recv()

                sends(s, there, there)

        loop(CHIPS, spread)


        @pl.when(ok(t - 1))
        def _():
            for s in (3, 0, 2, 1):
                remote(ps.at[prev, s], pr.at[prev, s], ps_s.at[prev, s], ps_r.at[prev, s], mate).wait_recv()
                value = chip[(t - 1) % SUMS, s] + pr[prev, s].astype(F32)
                chip[(t - 1) % SUMS, s] = value
                if s > 0:
                    @pl.when(z == 0)
                    def _():
                        su[slot, s] = value.astype(BF16)
                        remote(su.at[slot, s], ru.at[slot, s], su_s.at[slot, s], su_r.at[slot, s], above).start()
                if s < CHIPS - 1:
                    @pl.when(z == CHIPS - 1)
                    def _():
                        sd[slot, s] = value.astype(BF16)
                        remote(sd.at[slot, s], rd.at[slot, s], sd_s.at[slot, s], sd_r.at[slot, s], below).start()


        @pl.when(ok(t))
        def _():
            is_q = _is_q(t % PER_LAYER)
            for (rows, cols), test in ((Q_BLOCK, is_q), (P_BLOCK, jnp.logical_not(is_q))):
                @pl.when(test)
                def _():
                    wait_operands((rows, cols))
                    for own in range(2):
                        got = dot(ab[4 * rows * own : 4 * rows * (own + 1), :], db[:, :cols])
                        for s in range(CHIPS):
                            for j in range(cols // LANES):
                                piece = got[rows * s : rows * (s + 1), LANES * j : LANES * (j + 1)]
                                if own:
                                    chip[t % SUMS, s, rows * j : rows * (j + 1), :] = piece
                                else:
                                    ps[slot, s, rows * j : rows * (j + 1), :] = piece.astype(BF16)
                        if not own:
                            for s in (3, 0, 2, 1):
                                remote(ps.at[slot, s], pr.at[slot, s], ps_s.at[slot, s], ps_r.at[slot, s], mate).start()


        def arrived(s):
            @pl.when(ok(t - 5 - jnp.abs(z - s)))
            def _():
                there = wp.at[0, 0]
                remote(there, there, am_s.at[prev, s], am_r.at[prev, s], mate).wait_recv()

        loop(CHIPS, arrived)

        @pl.when(n < TICKS - 3)
        def _():
            tell(free_m, mate)

            @pl.when(has_above)
            def _():
                tell(free_d, above)

            @pl.when(has_below)
            def _():
                tell(free_u, below)

    loop(TICKS, tick)


def update(acts, given, w, m, v):
    vm, sem = pltpu.VMEM, pltpu.SemaphoreType
    block = (BLOCK, LANES)
    four = lambda: sem.DMA((SLOTS, CHIPS))
    scratch = [
        vm((D, T), BF16), vm((T, D), BF16), vm((SUMS, CHIPS, *block), F32),
        *(vm((SLOTS, CHIPS, *block), BF16) for _ in range(6)),
        vm((SLOTS, *block), BF16), vm((SLOTS, *block), BF16),
        vm((2, 112, D), F32), vm((2, 112, D), F32), vm((2, 112, D), BF16),
        vm((T, D), BF16), vm((T, D), BF16), vm((HEADS, T, HEAD), BF16),
        vm((2, D, TF), BF16), vm((2, D, TF), BF16), vm((2, TF, D), BF16), vm((T, D), F32),
        *(vm((TF, TF), BF16) for _ in range(3)),
        vm((GROUP, T, HEAD), BF16), vm((T, HEAD), BF16), vm((T, HEAD), BF16), vm((T, N_Q + 2 * N_K), BF16),
        vm((T, HALF), F32), vm((T, HALF), F32), vm((KV, GROUP, T), F32), vm((KV, GROUP, T), F32),
        sem.DMA, sem.DMA, sem.DMA((2, 3)), sem.DMA((SLOTS, 2)), sem.DMA((2, 3)), sem.DMA((2,)), sem.DMA, sem.DMA((3,)), sem.DMA, sem.DMA((3,)),
        *(four() for _ in range(12)),
        sem.REGULAR, sem.REGULAR, sem.REGULAR,
    ]
    refs = [a[name] for a in acts for name in LAYER_INPUTS] + [*w, *m, *v] + [given[name] for name in INPUTS]
    outs = [(CHUNKS, 8, *block), (CHUNKS, *block), (2, FF, T), (2, T, FF), (2, T, FF), (2, T, D), (2, T, N_Q + 2 * N_K), (T, D)]
    return pl.pallas_call(
        _update,
        in_specs=[pl.BlockSpec(memory_space=pl.ANY)] * len(refs),
        out_specs=[pl.BlockSpec(memory_space=pl.ANY)] * len(outs),
        out_shape=[jax.ShapeDtypeStruct(shape, BF16) for shape in outs],
        scratch_shapes=scratch,
        compiler_params=pltpu.CompilerParams(collective_id=0, has_side_effects=True, vmem_limit_bytes=63 * 2**20),
        name="update",
    )(*refs)[:2]


def _moments(m, v, g):
    return 0.9 * m + 0.1 * g, 0.95 * v + 0.05 * g * g


def _unpack(*refs):
    s = pl.program_id(1)
    ins, outs = refs[: 4 * len(NAMES)], refs[4 * len(NAMES) :]
    for i, name in enumerate(NAMES):
        wp_ref, gp_ref, m_ref, v_ref = ins[4 * i : 4 * i + 4]
        w_out, m_out, v_out = outs[i :: len(NAMES)]
        tall = name in ("w_down", "wo")
        rows, cols = Q_BLOCK if tall else P_BLOCK
        some = m_ref.shape[1]
        for j in range(cols // LANES):
            for n in range(wp_ref.shape[0]):
                over = slice(LANES * j, LANES * (j + 1)) if tall else slice(cols * n + LANES * j, cols * n + LANES * (j + 1))
                down = slice(rows * n, rows * (n + 1)) if tall else slice(0, rows)
                w_out[0, down, over] = wp_ref[n, 0, rows * j : rows * (j + 1), :]
                if tall and n:
                    continue
                if tall:
                    per = rows // some
                    g = gp_ref[s // per if name == "wo" else jnp.minimum(s, 6), pl.ds(pl.multiple_of(rows * j + some * (s % per), 16), some), :]
                else:
                    g = gp_ref[n, pl.ds(pl.multiple_of(rows * j + some * jnp.minimum(s, 6), 16), some), :]
                m_out[0, :, over], v_out[0, :, over] = _moments(m_ref[0, :, over], v_ref[0, :, over], g.astype(F32))


def unpack(wp, gp, m, v):
    block = (BLOCK, LANES)
    where = {"wq": (2, 22, 3), "wk": (1, 46, 6), "wv": (1, 47, 6), "wo": (2, 21, 3), "w_gate": (7, 0, 1), "w_up": (7, 2, 1), "w_down": (7, 4, 1)}
    in_specs, given, full, own = [], [], [], []
    for name in NAMES:
        count, start, step = where[name]
        _, height, width = m[name].shape
        some = 64 if name == "w_down" else 16
        last = height // some - 1
        mine = pl.BlockSpec((1, some, width), lambda layer, s, last=last: (layer, jnp.minimum(s, last), 0))
        in_specs += [
            pl.BlockSpec((count, 1, *block), lambda layer, s, start=start, step=step: (start + step * layer, s, 0, 0)),
            pl.BlockSpec((count, *block), lambda layer, s, start=start, step=step: (start + step * layer, 0, 0)), mine, mine,
        ]
        given += [wp, gp, m[name], v[name]]
        full.append((pl.BlockSpec((1, height, width), lambda layer, s: (layer, s, 0)), jax.ShapeDtypeStruct((2, 8 * height, width), BF16)))
        own.append((mine, jax.ShapeDtypeStruct(m[name].shape, F32)))
    outs = full + own + own
    return pl.pallas_call(
        _unpack,
        grid=(2, 8),
        in_specs=in_specs,
        out_specs=[o[0] for o in outs],
        out_shape=[o[1] for o in outs],
        compiler_params=pltpu.CompilerParams(vmem_limit_bytes=VMEM),
        name="unpack",
    )(*given)


def solution(mesh):
    def step(x, dy, *arrays):
        w, m, v = (dict(zip(NAMES, arrays[i : i + 7], strict=True)) for i in (0, 7, 14))
        angle = jnp.arange(T, dtype=F32)[:, None] * THETA ** (-jnp.arange(HALF, dtype=F32) / HALF)
        cos, sin = jnp.cos(angle), jnp.sin(angle)

        def attention_of(h, layer):
            q, k, v, at = before(h, w["wq"], w["wk"], w["wv"], cos, sin, layer)
            out, ot, lse = attend(q, k, v)
            return {"q": q, "k": k, "v": v, "o": out, "ot": ot, "at": at, "lse": lse}

        h0 = x[0]
        a0 = attention_of(h0, 0)
        a0["h1"], a0["b"], a0["bt"], h = mlp(a0["o"], h0, w["wo"], w["w_gate"], w["w_up"], w["w_down"], 0)
        a1 = attention_of(h, 1)
        a1["h1"], a1["b"], a1["bt"] = project(a1["o"], h, w["wo"], 1)
        wp, gp = update([a1, a0], {"dy": dy[0], "h": h, "cos": cos, "sin": sin}, w.values(), m.values(), v.values())
        return tuple(unpack(wp, gp, m, v))

    states, all_of, cut = P(("rep", "dp"), None, None), P(None, None, None), P(None, "dp", None)
    return jax.shard_map(
        step,
        mesh=mesh,
        in_specs=(states, states) + (all_of,) * 7 + (cut,) * 14,
        out_specs=(P("rep", None, None),) * 7 + (P("rep", "dp", None),) * 14,
        check_vma=False,
    )
```

```python
import functools

import jax
import jax.numpy as jnp
import numpy as np
from jax import lax
from jax.experimental import pallas as pl
from jax.experimental.pallas import tpu as pltpu
from jax.sharding import PartitionSpec as P

LOG2E = 1.4426950408889634
HIDDEN = -2e30
VMEM = 56 * 2**20
F32, BF16 = jnp.float32, jnp.bfloat16
MESH = pl.DeviceIdType.MESH
T, D, FF, HEADS, KV, HEAD = 1024, 896, 3584, 4, 2, 256
THETA = 10000
STRIDE = 32
NAMES = ("wq", "wk", "wv", "wo", "w_gate", "w_up", "w_down")
ROWS = 256
TF = 512
PIECES = T // ROWS


def loop(count, body):
    lax.fori_loop(0, count, lambda i, _: body(i), None)


def dot(a, b):
    return jnp.dot(a, b, preferred_element_type=F32)


def dot_t(a, b):
    return lax.dot_general(a, b, (((1,), (1,)), ((), ())), preferred_element_type=F32)


def _scale(wide):
    return lax.rsqrt(jnp.mean(wide * wide, -1, keepdims=True) + 1e-6)


def _norm_back(h, by):
    s = _scale(h)
    return by * s - h * (s * s * s * jnp.mean(by * h, -1, keepdims=True))


E = HEAD**-0.5 * LOG2E
GROUP = HEADS // KV


def _piece(i):
    return slice(ROWS * i, ROWS * (i + 1))


def _visible():
    shape = (ROWS, GROUP * ROWS)
    return lax.broadcasted_iota(jnp.int32, shape, 0) <= lax.rem(lax.broadcasted_iota(jnp.int32, shape, 1), ROWS)


LANES = 128
BLOCK = 448
SLOTS = 4
SUMS = 5
EARLY = 2
LAG = 22
P_BLOCK, Q_BLOCK = (112, 512), (64, 896)
TILES = FF // TF
DOWN_AT, WO_AT, QKV_AT, PER_LAYER = 14, 21, 23, 27
CHUNKS = 2 * PER_LAYER
TICKS = CHUNKS + 11 + EARLY
CHIPS = 4
HALF, T_HALF = HEAD // 2, T // 2
N_Q, N_K = HEADS * HEAD, KV * HEAD
LEAVE, HEADS_AT, AFTER = 13, 14, 17


def _is_q(r):
    return (r >= DOWN_AT) & (r < QKV_AT)


def _place(k):
    layer, r = 1 - k // PER_LAYER, k % PER_LAYER
    double, single = (r % 2) * DOWN_AT + layer * TILES + r // 2, 2 * DOWN_AT + layer * TILES + r - DOWN_AT
    return jnp.where(r < DOWN_AT, double, jnp.where(r < WO_AT, single, 3 * DOWN_AT + layer * (PER_LAYER - WO_AT) + r - WO_AT))


def _owners(layer, r):
    mlp_chunk = r < DOWN_AT
    return (
        ("w_gate", mlp_chunk & (r % 2 == 0), r // 2), ("w_up", mlp_chunk & (r % 2 == 1), r // 2),
        ("w_down", (r >= DOWN_AT) & (r < WO_AT), r - DOWN_AT), ("wo", (r >= WO_AT) & (r < QKV_AT), r - WO_AT),
        ("wq", (r >= QKV_AT) & (r < QKV_AT + 2), r - QKV_AT), ("wk", r == QKV_AT + 2, 0 * r), ("wv", r == QKV_AT + 3, 0 * r),
    )


INPUTS = ("x", "dy", "turns")
OUTPUTS = ("wp", "gp", "hidt", "dgate", "dup", "d1", "dqkv", "at", "ot", "bt", "b", "h1", "o", "qkv", "lse", "h", "by1")
SCRATCH = ("ab", "db", "chip", "ps", "pr", "su", "ru", "sd", "rd", "wn", "gn", "mb", "vb", "wb", "x1", "x2", "oo", "wg", "wu", "wd", "acc", "dg", "du", "ht",
           "qq", "kk", "vv", "dq", "st", "cosb", "sinb", "lseb", "delta", "tb",
           "ab_sem", "db_sem", "opt_sem", "out_sem", "tile_sem", "x_sem", "o_sem", "qkv_sem", "lse_sem", "write_sem", "save_sem",
           "ps_s", "ps_r", "su_s", "su_r", "sd_s", "sd_r", "am_s", "am_r", "au_s", "au_r", "ad_s", "ad_r", "free_m", "free_u", "free_d")


def _update(*refs):
    w_in, m_in, v_in = (dict(zip(NAMES, refs[i : i + 7])) for i in (0, 7, 14))
    r_ = dict(zip((*INPUTS, *OUTPUTS, *SCRATCH), refs[21:], strict=True))
    (ab, db, chip, ps, pr, su, ru, sd, rd, wn, gn, mb, vb, wb, x1, x2, oo, wg, wu, wd, acc, dg, du, ht, qq, kk, vv, dq, st, cosb, sinb, lseb, delta, tb,
     ab_sem, db_sem, opt_sem, out_sem, tile_sem, x_sem, o_sem, qkv_sem, lse_sem, write_sem, save_sem,
     ps_s, ps_r, su_s, su_r, sd_s, sd_r, am_s, am_r, au_s, au_r, ad_s, ad_r, free_m, free_u, free_d) = (r_[name] for name in SCRATCH)
    wp, gp = r_["wp"], r_["gp"]
    rep, me = lax.axis_index("rep"), lax.axis_index("dp")
    z, core = me // 2, me % 2
    mate, above, below = me + 1 - 2 * core, me + 2, me - 2
    has_above, has_below = z < CHIPS - 1, z > 0

    def remote(src, dst, send, recv, to):
        return pltpu.make_async_remote_copy(src_ref=src, dst_ref=dst, send_sem=send, recv_sem=recv, device_id=(rep, to), device_id_type=MESH)

    def tell(sem, to):
        pl.semaphore_signal(sem, inc=1, device_id=(rep, to), device_id_type=MESH)

    def local(src, dst, sem):
        return pltpu.make_async_copy(src, dst, sem)

    def ok(k):
        return (k >= 0) & (k < CHUNKS)

    def tokens(start, count):
        return pl.ds(pl.multiple_of(start, ROWS), count)


    def tile_copies(half, j, buf):
        layer, over = 1 - half, pl.ds(pl.multiple_of(TF * j, TF), TF)
        return [
            local(w_in["w_gate"].at[layer, :, over], wg.at[buf], tile_sem.at[buf, 0]),
            local(w_in["w_up"].at[layer, :, over], wu.at[buf], tile_sem.at[buf, 1]),
            local(w_in["w_down"].at[layer, over, :], wd.at[buf], tile_sem.at[buf, 2]),
        ]

    def wo_copies(half):
        return [local(w_in["wo"].at[1 - half, pl.ds(TF * n, TF), :], wd.at[n], tile_sem.at[n, 2]) for n in range(2)]

    def qkv_weight_copies(half):
        layer = 1 - half
        return [
            *(local(w_in["wq"].at[layer, :, pl.ds(TF * n, TF)], wg.at[n], tile_sem.at[n, 0]) for n in range(2)),
            local(w_in["wk"].at[layer], wu.at[0], tile_sem.at[0, 1]), local(w_in["wv"].at[layer], wu.at[1], tile_sem.at[1, 1]),
        ]

    def column(at):
        return pl.ds(pl.multiple_of(at, HEAD), HEAD)

    def head_copies(half, head):
        pair = pl.ds(pl.multiple_of(GROUP * HEAD * head, GROUP * HEAD), GROUP * HEAD)
        return [
            local(r_["qkv"].at[half, :, over], to, qkv_sem.at[n])
            for n, (over, to) in enumerate(((pair, qq), (column(N_Q + HEAD * head), kk), (column(N_Q + N_K + HEAD * head), vv)))
        ]

    def load_x2(ref):
        return local(ref, x2, x_sem.at[1])

    def unit_of(n):
        half = (n >= AFTER + 2 + EARLY).astype(jnp.int32)
        return half, n - EARLY - LAG * half

    def start(copies):
        for copy in copies:
            copy.start()

    def wait(copies):
        for copy in copies:
            copy.wait()

    def writes(half, tau):
        u = tau + EARLY
        j, first = u // 2, tokens(T_HALF * (u % 2), T_HALF)
        over = pl.ds(pl.multiple_of(TF * j, TF), TF)
        part = tokens(T_HALF * (tau - AFTER), T_HALF)
        after_at = (tau >= AFTER) & (tau < AFTER + 2)
        return (
            ((u >= 0) & (u < 2 * TILES), lambda: [
                local(dg, r_["dgate"].at[half, first, over], write_sem.at[0]), local(du, r_["dup"].at[half, first, over], write_sem.at[1]),
                local(ht, r_["hidt"].at[half, over, first], write_sem.at[2])]),
            (tau == LEAVE, lambda: [local(x1, r_["d1"].at[half], write_sem.at[0])]),
            (after_at, lambda: [local(dq.at[part, :], r_["dqkv"].at[half, part, :], write_sem.at[0])]),
            (after_at & (half == 0), lambda: [local(x1.at[part, :], r_["by1"].at[part, :], write_sem.at[1])]),
        )

    def fetch(n):
        half, tau = unit_of(n)
        u = tau + EARLY

        @pl.when((tau == -EARLY - 1) & (half == 1))
        def _():
            start([*tile_copies(half, 0, 0), load_x2(r_["b"].at[half])])

        @pl.when((u >= 0) & (u % 2 == 0) & (u < 2 * TILES - 2))
        def _():
            start(tile_copies(half, u // 2 + 1, (u // 2 + 1) % 2))

        @pl.when(tau == LEAVE - 1)
        def _():
            start([*wo_copies(half), load_x2(r_["h1"].at[half]), local(r_["o"].at[half], oo, o_sem)])

        @pl.when(tau == LEAVE)
        def _():
            start([*head_copies(half, 0), local(r_["lse"].at[half], lseb, lse_sem)])

        @pl.when(tau == HEADS_AT + 1)
        def _():
            start(head_copies(half, 1))

        @pl.when((tau == LEAVE - 1) & (half == 0))
        def _():
            start(qkv_weight_copies(0))

        @pl.when((tau == HEADS_AT) & (half == 0))
        def _():
            start([load_x2(r_["h"])])

    def mlp_unit(u, buf):
        rows = tokens(T_HALF * (u % 2), T_HALF)
        gate, up = dot(x2[rows, :], wg[buf]), dot(x2[rows, :], wu[buf])
        sig = 1.0 / (1.0 + jnp.exp(-gate))
        silu = gate * sig
        by = dot_t(x1[rows, :], wd[buf]).astype(BF16).astype(F32)
        ht[...] = (silu * up).astype(BF16).T
        du[...] = (by * silu).astype(BF16)
        dg[...] = (by * up * (sig * (1.0 + gate * (1.0 - sig)))).astype(BF16)
        acc[rows, :] += dot_t(dg[...], wg[buf]) + dot_t(du[...], wu[buf])

    def leave_unit(i):
        rows = tokens(ROWS * i, ROWS)
        inner = _norm_back(x2[rows, :].astype(F32), acc[rows, :].astype(BF16).astype(F32)).astype(BF16)
        d1 = (x1[rows, :].astype(F32) + inner.astype(F32)).astype(BF16)
        x1[rows, :] = d1
        for n in range(HEADS):
            low, over = HEAD * (n % 2), _piece(n)
            do = dot_t(d1, wd[n // 2, low : low + HEAD, :]).astype(BF16)
            both = do.astype(F32) * oo[rows, over].astype(F32)
            oo[rows, over] = do
            delta[n // GROUP, n % GROUP : n % GROUP + 1, rows] = both.T.sum(0, keepdims=True)

    def side(ref, i, head):
        return jnp.concatenate([ref[_piece(i), column(HEAD * (GROUP * head + n))] for n in range(GROUP)], axis=0)

    def turn_back(part, rows):
        cos, sin = cosb[rows, :], sinb[rows, :]
        x, y = part[:, :HALF].astype(F32), part[:, HALF:].astype(F32)
        return jnp.concatenate([x * cos + y * sin, y * cos - x * sin], -1).astype(BF16)

    def head_unit(head):
        seen = _visible()
        turned = kk[...].T
        line = lambda ref, i: jnp.concatenate([ref[head, n : n + 1, _piece(i)] for n in range(GROUP)], axis=1)
        dk_at, dv_at = slice(0, HEAD), slice(HEAD, 2 * HEAD)
        for i in range(PIECES):
            lse, dl = line(lseb, i), line(delta, i)
            q = jnp.concatenate([qq[_piece(i), _piece(n)] for n in range(GROUP)], axis=0)
            do = side(oo, i, head)
            by_q = 0.0
            for j in range(i + 1):
                at = _piece(j)
                p = jnp.exp2(dot_t(kk[at, :], q) * E - lse)
                if j == i:
                    p = jnp.where(seen, p, 0.0)
                ds = (p * (dot_t(vv[at, :], do) - dl)).astype(BF16)
                by_v, by_k = dot(p.astype(BF16), do), dot(ds, q)
                acc[at, dv_at] = by_v if j == i else acc[at, dv_at] + by_v
                acc[at, dk_at] = by_k if j == i else acc[at, dk_at] + by_k
                by_q = by_q + dot(turned[:, at], ds)
            by_q = (by_q * HEAD**-0.5).astype(BF16)
            for n in range(GROUP):
                dq[_piece(i), column(HEAD * (GROUP * head + n))] = turn_back(by_q[:, _piece(n)].T, _piece(i))
        for i in range(PIECES):
            dq[_piece(i), column(N_Q + HEAD * head)] = turn_back((acc[_piece(i), dk_at] * HEAD**-0.5).astype(BF16), _piece(i))
            dq[_piece(i), column(N_Q + N_K + HEAD * head)] = acc[_piece(i), dv_at].astype(BF16)

    def after_unit(rows):
        by = sum(dot_t(dq[rows, TF * n : TF * (n + 1)], (wg, wu)[n // 2][n % 2]) for n in range(4)).astype(BF16).astype(F32)
        inner = _norm_back(x2[rows, :].astype(F32), by).astype(BF16)
        x1[rows, :] = (x1[rows, :].astype(F32) + inner.astype(F32)).astype(BF16)

    def work(n):
        half, tau = unit_of(n)
        u = tau + EARLY

        @pl.when((u >= 0) & (u < 2 * TILES))
        def _():
            buf = u // 2 % 2

            @pl.when(u % 2 == 0)
            def _():
                wait(tile_copies(half, u // 2, buf))

            @pl.when(u == 0)
            def _():
                acc[...] = jnp.zeros((T, D), F32)

                @pl.when(half == 1)
                def _():
                    load_x2(r_["h"]).wait()

            mlp_unit(u, buf)

        @pl.when(tau == LEAVE)
        def _():
            wait([load_x2(r_["h"]), local(r_["o"].at[0], oo, o_sem), *wo_copies(half)])
            loop(PIECES, leave_unit)

        @pl.when((tau == HEADS_AT) | (tau == HEADS_AT + 2))
        def _():
            @pl.when(tau == HEADS_AT)
            def _():
                local(r_["lse"].at[0], lseb, lse_sem).wait()

            wait(head_copies(0, 0))
            head_unit((tau - HEADS_AT) // 2)

        @pl.when((tau >= AFTER) & (tau < AFTER + 2) & (half == 0))
        def _():
            @pl.when(tau == AFTER)
            def _():
                wait([load_x2(r_["h"]), *qkv_weight_copies(0)])

            loop(PIECES // 2, lambda i: after_unit(tokens(T_HALF * (tau - AFTER) + ROWS * i, ROWS)))

        for test, copies in writes(half, tau):
            pl.when(test)(lambda: start(copies()))


    def load_operands(k):
        half, r = k // PER_LAYER, k % PER_LAYER

        def from_rows(ref, block, down):
            rows, whole = block[0], ref.shape[0] // 8
            for e in range(8):
                owner = 2 * (e % 4) + (1 - core if e < 4 else core)
                at = pl.multiple_of(whole * owner + down, 16)
                local(ref.at[pl.ds(at, rows), :], ab.at[pl.ds(rows * e, rows), :], ab_sem).start()

        def from_columns(ref, j):
            local(ref.at[:, pl.ds(pl.multiple_of(TF * j, TF), TF)], db.at[:, pl.ds(0, TF)], db_sem).start()

        @pl.when(r < DOWN_AT)
        def _():
            from_rows(r_["bt"].at[half], P_BLOCK, 0)

        @pl.when((r < DOWN_AT) & (r % 2 == 0))
        def _():
            from_columns(r_["dgate"].at[half], r // 2)

        @pl.when((r < DOWN_AT) & (r % 2 == 1))
        def _():
            from_columns(r_["dup"].at[half], r // 2)

        @pl.when((r >= DOWN_AT) & (r < WO_AT))
        def _():
            from_rows(r_["hidt"].at[half], Q_BLOCK, Q_BLOCK[0] * (r - DOWN_AT))

            @pl.when(half == 0)
            def _():
                local(r_["dy"], db, db_sem).start()

            @pl.when(half == 1)
            def _():
                local(r_["by1"], db, db_sem).start()

        @pl.when((r >= WO_AT) & (r < QKV_AT))
        def _():
            from_rows(r_["ot"].at[half], Q_BLOCK, Q_BLOCK[0] * (r - WO_AT))
            local(r_["d1"].at[half], db, db_sem).start()

        @pl.when(r >= QKV_AT)
        def _():
            from_rows(r_["at"].at[half], P_BLOCK, 0)
            from_columns(r_["dqkv"].at[half], r - QKV_AT)

    def wait_operands(block):
        rows, cols = block
        local(r_["hidt"].at[0, pl.ds(0, 8 * rows), :], ab.at[pl.ds(0, 8 * rows), :], ab_sem).wait()
        local(r_["dgate"].at[0, :, pl.ds(0, cols)], db.at[:, pl.ds(0, cols)], db_sem).wait()

    def optimizer_copies(k, buf, do):
        layer, r = 1 - k // PER_LAYER, k % PER_LAYER
        for name, test, j in _owners(layer, r):
            rows, cols = block = Q_BLOCK if name in ("w_down", "wo") else P_BLOCK

            @pl.when(test)
            def _():
                whole = w_in[name].shape[1] // 8
                down = pl.multiple_of(rows * j if block == Q_BLOCK else 0 * j, 16)
                right = pl.ds(0, cols) if block == Q_BLOCK else pl.ds(pl.multiple_of(cols * j, cols), cols)
                for n, (ref, at, to) in enumerate(((m_in[name], down, mb), (v_in[name], down, vb), (w_in[name], pl.multiple_of(whole * me + down, 16), wb))):
                    do(local(ref.at[layer, pl.ds(at, rows), right], to.at[buf, pl.ds(0, rows), pl.ds(0, cols)], opt_sem.at[buf, n]))


    def save(n, source, to):
        return local(source, to, save_sem.at[n])

    def attend_head(head):
        seen = _visible()
        k_at, turned = column(N_Q + HEAD * head), dq[:, column(N_Q + N_K + HEAD * head)].T
        for i in range(PIECES):
            q = side(dq, i, head)
            scores = [dot_t(dq[_piece(j), k_at], q) for j in range(i + 1)]
            scores[i] = jnp.where(seen, scores[i], HIDDEN)
            top = functools.reduce(jnp.maximum, [s.max(axis=0, keepdims=True) for s in scores])
            total, mix = 0.0, 0.0
            for j, s in enumerate(scores):
                p = jnp.exp2((s - top) * E)
                total = total + p.sum(axis=0, keepdims=True)
                mix = mix + dot(turned[:, _piece(j)], p.astype(BF16))
            out = (mix * (1.0 / total)).astype(BF16)
            lse = top * E + jnp.log(total) * LOG2E
            for n in range(GROUP):
                over = column(HEAD * (GROUP * head + n))
                st[over, _piece(i)] = out[:, _piece(n)]
                oo[_piece(i), over] = out[:, _piece(n)].T
                lseb[head, n : n + 1, _piece(i)] = lse[:, _piece(n)]

    def forward(layer):
        half = 1 - layer
        kept = lambda name: r_[name].at[half]
        wait(qkv_weight_copies(half))
        saves = [save(0, ab, kept("at")), save(1, dq, kept("qkv"))]
        for i in range(PIECES):
            wide = x1[_piece(i), :].astype(F32)
            a = (wide * _scale(wide)).astype(BF16)
            ab[:, _piece(i)] = a.T
            cos, sin = cosb[_piece(i), :], sinb[_piece(i), :]
            for c, w in enumerate((wg[0], wg[1], wu[0], wu[1])):
                t = dot(a, w).astype(BF16)
                for n in range(2):
                    part = t[:, _piece(n)]
                    if c < 3:
                        p, q = part[:, :HALF].astype(F32), part[:, HALF:].astype(F32)
                        part = jnp.concatenate([p * cos - q * sin, q * cos + p * sin], -1).astype(BF16)
                    dq[_piece(i), TF * c + HEAD * n : TF * c + HEAD * (n + 1)] = part
        tile = tile_copies(half, 0, 0)
        start([*saves, *wo_copies(half), *tile[:2]])
        loop(KV, attend_head)
        wait([*saves, *wo_copies(half)])
        saves = [save(0, ab, kept("bt")), save(1, x1, kept("h1")), save(2, x2, kept("b")), save(3, st, kept("ot")), save(4, oo, kept("o")), save(5, lseb, kept("lse"))]
        start(saves[3:])
        for i in range(PIECES):
            rows = _piece(i)
            total = dot(oo[rows, :TF], wd[0]) + dot(oo[rows, TF:], wd[1])
            h1 = (x1[rows, :].astype(F32) + total.astype(BF16).astype(F32)).astype(BF16)
            x1[rows, :] = h1
            wide = h1.astype(F32)
            b = (wide * _scale(wide)).astype(BF16)
            x2[rows, :] = b
            ab[:, rows] = b.T
        start([*saves[:3], tile[2]])

        @pl.when(layer == 0)
        def _():
            acc[...] = jnp.zeros((T, D), F32)

            def one(j):
                buf = j % 2

                @pl.when(j < TILES - 1)
                def _():
                    start(tile_copies(half, j + 1, 1 - buf))

                wait(tile_copies(half, j, buf))
                for i in range(2):
                    rows = slice(T_HALF * i, T_HALF * (i + 1))
                    gate, up = dot(x2[rows, :], wg[buf]), dot(x2[rows, :], wu[buf])
                    hidden = (gate * (1.0 / (1.0 + jnp.exp(-gate))) * up).astype(BF16)
                    acc[rows, :] += dot(hidden, wd[buf])

            loop(TILES, one)
            start(qkv_weight_copies(0))

        wait(saves)

        @pl.when(layer == 0)
        def _():
            for i in range(PIECES):
                x1[_piece(i), :] = (x1[_piece(i), :].astype(F32) + acc[_piece(i), :].astype(BF16).astype(F32)).astype(BF16)
            save(0, x1, r_["h"]).start()
            save(0, x1, r_["h"]).wait()

    first = [local(r_["x"], x1, x_sem.at[0]), local(r_["turns"], tb, o_sem)]
    start([*first, *qkv_weight_copies(1)])


    barrier = pltpu.get_barrier_semaphore()
    tell(barrier, mate)

    @pl.when(has_above)
    def _():
        tell(barrier, above)

    @pl.when(has_below)
    def _():
        tell(barrier, below)

    wait(first)

    def spin(a):
        rows = pl.ds(pl.multiple_of(STRIDE * a, STRIDE), STRIDE)
        cos_a, sin_a, cos_b, sin_b = tb[0, pl.ds(a, 1), :], tb[1, pl.ds(a, 1), :], tb[2], tb[3]
        cosb[rows, :] = cos_a * cos_b - sin_a * sin_b
        sinb[rows, :] = sin_a * cos_b + cos_a * sin_b

    loop(T // STRIDE, spin)
    loop(2, forward)
    by_y = local(r_["dy"], x1, x_sem.at[0])
    by_y.start()

    @pl.when(has_above & has_below)
    def _():
        pl.semaphore_wait(barrier, 3)

    @pl.when(jnp.logical_not(has_above & has_below))
    def _():
        pl.semaphore_wait(barrier, 2)

    by_y.wait()

    def tick(n):
        t = n - EARLY
        slot, prev, late = n % SLOTS, (n + SLOTS - 1) % SLOTS, (n + 1) % SLOTS
        two = n % 2


        @pl.when(n >= 3)
        def _():
            pl.semaphore_wait(free_m, 1)

            @pl.when(has_above)
            def _():
                pl.semaphore_wait(free_u, 1)

            @pl.when(has_below)
            def _():
                pl.semaphore_wait(free_d, 1)

            @pl.when(ok(t - 3))
            def _():
                for s in range(CHIPS):
                    remote(ps.at[late, s], pr.at[late, s], ps_s.at[late, s], ps_r.at[late, s], mate).wait_send()

            @pl.when(ok(t - 4 - z))
            def _():
                for s in range(1, CHIPS):
                    @pl.when(s > z)
                    def _():
                        remote(su.at[late, s], ru.at[late, s], su_s.at[late, s], su_r.at[late, s], mate).wait_send()

            @pl.when(ok(t - 4 - (CHIPS - 1 - z)))
            def _():
                for s in range(CHIPS - 1):
                    @pl.when(s < z)
                    def _():
                        remote(sd.at[late, s], rd.at[late, s], sd_s.at[late, s], sd_r.at[late, s], mate).wait_send()

            def gone(s):
                @pl.when(ok(t - 7 - jnp.abs(z - s)))
                def _():
                    there = wp.at[0, 0]
                    remote(there, there, am_s.at[late, s], am_r.at[late, s], mate).wait_send()

                    @pl.when((s <= z) & has_above)
                    def _():
                        remote(there, there, au_s.at[late, s], au_r.at[late, s], mate).wait_send()

                    @pl.when((s >= z) & has_below)
                    def _():
                        remote(there, there, ad_s.at[late, s], ad_r.at[late, s], mate).wait_send()

            loop(CHIPS, gone)

            @pl.when(ok(t - 7))
            def _():
                local(wn.at[late], wp.at[0, 0], out_sem.at[late, 0]).wait()
                local(gn.at[late], gp.at[0], out_sem.at[late, 1]).wait()


        for test, copies in writes(*unit_of(n - 1)):
            pl.when(test & (n > 0))(lambda: wait(copies()))
        fetch(n)

        @pl.when(ok(t))
        def _():
            load_operands(t)

        @pl.when(ok(t - 3))
        def _():
            optimizer_copies(t - 3, 1 - two, lambda copy: copy.start())


        def pass_on(s, k, from_above):
            got, send, here, there, to = (rd, sd, sd_s, sd_r, below) if from_above else (ru, su, su_s, su_r, above)
            remote(send.at[prev, s], got.at[prev, s], here.at[prev, s], there.at[prev, s], mate).wait_recv()
            value = chip[k % SUMS, s] + got[prev, s].astype(F32)
            chip[k % SUMS, s] = value
            send[slot, s] = value.astype(BF16)

            @pl.when((s < z) if from_above else (s > z))
            def _():
                remote(send.at[slot, s], got.at[slot, s], here.at[slot, s], there.at[slot, s], to).start()

        up_k, down_k = t - 1 - z, t - 1 - (CHIPS - 1 - z)
        for i in range(CHIPS - 1):
            @pl.when(has_below & ok(up_k) & (CHIPS - 1 - i >= z))
            def _():
                pass_on(CHIPS - 1 - i, up_k, False)

            @pl.when(has_above & ok(down_k) & (i <= z))
            def _():
                pass_on(i, down_k, True)


        @pl.when(ok(t - 4))
        def _():
            k = t - 4
            optimizer_copies(k, two, lambda copy: copy.wait())
            is_q = _is_q(k % PER_LAYER)
            for (rows, cols), test in ((Q_BLOCK, is_q), (P_BLOCK, jnp.logical_not(is_q))):
                @pl.when(test)
                def _():
                    for j in range(cols // LANES):
                        at, over = slice(rows * j, rows * (j + 1)), slice(LANES * j, LANES * (j + 1))
                        low = chip[k % SUMS, z, at, :].astype(BF16)
                        m, v = _moments(mb[two, :rows, over], vb[two, :rows, over], low.astype(F32))
                        w = wb[two, :rows, over].astype(F32)
                        wn[slot, at, :] = (w - 0.02 * (m * lax.rsqrt(v + 1e-8) + 0.1 * w)).astype(BF16)
                        gn[slot, at, :] = low

            at = _place(k)
            local(wn.at[slot], wp.at[at, me], out_sem.at[slot, 0]).start()
            local(gn.at[slot], gp.at[at], out_sem.at[slot, 1]).start()


        def sends(s, source, there):
            @pl.when((s <= z) & has_above)
            def _():
                remote(source, there, au_s.at[slot, s], au_r.at[slot, s], above).start()

            @pl.when((s >= z) & has_below)
            def _():
                remote(source, there, ad_s.at[slot, s], ad_r.at[slot, s], below).start()

            remote(source, there, am_s.at[slot, s], am_r.at[slot, s], mate).start()

        @pl.when(ok(t - 4))
        def _():
            sends(z, wn.at[slot], wp.at[_place(t - 4), me])

        work(n)

        def spread(s):
            k = t - 4 - jnp.abs(z - s)

            @pl.when(ok(k) & (s != z))
            def _():
                there = wp.at[_place(k), 2 * s + core]

                @pl.when(s < z)
                def _():
                    remote(there, there, au_s.at[prev, s], au_r.at[prev, s], mate).wait_recv()

                @pl.when(s > z)
                def _():
                    remote(there, there, ad_s.at[prev, s], ad_r.at[prev, s], mate).wait_recv()

                sends(s, there, there)

        loop(CHIPS, spread)


        @pl.when(ok(t - 1))
        def _():
            for s in (3, 0, 2, 1):
                remote(ps.at[prev, s], pr.at[prev, s], ps_s.at[prev, s], ps_r.at[prev, s], mate).wait_recv()
                value = chip[(t - 1) % SUMS, s] + pr[prev, s].astype(F32)
                chip[(t - 1) % SUMS, s] = value
                if s > 0:
                    @pl.when(z == 0)
                    def _():
                        su[slot, s] = value.astype(BF16)
                        remote(su.at[slot, s], ru.at[slot, s], su_s.at[slot, s], su_r.at[slot, s], above).start()
                if s < CHIPS - 1:
                    @pl.when(z == CHIPS - 1)
                    def _():
                        sd[slot, s] = value.astype(BF16)
                        remote(sd.at[slot, s], rd.at[slot, s], sd_s.at[slot, s], sd_r.at[slot, s], below).start()


        @pl.when(ok(t))
        def _():
            is_q = _is_q(t % PER_LAYER)
            for (rows, cols), test in ((Q_BLOCK, is_q), (P_BLOCK, jnp.logical_not(is_q))):
                @pl.when(test)
                def _():
                    wait_operands((rows, cols))
                    for own in range(2):
                        got = dot(ab[4 * rows * own : 4 * rows * (own + 1), :], db[:, :cols])
                        for s in range(CHIPS):
                            for j in range(cols // LANES):
                                piece = got[rows * s : rows * (s + 1), LANES * j : LANES * (j + 1)]
                                if own:
                                    chip[t % SUMS, s, rows * j : rows * (j + 1), :] = piece
                                else:
                                    ps[slot, s, rows * j : rows * (j + 1), :] = piece.astype(BF16)
                        if not own:
                            for s in (3, 0, 2, 1):
                                remote(ps.at[slot, s], pr.at[slot, s], ps_s.at[slot, s], ps_r.at[slot, s], mate).start()


        def arrived(s):
            @pl.when(ok(t - 5 - jnp.abs(z - s)))
            def _():
                there = wp.at[0, 0]
                remote(there, there, am_s.at[prev, s], am_r.at[prev, s], mate).wait_recv()

        loop(CHIPS, arrived)

        @pl.when(n < TICKS - 3)
        def _():
            tell(free_m, mate)

            @pl.when(has_above)
            def _():
                tell(free_d, above)

            @pl.when(has_below)
            def _():
                tell(free_u, below)

    loop(TICKS, tick)


def update(given, w, m, v):
    vm, sem = pltpu.VMEM, pltpu.SemaphoreType
    block, wide = (BLOCK, LANES), N_Q + 2 * N_K
    scratch = [
        vm((D, T), BF16), vm((T, D), BF16), vm((SUMS, CHIPS, *block), F32),
        *(vm((SLOTS, CHIPS, *block), BF16) for _ in range(6)),
        vm((SLOTS, *block), BF16), vm((SLOTS, *block), BF16),
        *(vm((2, P_BLOCK[0], D), dtype) for dtype in (F32, F32, BF16)),
        vm((T, D), BF16), vm((T, D), BF16), vm((T, N_Q), BF16),
        vm((2, D, TF), BF16), vm((2, D, TF), BF16), vm((2, TF, D), BF16), vm((T, D), F32),
        *(vm((TF, TF), BF16) for _ in range(3)),
        vm((T, GROUP * HEAD), BF16), vm((T, HEAD), BF16), vm((T, HEAD), BF16), vm((T, wide), BF16), vm((N_Q, T), BF16),
        vm((T, HALF), F32), vm((T, HALF), F32), vm((KV, GROUP, T), F32), vm((KV, GROUP, T), F32), vm((4, STRIDE, HALF), F32),
        sem.DMA, sem.DMA, *(sem.DMA(shape) for shape in ((2, 3), (SLOTS, 2), (2, 3), (2,))), sem.DMA, sem.DMA((3,)), sem.DMA, sem.DMA((3,)), sem.DMA((6,)),
        *(sem.DMA((SLOTS, CHIPS)) for _ in range(12)),
        sem.REGULAR, sem.REGULAR, sem.REGULAR,
    ]
    refs = [*w, *m, *v, *(given[name] for name in INPUTS)]
    pair = [(FF, T), (T, FF), (T, FF), (T, D), (T, wide), (D, T), (N_Q, T), (D, T), (T, D), (T, D), (T, N_Q), (T, wide)]
    shapes = [(CHUNKS, 8, *block), (CHUNKS, *block), *((2, *shape) for shape in pair)]
    outs = [*((shape, BF16) for shape in shapes), ((2, KV, GROUP, T), F32), ((T, D), BF16), ((T, D), BF16)]
    return pl.pallas_call(
        _update,
        in_specs=[pl.BlockSpec(memory_space=pl.ANY)] * len(refs),
        out_specs=[pl.BlockSpec(memory_space=pl.ANY)] * len(outs),
        out_shape=[jax.ShapeDtypeStruct(*out) for out in outs],
        scratch_shapes=scratch,
        compiler_params=pltpu.CompilerParams(collective_id=0, has_side_effects=True, vmem_limit_bytes=63 * 2**20),
        name="update",
    )(*refs)[:2]


def _moments(m, v, g):
    return 0.9 * m + 0.1 * g, 0.95 * v + 0.05 * g * g


def _unpack(*refs):
    s = pl.program_id(1)
    ins, outs = refs[: 4 * len(NAMES)], refs[4 * len(NAMES) :]
    for i, name in enumerate(NAMES):
        wp_ref, gp_ref, m_ref, v_ref = ins[4 * i : 4 * i + 4]
        w_out, m_out, v_out = outs[i :: len(NAMES)]
        tall = name in ("w_down", "wo")
        rows, cols = Q_BLOCK if tall else P_BLOCK
        some = m_ref.shape[1]
        for j in range(cols // LANES):
            for n in range(wp_ref.shape[0]):
                over = slice(LANES * j, LANES * (j + 1)) if tall else slice(cols * n + LANES * j, cols * n + LANES * (j + 1))
                down = slice(rows * n, rows * (n + 1)) if tall else slice(0, rows)
                w_out[0, down, over] = wp_ref[n, 0, rows * j : rows * (j + 1), :]
                if tall and n:
                    continue
                if tall:
                    per = rows // some
                    g = gp_ref[s // per if name == "wo" else jnp.minimum(s, 6), pl.ds(pl.multiple_of(rows * j + some * (s % per), 16), some), :]
                else:
                    g = gp_ref[n, pl.ds(pl.multiple_of(rows * j + some * jnp.minimum(s, 6), 16), some), :]
                m_out[0, :, over], v_out[0, :, over] = _moments(m_ref[0, :, over], v_ref[0, :, over], g.astype(F32))


def unpack(wp, gp, m, v):
    block = (BLOCK, LANES)
    where = {"wq": (2, 22, 3), "wk": (1, 46, 6), "wv": (1, 47, 6), "wo": (2, 21, 3), "w_gate": (7, 0, 1), "w_up": (7, 2, 1), "w_down": (7, 4, 1)}
    in_specs, given, full, own = [], [], [], []
    for name in NAMES:
        count, start, step = where[name]
        _, height, width = m[name].shape
        some = 64 if name == "w_down" else 16
        last = height // some - 1
        mine = pl.BlockSpec((1, some, width), lambda layer, s, last=last: (layer, jnp.minimum(s, last), 0))
        in_specs += [
            pl.BlockSpec((count, 1, *block), lambda layer, s, start=start, step=step: (start + step * layer, s, 0, 0)),
            pl.BlockSpec((count, *block), lambda layer, s, start=start, step=step: (start + step * layer, 0, 0)), mine, mine,
        ]
        given += [wp, gp, m[name], v[name]]
        full.append((pl.BlockSpec((1, height, width), lambda layer, s: (layer, s, 0)), jax.ShapeDtypeStruct((2, 8 * height, width), BF16)))
        own.append((mine, jax.ShapeDtypeStruct(m[name].shape, F32)))
    outs = full + own + own
    return pl.pallas_call(
        _unpack,
        grid=(2, 8),
        in_specs=in_specs,
        out_specs=[o[0] for o in outs],
        out_shape=[o[1] for o in outs],
        compiler_params=pltpu.CompilerParams(vmem_limit_bytes=VMEM),
        name="unpack",
    )(*given)


def solution(mesh):
    angle = np.arange(STRIDE)[:, None] * float(THETA) ** (-np.arange(HALF) / HALF)
    turns = np.stack([turn(angle * step) for step in (STRIDE, 1) for turn in (np.cos, np.sin)]).astype(np.float32)

    def step(x, dy, *arrays):
        w, m, v = (dict(zip(NAMES, arrays[i : i + 7], strict=True)) for i in (0, 7, 14))
        wp, gp = update({"x": x[0], "dy": dy[0], "turns": jnp.asarray(turns)}, w.values(), m.values(), v.values())
        return tuple(unpack(wp, gp, m, v))

    states, all_of, cut = P(("rep", "dp"), None, None), P(None, None, None), P(None, "dp", None)
    return jax.shard_map(
        step,
        mesh=mesh,
        in_specs=(states, states) + (all_of,) * 7 + (cut,) * 14,
        out_specs=(P("rep", None, None),) * 7 + (P("rep", "dp", None),) * 14,
        check_vma=False,
    )
```

```python
import functools

import jax
import jax.numpy as jnp
import numpy as np
from jax import lax
from jax.experimental import pallas as pl
from jax.experimental.pallas import tpu as pltpu
from jax.sharding import PartitionSpec as P

LOG2E = 1.4426950408889634
HIDDEN = -2e30
VMEM = 56 * 2**20
F32, BF16 = jnp.float32, jnp.bfloat16
MESH = pl.DeviceIdType.MESH
T, D, FF, HEADS, KV, HEAD = 1024, 896, 3584, 4, 2, 256
THETA = 10000
STRIDE = 32
NAMES = ("wq", "wk", "wv", "wo", "w_gate", "w_up", "w_down")
ROWS = 256
TF = 512
PIECES = T // ROWS


def loop(count, body):
    lax.fori_loop(0, count, lambda i, _: body(i), None)


def dot(a, b):
    return jnp.dot(a, b, preferred_element_type=F32)


def dot_t(a, b):
    return lax.dot_general(a, b, (((1,), (1,)), ((), ())), preferred_element_type=F32)


def _scale(wide):
    return lax.rsqrt(jnp.mean(wide * wide, -1, keepdims=True) + 1e-6)


def _norm_back(h, by):
    s = _scale(h)
    return by * s - h * (s * s * s * jnp.mean(by * h, -1, keepdims=True))


E = HEAD**-0.5 * LOG2E
GROUP = HEADS // KV


def _piece(i):
    return slice(ROWS * i, ROWS * (i + 1))


def _visible():
    shape = (ROWS, GROUP * ROWS)
    return lax.broadcasted_iota(jnp.int32, shape, 0) <= lax.rem(lax.broadcasted_iota(jnp.int32, shape, 1), ROWS)


LANES = 128
BLOCK = 448
SLOTS = 4
SUMS = 5
EARLY = 2
LAG = 22
P_BLOCK, Q_BLOCK = (112, 512), (64, 896)
TILES = FF // TF
DOWN_AT, WO_AT, QKV_AT, PER_LAYER = 14, 21, 23, 27
CHUNKS = 2 * PER_LAYER
TICKS = CHUNKS + 11 + EARLY
CHIPS = 4
HALF, T_HALF = HEAD // 2, T // 2
N_Q, N_K = HEADS * HEAD, KV * HEAD
LEAVE, HEADS_AT, AFTER = 13, 14, 17


def _is_q(r):
    return (r >= DOWN_AT) & (r < QKV_AT)


def _place(k):
    layer, r = 1 - k // PER_LAYER, k % PER_LAYER
    double, single = (r % 2) * DOWN_AT + layer * TILES + r // 2, 2 * DOWN_AT + layer * TILES + r - DOWN_AT
    return jnp.where(r < DOWN_AT, double, jnp.where(r < WO_AT, single, 3 * DOWN_AT + layer * (PER_LAYER - WO_AT) + r - WO_AT))


def _owners(layer, r):
    mlp_chunk = r < DOWN_AT
    return (
        ("w_gate", mlp_chunk & (r % 2 == 0), r // 2), ("w_up", mlp_chunk & (r % 2 == 1), r // 2),
        ("w_down", (r >= DOWN_AT) & (r < WO_AT), r - DOWN_AT), ("wo", (r >= WO_AT) & (r < QKV_AT), r - WO_AT),
        ("wq", (r >= QKV_AT) & (r < QKV_AT + 2), r - QKV_AT), ("wk", r == QKV_AT + 2, 0 * r), ("wv", r == QKV_AT + 3, 0 * r),
    )


INPUTS = ("x", "dy", "turns")
OUTPUTS = ("wp", "gp", "hidt", "dgate", "dup", "d1", "dqkv", "at", "ot", "bt", "b", "h1", "o", "qkv", "lse", "h", "by1")
SCRATCH = ("ab", "db", "chip", "ps", "pr", "su", "ru", "sd", "rd", "wn", "gn", "mb", "vb", "wb", "x1", "x2", "oo", "wg", "wu", "wd", "acc", "dg", "du", "ht",
           "qq", "kk", "vv", "dq", "st", "cosb", "sinb", "lseb", "delta", "tb",
           "ab_sem", "db_sem", "opt_sem", "out_sem", "tile_sem", "x_sem", "o_sem", "qkv_sem", "lse_sem", "write_sem", "save_sem",
           "ps_s", "ps_r", "su_s", "su_r", "sd_s", "sd_r", "am_s", "am_r", "au_s", "au_r", "ad_s", "ad_r", "free_m", "free_u", "free_d")


def _update(*refs):
    w_in, m_in, v_in = (dict(zip(NAMES, refs[i : i + 7])) for i in (0, 7, 14))
    r_ = dict(zip((*INPUTS, *OUTPUTS, *SCRATCH), refs[21:], strict=True))
    (ab, db, chip, ps, pr, su, ru, sd, rd, wn, gn, mb, vb, wb, x1, x2, oo, wg, wu, wd, acc, dg, du, ht, qq, kk, vv, dq, st, cosb, sinb, lseb, delta, tb,
     ab_sem, db_sem, opt_sem, out_sem, tile_sem, x_sem, o_sem, qkv_sem, lse_sem, write_sem, save_sem,
     ps_s, ps_r, su_s, su_r, sd_s, sd_r, am_s, am_r, au_s, au_r, ad_s, ad_r, free_m, free_u, free_d) = (r_[name] for name in SCRATCH)
    wp, gp = r_["wp"], r_["gp"]
    rep, me = lax.axis_index("rep"), lax.axis_index("dp")
    z, core = me // 2, me % 2
    mate, above, below = me + 1 - 2 * core, me + 2, me - 2
    has_above, has_below = z < CHIPS - 1, z > 0

    def remote(src, dst, send, recv, to):
        return pltpu.make_async_remote_copy(src_ref=src, dst_ref=dst, send_sem=send, recv_sem=recv, device_id=(rep, to), device_id_type=MESH)

    def tell(sem, to):
        pl.semaphore_signal(sem, inc=1, device_id=(rep, to), device_id_type=MESH)

    def local(src, dst, sem):
        return pltpu.make_async_copy(src, dst, sem)

    def ok(k):
        return (k >= 0) & (k < CHUNKS)

    def tokens(start, count):
        return pl.ds(pl.multiple_of(start, ROWS), count)


    def tile_copies(half, j, buf):
        layer, over = 1 - half, pl.ds(pl.multiple_of(TF * j, TF), TF)
        return [
            local(w_in["w_gate"].at[layer, :, over], wg.at[buf], tile_sem.at[buf, 0]),
            local(w_in["w_up"].at[layer, :, over], wu.at[buf], tile_sem.at[buf, 1]),
            local(w_in["w_down"].at[layer, over, :], wd.at[buf], tile_sem.at[buf, 2]),
        ]

    def wo_copies(half):
        return [local(w_in["wo"].at[1 - half, pl.ds(TF * n, TF), :], wd.at[n], tile_sem.at[n, 2]) for n in range(2)]

    def qkv_weight_copies(half):
        layer = 1 - half
        return [
            *(local(w_in["wq"].at[layer, :, pl.ds(TF * n, TF)], wg.at[n], tile_sem.at[n, 0]) for n in range(2)),
            local(w_in["wk"].at[layer], wu.at[0], tile_sem.at[0, 1]), local(w_in["wv"].at[layer], wu.at[1], tile_sem.at[1, 1]),
        ]

    def column(at):
        return pl.ds(pl.multiple_of(at, HEAD), HEAD)

    def head_copies(half, head):
        pair = pl.ds(pl.multiple_of(GROUP * HEAD * head, GROUP * HEAD), GROUP * HEAD)
        return [
            local(r_["qkv"].at[half, :, over], to, qkv_sem.at[n])
            for n, (over, to) in enumerate(((pair, qq), (column(N_Q + HEAD * head), kk), (column(N_Q + N_K + HEAD * head), vv)))
        ]

    def load_x2(ref):
        return local(ref, x2, x_sem.at[1])

    def unit_of(n):
        half = (n >= AFTER + 2 + EARLY).astype(jnp.int32)
        return half, n - EARLY - LAG * half

    def start(copies):
        for copy in copies:
            copy.start()

    def wait(copies):
        for copy in copies:
            copy.wait()

    def writes(half, tau):
        u = tau + EARLY
        j, first = u // 2, tokens(T_HALF * (u % 2), T_HALF)
        over = pl.ds(pl.multiple_of(TF * j, TF), TF)
        part = tokens(T_HALF * (tau - AFTER), T_HALF)
        after_at = (tau >= AFTER) & (tau < AFTER + 2)
        return (
            ((u >= 0) & (u < 2 * TILES), lambda: [
                local(dg, r_["dgate"].at[half, first, over], write_sem.at[0]), local(du, r_["dup"].at[half, first, over], write_sem.at[1]),
                local(ht, r_["hidt"].at[half, over, first], write_sem.at[2])]),
            (tau == LEAVE, lambda: [local(x1, r_["d1"].at[half], write_sem.at[0])]),
            (after_at, lambda: [local(dq.at[part, :], r_["dqkv"].at[half, part, :], write_sem.at[0])]),
            (after_at & (half == 0), lambda: [local(x1.at[part, :], r_["by1"].at[part, :], write_sem.at[1])]),
        )

    def fetch(n):
        half, tau = unit_of(n)
        u = tau + EARLY

        @pl.when((tau == -EARLY - 1) & (half == 1))
        def _():
            start([*tile_copies(half, 0, 0), load_x2(r_["b"].at[half])])

        @pl.when((u >= 0) & (u % 2 == 0) & (u < 2 * TILES - 2))
        def _():
            start(tile_copies(half, u // 2 + 1, (u // 2 + 1) % 2))

        @pl.when(tau == LEAVE - 1)
        def _():
            start([*wo_copies(half), load_x2(r_["h1"].at[half]), local(r_["o"].at[half], oo, o_sem)])

        @pl.when(tau == LEAVE)
        def _():
            start([*head_copies(half, 0), local(r_["lse"].at[half], lseb, lse_sem)])

        @pl.when(tau == HEADS_AT + 1)
        def _():
            start(head_copies(half, 1))

        @pl.when((tau == LEAVE - 1) & (half == 0))
        def _():
            start(qkv_weight_copies(0))

        @pl.when((tau == HEADS_AT) & (half == 0))
        def _():
            start([load_x2(r_["h"])])

    def mlp_unit(u, buf):
        rows = tokens(T_HALF * (u % 2), T_HALF)
        gate, up = dot(x2[rows, :], wg[buf]), dot(x2[rows, :], wu[buf])
        sig = 1.0 / (1.0 + jnp.exp(-gate))
        silu = gate * sig
        by = dot_t(x1[rows, :], wd[buf]).astype(BF16).astype(F32)
        ht[...] = (silu * up).astype(BF16).T
        du[...] = (by * silu).astype(BF16)
        dg[...] = (by * up * (sig * (1.0 + gate * (1.0 - sig)))).astype(BF16)
        acc[rows, :] += dot_t(dg[...], wg[buf]) + dot_t(du[...], wu[buf])

    def leave_unit(i):
        rows = tokens(ROWS * i, ROWS)
        inner = _norm_back(x2[rows, :].astype(F32), acc[rows, :].astype(BF16).astype(F32)).astype(BF16)
        d1 = (x1[rows, :].astype(F32) + inner.astype(F32)).astype(BF16)
        x1[rows, :] = d1
        for n in range(HEADS):
            low, over = HEAD * (n % 2), _piece(n)
            do = dot_t(d1, wd[n // 2, low : low + HEAD, :]).astype(BF16)
            both = do.astype(F32) * oo[rows, over].astype(F32)
            oo[rows, over] = do
            delta[n // GROUP, n % GROUP : n % GROUP + 1, rows] = both.T.sum(0, keepdims=True)

    def side(ref, i, head):
        return jnp.concatenate([ref[_piece(i), column(HEAD * (GROUP * head + n))] for n in range(GROUP)], axis=0)

    def turn_back(part, rows):
        cos, sin = cosb[rows, :], sinb[rows, :]
        x, y = part[:, :HALF].astype(F32), part[:, HALF:].astype(F32)
        return jnp.concatenate([x * cos + y * sin, y * cos - x * sin], -1).astype(BF16)

    def head_unit(head):
        seen = _visible()
        turned = kk[...].T
        line = lambda ref, i: jnp.concatenate([ref[head, n : n + 1, _piece(i)] for n in range(GROUP)], axis=1)
        dk_at, dv_at = slice(0, HEAD), slice(HEAD, 2 * HEAD)
        for i in range(PIECES):
            lse, dl = line(lseb, i), line(delta, i)
            q = jnp.concatenate([qq[_piece(i), _piece(n)] for n in range(GROUP)], axis=0)
            do = side(oo, i, head)
            by_q = 0.0
            for j in range(i + 1):
                at = _piece(j)
                p = jnp.exp2(dot_t(kk[at, :], q) * E - lse)
                if j == i:
                    p = jnp.where(seen, p, 0.0)
                ds = (p * (dot_t(vv[at, :], do) - dl)).astype(BF16)
                by_v, by_k = dot(p.astype(BF16), do), dot(ds, q)
                acc[at, dv_at] = by_v if j == i else acc[at, dv_at] + by_v
                acc[at, dk_at] = by_k if j == i else acc[at, dk_at] + by_k
                by_q = by_q + dot(turned[:, at], ds)
            by_q = (by_q * HEAD**-0.5).astype(BF16)
            for n in range(GROUP):
                dq[_piece(i), column(HEAD * (GROUP * head + n))] = turn_back(by_q[:, _piece(n)].T, _piece(i))
        for i in range(PIECES):
            dq[_piece(i), column(N_Q + HEAD * head)] = turn_back((acc[_piece(i), dk_at] * HEAD**-0.5).astype(BF16), _piece(i))
            dq[_piece(i), column(N_Q + N_K + HEAD * head)] = acc[_piece(i), dv_at].astype(BF16)

    def after_unit(rows):
        by = sum(dot_t(dq[rows, TF * n : TF * (n + 1)], (wg, wu)[n // 2][n % 2]) for n in range(4)).astype(BF16).astype(F32)
        inner = _norm_back(x2[rows, :].astype(F32), by).astype(BF16)
        x1[rows, :] = (x1[rows, :].astype(F32) + inner.astype(F32)).astype(BF16)

    def work(n):
        half, tau = unit_of(n)
        u = tau + EARLY

        @pl.when((u >= 0) & (u < 2 * TILES))
        def _():
            buf = u // 2 % 2

            @pl.when(u % 2 == 0)
            def _():
                wait(tile_copies(half, u // 2, buf))

            @pl.when(u == 0)
            def _():
                acc[...] = jnp.zeros((T, D), F32)

                @pl.when(half == 1)
                def _():
                    load_x2(r_["h"]).wait()

            mlp_unit(u, buf)

        @pl.when(tau == LEAVE)
        def _():
            wait([load_x2(r_["h"]), local(r_["o"].at[0], oo, o_sem), *wo_copies(half)])
            loop(PIECES, leave_unit)

        @pl.when((tau == HEADS_AT) | (tau == HEADS_AT + 2))
        def _():
            @pl.when(tau == HEADS_AT)
            def _():
                local(r_["lse"].at[0], lseb, lse_sem).wait()

            wait(head_copies(0, 0))
            head_unit((tau - HEADS_AT) // 2)

        @pl.when((tau >= AFTER) & (tau < AFTER + 2) & (half == 0))
        def _():
            @pl.when(tau == AFTER)
            def _():
                wait([load_x2(r_["h"]), *qkv_weight_copies(0)])

            loop(PIECES // 2, lambda i: after_unit(tokens(T_HALF * (tau - AFTER) + ROWS * i, ROWS)))

        for test, copies in writes(half, tau):
            pl.when(test)(lambda: start(copies()))


    def load_operands(k):
        half, r = k // PER_LAYER, k % PER_LAYER

        def from_rows(ref, block, down):
            rows, whole = block[0], ref.shape[0] // 8
            for e in range(8):
                owner = 2 * (e % 4) + (1 - core if e < 4 else core)
                at = pl.multiple_of(whole * owner + down, 16)
                local(ref.at[pl.ds(at, rows), :], ab.at[pl.ds(rows * e, rows), :], ab_sem).start()

        def from_columns(ref, j):
            local(ref.at[:, pl.ds(pl.multiple_of(TF * j, TF), TF)], db.at[:, pl.ds(0, TF)], db_sem).start()

        @pl.when(r < DOWN_AT)
        def _():
            from_rows(r_["bt"].at[half], P_BLOCK, 0)

        @pl.when((r < DOWN_AT) & (r % 2 == 0))
        def _():
            from_columns(r_["dgate"].at[half], r // 2)

        @pl.when((r < DOWN_AT) & (r % 2 == 1))
        def _():
            from_columns(r_["dup"].at[half], r // 2)

        @pl.when((r >= DOWN_AT) & (r < WO_AT))
        def _():
            from_rows(r_["hidt"].at[half], Q_BLOCK, Q_BLOCK[0] * (r - DOWN_AT))

            @pl.when(half == 0)
            def _():
                local(r_["dy"], db, db_sem).start()

            @pl.when(half == 1)
            def _():
                local(r_["by1"], db, db_sem).start()

        @pl.when((r >= WO_AT) & (r < QKV_AT))
        def _():
            from_rows(r_["ot"].at[half], Q_BLOCK, Q_BLOCK[0] * (r - WO_AT))
            local(r_["d1"].at[half], db, db_sem).start()

        @pl.when(r >= QKV_AT)
        def _():
            from_rows(r_["at"].at[half], P_BLOCK, 0)
            from_columns(r_["dqkv"].at[half], r - QKV_AT)

    def wait_operands(block):
        rows, cols = block
        local(r_["hidt"].at[0, pl.ds(0, 8 * rows), :], ab.at[pl.ds(0, 8 * rows), :], ab_sem).wait()
        local(r_["dgate"].at[0, :, pl.ds(0, cols)], db.at[:, pl.ds(0, cols)], db_sem).wait()

    def optimizer_copies(k, buf, do):
        layer, r = 1 - k // PER_LAYER, k % PER_LAYER
        for name, test, j in _owners(layer, r):
            rows, cols = block = Q_BLOCK if name in ("w_down", "wo") else P_BLOCK

            @pl.when(test)
            def _():
                whole = w_in[name].shape[1] // 8
                down = pl.multiple_of(rows * j if block == Q_BLOCK else 0 * j, 16)
                right = pl.ds(0, cols) if block == Q_BLOCK else pl.ds(pl.multiple_of(cols * j, cols), cols)
                for n, (ref, at, to) in enumerate(((m_in[name], down, mb), (v_in[name], down, vb), (w_in[name], pl.multiple_of(whole * me + down, 16), wb))):
                    do(local(ref.at[layer, pl.ds(at, rows), right], to.at[buf, pl.ds(0, rows), pl.ds(0, cols)], opt_sem.at[buf, n]))


    def save(n, source, to):
        return local(source, to, save_sem.at[n])

    def attend_head(head):
        seen = _visible()
        k_at, turned = column(N_Q + HEAD * head), dq[:, column(N_Q + N_K + HEAD * head)].T
        for i in range(PIECES):
            q = side(dq, i, head)
            scores = [dot_t(dq[_piece(j), k_at], q) for j in range(i + 1)]
            scores[i] = jnp.where(seen, scores[i], HIDDEN)
            top = functools.reduce(jnp.maximum, [s.max(axis=0, keepdims=True) for s in scores])
            total, mix = 0.0, 0.0
            for j, s in enumerate(scores):
                p = jnp.exp2((s - top) * E)
                total = total + p.sum(axis=0, keepdims=True)
                mix = mix + dot(turned[:, _piece(j)], p.astype(BF16))
            out = (mix * (1.0 / total)).astype(BF16)
            lse = top * E + jnp.log(total) * LOG2E
            for n in range(GROUP):
                over = column(HEAD * (GROUP * head + n))
                st[over, _piece(i)] = out[:, _piece(n)]
                oo[_piece(i), over] = out[:, _piece(n)].T
                lseb[head, n : n + 1, _piece(i)] = lse[:, _piece(n)]

    def forward(layer):
        half = 1 - layer
        kept = lambda name: r_[name].at[half]
        wait(qkv_weight_copies(half))
        saves = [save(0, ab, kept("at")), save(1, dq, kept("qkv"))]
        for i in range(PIECES):
            wide = x1[_piece(i), :].astype(F32)
            a = (wide * _scale(wide)).astype(BF16)
            ab[:, _piece(i)] = a.T
            cos, sin = cosb[_piece(i), :], sinb[_piece(i), :]
            for c, w in enumerate((wg[0], wg[1], wu[0], wu[1])):
                t = dot(a, w).astype(BF16)
                for n in range(2):
                    part = t[:, _piece(n)]
                    if c < 3:
                        p, q = part[:, :HALF].astype(F32), part[:, HALF:].astype(F32)
                        part = jnp.concatenate([p * cos - q * sin, q * cos + p * sin], -1).astype(BF16)
                    dq[_piece(i), TF * c + HEAD * n : TF * c + HEAD * (n + 1)] = part
        tile = tile_copies(half, 0, 0)
        start([*saves, *wo_copies(half), *tile[:2]])
        loop(KV, attend_head)
        wait([*saves, *wo_copies(half)])
        saves = [save(0, ab, kept("bt")), save(1, x1, kept("h1")), save(2, x2, kept("b")), save(3, st, kept("ot")), save(4, oo, kept("o")), save(5, lseb, kept("lse"))]
        start(saves[3:])
        for i in range(PIECES):
            rows = _piece(i)
            total = dot(oo[rows, :TF], wd[0]) + dot(oo[rows, TF:], wd[1])
            h1 = (x1[rows, :].astype(F32) + total.astype(BF16).astype(F32)).astype(BF16)
            x1[rows, :] = h1
            wide = h1.astype(F32)
            b = (wide * _scale(wide)).astype(BF16)
            x2[rows, :] = b
            ab[:, rows] = b.T
        start([*saves[:3], tile[2]])

        @pl.when(layer == 0)
        def _():
            acc[...] = jnp.zeros((T, D), F32)

            def one(j):
                buf = j % 2

                @pl.when(j < TILES - 1)
                def _():
                    start(tile_copies(half, j + 1, 1 - buf))

                wait(tile_copies(half, j, buf))
                for i in range(2):
                    rows = slice(T_HALF * i, T_HALF * (i + 1))
                    gate, up = dot(x2[rows, :], wg[buf]), dot(x2[rows, :], wu[buf])
                    hidden = (gate * (1.0 / (1.0 + jnp.exp(-gate))) * up).astype(BF16)
                    acc[rows, :] += dot(hidden, wd[buf])

            loop(TILES, one)
            start(qkv_weight_copies(0))

        wait(saves)

        @pl.when(layer == 0)
        def _():
            for i in range(PIECES):
                x1[_piece(i), :] = (x1[_piece(i), :].astype(F32) + acc[_piece(i), :].astype(BF16).astype(F32)).astype(BF16)
            save(0, x1, r_["h"]).start()
            save(0, x1, r_["h"]).wait()

    first = [local(r_["x"], x1, x_sem.at[0]), local(r_["turns"], tb, o_sem)]
    start([*first, *qkv_weight_copies(1)])


    barrier = pltpu.get_barrier_semaphore()
    tell(barrier, mate)

    @pl.when(has_above)
    def _():
        tell(barrier, above)

    @pl.when(has_below)
    def _():
        tell(barrier, below)

    wait(first)

    def spin(a):
        rows = pl.ds(pl.multiple_of(STRIDE * a, STRIDE), STRIDE)
        cos_a, sin_a, cos_b, sin_b = tb[0, pl.ds(a, 1), :], tb[1, pl.ds(a, 1), :], tb[2], tb[3]
        cosb[rows, :] = cos_a * cos_b - sin_a * sin_b
        sinb[rows, :] = sin_a * cos_b + cos_a * sin_b

    loop(T // STRIDE, spin)
    loop(2, forward)
    by_y = local(r_["dy"], x1, x_sem.at[0])
    by_y.start()

    @pl.when(has_above & has_below)
    def _():
        pl.semaphore_wait(barrier, 3)

    @pl.when(jnp.logical_not(has_above & has_below))
    def _():
        pl.semaphore_wait(barrier, 2)

    by_y.wait()

    def tick(n):
        t = n - EARLY
        slot, prev, late = n % SLOTS, (n + SLOTS - 1) % SLOTS, (n + 1) % SLOTS
        two = n % 2


        @pl.when(n >= 3)
        def _():
            pl.semaphore_wait(free_m, 1)

            @pl.when(has_above)
            def _():
                pl.semaphore_wait(free_u, 1)

            @pl.when(has_below)
            def _():
                pl.semaphore_wait(free_d, 1)

            @pl.when(ok(t - 3))
            def _():
                for s in range(CHIPS):
                    remote(ps.at[late, s], pr.at[late, s], ps_s.at[late, s], ps_r.at[late, s], mate).wait_send()

            @pl.when(ok(t - 4 - z))
            def _():
                for s in range(1, CHIPS):
                    @pl.when(s > z)
                    def _():
                        remote(su.at[late, s], ru.at[late, s], su_s.at[late, s], su_r.at[late, s], mate).wait_send()

            @pl.when(ok(t - 4 - (CHIPS - 1 - z)))
            def _():
                for s in range(CHIPS - 1):
                    @pl.when(s < z)
                    def _():
                        remote(sd.at[late, s], rd.at[late, s], sd_s.at[late, s], sd_r.at[late, s], mate).wait_send()

            def gone(s):
                @pl.when(ok(t - 7 - jnp.abs(z - s)))
                def _():
                    there = wp.at[0, 0]
                    remote(there, there, am_s.at[late, s], am_r.at[late, s], mate).wait_send()

                    @pl.when((s <= z) & has_above)
                    def _():
                        remote(there, there, au_s.at[late, s], au_r.at[late, s], mate).wait_send()

                    @pl.when((s >= z) & has_below)
                    def _():
                        remote(there, there, ad_s.at[late, s], ad_r.at[late, s], mate).wait_send()

            loop(CHIPS, gone)

            @pl.when(ok(t - 7))
            def _():
                local(wn.at[late], wp.at[0, 0], out_sem.at[late, 0]).wait()
                local(gn.at[late], gp.at[0], out_sem.at[late, 1]).wait()


        for test, copies in writes(*unit_of(n - 1)):
            pl.when(test & (n > 0))(lambda: wait(copies()))
        fetch(n)

        @pl.when(ok(t))
        def _():
            load_operands(t)

        @pl.when(ok(t - 3))
        def _():
            optimizer_copies(t - 3, 1 - two, lambda copy: copy.start())


        @pl.when(ok(t - 1))
        def _():
            for s in (3, 0, 2, 1):
                remote(ps.at[prev, s], pr.at[prev, s], ps_s.at[prev, s], ps_r.at[prev, s], mate).wait_recv()
                value = chip[(t - 1) % SUMS, s] + pr[prev, s].astype(F32)
                chip[(t - 1) % SUMS, s] = value
                if s > 0:
                    @pl.when(z == 0)
                    def _():
                        su[slot, s] = value.astype(BF16)
                        remote(su.at[slot, s], ru.at[slot, s], su_s.at[slot, s], su_r.at[slot, s], above).start()
                if s < CHIPS - 1:
                    @pl.when(z == CHIPS - 1)
                    def _():
                        sd[slot, s] = value.astype(BF16)
                        remote(sd.at[slot, s], rd.at[slot, s], sd_s.at[slot, s], sd_r.at[slot, s], below).start()


        def pass_on(s, k, from_above):
            got, send, here, there, to = (rd, sd, sd_s, sd_r, below) if from_above else (ru, su, su_s, su_r, above)
            remote(send.at[prev, s], got.at[prev, s], here.at[prev, s], there.at[prev, s], mate).wait_recv()
            value = chip[k % SUMS, s] + got[prev, s].astype(F32)
            chip[k % SUMS, s] = value
            send[slot, s] = value.astype(BF16)

            @pl.when((s < z) if from_above else (s > z))
            def _():
                remote(send.at[slot, s], got.at[slot, s], here.at[slot, s], there.at[slot, s], to).start()

        up_k, down_k = t - 1 - z, t - 1 - (CHIPS - 1 - z)
        for i in range(CHIPS - 1):
            @pl.when(has_below & ok(up_k) & (CHIPS - 1 - i >= z))
            def _():
                pass_on(CHIPS - 1 - i, up_k, False)

            @pl.when(has_above & ok(down_k) & (i <= z))
            def _():
                pass_on(i, down_k, True)


        @pl.when(ok(t - 4))
        def _():
            k = t - 4
            optimizer_copies(k, two, lambda copy: copy.wait())
            is_q = _is_q(k % PER_LAYER)
            for (rows, cols), test in ((Q_BLOCK, is_q), (P_BLOCK, jnp.logical_not(is_q))):
                @pl.when(test)
                def _():
                    for j in range(cols // LANES):
                        at, over = slice(rows * j, rows * (j + 1)), slice(LANES * j, LANES * (j + 1))
                        low = chip[k % SUMS, z, at, :].astype(BF16)
                        m, v = _moments(mb[two, :rows, over], vb[two, :rows, over], low.astype(F32))
                        w = wb[two, :rows, over].astype(F32)
                        wn[slot, at, :] = (w - 0.02 * (m * lax.rsqrt(v + 1e-8) + 0.1 * w)).astype(BF16)
                        gn[slot, at, :] = low

            at = _place(k)
            local(wn.at[slot], wp.at[at, me], out_sem.at[slot, 0]).start()
            local(gn.at[slot], gp.at[at], out_sem.at[slot, 1]).start()


        def sends(s, source, there):
            @pl.when((s <= z) & has_above)
            def _():
                remote(source, there, au_s.at[slot, s], au_r.at[slot, s], above).start()

            @pl.when((s >= z) & has_below)
            def _():
                remote(source, there, ad_s.at[slot, s], ad_r.at[slot, s], below).start()

            remote(source, there, am_s.at[slot, s], am_r.at[slot, s], mate).start()

        @pl.when(ok(t - 4))
        def _():
            sends(z, wn.at[slot], wp.at[_place(t - 4), me])


        @pl.when(ok(t))
        def _():
            is_q = _is_q(t % PER_LAYER)
            for (rows, cols), test in ((Q_BLOCK, is_q), (P_BLOCK, jnp.logical_not(is_q))):
                @pl.when(test)
                def _():
                    wait_operands((rows, cols))
                    for own in range(2):
                        got = dot(ab[4 * rows * own : 4 * rows * (own + 1), :], db[:, :cols])
                        for s in range(CHIPS):
                            for j in range(cols // LANES):
                                piece = got[rows * s : rows * (s + 1), LANES * j : LANES * (j + 1)]
                                if own:
                                    chip[t % SUMS, s, rows * j : rows * (j + 1), :] = piece
                                else:
                                    ps[slot, s, rows * j : rows * (j + 1), :] = piece.astype(BF16)
                        if not own:
                            for s in (3, 0, 2, 1):
                                remote(ps.at[slot, s], pr.at[slot, s], ps_s.at[slot, s], ps_r.at[slot, s], mate).start()

        work(n)


        def spread(s):
            k = t - 4 - jnp.abs(z - s)

            @pl.when(ok(k) & (s != z))
            def _():
                there = wp.at[_place(k), 2 * s + core]

                @pl.when(s < z)
                def _():
                    remote(there, there, au_s.at[prev, s], au_r.at[prev, s], mate).wait_recv()

                @pl.when(s > z)
                def _():
                    remote(there, there, ad_s.at[prev, s], ad_r.at[prev, s], mate).wait_recv()

                sends(s, there, there)

        loop(CHIPS, spread)


        def arrived(s):
            @pl.when(ok(t - 5 - jnp.abs(z - s)))
            def _():
                there = wp.at[0, 0]
                remote(there, there, am_s.at[prev, s], am_r.at[prev, s], mate).wait_recv()

        loop(CHIPS, arrived)

        @pl.when(n < TICKS - 3)
        def _():
            tell(free_m, mate)

            @pl.when(has_above)
            def _():
                tell(free_d, above)

            @pl.when(has_below)
            def _():
                tell(free_u, below)

    loop(TICKS, tick)


def update(given, w, m, v):
    vm, sem = pltpu.VMEM, pltpu.SemaphoreType
    block, wide = (BLOCK, LANES), N_Q + 2 * N_K
    scratch = [
        vm((D, T), BF16), vm((T, D), BF16), vm((SUMS, CHIPS, *block), F32),
        *(vm((SLOTS, CHIPS, *block), BF16) for _ in range(6)),
        vm((SLOTS, *block), BF16), vm((SLOTS, *block), BF16),
        *(vm((2, P_BLOCK[0], D), dtype) for dtype in (F32, F32, BF16)),
        vm((T, D), BF16), vm((T, D), BF16), vm((T, N_Q), BF16),
        vm((2, D, TF), BF16), vm((2, D, TF), BF16), vm((2, TF, D), BF16), vm((T, D), F32),
        *(vm((TF, TF), BF16) for _ in range(3)),
        vm((T, GROUP * HEAD), BF16), vm((T, HEAD), BF16), vm((T, HEAD), BF16), vm((T, wide), BF16), vm((N_Q, T), BF16),
        vm((T, HALF), F32), vm((T, HALF), F32), vm((KV, GROUP, T), F32), vm((KV, GROUP, T), F32), vm((4, STRIDE, HALF), F32),
        sem.DMA, sem.DMA, *(sem.DMA(shape) for shape in ((2, 3), (SLOTS, 2), (2, 3), (2,))), sem.DMA, sem.DMA((3,)), sem.DMA, sem.DMA((3,)), sem.DMA((6,)),
        *(sem.DMA((SLOTS, CHIPS)) for _ in range(12)),
        sem.REGULAR, sem.REGULAR, sem.REGULAR,
    ]
    refs = [*w, *m, *v, *(given[name] for name in INPUTS)]
    pair = [(FF, T), (T, FF), (T, FF), (T, D), (T, wide), (D, T), (N_Q, T), (D, T), (T, D), (T, D), (T, N_Q), (T, wide)]
    shapes = [(CHUNKS, 8, *block), (CHUNKS, *block), *((2, *shape) for shape in pair)]
    outs = [*((shape, BF16) for shape in shapes), ((2, KV, GROUP, T), F32), ((T, D), BF16), ((T, D), BF16)]
    return pl.pallas_call(
        _update,
        in_specs=[pl.BlockSpec(memory_space=pl.ANY)] * len(refs),
        out_specs=[pl.BlockSpec(memory_space=pl.ANY)] * len(outs),
        out_shape=[jax.ShapeDtypeStruct(*out) for out in outs],
        scratch_shapes=scratch,
        compiler_params=pltpu.CompilerParams(collective_id=0, has_side_effects=True, vmem_limit_bytes=63 * 2**20),
        name="update",
    )(*refs)[:2]


def _moments(m, v, g):
    return 0.9 * m + 0.1 * g, 0.95 * v + 0.05 * g * g


def _unpack(*refs):
    s = pl.program_id(1)
    ins, outs = refs[: 4 * len(NAMES)], refs[4 * len(NAMES) :]
    for i, name in enumerate(NAMES):
        wp_ref, gp_ref, m_ref, v_ref = ins[4 * i : 4 * i + 4]
        w_out, m_out, v_out = outs[i :: len(NAMES)]
        tall = name in ("w_down", "wo")
        rows, cols = Q_BLOCK if tall else P_BLOCK
        some = m_ref.shape[1]
        for j in range(cols // LANES):
            for n in range(wp_ref.shape[0]):
                over = slice(LANES * j, LANES * (j + 1)) if tall else slice(cols * n + LANES * j, cols * n + LANES * (j + 1))
                down = slice(rows * n, rows * (n + 1)) if tall else slice(0, rows)
                w_out[0, down, over] = wp_ref[n, 0, rows * j : rows * (j + 1), :]
                if tall and n:
                    continue
                if tall:
                    per = rows // some
                    g = gp_ref[s // per if name == "wo" else jnp.minimum(s, 6), pl.ds(pl.multiple_of(rows * j + some * (s % per), 16), some), :]
                else:
                    g = gp_ref[n, pl.ds(pl.multiple_of(rows * j + some * jnp.minimum(s, 6), 16), some), :]
                m_out[0, :, over], v_out[0, :, over] = _moments(m_ref[0, :, over], v_ref[0, :, over], g.astype(F32))


def unpack(wp, gp, m, v):
    block = (BLOCK, LANES)
    where = {"wq": (2, 22, 3), "wk": (1, 46, 6), "wv": (1, 47, 6), "wo": (2, 21, 3), "w_gate": (7, 0, 1), "w_up": (7, 2, 1), "w_down": (7, 4, 1)}
    in_specs, given, full, own = [], [], [], []
    for name in NAMES:
        count, start, step = where[name]
        _, height, width = m[name].shape
        some = 64 if name == "w_down" else 16
        last = height // some - 1
        mine = pl.BlockSpec((1, some, width), lambda layer, s, last=last: (layer, jnp.minimum(s, last), 0))
        in_specs += [
            pl.BlockSpec((count, 1, *block), lambda layer, s, start=start, step=step: (start + step * layer, s, 0, 0)),
            pl.BlockSpec((count, *block), lambda layer, s, start=start, step=step: (start + step * layer, 0, 0)), mine, mine,
        ]
        given += [wp, gp, m[name], v[name]]
        full.append((pl.BlockSpec((1, height, width), lambda layer, s: (layer, s, 0)), jax.ShapeDtypeStruct((2, 8 * height, width), BF16)))
        own.append((mine, jax.ShapeDtypeStruct(m[name].shape, F32)))
    outs = full + own + own
    return pl.pallas_call(
        _unpack,
        grid=(2, 8),
        in_specs=in_specs,
        out_specs=[o[0] for o in outs],
        out_shape=[o[1] for o in outs],
        compiler_params=pltpu.CompilerParams(vmem_limit_bytes=VMEM),
        name="unpack",
    )(*given)


def solution(mesh):
    angle = np.arange(STRIDE)[:, None] * float(THETA) ** (-np.arange(HALF) / HALF)
    turns = np.stack([turn(angle * step) for step in (STRIDE, 1) for turn in (np.cos, np.sin)]).astype(np.float32)

    def step(x, dy, *arrays):
        w, m, v = (dict(zip(NAMES, arrays[i : i + 7], strict=True)) for i in (0, 7, 14))
        wp, gp = update({"x": x[0], "dy": dy[0], "turns": jnp.asarray(turns)}, w.values(), m.values(), v.values())
        return tuple(unpack(wp, gp, m, v))

    states, all_of, cut = P(("rep", "dp"), None, None), P(None, None, None), P(None, "dp", None)
    return jax.shard_map(
        step,
        mesh=mesh,
        in_specs=(states, states) + (all_of,) * 7 + (cut,) * 14,
        out_specs=(P("rep", None, None),) * 7 + (P("rep", "dp", None),) * 14,
        check_vma=False,
    )
```

```python
import functools

import jax
import jax.numpy as jnp
import numpy as np
from jax import lax
from jax.experimental import pallas as pl
from jax.experimental.pallas import tpu as pltpu
from jax.sharding import PartitionSpec as P

LOG2E = 1.4426950408889634
HIDDEN = -2e30
VMEM = 56 * 2**20
F32, BF16 = jnp.float32, jnp.bfloat16
MESH = pl.DeviceIdType.MESH
T, D, FF, HEADS, KV, HEAD = 1024, 896, 3584, 4, 2, 256
THETA = 10000
STRIDE = 32
NAMES = ("wq", "wk", "wv", "wo", "w_gate", "w_up", "w_down")
ROWS = 256
TF = 512
PIECES = T // ROWS


def loop(count, body):
    lax.fori_loop(0, count, lambda i, _: body(i), None)


def dot(a, b):
    return jnp.dot(a, b, preferred_element_type=F32)


def dot_t(a, b):
    return lax.dot_general(a, b, (((1,), (1,)), ((), ())), preferred_element_type=F32)


def _scale(wide):
    return lax.rsqrt(jnp.mean(wide * wide, -1, keepdims=True) + 1e-6)


def _norm_back(h, by):
    s = _scale(h)
    return by * s - h * (s * s * s * jnp.mean(by * h, -1, keepdims=True))


E = HEAD**-0.5 * LOG2E
GROUP = HEADS // KV


def _piece(i):
    return slice(ROWS * i, ROWS * (i + 1))


def _visible():
    shape = (ROWS, GROUP * ROWS)
    return lax.broadcasted_iota(jnp.int32, shape, 0) <= lax.rem(lax.broadcasted_iota(jnp.int32, shape, 1), ROWS)


LANES = 128
BLOCK = 448
SLOTS = 4
SUMS = 5
EARLY = 2
LAG = 22
P_BLOCK, Q_BLOCK = (112, 512), (64, 896)
TILES = FF // TF
DOWN_AT, WO_AT, QKV_AT, PER_LAYER = 14, 21, 23, 27
CHUNKS = 2 * PER_LAYER
TICKS = CHUNKS + 11 + EARLY
CHIPS = 4
HALF, T_HALF = HEAD // 2, T // 2
N_Q, N_K = HEADS * HEAD, KV * HEAD
LEAVE, HEADS_AT, AFTER = 13, 14, 17


def _is_q(r):
    return (r >= DOWN_AT) & (r < QKV_AT)


def _place(k):
    layer, r = 1 - k // PER_LAYER, k % PER_LAYER
    double, single = (r % 2) * DOWN_AT + layer * TILES + r // 2, 2 * DOWN_AT + layer * TILES + r - DOWN_AT
    return jnp.where(r < DOWN_AT, double, jnp.where(r < WO_AT, single, 3 * DOWN_AT + layer * (PER_LAYER - WO_AT) + r - WO_AT))


def _owners(layer, r):
    mlp_chunk = r < DOWN_AT
    return (
        ("w_gate", mlp_chunk & (r % 2 == 0), r // 2), ("w_up", mlp_chunk & (r % 2 == 1), r // 2),
        ("w_down", (r >= DOWN_AT) & (r < WO_AT), r - DOWN_AT), ("wo", (r >= WO_AT) & (r < QKV_AT), r - WO_AT),
        ("wq", (r >= QKV_AT) & (r < QKV_AT + 2), r - QKV_AT), ("wk", r == QKV_AT + 2, 0 * r), ("wv", r == QKV_AT + 3, 0 * r),
    )


INPUTS = ("x", "dy", "turns")
OUTPUTS = ("wp", "gp", "hidt", "dgate", "dup", "d1", "dqkv", "at", "ot", "bt", "b", "h1", "o", "qkv", "lse", "h", "by1")
SCRATCH = ("ab", "db", "chip", "ps", "pr", "su", "ru", "sd", "rd", "wn", "gn", "mb", "vb", "wb", "x1", "x2", "oo", "wg", "wu", "wd", "acc", "dg", "du", "ht",
           "qq", "kk", "vv", "dq", "st", "cosb", "sinb", "lseb", "delta", "tb",
           "ab_sem", "db_sem", "opt_sem", "out_sem", "tile_sem", "x_sem", "o_sem", "qkv_sem", "lse_sem", "write_sem", "save_sem",
           "ps_s", "ps_r", "su_s", "su_r", "sd_s", "sd_r", "am_s", "am_r", "au_s", "au_r", "ad_s", "ad_r", "free_m", "free_u", "free_d")


def _update(*refs):
    w_in, m_in, v_in = (dict(zip(NAMES, refs[i : i + 7])) for i in (0, 7, 14))
    r_ = dict(zip((*INPUTS, *OUTPUTS, *SCRATCH), refs[21:], strict=True))
    (ab, db, chip, ps, pr, su, ru, sd, rd, wn, gn, mb, vb, wb, x1, x2, oo, wg, wu, wd, acc, dg, du, ht, qq, kk, vv, dq, st, cosb, sinb, lseb, delta, tb,
     ab_sem, db_sem, opt_sem, out_sem, tile_sem, x_sem, o_sem, qkv_sem, lse_sem, write_sem, save_sem,
     ps_s, ps_r, su_s, su_r, sd_s, sd_r, am_s, am_r, au_s, au_r, ad_s, ad_r, free_m, free_u, free_d) = (r_[name] for name in SCRATCH)
    wp, gp = r_["wp"], r_["gp"]
    rep, me = lax.axis_index("rep"), lax.axis_index("dp")
    z, core = me // 2, me % 2
    mate, above, below = me + 1 - 2 * core, me + 2, me - 2
    has_above, has_below = z < CHIPS - 1, z > 0

    def remote(src, dst, send, recv, to):
        return pltpu.make_async_remote_copy(src_ref=src, dst_ref=dst, send_sem=send, recv_sem=recv, device_id=(rep, to), device_id_type=MESH)

    def tell(sem, to):
        pl.semaphore_signal(sem, inc=1, device_id=(rep, to), device_id_type=MESH)

    def local(src, dst, sem):
        return pltpu.make_async_copy(src, dst, sem)

    def ok(k):
        return (k >= 0) & (k < CHUNKS)

    def wait_of(s):
        return 3 + ((s == 0) | (s == CHIPS - 1)).astype(jnp.int32)

    mine = wait_of(z)

    def tokens(start, count):
        return pl.ds(pl.multiple_of(start, ROWS), count)


    def tile_copies(half, j, buf):
        layer, over = 1 - half, pl.ds(pl.multiple_of(TF * j, TF), TF)
        return [
            local(w_in["w_gate"].at[layer, :, over], wg.at[buf], tile_sem.at[buf, 0]),
            local(w_in["w_up"].at[layer, :, over], wu.at[buf], tile_sem.at[buf, 1]),
            local(w_in["w_down"].at[layer, over, :], wd.at[buf], tile_sem.at[buf, 2]),
        ]

    def wo_copies(half):
        return [local(w_in["wo"].at[1 - half, pl.ds(TF * n, TF), :], wd.at[n], tile_sem.at[n, 2]) for n in range(2)]

    def qkv_weight_copies(half):
        layer = 1 - half
        return [
            *(local(w_in["wq"].at[layer, :, pl.ds(TF * n, TF)], wg.at[n], tile_sem.at[n, 0]) for n in range(2)),
            local(w_in["wk"].at[layer], wu.at[0], tile_sem.at[0, 1]), local(w_in["wv"].at[layer], wu.at[1], tile_sem.at[1, 1]),
        ]

    def column(at):
        return pl.ds(pl.multiple_of(at, HEAD), HEAD)

    def head_copies(half, head):
        pair = pl.ds(pl.multiple_of(GROUP * HEAD * head, GROUP * HEAD), GROUP * HEAD)
        return [
            local(r_["qkv"].at[half, :, over], to, qkv_sem.at[n])
            for n, (over, to) in enumerate(((pair, qq), (column(N_Q + HEAD * head), kk), (column(N_Q + N_K + HEAD * head), vv)))
        ]

    def late_copies():
        first = pl.ds(0, TF)
        return [
            *tile_copies(0, 0, 0)[:2], local(r_["dgate"].at[0, :, first], st.at[:, first], qkv_sem.at[0]),
            local(r_["dup"].at[0, :, first], st.at[:, pl.ds(TF, TF)], qkv_sem.at[1]),
        ]

    def load_x2(ref):
        return local(ref, x2, x_sem.at[1])

    def unit_of(n):
        half = (n >= AFTER + 2 + EARLY).astype(jnp.int32)
        return half, n - EARLY - LAG * half

    def start(copies):
        for copy in copies:
            copy.start()

    def wait(copies):
        for copy in copies:
            copy.wait()

    def writes(half, tau):
        u = tau + EARLY
        j, first = u // 2, tokens(T_HALF * (u % 2), T_HALF)
        over = pl.ds(pl.multiple_of(TF * j, TF), TF)
        part = tokens(T_HALF * (tau - AFTER), T_HALF)
        after_at = (tau >= AFTER) & (tau < AFTER + 2)
        return (
            ((u >= 0) & (u < 2 * TILES), lambda: [
                local(dg, r_["dgate"].at[half, first, over], write_sem.at[0]), local(du, r_["dup"].at[half, first, over], write_sem.at[1]),
                local(ht, r_["hidt"].at[half, over, first], write_sem.at[2])]),
            (tau == LEAVE, lambda: [local(x1, r_["d1"].at[half], write_sem.at[0])]),
            (after_at, lambda: [local(dq.at[part, :], r_["dqkv"].at[half, part, :], write_sem.at[0])]),
            (after_at & (half == 0), lambda: [local(x1.at[part, :], r_["by1"].at[part, :], write_sem.at[1])]),
        )

    def fetch(n):
        half, tau = unit_of(n)
        u = tau + EARLY

        @pl.when((tau == -EARLY - 1) & (half == 1))
        def _():
            start([*tile_copies(half, 0, 0), load_x2(r_["b"].at[half])])

        @pl.when((u >= 0) & (u % 2 == 0) & (u < 2 * TILES - 2))
        def _():
            start(tile_copies(half, u // 2 + 1, (u // 2 + 1) % 2))

        @pl.when(tau == LEAVE - 1)
        def _():
            start([*wo_copies(half), load_x2(r_["h1"].at[half]), local(r_["o"].at[half], oo, o_sem)])

        @pl.when(tau == LEAVE)
        def _():
            start([*head_copies(half, 0), local(r_["lse"].at[half], lseb, lse_sem)])

        @pl.when(tau == HEADS_AT + 1)
        def _():
            start(head_copies(half, 1))

        @pl.when((tau == LEAVE - 1) & (half == 0))
        def _():
            start(late_copies())

        @pl.when((tau == LEAVE) & (half == 0))
        def _():
            start(qkv_weight_copies(0))

        @pl.when((tau == HEADS_AT) & (half == 0))
        def _():
            start([load_x2(r_["h"])])

    def mlp_unit(u, buf, later):
        rows = tokens(T_HALF * (u % 2), T_HALF)
        gate, up = dot(x2[rows, :], wg[buf]), dot(x2[rows, :], wu[buf])
        sig = 1.0 / (1.0 + jnp.exp(-gate))
        silu = gate * sig
        by = dot_t(x1[rows, :], wd[buf]).astype(BF16).astype(F32)
        ht[...] = (silu * up).astype(BF16).T
        du[...] = (by * silu).astype(BF16)
        dg[...] = (by * up * (sig * (1.0 + gate * (1.0 - sig)))).astype(BF16)

        @pl.when(jnp.logical_not(later))
        def _():
            acc[rows, :] += dot_t(dg[...], wg[buf]) + dot_t(du[...], wu[buf])

    def late_unit(i):
        rows = tokens(ROWS * i, ROWS)
        acc[rows, :] += dot_t(st[rows, :TF], wg[0]) + dot_t(st[rows, TF:], wu[0])

    def leave_unit(i):
        rows = tokens(ROWS * i, ROWS)
        inner = _norm_back(x2[rows, :].astype(F32), acc[rows, :].astype(BF16).astype(F32)).astype(BF16)
        d1 = (x1[rows, :].astype(F32) + inner.astype(F32)).astype(BF16)
        x1[rows, :] = d1
        for n in range(HEADS):
            low, over = HEAD * (n % 2), _piece(n)
            do = dot_t(d1, wd[n // 2, low : low + HEAD, :]).astype(BF16)
            both = do.astype(F32) * oo[rows, over].astype(F32)
            oo[rows, over] = do
            delta[n // GROUP, n % GROUP : n % GROUP + 1, rows] = both.T.sum(0, keepdims=True)

    def side(ref, i, head):
        return jnp.concatenate([ref[_piece(i), column(HEAD * (GROUP * head + n))] for n in range(GROUP)], axis=0)

    def turn_back(part, rows):
        cos, sin = cosb[rows, :], sinb[rows, :]
        x, y = part[:, :HALF].astype(F32), part[:, HALF:].astype(F32)
        return jnp.concatenate([x * cos + y * sin, y * cos - x * sin], -1).astype(BF16)

    def head_unit(head):
        seen = _visible()
        turned = kk[...].T
        line = lambda ref, i: jnp.concatenate([ref[head, n : n + 1, _piece(i)] for n in range(GROUP)], axis=1)
        dk_at, dv_at = slice(0, HEAD), slice(HEAD, 2 * HEAD)
        for i in range(PIECES):
            lse, dl = line(lseb, i), line(delta, i)
            q = jnp.concatenate([qq[_piece(i), _piece(n)] for n in range(GROUP)], axis=0)
            do = side(oo, i, head)
            by_q = 0.0
            for j in range(i + 1):
                at = _piece(j)
                p = jnp.exp2(dot_t(kk[at, :], q) * E - lse)
                if j == i:
                    p = jnp.where(seen, p, 0.0)
                ds = (p * (dot_t(vv[at, :], do) - dl)).astype(BF16)
                by_v, by_k = dot(p.astype(BF16), do), dot(ds, q)
                acc[at, dv_at] = by_v if j == i else acc[at, dv_at] + by_v
                acc[at, dk_at] = by_k if j == i else acc[at, dk_at] + by_k
                by_q = by_q + dot(turned[:, at], ds)
            by_q = (by_q * HEAD**-0.5).astype(BF16)
            for n in range(GROUP):
                dq[_piece(i), column(HEAD * (GROUP * head + n))] = turn_back(by_q[:, _piece(n)].T, _piece(i))
        for i in range(PIECES):
            dq[_piece(i), column(N_Q + HEAD * head)] = turn_back((acc[_piece(i), dk_at] * HEAD**-0.5).astype(BF16), _piece(i))
            dq[_piece(i), column(N_Q + N_K + HEAD * head)] = acc[_piece(i), dv_at].astype(BF16)

    def after_unit(rows):
        by = sum(dot_t(dq[rows, TF * n : TF * (n + 1)], (wg, wu)[n // 2][n % 2]) for n in range(4)).astype(BF16).astype(F32)
        inner = _norm_back(x2[rows, :].astype(F32), by).astype(BF16)
        x1[rows, :] = (x1[rows, :].astype(F32) + inner.astype(F32)).astype(BF16)

    def work(n):
        half, tau = unit_of(n)
        u = tau + EARLY

        @pl.when((u >= 0) & (u < 2 * TILES))
        def _():
            buf = u // 2 % 2

            @pl.when(u % 2 == 0)
            def _():
                wait(tile_copies(half, u // 2, buf))

            @pl.when(u == 0)
            def _():
                acc[...] = jnp.zeros((T, D), F32)

                @pl.when(half == 1)
                def _():
                    load_x2(r_["h"]).wait()

            mlp_unit(u, buf, (half == 0) & (u < 2))

        @pl.when((tau == LEAVE - 1) & (half == 0))
        def _():
            wait(late_copies())
            loop(PIECES, late_unit)

        @pl.when(tau == LEAVE)
        def _():
            wait([load_x2(r_["h"]), local(r_["o"].at[0], oo, o_sem), *wo_copies(half)])
            loop(PIECES, leave_unit)

        @pl.when((tau == HEADS_AT) | (tau == HEADS_AT + 2))
        def _():
            @pl.when(tau == HEADS_AT)
            def _():
                local(r_["lse"].at[0], lseb, lse_sem).wait()

            wait(head_copies(0, 0))
            head_unit((tau - HEADS_AT) // 2)

        @pl.when((tau >= AFTER) & (tau < AFTER + 2) & (half == 0))
        def _():
            @pl.when(tau == AFTER)
            def _():
                wait([load_x2(r_["h"]), *qkv_weight_copies(0)])

            loop(PIECES // 2, lambda i: after_unit(tokens(T_HALF * (tau - AFTER) + ROWS * i, ROWS)))

        for test, copies in writes(half, tau):
            pl.when(test)(lambda: start(copies()))


    def load_operands(k):
        half, r = k // PER_LAYER, k % PER_LAYER

        def from_rows(ref, block, down):
            rows, whole = block[0], ref.shape[0] // 8
            for e in range(8):
                owner = 2 * (e % 4) + (1 - core if e < 4 else core)
                at = pl.multiple_of(whole * owner + down, 16)
                local(ref.at[pl.ds(at, rows), :], ab.at[pl.ds(rows * e, rows), :], ab_sem).start()

        def from_columns(ref, j):
            local(ref.at[:, pl.ds(pl.multiple_of(TF * j, TF), TF)], db.at[:, pl.ds(0, TF)], db_sem).start()

        @pl.when(r < DOWN_AT)
        def _():
            from_rows(r_["bt"].at[half], P_BLOCK, 0)

        @pl.when((r < DOWN_AT) & (r % 2 == 0))
        def _():
            from_columns(r_["dgate"].at[half], r // 2)

        @pl.when((r < DOWN_AT) & (r % 2 == 1))
        def _():
            from_columns(r_["dup"].at[half], r // 2)

        @pl.when((r >= DOWN_AT) & (r < WO_AT))
        def _():
            from_rows(r_["hidt"].at[half], Q_BLOCK, Q_BLOCK[0] * (r - DOWN_AT))

            @pl.when(half == 0)
            def _():
                local(r_["dy"], db, db_sem).start()

            @pl.when(half == 1)
            def _():
                local(r_["by1"], db, db_sem).start()

        @pl.when((r >= WO_AT) & (r < QKV_AT))
        def _():
            from_rows(r_["ot"].at[half], Q_BLOCK, Q_BLOCK[0] * (r - WO_AT))
            local(r_["d1"].at[half], db, db_sem).start()

        @pl.when(r >= QKV_AT)
        def _():
            from_rows(r_["at"].at[half], P_BLOCK, 0)
            from_columns(r_["dqkv"].at[half], r - QKV_AT)

    def wait_operands(block):
        rows, cols = block
        local(r_["hidt"].at[0, pl.ds(0, 8 * rows), :], ab.at[pl.ds(0, 8 * rows), :], ab_sem).wait()
        local(r_["dgate"].at[0, :, pl.ds(0, cols)], db.at[:, pl.ds(0, cols)], db_sem).wait()

    def optimizer_copies(k, buf, do):
        layer, r = 1 - k // PER_LAYER, k % PER_LAYER
        for name, test, j in _owners(layer, r):
            rows, cols = block = Q_BLOCK if name in ("w_down", "wo") else P_BLOCK

            @pl.when(test)
            def _():
                whole = w_in[name].shape[1] // 8
                down = pl.multiple_of(rows * j if block == Q_BLOCK else 0 * j, 16)
                right = pl.ds(0, cols) if block == Q_BLOCK else pl.ds(pl.multiple_of(cols * j, cols), cols)
                for n, (ref, at, to) in enumerate(((m_in[name], down, mb), (v_in[name], down, vb), (w_in[name], pl.multiple_of(whole * me + down, 16), wb))):
                    do(local(ref.at[layer, pl.ds(at, rows), right], to.at[buf, pl.ds(0, rows), pl.ds(0, cols)], opt_sem.at[buf, n]))


    def save(n, source, to):
        return local(source, to, save_sem.at[n])

    def attend_head(head):
        seen = _visible()
        k_at, turned = column(N_Q + HEAD * head), dq[:, column(N_Q + N_K + HEAD * head)].T

        def scores_of(i):
            q = side(dq, i, head)
            scores = [dot_t(dq[_piece(j), k_at], q) for j in range(i + 1)]
            return [*scores[:i], jnp.where(seen, scores[i], HIDDEN)]

        coming = scores_of(0)
        for i in range(PIECES):
            scores, coming = coming, scores_of(i + 1) if i + 1 < PIECES else None
            top = functools.reduce(jnp.maximum, [s.max(axis=0, keepdims=True) for s in scores])
            total, mix = 0.0, 0.0
            for j, s in enumerate(scores):
                p = jnp.exp2((s - top) * E)
                total = total + p.sum(axis=0, keepdims=True)
                mix = mix + dot(turned[:, _piece(j)], p.astype(BF16))
            out = (mix * (1.0 / total)).astype(BF16)
            lse = top * E + jnp.log(total) * LOG2E
            for n in range(GROUP):
                over = column(HEAD * (GROUP * head + n))
                st[over, _piece(i)] = out[:, _piece(n)]
                oo[_piece(i), over] = out[:, _piece(n)].T
                lseb[head, n : n + 1, _piece(i)] = lse[:, _piece(n)]

    def forward(layer):
        half = 1 - layer
        kept = lambda name: r_[name].at[half]
        wait(qkv_weight_copies(half))
        saves = [save(0, ab, kept("at")), save(1, dq, kept("qkv"))]
        for i in range(PIECES):
            wide = x1[_piece(i), :].astype(F32)
            a = (wide * _scale(wide)).astype(BF16)
            ab[:, _piece(i)] = a.T
            cos, sin = cosb[_piece(i), :], sinb[_piece(i), :]
            for c, w in enumerate((wg[0], wg[1], wu[0], wu[1])):
                t = dot(a, w).astype(BF16)
                for n in range(2):
                    part = t[:, _piece(n)]
                    if c < 3:
                        p, q = part[:, :HALF].astype(F32), part[:, HALF:].astype(F32)
                        part = jnp.concatenate([p * cos - q * sin, q * cos + p * sin], -1).astype(BF16)
                    dq[_piece(i), TF * c + HEAD * n : TF * c + HEAD * (n + 1)] = part
        tile = tile_copies(half, 0, 0)
        start([*saves, *wo_copies(half), *tile[:2]])
        loop(KV, attend_head)
        wait([*saves, *wo_copies(half)])
        saves = [save(0, ab, kept("bt")), save(1, x1, kept("h1")), save(2, x2, kept("b")), save(3, st, kept("ot")), save(4, oo, kept("o")), save(5, lseb, kept("lse"))]
        start(saves[3:])
        projected = lambda i: dot(oo[_piece(i), :TF], wd[0]) + dot(oo[_piece(i), TF:], wd[1])
        coming = projected(0)
        for i in range(PIECES):
            rows = _piece(i)
            total, coming = coming, projected(i + 1) if i + 1 < PIECES else None
            h1 = (x1[rows, :].astype(F32) + total.astype(BF16).astype(F32)).astype(BF16)
            x1[rows, :] = h1
            wide = h1.astype(F32)
            b = (wide * _scale(wide)).astype(BF16)
            x2[rows, :] = b
            ab[:, rows] = b.T
        start([*saves[:3], tile[2]])

        @pl.when(layer == 0)
        def _():
            acc[...] = jnp.zeros((T, D), F32)

            def one(j):
                buf = j % 2

                @pl.when(j < TILES - 1)
                def _():
                    start(tile_copies(half, j + 1, 1 - buf))

                wait(tile_copies(half, j, buf))
                for i in range(2):
                    rows = slice(T_HALF * i, T_HALF * (i + 1))
                    gate, up = dot(x2[rows, :], wg[buf]), dot(x2[rows, :], wu[buf])
                    hidden = (gate * (1.0 / (1.0 + jnp.exp(-gate))) * up).astype(BF16)
                    acc[rows, :] += dot(hidden, wd[buf])

            loop(TILES, one)
            start(qkv_weight_copies(0))

        wait(saves)

        @pl.when(layer == 0)
        def _():
            for i in range(PIECES):
                x1[_piece(i), :] = (x1[_piece(i), :].astype(F32) + acc[_piece(i), :].astype(BF16).astype(F32)).astype(BF16)
            save(0, x1, r_["h"]).start()
            save(0, x1, r_["h"]).wait()

    first = [local(r_["x"], x1, x_sem.at[0]), local(r_["turns"], tb, o_sem)]
    start([*first, *qkv_weight_copies(1)])


    barrier = pltpu.get_barrier_semaphore()
    tell(barrier, mate)

    @pl.when(has_above)
    def _():
        tell(barrier, above)

    @pl.when(has_below)
    def _():
        tell(barrier, below)

    wait(first)

    def spin(a):
        rows = pl.ds(pl.multiple_of(STRIDE * a, STRIDE), STRIDE)
        cos_a, sin_a, cos_b, sin_b = tb[0, pl.ds(a, 1), :], tb[1, pl.ds(a, 1), :], tb[2], tb[3]
        cosb[rows, :] = cos_a * cos_b - sin_a * sin_b
        sinb[rows, :] = sin_a * cos_b + cos_a * sin_b

    loop(T // STRIDE, spin)
    loop(2, forward)
    by_y = local(r_["dy"], x1, x_sem.at[0])
    by_y.start()

    @pl.when(has_above & has_below)
    def _():
        pl.semaphore_wait(barrier, 3)

    @pl.when(jnp.logical_not(has_above & has_below))
    def _():
        pl.semaphore_wait(barrier, 2)

    by_y.wait()

    def tick(n):
        t = n - EARLY
        slot, prev, late = n % SLOTS, (n + SLOTS - 1) % SLOTS, (n + 1) % SLOTS
        two = n % 2


        @pl.when(n >= 3)
        def _():
            pl.semaphore_wait(free_m, 1)

            @pl.when(has_above)
            def _():
                pl.semaphore_wait(free_u, 1)

            @pl.when(has_below)
            def _():
                pl.semaphore_wait(free_d, 1)

            @pl.when(ok(t - 3))
            def _():
                for s in range(CHIPS):
                    remote(ps.at[late, s], pr.at[late, s], ps_s.at[late, s], ps_r.at[late, s], mate).wait_send()

            @pl.when(ok(t - 4 - z))
            def _():
                for s in range(1, CHIPS):
                    @pl.when(s > z)
                    def _():
                        remote(su.at[late, s], ru.at[late, s], su_s.at[late, s], su_r.at[late, s], mate).wait_send()

            @pl.when(ok(t - 4 - (CHIPS - 1 - z)))
            def _():
                for s in range(CHIPS - 1):
                    @pl.when(s < z)
                    def _():
                        remote(sd.at[late, s], rd.at[late, s], sd_s.at[late, s], sd_r.at[late, s], mate).wait_send()

            def gone(s):
                @pl.when(ok(t - 3 - wait_of(s) - jnp.abs(z - s)))
                def _():
                    there = wp.at[0, 0]
                    remote(there, there, am_s.at[late, s], am_r.at[late, s], mate).wait_send()

                    @pl.when((s <= z) & has_above)
                    def _():
                        remote(there, there, au_s.at[late, s], au_r.at[late, s], mate).wait_send()

                    @pl.when((s >= z) & has_below)
                    def _():
                        remote(there, there, ad_s.at[late, s], ad_r.at[late, s], mate).wait_send()

            loop(CHIPS, gone)

            @pl.when(ok(t - 3 - mine))
            def _():
                local(wn.at[late], wp.at[0, 0], out_sem.at[late, 0]).wait()
                local(gn.at[late], gp.at[0], out_sem.at[late, 1]).wait()


        for test, copies in writes(*unit_of(n - 1)):
            pl.when(test & (n > 0))(lambda: wait(copies()))
        fetch(n)

        @pl.when(ok(t))
        def _():
            load_operands(t)

        @pl.when(ok(t + 1 - mine))
        def _():
            optimizer_copies(t + 1 - mine, 1 - two, lambda copy: copy.start())


        @pl.when(ok(t - 1))
        def _():
            for s in (3, 0, 2, 1):
                remote(ps.at[prev, s], pr.at[prev, s], ps_s.at[prev, s], ps_r.at[prev, s], mate).wait_recv()
                value = chip[(t - 1) % SUMS, s] + pr[prev, s].astype(F32)
                chip[(t - 1) % SUMS, s] = value
                if s > 0:
                    @pl.when(z == 0)
                    def _():
                        su[slot, s] = value.astype(BF16)
                        remote(su.at[slot, s], ru.at[slot, s], su_s.at[slot, s], su_r.at[slot, s], above).start()
                if s < CHIPS - 1:
                    @pl.when(z == CHIPS - 1)
                    def _():
                        sd[slot, s] = value.astype(BF16)
                        remote(sd.at[slot, s], rd.at[slot, s], sd_s.at[slot, s], sd_r.at[slot, s], below).start()


        def pass_on(s, k, from_above):
            got, send, here, there, to = (rd, sd, sd_s, sd_r, below) if from_above else (ru, su, su_s, su_r, above)
            remote(send.at[prev, s], got.at[prev, s], here.at[prev, s], there.at[prev, s], mate).wait_recv()
            value = chip[k % SUMS, s] + got[prev, s].astype(F32)
            chip[k % SUMS, s] = value
            send[slot, s] = value.astype(BF16)

            @pl.when((s < z) if from_above else (s > z))
            def _():
                remote(send.at[slot, s], got.at[slot, s], here.at[slot, s], there.at[slot, s], to).start()

        up_k, down_k = t - 1 - z, t - 1 - (CHIPS - 1 - z)
        for i in range(CHIPS - 1):
            @pl.when(has_below & ok(up_k) & (CHIPS - 1 - i >= z))
            def _():
                pass_on(CHIPS - 1 - i, up_k, False)

            @pl.when(has_above & ok(down_k) & (i <= z))
            def _():
                pass_on(i, down_k, True)


        @pl.when(ok(t - mine))
        def _():
            k = t - mine
            optimizer_copies(k, two, lambda copy: copy.wait())
            is_q = _is_q(k % PER_LAYER)
            for (rows, cols), test in ((Q_BLOCK, is_q), (P_BLOCK, jnp.logical_not(is_q))):
                @pl.when(test)
                def _():
                    for j in range(cols // LANES):
                        at, over = slice(rows * j, rows * (j + 1)), slice(LANES * j, LANES * (j + 1))
                        low = chip[k % SUMS, z, at, :].astype(BF16)
                        m, v = _moments(mb[two, :rows, over], vb[two, :rows, over], low.astype(F32))
                        w = wb[two, :rows, over].astype(F32)
                        wn[slot, at, :] = (w - 0.02 * (m * lax.rsqrt(v + 1e-8) + 0.1 * w)).astype(BF16)
                        gn[slot, at, :] = low

            at = _place(k)
            local(wn.at[slot], wp.at[at, me], out_sem.at[slot, 0]).start()
            local(gn.at[slot], gp.at[at], out_sem.at[slot, 1]).start()


        def sends(s, source, there):
            @pl.when((s <= z) & has_above)
            def _():
                remote(source, there, au_s.at[slot, s], au_r.at[slot, s], above).start()

            @pl.when((s >= z) & has_below)
            def _():
                remote(source, there, ad_s.at[slot, s], ad_r.at[slot, s], below).start()

            remote(source, there, am_s.at[slot, s], am_r.at[slot, s], mate).start()

        @pl.when(ok(t - mine))
        def _():
            sends(z, wn.at[slot], wp.at[_place(t - mine), me])


        @pl.when(ok(t))
        def _():
            is_q = _is_q(t % PER_LAYER)
            for (rows, cols), test in ((Q_BLOCK, is_q), (P_BLOCK, jnp.logical_not(is_q))):
                @pl.when(test)
                def _():
                    wait_operands((rows, cols))
                    for own in range(2):
                        got = dot(ab[4 * rows * own : 4 * rows * (own + 1), :], db[:, :cols])
                        for s in range(CHIPS):
                            for j in range(cols // LANES):
                                piece = got[rows * s : rows * (s + 1), LANES * j : LANES * (j + 1)]
                                if own:
                                    chip[t % SUMS, s, rows * j : rows * (j + 1), :] = piece
                                else:
                                    ps[slot, s, rows * j : rows * (j + 1), :] = piece.astype(BF16)
                        if not own:
                            for s in (3, 0, 2, 1):
                                remote(ps.at[slot, s], pr.at[slot, s], ps_s.at[slot, s], ps_r.at[slot, s], mate).start()

        work(n)


        def spread(s):
            k = t - wait_of(s) - jnp.abs(z - s)

            @pl.when(ok(k) & (s != z))
            def _():
                there = wp.at[_place(k), 2 * s + core]

                @pl.when(s < z)
                def _():
                    remote(there, there, au_s.at[prev, s], au_r.at[prev, s], mate).wait_recv()

                @pl.when(s > z)
                def _():
                    remote(there, there, ad_s.at[prev, s], ad_r.at[prev, s], mate).wait_recv()

                sends(s, there, there)

        loop(CHIPS, spread)


        def arrived(s):
            @pl.when(ok(t - 1 - wait_of(s) - jnp.abs(z - s)))
            def _():
                there = wp.at[0, 0]
                remote(there, there, am_s.at[prev, s], am_r.at[prev, s], mate).wait_recv()

        loop(CHIPS, arrived)

        @pl.when(n < TICKS - 3)
        def _():
            tell(free_m, mate)

            @pl.when(has_above)
            def _():
                tell(free_d, above)

            @pl.when(has_below)
            def _():
                tell(free_u, below)

    loop(TICKS, tick)


def update(given, w, m, v):
    vm, sem = pltpu.VMEM, pltpu.SemaphoreType
    block, wide = (BLOCK, LANES), N_Q + 2 * N_K
    scratch = [
        vm((D, T), BF16), vm((T, D), BF16), vm((SUMS, CHIPS, *block), F32),
        *(vm((SLOTS, CHIPS, *block), BF16) for _ in range(6)),
        vm((SLOTS, *block), BF16), vm((SLOTS, *block), BF16),
        *(vm((2, P_BLOCK[0], D), dtype) for dtype in (F32, F32, BF16)),
        vm((T, D), BF16), vm((T, D), BF16), vm((T, N_Q), BF16),
        vm((2, D, TF), BF16), vm((2, D, TF), BF16), vm((2, TF, D), BF16), vm((T, D), F32),
        *(vm((TF, TF), BF16) for _ in range(3)),
        vm((T, GROUP * HEAD), BF16), vm((T, HEAD), BF16), vm((T, HEAD), BF16), vm((T, wide), BF16), vm((N_Q, T), BF16),
        vm((T, HALF), F32), vm((T, HALF), F32), vm((KV, GROUP, T), F32), vm((KV, GROUP, T), F32), vm((4, STRIDE, HALF), F32),
        sem.DMA, sem.DMA, *(sem.DMA(shape) for shape in ((2, 3), (SLOTS, 2), (2, 3), (2,))), sem.DMA, sem.DMA((3,)), sem.DMA, sem.DMA((3,)), sem.DMA((6,)),
        *(sem.DMA((SLOTS, CHIPS)) for _ in range(12)),
        sem.REGULAR, sem.REGULAR, sem.REGULAR,
    ]
    refs = [*w, *m, *v, *(given[name] for name in INPUTS)]
    pair = [(FF, T), (T, FF), (T, FF), (T, D), (T, wide), (D, T), (N_Q, T), (D, T), (T, D), (T, D), (T, N_Q), (T, wide)]
    shapes = [(CHUNKS, 8, *block), (CHUNKS, *block), *((2, *shape) for shape in pair)]
    outs = [*((shape, BF16) for shape in shapes), ((2, KV, GROUP, T), F32), ((T, D), BF16), ((T, D), BF16)]
    return pl.pallas_call(
        _update,
        in_specs=[pl.BlockSpec(memory_space=pl.ANY)] * len(refs),
        out_specs=[pl.BlockSpec(memory_space=pl.ANY)] * len(outs),
        out_shape=[jax.ShapeDtypeStruct(*out) for out in outs],
        scratch_shapes=scratch,
        compiler_params=pltpu.CompilerParams(collective_id=0, has_side_effects=True, vmem_limit_bytes=63 * 2**20),
        name="update",
    )(*refs)[:2]


def _moments(m, v, g):
    return 0.9 * m + 0.1 * g, 0.95 * v + 0.05 * g * g


def _unpack(*refs):
    s = pl.program_id(1)
    ins, outs = refs[: 4 * len(NAMES)], refs[4 * len(NAMES) :]
    for i, name in enumerate(NAMES):
        wp_ref, gp_ref, m_ref, v_ref = ins[4 * i : 4 * i + 4]
        w_out, m_out, v_out = outs[i :: len(NAMES)]
        tall = name in ("w_down", "wo")
        rows, cols = Q_BLOCK if tall else P_BLOCK
        some = m_ref.shape[1]
        for j in range(cols // LANES):
            for n in range(wp_ref.shape[0]):
                over = slice(LANES * j, LANES * (j + 1)) if tall else slice(cols * n + LANES * j, cols * n + LANES * (j + 1))
                down = slice(rows * n, rows * (n + 1)) if tall else slice(0, rows)
                w_out[0, down, over] = wp_ref[n, 0, rows * j : rows * (j + 1), :]
                if tall and n:
                    continue
                if tall:
                    per = rows // some
                    g = gp_ref[s // per if name == "wo" else jnp.minimum(s, 6), pl.ds(pl.multiple_of(rows * j + some * (s % per), 16), some), :]
                else:
                    g = gp_ref[n, pl.ds(pl.multiple_of(rows * j + some * jnp.minimum(s, 6), 16), some), :]
                m_out[0, :, over], v_out[0, :, over] = _moments(m_ref[0, :, over], v_ref[0, :, over], g.astype(F32))


def unpack(wp, gp, m, v):
    block = (BLOCK, LANES)
    where = {"wq": (2, 22, 3), "wk": (1, 46, 6), "wv": (1, 47, 6), "wo": (2, 21, 3), "w_gate": (7, 0, 1), "w_up": (7, 2, 1), "w_down": (7, 4, 1)}
    in_specs, given, full, own = [], [], [], []
    for name in NAMES:
        count, start, step = where[name]
        _, height, width = m[name].shape
        some = 64 if name == "w_down" else 16
        last = height // some - 1
        mine = pl.BlockSpec((1, some, width), lambda layer, s, last=last: (layer, jnp.minimum(s, last), 0))
        in_specs += [
            pl.BlockSpec((count, 1, *block), lambda layer, s, start=start, step=step: (start + step * layer, s, 0, 0)),
            pl.BlockSpec((count, *block), lambda layer, s, start=start, step=step: (start + step * layer, 0, 0)), mine, mine,
        ]
        given += [wp, gp, m[name], v[name]]
        full.append((pl.BlockSpec((1, height, width), lambda layer, s: (layer, s, 0)), jax.ShapeDtypeStruct((2, 8 * height, width), BF16)))
        own.append((mine, jax.ShapeDtypeStruct(m[name].shape, F32)))
    outs = full + own + own
    return pl.pallas_call(
        _unpack,
        grid=(2, 8),
        in_specs=in_specs,
        out_specs=[o[0] for o in outs],
        out_shape=[o[1] for o in outs],
        compiler_params=pltpu.CompilerParams(vmem_limit_bytes=VMEM),
        name="unpack",
    )(*given)


def solution(mesh):
    angle = np.arange(STRIDE)[:, None] * float(THETA) ** (-np.arange(HALF) / HALF)
    turns = np.stack([turn(angle * step) for step in (STRIDE, 1) for turn in (np.cos, np.sin)]).astype(np.float32)

    def step(x, dy, *arrays):
        w, m, v = (dict(zip(NAMES, arrays[i : i + 7], strict=True)) for i in (0, 7, 14))
        wp, gp = update({"x": x[0], "dy": dy[0], "turns": jnp.asarray(turns)}, w.values(), m.values(), v.values())
        return tuple(unpack(wp, gp, m, v))

    states, all_of, cut = P(("rep", "dp"), None, None), P(None, None, None), P(None, "dp", None)
    return jax.shard_map(
        step,
        mesh=mesh,
        in_specs=(states, states) + (all_of,) * 7 + (cut,) * 14,
        out_specs=(P("rep", None, None),) * 7 + (P("rep", "dp", None),) * 14,
        check_vma=False,
    )
```

```python
import functools

import jax
import jax.numpy as jnp
import numpy as np
from jax import lax
from jax.experimental import pallas as pl
from jax.experimental.pallas import tpu as pltpu
from jax.sharding import PartitionSpec as P

LOG2E = 1.4426950408889634
HIDDEN = -2e30
VMEM = 56 * 2**20
F32, BF16 = jnp.float32, jnp.bfloat16
MESH = pl.DeviceIdType.MESH
T, D, FF, HEADS, KV, HEAD = 1024, 896, 3584, 4, 2, 256
THETA = 10000
STRIDE = 32
NAMES = ("wq", "wk", "wv", "wo", "w_gate", "w_up", "w_down")
ROWS = 256
TF = 512
PIECES = T // ROWS


def loop(count, body):
    lax.fori_loop(0, count, lambda i, _: body(i), None)


def dot(a, b):
    return jnp.dot(a, b, preferred_element_type=F32)


def dot_t(a, b):
    return lax.dot_general(a, b, (((1,), (1,)), ((), ())), preferred_element_type=F32)


def _scale(wide):
    return lax.rsqrt(jnp.mean(wide * wide, -1, keepdims=True) + 1e-6)


def _norm_back(h, by):
    s = _scale(h)
    return by * s - h * (s * s * s * jnp.mean(by * h, -1, keepdims=True))


E = HEAD**-0.5 * LOG2E
GROUP = HEADS // KV


def _piece(i):
    return slice(ROWS * i, ROWS * (i + 1))


def _visible():
    shape = (ROWS, GROUP * ROWS)
    return lax.broadcasted_iota(jnp.int32, shape, 0) <= lax.rem(lax.broadcasted_iota(jnp.int32, shape, 1), ROWS)


LANES = 128
BLOCK = 448
SLOTS = 4
SUMS = 5
EARLY = 2
LAG = 27
P_BLOCK, Q_BLOCK = (112, 512), (64, 896)
TILES = FF // TF
DOWN_AT, WO_AT, QKV_AT, PER_LAYER = 14, 21, 23, 27
CHUNKS = 2 * PER_LAYER
TICKS = CHUNKS + 11 + EARLY
CHIPS = 4
QKV_ORDER = (1, 3, 0, 2)
HALF, T_HALF = HEAD // 2, T // 2
N_Q, N_K = HEADS * HEAD, KV * HEAD
LEAVE, HEADS_AT, AFTER = 13, 14, 17


def _is_q(r):
    return (r >= DOWN_AT) & (r < QKV_AT)


def _place(k):
    layer, r = 1 - k // PER_LAYER, k % PER_LAYER
    double, single = (r % 2) * DOWN_AT + layer * TILES + r // 2, 2 * DOWN_AT + layer * TILES + r - DOWN_AT
    return jnp.where(r < DOWN_AT, double, jnp.where(r < WO_AT, single, 3 * DOWN_AT + layer * (PER_LAYER - WO_AT) + r - WO_AT))


def _owners(layer, r):
    mlp_chunk = r < DOWN_AT
    return (
        ("w_gate", mlp_chunk & (r % 2 == 0), r // 2), ("w_up", mlp_chunk & (r % 2 == 1), r // 2),
        ("w_down", (r >= DOWN_AT) & (r < WO_AT), r - DOWN_AT), ("wo", (r >= WO_AT) & (r < QKV_AT), r - WO_AT),
        ("wq", (r >= QKV_AT) & (r < QKV_AT + 2), r - QKV_AT), ("wk", r == QKV_AT + 2, 0 * r), ("wv", r == QKV_AT + 3, 0 * r),
    )


INPUTS = ("x", "dy", "turns")
OUTPUTS = ("wp", "gp", "hidt", "d1", "dqkv", "at", "ot", "bt", "b", "h1", "o", "qkv", "lse", "h", "by1")
SCRATCH = ("ab", "db", "chip", "ps", "pr", "su", "ru", "sd", "rd", "wn", "gn", "mb", "vb", "wb", "x1", "x2", "oo", "wg", "wu", "wd", "acc", "dg", "du", "ht",
           "qq", "kk", "vv", "dq", "st", "cosb", "sinb", "lseb", "delta", "tb",
           "ab_sem", "db_sem", "opt_sem", "out_sem", "tile_sem", "x_sem", "o_sem", "qkv_sem", "lse_sem", "write_sem", "save_sem",
           "ps_s", "ps_r", "su_s", "su_r", "sd_s", "sd_r", "am_s", "am_r", "au_s", "au_r", "ad_s", "ad_r", "free_m", "free_u", "free_d")


def _update(*refs):
    w_in, m_in, v_in = (dict(zip(NAMES, refs[i : i + 7])) for i in (0, 7, 14))
    r_ = dict(zip((*INPUTS, *OUTPUTS, *SCRATCH), refs[21:], strict=True))
    (ab, db, chip, ps, pr, su, ru, sd, rd, wn, gn, mb, vb, wb, x1, x2, oo, wg, wu, wd, acc, dg, du, ht, qq, kk, vv, dq, st, cosb, sinb, lseb, delta, tb,
     ab_sem, db_sem, opt_sem, out_sem, tile_sem, x_sem, o_sem, qkv_sem, lse_sem, write_sem, save_sem,
     ps_s, ps_r, su_s, su_r, sd_s, sd_r, am_s, am_r, au_s, au_r, ad_s, ad_r, free_m, free_u, free_d) = (r_[name] for name in SCRATCH)
    wp, gp = r_["wp"], r_["gp"]
    rep, me = lax.axis_index("rep"), lax.axis_index("dp")
    z, core = me // 2, me % 2
    mate, above, below = me + 1 - 2 * core, me + 2, me - 2
    has_above, has_below = z < CHIPS - 1, z > 0

    def remote(src, dst, send, recv, to):
        return pltpu.make_async_remote_copy(src_ref=src, dst_ref=dst, send_sem=send, recv_sem=recv, device_id=(rep, to), device_id_type=MESH)

    def tell(sem, to):
        pl.semaphore_signal(sem, inc=1, device_id=(rep, to), device_id_type=MESH)

    def local(src, dst, sem):
        return pltpu.make_async_copy(src, dst, sem)

    def ok(k):
        return (k >= 0) & (k < CHUNKS)

    def wait_of(s):
        return 3 + ((s == 0) | (s == CHIPS - 1)).astype(jnp.int32)

    mine = wait_of(z)

    def tokens(start, count):
        return pl.ds(pl.multiple_of(start, ROWS), count)


    def tile_copies(half, j, buf):
        layer, over = 1 - half, pl.ds(pl.multiple_of(TF * j, TF), TF)
        return [
            local(w_in["w_gate"].at[layer, :, over], wg.at[buf], tile_sem.at[buf, 0]),
            local(w_in["w_up"].at[layer, :, over], wu.at[buf], tile_sem.at[buf, 1]),
            local(w_in["w_down"].at[layer, over, :], wd.at[buf], tile_sem.at[buf, 2]),
        ]

    def wo_copies(half):
        return [local(w_in["wo"].at[1 - half, pl.ds(TF * n, TF), :], wd.at[n], tile_sem.at[n, 2]) for n in range(2)]

    def qkv_weight_copies(half):
        layer = 1 - half
        return [
            *(local(w_in["wq"].at[layer, :, pl.ds(TF * n, TF)], wg.at[n], tile_sem.at[n, 0]) for n in range(2)),
            local(w_in["wk"].at[layer], wu.at[0], tile_sem.at[0, 1]), local(w_in["wv"].at[layer], wu.at[1], tile_sem.at[1, 1]),
        ]

    def column(at):
        return pl.ds(pl.multiple_of(at, HEAD), HEAD)

    def head_copies(half, head):
        pair = pl.ds(pl.multiple_of(GROUP * HEAD * head, GROUP * HEAD), GROUP * HEAD)
        return [
            local(r_["qkv"].at[half, :, over], to, qkv_sem.at[n])
            for n, (over, to) in enumerate(((pair, qq), (column(N_Q + HEAD * head), kk), (column(N_Q + N_K + HEAD * head), vv)))
        ]

    def load_x2(ref):
        return local(ref, x2, x_sem.at[1])

    def unit_of(n):
        half = (n >= AFTER + 2 + EARLY).astype(jnp.int32)
        return half, n - EARLY - LAG * half

    def start(copies):
        for copy in copies:
            copy.start()

    def wait(copies):
        for copy in copies:
            copy.wait()

    def writes(half, tau):
        u = tau + EARLY
        j, first = u // 2, tokens(T_HALF * (u % 2), T_HALF)
        over = pl.ds(pl.multiple_of(TF * j, TF), TF)
        part = tokens(T_HALF * (tau - AFTER), T_HALF)
        after_at = (tau >= AFTER) & (tau < AFTER + 2)
        return (
            ((u >= 0) & (u < 2 * TILES), lambda: [local(ht, r_["hidt"].at[half, over, first], write_sem.at[0])]),
            (tau == LEAVE, lambda: [local(x1, r_["d1"].at[half], write_sem.at[0])]),
            (after_at, lambda: [local(dq.at[part, :], r_["dqkv"].at[half, part, :], write_sem.at[0])]),
            (after_at & (half == 0), lambda: [local(x1.at[part, :], r_["by1"].at[part, :], write_sem.at[1])]),
        )

    def fetch(n):
        half, tau = unit_of(n)
        u = tau + EARLY

        @pl.when((tau == -EARLY - 1) & (half == 1))
        def _():
            start([*tile_copies(half, 0, 0), load_x2(r_["b"].at[half])])

        @pl.when((u >= 0) & (u % 2 == 0) & (u < 2 * TILES - 2))
        def _():
            start(tile_copies(half, u // 2 + 1, (u // 2 + 1) % 2))

        @pl.when(tau == LEAVE - 1)
        def _():
            start([*wo_copies(half), load_x2(r_["h1"].at[half]), local(r_["o"].at[half], oo, o_sem)])

        @pl.when(tau == LEAVE)
        def _():
            start([*head_copies(half, 0), local(r_["lse"].at[half], lseb, lse_sem)])

        @pl.when(tau == HEADS_AT + 1)
        def _():
            start(head_copies(half, 1))

        @pl.when((tau == LEAVE - 1) & (half == 0))
        def _():
            start(tile_copies(0, 0, 0)[:2])

        @pl.when((tau == LEAVE) & (half == 0))
        def _():
            start(qkv_weight_copies(0))

        @pl.when((tau == HEADS_AT) & (half == 0))
        def _():
            start([load_x2(r_["h"])])

    def mlp_unit(u, buf, later):
        rows = tokens(T_HALF * (u % 2), T_HALF)
        gate, up = dot(x2[rows, :], wg[buf]), dot(x2[rows, :], wu[buf])
        sig = 1.0 / (1.0 + jnp.exp(-gate))
        silu = gate * sig
        by = dot_t(x1[rows, :], wd[buf]).astype(BF16).astype(F32)
        ht[...] = (silu * up).astype(BF16).T
        du[buf, rows, :] = (by * silu).astype(BF16)
        dg[buf, rows, :] = (by * up * (sig * (1.0 + gate * (1.0 - sig)))).astype(BF16)

        @pl.when(jnp.logical_not(later))
        def _():
            acc[rows, :] += dot_t(dg[buf, rows, :], wg[buf]) + dot_t(du[buf, rows, :], wu[buf])

    def late_unit(i):
        rows = tokens(ROWS * i, ROWS)
        acc[rows, :] += dot_t(st[rows, :TF], wg[0]) + dot_t(st[rows, TF:], wu[0])

    def leave_unit(i):
        rows = tokens(ROWS * i, ROWS)
        inner = _norm_back(x2[rows, :].astype(F32), acc[rows, :].astype(BF16).astype(F32)).astype(BF16)
        d1 = (x1[rows, :].astype(F32) + inner.astype(F32)).astype(BF16)
        x1[rows, :] = d1
        for n in range(HEADS):
            low, over = HEAD * (n % 2), _piece(n)
            do = dot_t(d1, wd[n // 2, low : low + HEAD, :]).astype(BF16)
            both = do.astype(F32) * oo[rows, over].astype(F32)
            oo[rows, over] = do
            delta[n // GROUP, n % GROUP : n % GROUP + 1, rows] = both.T.sum(0, keepdims=True)

    def side(ref, i, head):
        return jnp.concatenate([ref[_piece(i), column(HEAD * (GROUP * head + n))] for n in range(GROUP)], axis=0)

    def turn_back(part, rows):
        cos, sin = cosb[rows, :], sinb[rows, :]
        x, y = part[:, :HALF].astype(F32), part[:, HALF:].astype(F32)
        return jnp.concatenate([x * cos + y * sin, y * cos - x * sin], -1).astype(BF16)

    def head_unit(head):
        seen = _visible()
        turned = kk[...].T
        line = lambda ref, i: jnp.concatenate([ref[head, n : n + 1, _piece(i)] for n in range(GROUP)], axis=1)
        dk_at, dv_at = slice(0, HEAD), slice(HEAD, 2 * HEAD)
        for i in range(PIECES):
            lse, dl = line(lseb, i), line(delta, i)
            q = jnp.concatenate([qq[_piece(i), _piece(n)] for n in range(GROUP)], axis=0)
            do = side(oo, i, head)
            by_q = 0.0
            for j in range(i + 1):
                at = _piece(j)
                p = jnp.exp2(dot_t(kk[at, :], q) * E - lse)
                if j == i:
                    p = jnp.where(seen, p, 0.0)
                ds = (p * (dot_t(vv[at, :], do) - dl)).astype(BF16)
                by_v, by_k = dot(p.astype(BF16), do), dot(ds, q)
                acc[at, dv_at] = by_v if j == i else acc[at, dv_at] + by_v
                acc[at, dk_at] = by_k if j == i else acc[at, dk_at] + by_k
                by_q = by_q + dot(turned[:, at], ds)
            by_q = (by_q * HEAD**-0.5).astype(BF16)
            for n in range(GROUP):
                dq[_piece(i), column(HEAD * (GROUP * head + n))] = turn_back(by_q[:, _piece(n)].T, _piece(i))
        for i in range(PIECES):
            dq[_piece(i), column(N_Q + HEAD * head)] = turn_back((acc[_piece(i), dk_at] * HEAD**-0.5).astype(BF16), _piece(i))
            dq[_piece(i), column(N_Q + N_K + HEAD * head)] = acc[_piece(i), dv_at].astype(BF16)

    def after_unit(rows):
        by = sum(dot_t(dq[rows, TF * n : TF * (n + 1)], (wg, wu)[n // 2][n % 2]) for n in range(4)).astype(BF16).astype(F32)
        inner = _norm_back(x2[rows, :].astype(F32), by).astype(BF16)
        x1[rows, :] = (x1[rows, :].astype(F32) + inner.astype(F32)).astype(BF16)

    def work(n):
        half, tau = unit_of(n)
        u = tau + EARLY

        @pl.when((u >= 0) & (u < 2 * TILES))
        def _():
            buf = u // 2 % 2

            @pl.when(u % 2 == 0)
            def _():
                wait(tile_copies(half, u // 2, buf))

            @pl.when(u == 0)
            def _():
                acc[...] = jnp.zeros((T, D), F32)

                @pl.when(half == 1)
                def _():
                    load_x2(r_["h"]).wait()

            mlp_unit(u, buf, (half == 0) & (u < 2))

            @pl.when((half == 0) & (u == 1))
            def _():
                st[:, :TF] = dg[0]
                st[:, TF:] = du[0]

        @pl.when((tau == LEAVE - 1) & (half == 0))
        def _():
            wait(tile_copies(0, 0, 0)[:2])
            loop(PIECES, late_unit)

        @pl.when(tau == LEAVE)
        def _():
            wait([load_x2(r_["h"]), local(r_["o"].at[0], oo, o_sem), *wo_copies(half)])
            loop(PIECES, leave_unit)

        @pl.when((tau == HEADS_AT) | (tau == HEADS_AT + 2))
        def _():
            @pl.when(tau == HEADS_AT)
            def _():
                local(r_["lse"].at[0], lseb, lse_sem).wait()

            wait(head_copies(0, 0))
            head_unit((tau - HEADS_AT) // 2)

        @pl.when((tau >= AFTER) & (tau < AFTER + 2) & (half == 0))
        def _():
            @pl.when(tau == AFTER)
            def _():
                wait([load_x2(r_["h"]), *qkv_weight_copies(0)])

            loop(PIECES // 2, lambda i: after_unit(tokens(T_HALF * (tau - AFTER) + ROWS * i, ROWS)))

        for test, copies in writes(half, tau):
            pl.when(test)(lambda: start(copies()))


    def load_operands(k):
        half, r = k // PER_LAYER, k % PER_LAYER

        def from_rows(ref, block, down):
            rows, whole = block[0], ref.shape[0] // 8
            for e in range(8):
                owner = 2 * (e % 4) + (1 - core if e < 4 else core)
                at = pl.multiple_of(whole * owner + down, 16)
                local(ref.at[pl.ds(at, rows), :], ab.at[pl.ds(rows * e, rows), :], ab_sem).start()

        @pl.when(r < DOWN_AT)
        def _():
            from_rows(r_["bt"].at[half], P_BLOCK, 0)

        @pl.when((r >= DOWN_AT) & (r < WO_AT))
        def _():
            from_rows(r_["hidt"].at[half], Q_BLOCK, Q_BLOCK[0] * (r - DOWN_AT))

            @pl.when(half == 0)
            def _():
                local(r_["dy"], db, db_sem).start()

            @pl.when(half == 1)
            def _():
                local(r_["by1"], db, db_sem).start()

        @pl.when((r >= WO_AT) & (r < QKV_AT))
        def _():
            from_rows(r_["ot"].at[half], Q_BLOCK, Q_BLOCK[0] * (r - WO_AT))
            local(r_["d1"].at[half], db, db_sem).start()

        @pl.when(r >= QKV_AT)
        def _():
            from_rows(r_["at"].at[half], P_BLOCK, 0)
            local(r_["dqkv"].at[half, :, pl.ds(pl.multiple_of(TF * (r - QKV_AT), TF), TF)], db.at[:, pl.ds(0, TF)], db_sem).start()

    def wait_operands(block, r):
        rows, cols = block
        local(r_["hidt"].at[0, pl.ds(0, 8 * rows), :], ab.at[pl.ds(0, 8 * rows), :], ab_sem).wait()

        @pl.when(r >= DOWN_AT)
        def _():
            local(r_["dqkv"].at[0, :, pl.ds(0, cols)], db.at[:, pl.ds(0, cols)], db_sem).wait()

        for which, ref in enumerate((dg, du)):
            @pl.when((r < DOWN_AT) & (r % 2 == which))
            def _():
                db[:, :TF] = ref[r // 2 % 2]

    def optimizer_copies(k, buf, do):
        layer, r = 1 - k // PER_LAYER, k % PER_LAYER
        for name, test, j in _owners(layer, r):
            rows, cols = block = Q_BLOCK if name in ("w_down", "wo") else P_BLOCK

            @pl.when(test)
            def _():
                whole = w_in[name].shape[1] // 8
                down = pl.multiple_of(rows * j if block == Q_BLOCK else 0 * j, 16)
                right = pl.ds(0, cols) if block == Q_BLOCK else pl.ds(pl.multiple_of(cols * j, cols), cols)
                for n, (ref, at, to) in enumerate(((m_in[name], down, mb), (v_in[name], down, vb), (w_in[name], pl.multiple_of(whole * me + down, 16), wb))):
                    do(local(ref.at[layer, pl.ds(at, rows), right], to.at[buf, pl.ds(0, rows), pl.ds(0, cols)], opt_sem.at[buf, n]))


    def save(n, source, to):
        return local(source, to, save_sem.at[n])

    def attend_head(head):
        seen = _visible()
        k_at, turned = column(N_Q + HEAD * head), dq[:, column(N_Q + N_K + HEAD * head)].T

        def scores_of(i):
            q = side(dq, i, head)
            scores = [dot_t(dq[_piece(j), k_at], q) for j in range(i + 1)]
            return [*scores[:i], jnp.where(seen, scores[i], HIDDEN)]

        coming = scores_of(0)
        for i in range(PIECES):
            scores, coming = coming, scores_of(i + 1) if i + 1 < PIECES else None
            top = functools.reduce(jnp.maximum, [s.max(axis=0, keepdims=True) for s in scores])
            total, mix = 0.0, 0.0
            for j, s in enumerate(scores):
                p = jnp.exp2((s - top) * E)
                total = total + p.sum(axis=0, keepdims=True)
                mix = mix + dot(turned[:, _piece(j)], p.astype(BF16))
            out = (mix * (1.0 / total)).astype(BF16)
            lse = top * E + jnp.log(total) * LOG2E
            for n in range(GROUP):
                over = column(HEAD * (GROUP * head + n))
                st[over, _piece(i)] = out[:, _piece(n)]
                oo[_piece(i), over] = out[:, _piece(n)].T
                lseb[head, n : n + 1, _piece(i)] = lse[:, _piece(n)]

    def saves(half):
        kept = lambda name: r_[name].at[half]
        return [
            save(0, ab, kept("bt")), save(1, dq.at[:, pl.ds(0, D)], kept("h1")), save(2, x2, kept("b")),
            save(3, st, kept("ot")), save(4, oo, kept("o")), save(5, lseb, kept("lse")),
        ]

    by_y, by_h = local(r_["dy"], x1, x_sem.at[0]), save(6, x1, r_["h"])

    def forward(layer):
        half = 1 - layer
        weights = qkv_weight_copies(half)
        early = [save(0, ab, r_["at"].at[half]), save(1, dq, r_["qkv"].at[half])]
        for i in range(PIECES):
            wide = x1[_piece(i), :].astype(F32)
            a = (wide * _scale(wide)).astype(BF16)
            ab[:, _piece(i)] = a.T
            cos, sin = cosb[_piece(i), :], sinb[_piece(i), :]
            for c in QKV_ORDER:
                if i == 0:
                    weights[c].wait()
                t = dot(a, (wg, wu)[c // 2][c % 2]).astype(BF16)
                for n in range(2):
                    part = t[:, _piece(n)]
                    if c < 3:
                        p, q = part[:, :HALF].astype(F32), part[:, HALF:].astype(F32)
                        part = jnp.concatenate([p * cos - q * sin, q * cos + p * sin], -1).astype(BF16)
                    dq[_piece(i), TF * c + HEAD * n : TF * c + HEAD * (n + 1)] = part
        wo = local(w_in["wo"].at[layer], db, db_sem)
        start([*early, wo, *tile_copies(half, 0, 0)])
        loop(KV, attend_head)
        wait([*early, wo])
        start(saves(half)[3:])

        @pl.when(layer == 1)
        def _():
            by_h.wait()

        projected = lambda i: dot(oo[_piece(i), :], db[...])
        coming = projected(0)
        for i in range(PIECES):
            rows = _piece(i)
            total, coming = coming, projected(i + 1) if i + 1 < PIECES else None
            h1 = (x1[rows, :].astype(F32) + total.astype(BF16).astype(F32)).astype(BF16)
            dq[rows, :D] = h1
            wide = h1.astype(F32)
            b = (wide * _scale(wide)).astype(BF16)
            x2[rows, :] = b
            ab[:, rows] = b.T
        start(saves(half)[:3])

        @pl.when(layer == 1)
        def _():
            by_y.start()

        @pl.when(layer == 0)
        def _():
            acc[...] = jnp.zeros((T, D), F32)
            coming = qkv_weight_copies(0)

            def one(j):
                buf = j % 2

                @pl.when(j < TILES - 1)
                def _():
                    start(tile_copies(half, j + 1, 1 - buf))

                @pl.when(j == TILES - 1)
                def _():
                    start([coming[c] for c in QKV_ORDER[:2]])

                wait(tile_copies(half, j, buf))
                for i in range(2):
                    rows = slice(T_HALF * i, T_HALF * (i + 1))
                    gate, up = dot(x2[rows, :], wg[buf]), dot(x2[rows, :], wu[buf])
                    hidden = (gate * (1.0 / (1.0 + jnp.exp(-gate))) * up).astype(BF16)
                    acc[rows, :] += dot(hidden, wd[buf])

            loop(TILES, one)
            start([coming[c] for c in QKV_ORDER[2:]])
            wait(saves(half))
            for i in range(PIECES):
                x1[_piece(i), :] = (dq[_piece(i), :D].astype(F32) + acc[_piece(i), :].astype(BF16).astype(F32)).astype(BF16)
            by_h.start()

    first = [local(r_["x"], x1, x_sem.at[0]), local(r_["turns"], tb, o_sem)]
    start([*first, *(qkv_weight_copies(1)[c] for c in QKV_ORDER)])


    barrier = pltpu.get_barrier_semaphore()
    tell(barrier, mate)

    @pl.when(has_above)
    def _():
        tell(barrier, above)

    @pl.when(has_below)
    def _():
        tell(barrier, below)

    wait(first)

    def spin(a):
        rows = pl.ds(pl.multiple_of(STRIDE * a, STRIDE), STRIDE)
        cos_a, sin_a, cos_b, sin_b = tb[0, pl.ds(a, 1), :], tb[1, pl.ds(a, 1), :], tb[2], tb[3]
        cosb[rows, :] = cos_a * cos_b - sin_a * sin_b
        sinb[rows, :] = sin_a * cos_b + cos_a * sin_b

    loop(T // STRIDE, spin)
    loop(2, forward)
    @pl.when(has_above & has_below)
    def _():
        pl.semaphore_wait(barrier, 3)

    @pl.when(jnp.logical_not(has_above & has_below))
    def _():
        pl.semaphore_wait(barrier, 2)

    by_y.wait()

    def tick(n):
        t = n - EARLY
        slot, prev, late = n % SLOTS, (n + SLOTS - 1) % SLOTS, (n + 1) % SLOTS
        two = n % 2


        @pl.when(n >= 3)
        def _():
            pl.semaphore_wait(free_m, 1)

            @pl.when(has_above)
            def _():
                pl.semaphore_wait(free_u, 1)

            @pl.when(has_below)
            def _():
                pl.semaphore_wait(free_d, 1)

            @pl.when(ok(t - 3))
            def _():
                for s in range(CHIPS):
                    remote(ps.at[late, s], pr.at[late, s], ps_s.at[late, s], ps_r.at[late, s], mate).wait_send()

            @pl.when(ok(t - 4 - z))
            def _():
                for s in range(1, CHIPS):
                    @pl.when(s > z)
                    def _():
                        remote(su.at[late, s], ru.at[late, s], su_s.at[late, s], su_r.at[late, s], mate).wait_send()

            @pl.when(ok(t - 4 - (CHIPS - 1 - z)))
            def _():
                for s in range(CHIPS - 1):
                    @pl.when(s < z)
                    def _():
                        remote(sd.at[late, s], rd.at[late, s], sd_s.at[late, s], sd_r.at[late, s], mate).wait_send()

            def gone(s):
                @pl.when(ok(t - 3 - wait_of(s) - jnp.abs(z - s)))
                def _():
                    there = wp.at[0, 0]
                    remote(there, there, am_s.at[late, s], am_r.at[late, s], mate).wait_send()

                    @pl.when((s <= z) & has_above)
                    def _():
                        remote(there, there, au_s.at[late, s], au_r.at[late, s], mate).wait_send()

                    @pl.when((s >= z) & has_below)
                    def _():
                        remote(there, there, ad_s.at[late, s], ad_r.at[late, s], mate).wait_send()

            loop(CHIPS, gone)

            @pl.when(ok(t - 3 - mine))
            def _():
                local(wn.at[late], wp.at[0, 0], out_sem.at[late, 0]).wait()
                local(gn.at[late], gp.at[0], out_sem.at[late, 1]).wait()


        @pl.when(n == EARLY - 1)
        def _():
            wait(saves(0))

        for test, copies in writes(*unit_of(n - 1)):
            pl.when(test & (n > 0))(lambda: wait(copies()))
        fetch(n)

        @pl.when(ok(t + 1 - mine))
        def _():
            optimizer_copies(t + 1 - mine, 1 - two, lambda copy: copy.start())


        @pl.when(ok(t - 1))
        def _():
            for s in (3, 0, 2, 1):
                remote(ps.at[prev, s], pr.at[prev, s], ps_s.at[prev, s], ps_r.at[prev, s], mate).wait_recv()
                value = chip[(t - 1) % SUMS, s] + pr[prev, s].astype(F32)
                chip[(t - 1) % SUMS, s] = value
                if s > 0:
                    @pl.when(z == 0)
                    def _():
                        su[slot, s] = value.astype(BF16)
                        remote(su.at[slot, s], ru.at[slot, s], su_s.at[slot, s], su_r.at[slot, s], above).start()
                if s < CHIPS - 1:
                    @pl.when(z == CHIPS - 1)
                    def _():
                        sd[slot, s] = value.astype(BF16)
                        remote(sd.at[slot, s], rd.at[slot, s], sd_s.at[slot, s], sd_r.at[slot, s], below).start()


        def pass_on(s, k, from_above):
            got, send, here, there, to = (rd, sd, sd_s, sd_r, below) if from_above else (ru, su, su_s, su_r, above)
            remote(send.at[prev, s], got.at[prev, s], here.at[prev, s], there.at[prev, s], mate).wait_recv()
            value = chip[k % SUMS, s] + got[prev, s].astype(F32)
            chip[k % SUMS, s] = value
            send[slot, s] = value.astype(BF16)

            @pl.when((s < z) if from_above else (s > z))
            def _():
                remote(send.at[slot, s], got.at[slot, s], here.at[slot, s], there.at[slot, s], to).start()

        up_k, down_k = t - 1 - z, t - 1 - (CHIPS - 1 - z)
        for i in range(CHIPS - 1):
            @pl.when(has_below & ok(up_k) & (CHIPS - 1 - i >= z))
            def _():
                pass_on(CHIPS - 1 - i, up_k, False)

            @pl.when(has_above & ok(down_k) & (i <= z))
            def _():
                pass_on(i, down_k, True)


        @pl.when(ok(t - mine))
        def _():
            k = t - mine
            optimizer_copies(k, two, lambda copy: copy.wait())
            is_q = _is_q(k % PER_LAYER)
            for (rows, cols), test in ((Q_BLOCK, is_q), (P_BLOCK, jnp.logical_not(is_q))):
                @pl.when(test)
                def _():
                    for j in range(cols // LANES):
                        at, over = slice(rows * j, rows * (j + 1)), slice(LANES * j, LANES * (j + 1))
                        low = chip[k % SUMS, z, at, :].astype(BF16)
                        m, v = _moments(mb[two, :rows, over], vb[two, :rows, over], low.astype(F32))
                        w = wb[two, :rows, over].astype(F32)
                        wn[slot, at, :] = (w - 0.02 * (m * lax.rsqrt(v + 1e-8) + 0.1 * w)).astype(BF16)
                        gn[slot, at, :] = low

            at = _place(k)
            local(wn.at[slot], wp.at[at, me], out_sem.at[slot, 0]).start()
            local(gn.at[slot], gp.at[at], out_sem.at[slot, 1]).start()


        def sends(s, source, there):
            @pl.when((s <= z) & has_above)
            def _():
                remote(source, there, au_s.at[slot, s], au_r.at[slot, s], above).start()

            @pl.when((s >= z) & has_below)
            def _():
                remote(source, there, ad_s.at[slot, s], ad_r.at[slot, s], below).start()

            remote(source, there, am_s.at[slot, s], am_r.at[slot, s], mate).start()

        @pl.when(ok(t - mine))
        def _():
            sends(z, wn.at[slot], wp.at[_place(t - mine), me])


        @pl.when(ok(t))
        def _():
            r = t % PER_LAYER
            is_q = _is_q(r)
            for (rows, cols), test in ((Q_BLOCK, is_q), (P_BLOCK, jnp.logical_not(is_q))):
                @pl.when(test)
                def _():
                    wait_operands((rows, cols), r)
                    for own in range(2):
                        got = dot(ab[4 * rows * own : 4 * rows * (own + 1), :], db[:, :cols])
                        for s in range(CHIPS):
                            for j in range(cols // LANES):
                                piece = got[rows * s : rows * (s + 1), LANES * j : LANES * (j + 1)]
                                if own:
                                    chip[t % SUMS, s, rows * j : rows * (j + 1), :] = piece
                                else:
                                    ps[slot, s, rows * j : rows * (j + 1), :] = piece.astype(BF16)
                        if not own:
                            for s in (3, 0, 2, 1):
                                remote(ps.at[slot, s], pr.at[slot, s], ps_s.at[slot, s], ps_r.at[slot, s], mate).start()

        @pl.when(ok(t + 1))
        def _():
            load_operands(t + 1)

        work(n)


        def spread(s):
            k = t - wait_of(s) - jnp.abs(z - s)

            @pl.when(ok(k) & (s != z))
            def _():
                there = wp.at[_place(k), 2 * s + core]

                @pl.when(s < z)
                def _():
                    remote(there, there, au_s.at[prev, s], au_r.at[prev, s], mate).wait_recv()

                @pl.when(s > z)
                def _():
                    remote(there, there, ad_s.at[prev, s], ad_r.at[prev, s], mate).wait_recv()

                sends(s, there, there)

        loop(CHIPS, spread)


        def arrived(s):
            @pl.when(ok(t - 1 - wait_of(s) - jnp.abs(z - s)))
            def _():
                there = wp.at[0, 0]
                remote(there, there, am_s.at[prev, s], am_r.at[prev, s], mate).wait_recv()

        loop(CHIPS, arrived)

        @pl.when(n < TICKS - 3)
        def _():
            tell(free_m, mate)

            @pl.when(has_above)
            def _():
                tell(free_d, above)

            @pl.when(has_below)
            def _():
                tell(free_u, below)

    loop(TICKS, tick)


def update(given, w, m, v):
    vm, sem = pltpu.VMEM, pltpu.SemaphoreType
    block, wide = (BLOCK, LANES), N_Q + 2 * N_K
    scratch = [
        vm((D, T), BF16), vm((T, D), BF16), vm((SUMS, CHIPS, *block), F32),
        *(vm((SLOTS, CHIPS, *block), BF16) for _ in range(6)),
        vm((SLOTS, *block), BF16), vm((SLOTS, *block), BF16),
        *(vm((2, P_BLOCK[0], D), dtype) for dtype in (F32, F32, BF16)),
        vm((T, D), BF16), vm((T, D), BF16), vm((T, N_Q), BF16),
        vm((2, D, TF), BF16), vm((2, D, TF), BF16), vm((2, TF, D), BF16), vm((T, D), F32),
        vm((2, T, TF), BF16), vm((2, T, TF), BF16), vm((TF, TF), BF16),
        vm((T, GROUP * HEAD), BF16), vm((T, HEAD), BF16), vm((T, HEAD), BF16), vm((T, wide), BF16), vm((N_Q, T), BF16),
        vm((T, HALF), F32), vm((T, HALF), F32), vm((KV, GROUP, T), F32), vm((KV, GROUP, T), F32), vm((4, STRIDE, HALF), F32),
        sem.DMA, sem.DMA, *(sem.DMA(shape) for shape in ((2, 3), (SLOTS, 2), (2, 3), (2,))), sem.DMA, sem.DMA((3,)), sem.DMA, sem.DMA((2,)), sem.DMA((7,)),
        *(sem.DMA((SLOTS, CHIPS)) for _ in range(12)),
        sem.REGULAR, sem.REGULAR, sem.REGULAR,
    ]
    refs = [*w, *m, *v, *(given[name] for name in INPUTS)]
    pair = [(FF, T), (T, D), (T, wide), (D, T), (N_Q, T), (D, T), (T, D), (T, D), (T, N_Q), (T, wide)]
    shapes = [(CHUNKS, 8, *block), (CHUNKS, *block), *((2, *shape) for shape in pair)]
    outs = [*((shape, BF16) for shape in shapes), ((2, KV, GROUP, T), F32), ((T, D), BF16), ((T, D), BF16)]
    return pl.pallas_call(
        _update,
        in_specs=[pl.BlockSpec(memory_space=pl.ANY)] * len(refs),
        out_specs=[pl.BlockSpec(memory_space=pl.ANY)] * len(outs),
        out_shape=[jax.ShapeDtypeStruct(*out) for out in outs],
        scratch_shapes=scratch,
        compiler_params=pltpu.CompilerParams(collective_id=0, has_side_effects=True, vmem_limit_bytes=63 * 2**20),
        name="update",
    )(*refs)[:2]


def _moments(m, v, g):
    return 0.9 * m + 0.1 * g, 0.95 * v + 0.05 * g * g


def _unpack(*refs):
    s = pl.program_id(1)
    ins, outs = refs[: 4 * len(NAMES)], refs[4 * len(NAMES) :]
    for i, name in enumerate(NAMES):
        wp_ref, gp_ref, m_ref, v_ref = ins[4 * i : 4 * i + 4]
        w_out, m_out, v_out = outs[i :: len(NAMES)]
        tall = name in ("w_down", "wo")
        rows, cols = Q_BLOCK if tall else P_BLOCK
        some = m_ref.shape[1]
        for j in range(cols // LANES):
            for n in range(wp_ref.shape[0]):
                over = slice(LANES * j, LANES * (j + 1)) if tall else slice(cols * n + LANES * j, cols * n + LANES * (j + 1))
                down = slice(rows * n, rows * (n + 1)) if tall else slice(0, rows)
                w_out[0, down, over] = wp_ref[n, 0, rows * j : rows * (j + 1), :]
                if tall and n:
                    continue
                if tall:
                    per = rows // some
                    g = gp_ref[s // per if name == "wo" else jnp.minimum(s, 6), pl.ds(pl.multiple_of(rows * j + some * (s % per), 16), some), :]
                else:
                    g = gp_ref[n, pl.ds(pl.multiple_of(rows * j + some * jnp.minimum(s, 6), 16), some), :]
                m_out[0, :, over], v_out[0, :, over] = _moments(m_ref[0, :, over], v_ref[0, :, over], g.astype(F32))


def unpack(wp, gp, m, v):
    block = (BLOCK, LANES)
    where = {"wq": (2, 22, 3), "wk": (1, 46, 6), "wv": (1, 47, 6), "wo": (2, 21, 3), "w_gate": (7, 0, 1), "w_up": (7, 2, 1), "w_down": (7, 4, 1)}
    in_specs, given, full, own = [], [], [], []
    for name in NAMES:
        count, start, step = where[name]
        _, height, width = m[name].shape
        some = 64 if name == "w_down" else 16
        last = height // some - 1
        mine = pl.BlockSpec((1, some, width), lambda layer, s, last=last: (layer, jnp.minimum(s, last), 0))
        in_specs += [
            pl.BlockSpec((count, 1, *block), lambda layer, s, start=start, step=step: (start + step * layer, s, 0, 0)),
            pl.BlockSpec((count, *block), lambda layer, s, start=start, step=step: (start + step * layer, 0, 0)), mine, mine,
        ]
        given += [wp, gp, m[name], v[name]]
        full.append((pl.BlockSpec((1, height, width), lambda layer, s: (layer, s, 0)), jax.ShapeDtypeStruct((2, 8 * height, width), BF16)))
        own.append((mine, jax.ShapeDtypeStruct(m[name].shape, F32)))
    outs = full + own + own
    return pl.pallas_call(
        _unpack,
        grid=(2, 8),
        in_specs=in_specs,
        out_specs=[o[0] for o in outs],
        out_shape=[o[1] for o in outs],
        compiler_params=pltpu.CompilerParams(vmem_limit_bytes=VMEM),
        name="unpack",
    )(*given)


def solution(mesh):
    angle = np.arange(STRIDE)[:, None] * float(THETA) ** (-np.arange(HALF) / HALF)
    turns = np.stack([turn(angle * step) for step in (STRIDE, 1) for turn in (np.cos, np.sin)]).astype(np.float32)

    def step(x, dy, *arrays):
        w, m, v = (dict(zip(NAMES, arrays[i : i + 7], strict=True)) for i in (0, 7, 14))
        wp, gp = update({"x": x[0], "dy": dy[0], "turns": jnp.asarray(turns)}, w.values(), m.values(), v.values())
        return tuple(unpack(wp, gp, m, v))

    states, all_of, cut = P(("rep", "dp"), None, None), P(None, None, None), P(None, "dp", None)
    return jax.shard_map(
        step,
        mesh=mesh,
        in_specs=(states, states) + (all_of,) * 7 + (cut,) * 14,
        out_specs=(P("rep", None, None),) * 7 + (P("rep", "dp", None),) * 14,
        check_vma=False,
    )
```

```python
import functools

import jax
import jax.numpy as jnp
import numpy as np
from jax import lax
from jax.experimental import pallas as pl
from jax.experimental.pallas import tpu as pltpu
from jax.sharding import PartitionSpec as P

LOG2E = 1.4426950408889634
HIDDEN = -2e30
VMEM = 56 * 2**20
F32, BF16 = jnp.float32, jnp.bfloat16
MESH = pl.DeviceIdType.MESH
T, D, FF, HEADS, KV, HEAD = 1024, 896, 3584, 4, 2, 256
THETA = 10000
STRIDE = 32
NAMES = ("wq", "wk", "wv", "wo", "w_gate", "w_up", "w_down")
ROWS = 256
TF = 512
PIECES = T // ROWS


def loop(count, body):
    lax.fori_loop(0, count, lambda i, _: body(i), None)


def dot(a, b):
    return jnp.dot(a, b, preferred_element_type=F32)


def dot_t(a, b):
    return lax.dot_general(a, b, (((1,), (1,)), ((), ())), preferred_element_type=F32)


def _scale(wide):
    return lax.rsqrt(jnp.mean(wide * wide, -1, keepdims=True) + 1e-6)


def _norm_back(h, by):
    s = _scale(h)
    return by * s - h * (s * s * s * jnp.mean(by * h, -1, keepdims=True))


E = HEAD**-0.5 * LOG2E
GROUP = HEADS // KV


def part_of(i, size):
    return slice(size * i, size * (i + 1))


def _piece(i):
    return part_of(i, ROWS)


def _visible():
    shape = (ROWS, GROUP * ROWS)
    return lax.broadcasted_iota(jnp.int32, shape, 0) <= lax.rem(lax.broadcasted_iota(jnp.int32, shape, 1), ROWS)


LANES = 128
BLOCK = 448
SLOTS = 4
SUMS = 5
EARLY = 2
LAG = 27
P_BLOCK, Q_BLOCK = (112, 512), (64, 896)
TILES = FF // TF
DOWN_AT, WO_AT, QKV_AT, PER_LAYER = 14, 21, 23, 27
CHUNKS = 2 * PER_LAYER
SPREAD = CHUNKS - 2
TICKS = CHUNKS + 9 + EARLY
CHIPS = 4
MATE_ORDER = (3, 0, 2, 1)
QKV_ORDER = (1, 3, 0, 2)
HALF, T_HALF = HEAD // 2, T // 2
N_Q, N_K = HEADS * HEAD, KV * HEAD
BEFORE, LEAVE, HEADS_AT, AFTER = 12, 13, 14, 17


def _is_q(r):
    return (r >= DOWN_AT) & (r < QKV_AT)


def _place(k):
    layer, r = 1 - k // PER_LAYER, k % PER_LAYER
    double, single = (r % 2) * DOWN_AT + layer * TILES + r // 2, 2 * DOWN_AT + layer * TILES + r - DOWN_AT
    return jnp.where(r < DOWN_AT, double, jnp.where(r < WO_AT, single, 3 * DOWN_AT + layer * (PER_LAYER - WO_AT) + r - WO_AT))


def _owners(layer, r):
    mlp_chunk = r < DOWN_AT
    return (
        ("w_gate", mlp_chunk & (r % 2 == 0), r // 2), ("w_up", mlp_chunk & (r % 2 == 1), r // 2),
        ("w_down", (r >= DOWN_AT) & (r < WO_AT), r - DOWN_AT), ("wo", (r >= WO_AT) & (r < QKV_AT), r - WO_AT),
        ("wq", (r >= QKV_AT) & (r < QKV_AT + 2), r - QKV_AT), ("wk", r == QKV_AT + 2, 0 * r), ("wv", r == QKV_AT + 3, 0 * r),
    )


INPUTS = ("x", "dy", "turns")
OUTPUTS = ("wp", "gp", "last", "hidt", "d1", "dqkv", "at", "ot", "bt", "b", "h1", "o", "qkv", "lse", "h", "by1")
SCRATCH = ("ab", "db", "chip", "ps", "pr", "su", "ru", "sd", "rd", "wn", "gn", "mb", "vb", "wb", "x1", "x2", "oo", "wg", "wu", "wd", "acc", "dg", "du", "ht",
           "qq", "kk", "vv", "dq", "st", "cosb", "sinb", "lseb", "delta", "tb",
           "ab_sem", "db_sem", "opt_sem", "out_sem", "tile_sem", "x_sem", "o_sem", "qkv_sem", "lse_sem", "write_sem", "save_sem",
           "ps_s", "ps_r", "su_s", "su_r", "sd_s", "sd_r", "am_s", "am_r", "au_s", "au_r", "ad_s", "ad_r", "free_m", "free_u", "free_d")


def _update(*refs):
    count = len(NAMES)
    w_in, m_in, v_in = (dict(zip(NAMES, some)) for some in (refs[:count], refs[count : 2 * count], refs[2 * count :]))
    r_ = dict(zip((*INPUTS, *OUTPUTS, *SCRATCH), refs[3 * count :], strict=True))
    (ab, db, chip, ps, pr, su, ru, sd, rd, wn, gn, mb, vb, wb, x1, x2, oo, wg, wu, wd, acc, dg, du, ht, qq, kk, vv, dq, st, cosb, sinb, lseb, delta, tb,
     ab_sem, db_sem, opt_sem, out_sem, tile_sem, x_sem, o_sem, qkv_sem, lse_sem, write_sem, save_sem,
     ps_s, ps_r, su_s, su_r, sd_s, sd_r, am_s, am_r, au_s, au_r, ad_s, ad_r, free_m, free_u, free_d) = (r_[name] for name in SCRATCH)
    wp, gp = r_["wp"], r_["gp"]
    any_block = wp.at[0, 0]
    rep, me = lax.axis_index("rep"), lax.axis_index("dp")
    z, core = me // 2, me % 2
    mate, above, below = me + 1 - 2 * core, me + 2, me - 2
    has_above, has_below = z < CHIPS - 1, z > 0

    def remote(src, dst, send, recv, to):
        return pltpu.make_async_remote_copy(src_ref=src, dst_ref=dst, send_sem=send, recv_sem=recv, device_id=(rep, to), device_id_type=MESH)

    def tell(sem, to):
        pl.semaphore_signal(sem, inc=1, device_id=(rep, to), device_id_type=MESH)

    def local(src, dst, sem):
        return pltpu.make_async_copy(src, dst, sem)

    def ok(k):
        return (k >= 0) & (k < CHUNKS)

    def spread_here(k):
        return (k >= 0) & (k < SPREAD)

    def wait_of(s):
        return 3 + ((s == 0) | (s == CHIPS - 1)).astype(jnp.int32)

    mine = wait_of(z)

    def tokens(start, count):
        return pl.ds(pl.multiple_of(start, ROWS), count)


    def tile_copies(half, j, buf):
        layer, over = 1 - half, pl.ds(pl.multiple_of(TF * j, TF), TF)
        return [
            local(w_in["w_gate"].at[layer, :, over], wg.at[buf], tile_sem.at[buf, 0]),
            local(w_in["w_up"].at[layer, :, over], wu.at[buf], tile_sem.at[buf, 1]),
            local(w_in["w_down"].at[layer, over, :], wd.at[buf], tile_sem.at[buf, 2]),
        ]

    def wo_copies(half):
        return [local(w_in["wo"].at[1 - half, pl.ds(TF * n, TF), :], wd.at[n], tile_sem.at[n, 2]) for n in range(2)]

    def qkv_weight_copies(half):
        layer = 1 - half
        return [
            *(local(w_in["wq"].at[layer, :, pl.ds(TF * n, TF)], wg.at[n], tile_sem.at[n, 0]) for n in range(2)),
            local(w_in["wk"].at[layer], wu.at[0], tile_sem.at[0, 1]), local(w_in["wv"].at[layer], wu.at[1], tile_sem.at[1, 1]),
        ]

    def column(at):
        return pl.ds(pl.multiple_of(at, HEAD), HEAD)

    def head_copies(half, head):
        pair = pl.ds(pl.multiple_of(GROUP * HEAD * head, GROUP * HEAD), GROUP * HEAD)
        return [
            local(r_["qkv"].at[half, :, over], to, qkv_sem.at[n])
            for n, (over, to) in enumerate(((pair, qq), (column(N_Q + HEAD * head), kk), (column(N_Q + N_K + HEAD * head), vv)))
        ]

    def load_x2(ref):
        return local(ref, x2, x_sem.at[1])

    def unit_of(n):
        half = (n >= AFTER + 2 + EARLY).astype(jnp.int32)
        return half, n - EARLY - LAG * half

    def start(copies):
        for copy in copies:
            copy.start()

    def wait(copies):
        for copy in copies:
            copy.wait()

    def writes(half, tau):
        u = tau + EARLY
        j, first = u // 2, tokens(T_HALF * (u % 2), T_HALF)
        over = pl.ds(pl.multiple_of(TF * j, TF), TF)
        part = tokens(T_HALF * (tau - AFTER), T_HALF)
        after_at = (tau >= AFTER) & (tau < AFTER + 2)
        return (
            ((u >= 0) & (u < 2 * TILES), lambda: [local(ht, r_["hidt"].at[half, over, first], write_sem.at[0])]),
            (tau == LEAVE, lambda: [local(x1, r_["d1"].at[half], write_sem.at[0])]),
            (after_at, lambda: [local(dq.at[part, :], r_["dqkv"].at[half, part, :], write_sem.at[0])]),
            (after_at & (half == 0), lambda: [local(x1.at[part, :], r_["by1"].at[part, :], write_sem.at[1])]),
        )

    def fetch(n):
        half, tau = unit_of(n)
        u = tau + EARLY

        @pl.when((tau == -EARLY - 1) & (half == 1))
        def _():
            start([*tile_copies(half, 0, 0), load_x2(r_["b"].at[half])])

        @pl.when((u >= 0) & (u % 2 == 0) & (u < 2 * TILES - 2))
        def _():
            start(tile_copies(half, u // 2 + 1, (u // 2 + 1) % 2))

        @pl.when(tau == BEFORE)
        def _():
            start([*wo_copies(half), load_x2(r_["h1"].at[half]), local(r_["o"].at[half], oo, o_sem)])

        @pl.when(tau == LEAVE)
        def _():
            start([*head_copies(half, 0), local(r_["lse"].at[half], lseb, lse_sem)])

        @pl.when(tau == HEADS_AT + 1)
        def _():
            start(head_copies(half, 1))

        @pl.when((tau == BEFORE) & (half == 0))
        def _():
            start(tile_copies(0, 0, 0)[:2])

        @pl.when((tau == LEAVE) & (half == 0))
        def _():
            start(qkv_weight_copies(0))

        @pl.when((tau == HEADS_AT) & (half == 0))
        def _():
            start([load_x2(r_["h"])])

    def mlp_unit(u, buf, later):
        rows = tokens(T_HALF * (u % 2), T_HALF)
        gate, up = dot(x2[rows, :], wg[buf]), dot(x2[rows, :], wu[buf])
        sig = 1.0 / (1.0 + jnp.exp(-gate))
        silu = gate * sig
        by = dot_t(x1[rows, :], wd[buf]).astype(BF16).astype(F32)
        ht[...] = (silu * up).astype(BF16).T
        du[buf, rows, :] = (by * silu).astype(BF16)
        dg[buf, rows, :] = (by * up * (sig * (1.0 + gate * (1.0 - sig)))).astype(BF16)

        @pl.when(jnp.logical_not(later))
        def _():
            acc[rows, :] += dot_t(dg[buf, rows, :], wg[buf]) + dot_t(du[buf, rows, :], wu[buf])

    def late_unit(i):
        rows = tokens(ROWS * i, ROWS)
        acc[rows, :] += dot_t(st[rows, :TF], wg[0]) + dot_t(st[rows, TF:], wu[0])

    def leave_unit(i):
        rows = tokens(ROWS * i, ROWS)
        inner = _norm_back(x2[rows, :].astype(F32), acc[rows, :].astype(BF16).astype(F32)).astype(BF16)
        d1 = (x1[rows, :].astype(F32) + inner.astype(F32)).astype(BF16)
        x1[rows, :] = d1
        for n in range(HEADS):
            low, over = HEAD * (n % 2), _piece(n)
            do = dot_t(d1, wd[n // 2, low : low + HEAD, :]).astype(BF16)
            both = do.astype(F32) * oo[rows, over].astype(F32)
            oo[rows, over] = do
            delta[n // GROUP, n % GROUP : n % GROUP + 1, rows] = both.T.sum(0, keepdims=True)

    def side(ref, i, head):
        return jnp.concatenate([ref[_piece(i), column(HEAD * (GROUP * head + n))] for n in range(GROUP)], axis=0)

    def turn_back(part, rows):
        cos, sin = cosb[rows, :], sinb[rows, :]
        x, y = part[:, :HALF].astype(F32), part[:, HALF:].astype(F32)
        return jnp.concatenate([x * cos + y * sin, y * cos - x * sin], -1).astype(BF16)

    def head_unit(head):
        seen = _visible()
        turned = kk[...].T
        line = lambda ref, i: jnp.concatenate([ref[head, n : n + 1, _piece(i)] for n in range(GROUP)], axis=1)
        dk_at, dv_at = slice(0, HEAD), slice(HEAD, 2 * HEAD)
        for i in range(PIECES):
            lse, dl = line(lseb, i), line(delta, i)
            q = jnp.concatenate([qq[_piece(i), _piece(n)] for n in range(GROUP)], axis=0)
            do = side(oo, i, head)
            by_q = 0.0
            for j in range(i + 1):
                at = _piece(j)
                p = jnp.exp2(dot_t(kk[at, :], q) * E - lse)
                if j == i:
                    p = jnp.where(seen, p, 0.0)
                ds = (p * (dot_t(vv[at, :], do) - dl)).astype(BF16)
                by_v, by_k = dot(p.astype(BF16), do), dot(ds, q)
                acc[at, dv_at] = by_v if j == i else acc[at, dv_at] + by_v
                acc[at, dk_at] = by_k if j == i else acc[at, dk_at] + by_k
                by_q = by_q + dot(turned[:, at], ds)
            by_q = (by_q * HEAD**-0.5).astype(BF16)
            for n in range(GROUP):
                dq[_piece(i), column(HEAD * (GROUP * head + n))] = turn_back(by_q[:, _piece(n)].T, _piece(i))
        for i in range(PIECES):
            dq[_piece(i), column(N_Q + HEAD * head)] = turn_back((acc[_piece(i), dk_at] * HEAD**-0.5).astype(BF16), _piece(i))
            dq[_piece(i), column(N_Q + N_K + HEAD * head)] = acc[_piece(i), dv_at].astype(BF16)

    def after_unit(rows):
        by = sum(dot_t(dq[rows, part_of(n, TF)], (wg, wu)[n // 2][n % 2]) for n in range(4)).astype(BF16).astype(F32)
        inner = _norm_back(x2[rows, :].astype(F32), by).astype(BF16)
        x1[rows, :] = (x1[rows, :].astype(F32) + inner.astype(F32)).astype(BF16)

    def work(n):
        half, tau = unit_of(n)
        u = tau + EARLY

        @pl.when((u >= 0) & (u < 2 * TILES))
        def _():
            buf = u // 2 % 2

            @pl.when(u % 2 == 0)
            def _():
                wait(tile_copies(half, u // 2, buf))

            @pl.when(u == 0)
            def _():
                acc[...] = jnp.zeros((T, D), F32)

                @pl.when(half == 1)
                def _():
                    load_x2(r_["h"]).wait()

            mlp_unit(u, buf, (half == 0) & (u < 2))

            @pl.when((half == 0) & (u == 1))
            def _():
                st[:, :TF] = dg[0]
                st[:, TF:] = du[0]

        @pl.when((tau == BEFORE) & (half == 0))
        def _():
            wait(tile_copies(0, 0, 0)[:2])
            loop(PIECES, late_unit)

        @pl.when(tau == LEAVE)
        def _():
            wait([load_x2(r_["h"]), local(r_["o"].at[0], oo, o_sem), *wo_copies(half)])
            loop(PIECES, leave_unit)

        @pl.when((tau == HEADS_AT) | (tau == HEADS_AT + 2))
        def _():
            @pl.when(tau == HEADS_AT)
            def _():
                local(r_["lse"].at[0], lseb, lse_sem).wait()

            wait(head_copies(0, 0))
            head_unit((tau - HEADS_AT) // 2)

        @pl.when((tau >= AFTER) & (tau < AFTER + 2) & (half == 0))
        def _():
            @pl.when(tau == AFTER)
            def _():
                wait([load_x2(r_["h"]), *qkv_weight_copies(0)])

            loop(PIECES // 2, lambda i: after_unit(tokens(T_HALF * (tau - AFTER) + ROWS * i, ROWS)))

        for test, copies in writes(half, tau):
            pl.when(test)(lambda: start(copies()))


    def load_operands(k):
        half, r = k // PER_LAYER, k % PER_LAYER

        def from_rows(ref, block, down):
            rows, whole = block[0], ref.shape[0] // 8
            for e in range(8):
                owner = 2 * (e % 4) + (1 - core if e < 4 else core)
                at = pl.multiple_of(whole * owner + down, 16)
                local(ref.at[pl.ds(at, rows), :], ab.at[pl.ds(rows * e, rows), :], ab_sem).start()

        @pl.when(r < DOWN_AT)
        def _():
            from_rows(r_["bt"].at[half], P_BLOCK, 0)

        @pl.when((r >= DOWN_AT) & (r < WO_AT))
        def _():
            from_rows(r_["hidt"].at[half], Q_BLOCK, Q_BLOCK[0] * (r - DOWN_AT))

            @pl.when(half == 0)
            def _():
                local(r_["dy"], db, db_sem).start()

            @pl.when(half == 1)
            def _():
                local(r_["by1"], db, db_sem).start()

        @pl.when((r >= WO_AT) & (r < QKV_AT))
        def _():
            from_rows(r_["ot"].at[half], Q_BLOCK, Q_BLOCK[0] * (r - WO_AT))
            local(r_["d1"].at[half], db, db_sem).start()

        @pl.when(r >= QKV_AT)
        def _():
            from_rows(r_["at"].at[half], P_BLOCK, 0)
            local(r_["dqkv"].at[half, :, pl.ds(pl.multiple_of(TF * (r - QKV_AT), TF), TF)], db.at[:, pl.ds(0, TF)], db_sem).start()

    def wait_operands(block, r):
        rows, cols = block
        local(r_["hidt"].at[0, pl.ds(0, 8 * rows), :], ab.at[pl.ds(0, 8 * rows), :], ab_sem).wait()

        @pl.when(r >= DOWN_AT)
        def _():
            local(r_["dqkv"].at[0, :, pl.ds(0, cols)], db.at[:, pl.ds(0, cols)], db_sem).wait()

        for which, ref in enumerate((dg, du)):
            @pl.when((r < DOWN_AT) & (r % 2 == which))
            def _():
                db[:, :TF] = ref[r // 2 % 2]

    def optimizer_copies(k, buf, do):
        layer, r = 1 - k // PER_LAYER, k % PER_LAYER
        for name, test, j in _owners(layer, r):
            rows, cols = block = Q_BLOCK if name in ("w_down", "wo") else P_BLOCK

            @pl.when(test)
            def _():
                whole = w_in[name].shape[1] // 8
                down = pl.multiple_of(rows * j if block == Q_BLOCK else 0 * j, 16)
                right = pl.ds(0, cols) if block == Q_BLOCK else pl.ds(pl.multiple_of(cols * j, cols), cols)
                for n, (ref, at, to) in enumerate(((m_in[name], down, mb), (v_in[name], down, vb), (w_in[name], pl.multiple_of(whole * me + down, 16), wb))):
                    do(local(ref.at[layer, pl.ds(at, rows), right], to.at[buf, pl.ds(0, rows), pl.ds(0, cols)], opt_sem.at[buf, n]))


    def save(n, source, to):
        return local(source, to, save_sem.at[n])

    def attend_head(head):
        seen = _visible()
        k_at, turned = column(N_Q + HEAD * head), dq[:, column(N_Q + N_K + HEAD * head)].T

        def scores_of(i):
            q = side(dq, i, head)
            scores = [dot_t(dq[_piece(j), k_at], q) for j in range(i + 1)]
            return [*scores[:i], jnp.where(seen, scores[i], HIDDEN)]

        coming = scores_of(0)
        for i in range(PIECES):
            scores, coming = coming, scores_of(i + 1) if i + 1 < PIECES else None
            top = functools.reduce(jnp.maximum, [s.max(axis=0, keepdims=True) for s in scores])
            total, mix = 0.0, 0.0
            for j, s in enumerate(scores):
                p = jnp.exp2((s - top) * E)
                total = total + p.sum(axis=0, keepdims=True)
                mix = mix + dot(turned[:, _piece(j)], p.astype(BF16))
            out = (mix * (1.0 / total)).astype(BF16)
            lse = top * E + jnp.log(total) * LOG2E
            for n in range(GROUP):
                over = column(HEAD * (GROUP * head + n))
                st[over, _piece(i)] = out[:, _piece(n)]
                oo[_piece(i), over] = out[:, _piece(n)].T
                lseb[head, n : n + 1, _piece(i)] = lse[:, _piece(n)]

    def saves(half):
        kept = lambda name: r_[name].at[half]
        return [
            save(0, ab, kept("bt")), save(1, dq.at[:, pl.ds(0, D)], kept("h1")), save(2, x2, kept("b")),
            save(3, st, kept("ot")), save(4, oo, kept("o")), save(5, lseb, kept("lse")),
        ]

    by_y, by_h = local(r_["dy"], x1, x_sem.at[0]), save(6, x1, r_["h"])

    def forward(layer):
        half = 1 - layer
        weights = qkv_weight_copies(half)
        early = [save(0, ab, r_["at"].at[half]), save(1, dq, r_["qkv"].at[half])]
        for i in range(PIECES):
            wide = x1[_piece(i), :].astype(F32)
            a = (wide * _scale(wide)).astype(BF16)
            ab[:, _piece(i)] = a.T
            cos, sin = cosb[_piece(i), :], sinb[_piece(i), :]
            for c in QKV_ORDER:
                if i == 0:
                    weights[c].wait()
                t = dot(a, (wg, wu)[c // 2][c % 2]).astype(BF16)
                for n in range(2):
                    part = t[:, _piece(n)]
                    if c < 3:
                        p, q = part[:, :HALF].astype(F32), part[:, HALF:].astype(F32)
                        part = jnp.concatenate([p * cos - q * sin, q * cos + p * sin], -1).astype(BF16)
                    dq[_piece(i), TF * c + HEAD * n : TF * c + HEAD * (n + 1)] = part
        wo = local(w_in["wo"].at[layer], db, db_sem)
        start([*early, wo, *tile_copies(half, 0, 0)])
        loop(KV, attend_head)
        wait([*early, wo])
        start(saves(half)[3:])

        @pl.when(layer == 1)
        def _():
            by_h.wait()

        projected = lambda i: dot(oo[_piece(i), :], db[...])
        coming = projected(0)
        for i in range(PIECES):
            rows = _piece(i)
            total, coming = coming, projected(i + 1) if i + 1 < PIECES else None
            h1 = (x1[rows, :].astype(F32) + total.astype(BF16).astype(F32)).astype(BF16)
            dq[rows, :D] = h1
            wide = h1.astype(F32)
            b = (wide * _scale(wide)).astype(BF16)
            x2[rows, :] = b
            ab[:, rows] = b.T
        start(saves(half)[:3])

        @pl.when(layer == 1)
        def _():
            by_y.start()

        @pl.when(layer == 0)
        def _():
            acc[...] = jnp.zeros((T, D), F32)
            coming = qkv_weight_copies(0)

            def one(j):
                buf = j % 2

                @pl.when(j < TILES - 1)
                def _():
                    start(tile_copies(half, j + 1, 1 - buf))

                @pl.when(j == TILES - 1)
                def _():
                    start([coming[c] for c in QKV_ORDER[:2]])

                wait(tile_copies(half, j, buf))
                for i in range(2):
                    rows = part_of(i, T_HALF)
                    gate, up = dot(x2[rows, :], wg[buf]), dot(x2[rows, :], wu[buf])
                    hidden = (gate * (1.0 / (1.0 + jnp.exp(-gate))) * up).astype(BF16)
                    acc[rows, :] += dot(hidden, wd[buf])

            loop(TILES, one)
            start([coming[c] for c in QKV_ORDER[2:]])
            wait(saves(half))
            for i in range(PIECES):
                x1[_piece(i), :] = (dq[_piece(i), :D].astype(F32) + acc[_piece(i), :].astype(BF16).astype(F32)).astype(BF16)
            by_h.start()

    first = [local(r_["x"], x1, x_sem.at[0]), local(r_["turns"], tb, o_sem)]
    start([*first, *(qkv_weight_copies(1)[c] for c in QKV_ORDER)])


    barrier = pltpu.get_barrier_semaphore()
    tell(barrier, mate)

    @pl.when(has_above)
    def _():
        tell(barrier, above)

    @pl.when(has_below)
    def _():
        tell(barrier, below)

    wait(first)

    def spin(a):
        rows = pl.ds(pl.multiple_of(STRIDE * a, STRIDE), STRIDE)
        cos_a, sin_a, cos_b, sin_b = tb[0, pl.ds(a, 1), :], tb[1, pl.ds(a, 1), :], tb[2], tb[3]
        cosb[rows, :] = cos_a * cos_b - sin_a * sin_b
        sinb[rows, :] = sin_a * cos_b + cos_a * sin_b

    loop(T // STRIDE, spin)
    loop(2, forward)
    @pl.when(has_above & has_below)
    def _():
        pl.semaphore_wait(barrier, 3)

    @pl.when(jnp.logical_not(has_above & has_below))
    def _():
        pl.semaphore_wait(barrier, 2)

    by_y.wait()

    def tick(n):
        t = n - EARLY
        slot, prev, late = n % SLOTS, (n + SLOTS - 1) % SLOTS, (n + 1) % SLOTS
        two = n % 2


        @pl.when(n >= 3)
        def _():
            pl.semaphore_wait(free_m, 1)

            @pl.when(has_above)
            def _():
                pl.semaphore_wait(free_u, 1)

            @pl.when(has_below)
            def _():
                pl.semaphore_wait(free_d, 1)

            @pl.when(ok(t - 3))
            def _():
                for s in range(CHIPS):
                    remote(ps.at[late, s], pr.at[late, s], ps_s.at[late, s], ps_r.at[late, s], mate).wait_send()

            @pl.when(ok(t - 4 - z))
            def _():
                for s in range(1, CHIPS):
                    @pl.when(s > z)
                    def _():
                        remote(su.at[late, s], ru.at[late, s], su_s.at[late, s], su_r.at[late, s], mate).wait_send()

            @pl.when(ok(t - 4 - (CHIPS - 1 - z)))
            def _():
                for s in range(CHIPS - 1):
                    @pl.when(s < z)
                    def _():
                        remote(sd.at[late, s], rd.at[late, s], sd_s.at[late, s], sd_r.at[late, s], mate).wait_send()

            def gone(s):
                @pl.when(spread_here(t - 3 - wait_of(s) - jnp.abs(z - s)))
                def _():
                    there = any_block
                    remote(there, there, am_s.at[late, s], am_r.at[late, s], mate).wait_send()

                    @pl.when((s <= z) & has_above)
                    def _():
                        remote(there, there, au_s.at[late, s], au_r.at[late, s], mate).wait_send()

                    @pl.when((s >= z) & has_below)
                    def _():
                        remote(there, there, ad_s.at[late, s], ad_r.at[late, s], mate).wait_send()

            loop(CHIPS, gone)

            @pl.when(ok(t - 3 - mine))
            def _():
                local(wn.at[late], any_block, out_sem.at[late, 0]).wait()
                local(gn.at[late], gp.at[0], out_sem.at[late, 1]).wait()


        @pl.when(n == EARLY - 1)
        def _():
            wait(saves(0))

        for test, copies in writes(*unit_of(n - 1)):
            pl.when(test & (n > 0))(lambda: wait(copies()))
        fetch(n)

        @pl.when(ok(t + 1 - mine))
        def _():
            optimizer_copies(t + 1 - mine, 1 - two, lambda copy: copy.start())


        @pl.when(ok(t - 1))
        def _():
            for s in MATE_ORDER:
                remote(ps.at[prev, s], pr.at[prev, s], ps_s.at[prev, s], ps_r.at[prev, s], mate).wait_recv()
                value = chip[(t - 1) % SUMS, s] + pr[prev, s].astype(F32)
                chip[(t - 1) % SUMS, s] = value
                if s > 0:
                    @pl.when(z == 0)
                    def _():
                        su[slot, s] = value.astype(BF16)
                        remote(su.at[slot, s], ru.at[slot, s], su_s.at[slot, s], su_r.at[slot, s], above).start()
                if s < CHIPS - 1:
                    @pl.when(z == CHIPS - 1)
                    def _():
                        sd[slot, s] = value.astype(BF16)
                        remote(sd.at[slot, s], rd.at[slot, s], sd_s.at[slot, s], sd_r.at[slot, s], below).start()


        def pass_on(s, k, from_above):
            got, send, here, there, to = (rd, sd, sd_s, sd_r, below) if from_above else (ru, su, su_s, su_r, above)
            remote(send.at[prev, s], got.at[prev, s], here.at[prev, s], there.at[prev, s], mate).wait_recv()
            value = chip[k % SUMS, s] + got[prev, s].astype(F32)
            chip[k % SUMS, s] = value
            send[slot, s] = value.astype(BF16)

            @pl.when((s < z) if from_above else (s > z))
            def _():
                remote(send.at[slot, s], got.at[slot, s], here.at[slot, s], there.at[slot, s], to).start()

        up_k, down_k = t - 1 - z, t - 1 - (CHIPS - 1 - z)
        for i in range(CHIPS - 1):
            @pl.when(has_below & ok(up_k) & (CHIPS - 1 - i >= z))
            def _():
                pass_on(CHIPS - 1 - i, up_k, False)

            @pl.when(has_above & ok(down_k) & (i <= z))
            def _():
                pass_on(i, down_k, True)


        @pl.when(ok(t - mine))
        def _():
            k = t - mine
            optimizer_copies(k, two, lambda copy: copy.wait())
            is_q = _is_q(k % PER_LAYER)
            for (rows, cols), test in ((Q_BLOCK, is_q), (P_BLOCK, jnp.logical_not(is_q))):
                @pl.when(test)
                def _():
                    for j in range(cols // LANES):
                        at, over = part_of(j, rows), part_of(j, LANES)
                        low = chip[k % SUMS, z, at, :].astype(BF16)
                        m, v = _moments(mb[two, :rows, over], vb[two, :rows, over], low.astype(F32))
                        w = wb[two, :rows, over].astype(F32)
                        wn[slot, at, :] = (w - 0.02 * (m * lax.rsqrt(v + 1e-8) + 0.1 * w)).astype(BF16)
                        gn[slot, at, :] = low

            local(gn.at[slot], gp.at[_place(k)], out_sem.at[slot, 1]).start()

            @pl.when(k < SPREAD)
            def _():
                local(wn.at[slot], wp.at[_place(k), me], out_sem.at[slot, 0]).start()

            @pl.when(k >= SPREAD)
            def _():
                local(wn.at[slot], r_["last"].at[k - SPREAD], out_sem.at[slot, 0]).start()


        def sends(s, source, there):
            @pl.when((s <= z) & has_above)
            def _():
                remote(source, there, au_s.at[slot, s], au_r.at[slot, s], above).start()

            @pl.when((s >= z) & has_below)
            def _():
                remote(source, there, ad_s.at[slot, s], ad_r.at[slot, s], below).start()

            remote(source, there, am_s.at[slot, s], am_r.at[slot, s], mate).start()

        @pl.when(spread_here(t - mine))
        def _():
            sends(z, wn.at[slot], wp.at[_place(t - mine), me])


        @pl.when(ok(t))
        def _():
            r = t % PER_LAYER
            is_q = _is_q(r)
            for (rows, cols), test in ((Q_BLOCK, is_q), (P_BLOCK, jnp.logical_not(is_q))):
                @pl.when(test)
                def _():
                    wait_operands((rows, cols), r)
                    for own in range(2):
                        got = dot(ab[4 * rows * own : 4 * rows * (own + 1), :], db[:, :cols])
                        for s in range(CHIPS):
                            for j in range(cols // LANES):
                                piece = got[part_of(s, rows), part_of(j, LANES)]
                                if own:
                                    chip[t % SUMS, s, part_of(j, rows), :] = piece
                                else:
                                    ps[slot, s, part_of(j, rows), :] = piece.astype(BF16)
                        if not own:
                            for s in MATE_ORDER:
                                remote(ps.at[slot, s], pr.at[slot, s], ps_s.at[slot, s], ps_r.at[slot, s], mate).start()

        @pl.when(ok(t + 1))
        def _():
            load_operands(t + 1)

        work(n)


        def spread(s):
            k = t - wait_of(s) - jnp.abs(z - s)

            @pl.when(spread_here(k) & (s != z))
            def _():
                there = wp.at[_place(k), 2 * s + core]

                @pl.when(s < z)
                def _():
                    remote(there, there, au_s.at[prev, s], au_r.at[prev, s], mate).wait_recv()

                @pl.when(s > z)
                def _():
                    remote(there, there, ad_s.at[prev, s], ad_r.at[prev, s], mate).wait_recv()

                sends(s, there, there)

        loop(CHIPS, spread)


        def arrived(s):
            @pl.when(spread_here(t - 1 - wait_of(s) - jnp.abs(z - s)))
            def _():
                there = any_block
                remote(there, there, am_s.at[prev, s], am_r.at[prev, s], mate).wait_recv()

        loop(CHIPS, arrived)

        @pl.when(n < TICKS - 3)
        def _():
            tell(free_m, mate)

            @pl.when(has_above)
            def _():
                tell(free_d, above)

            @pl.when(has_below)
            def _():
                tell(free_u, below)

    loop(TICKS, tick)


def update(given, w, m, v):
    vm, sem = pltpu.VMEM, pltpu.SemaphoreType
    block, wide = (BLOCK, LANES), N_Q + 2 * N_K
    scratch = [
        vm((D, T), BF16), vm((T, D), BF16), vm((SUMS, CHIPS, *block), F32),
        *(vm((SLOTS, CHIPS, *block), BF16) for _ in range(6)),
        vm((SLOTS, *block), BF16), vm((SLOTS, *block), BF16),
        *(vm((2, P_BLOCK[0], D), dtype) for dtype in (F32, F32, BF16)),
        vm((T, D), BF16), vm((T, D), BF16), vm((T, N_Q), BF16),
        vm((2, D, TF), BF16), vm((2, D, TF), BF16), vm((2, TF, D), BF16), vm((T, D), F32),
        vm((2, T, TF), BF16), vm((2, T, TF), BF16), vm((TF, TF), BF16),
        vm((T, GROUP * HEAD), BF16), vm((T, HEAD), BF16), vm((T, HEAD), BF16), vm((T, wide), BF16), vm((N_Q, T), BF16),
        vm((T, HALF), F32), vm((T, HALF), F32), vm((KV, GROUP, T), F32), vm((KV, GROUP, T), F32), vm((4, STRIDE, HALF), F32),
        sem.DMA, sem.DMA, *(sem.DMA(shape) for shape in ((2, 3), (SLOTS, 2), (2, 3), (2,))), sem.DMA, sem.DMA((3,)), sem.DMA, sem.DMA((2,)), sem.DMA((7,)),
        *(sem.DMA((SLOTS, CHIPS)) for _ in range(12)),
        sem.REGULAR, sem.REGULAR, sem.REGULAR,
    ]
    refs = [*w, *m, *v, *(given[name] for name in INPUTS)]
    pair = [(FF, T), (T, D), (T, wide), (D, T), (N_Q, T), (D, T), (T, D), (T, D), (T, N_Q), (T, wide)]
    shapes = [(CHUNKS, 8, *block), (CHUNKS, *block), (2, *block), *((2, *shape) for shape in pair)]
    outs = [*((shape, BF16) for shape in shapes), ((2, KV, GROUP, T), F32), ((T, D), BF16), ((T, D), BF16)]
    return pl.pallas_call(
        _update,
        in_specs=[pl.BlockSpec(memory_space=pl.ANY)] * len(refs),
        out_specs=[pl.BlockSpec(memory_space=pl.ANY)] * len(outs),
        out_shape=[jax.ShapeDtypeStruct(*out) for out in outs],
        scratch_shapes=scratch,
        compiler_params=pltpu.CompilerParams(collective_id=0, has_side_effects=True, vmem_limit_bytes=63 * 2**20),
        name="update",
    )(*refs)[:3]


def _moments(m, v, g):
    return 0.9 * m + 0.1 * g, 0.95 * v + 0.05 * g * g


LATE = ("wk", "wv")


def _unpack(*refs):
    s = pl.program_id(1)
    refs = list(refs)
    ins = [[refs.pop(0) for _ in range(3 if name in LATE else 4)] for name in NAMES]
    for i, name in enumerate(NAMES):
        gp_ref, m_ref, v_ref = ins[i][:3]
        w_out = None if name in LATE else refs.pop(0)
        m_out, v_out = refs[i - 2 * len(NAMES)], refs[i - len(NAMES)]
        tall = name in ("w_down", "wo")
        rows, cols = Q_BLOCK if tall else P_BLOCK
        some = m_ref.shape[1]
        for j in range(cols // LANES):
            for n in range(gp_ref.shape[0]):
                over = part_of(j, LANES) if tall else slice(cols * n + LANES * j, cols * n + LANES * (j + 1))
                down = part_of(n, rows) if tall else slice(0, rows)
                if w_out is not None:
                    w_out[0, down, over] = ins[i][3][n, 0, part_of(j, rows), :]
                if tall and n:
                    continue
                if tall:
                    per = rows // some
                    g = gp_ref[s // per if name == "wo" else jnp.minimum(s, 6), pl.ds(pl.multiple_of(rows * j + some * (s % per), 16), some), :]
                else:
                    g = gp_ref[n, pl.ds(pl.multiple_of(rows * j + some * jnp.minimum(s, 6), 16), some), :]
                m_out[0, :, over], v_out[0, :, over] = _moments(m_ref[0, :, over], v_ref[0, :, over], g.astype(F32))


def unpack(wp, gp, m, v):
    block = (BLOCK, LANES)
    where = {name: (TILES, 2 * i, 1) for i, name in enumerate(("w_gate", "w_up", "w_down"))}
    at = 3 * DOWN_AT
    for name, count in (("wo", 2), ("wq", 2), ("wk", 1), ("wv", 1)):
        where[name] = (count, at // count, (PER_LAYER - WO_AT) // count)
        at += count
    in_specs, given, full, own_m, own_v = [], [], {}, [], []
    for name in NAMES:
        count, start, step = where[name]
        _, height, width = m[name].shape
        some = Q_BLOCK[0] if name == "w_down" else 16
        last = height // some - 1
        mine = pl.BlockSpec((1, some, width), lambda layer, s, last=last: (layer, jnp.minimum(s, last), 0))
        in_specs += [pl.BlockSpec((count, *block), lambda layer, s, start=start, step=step: (start + step * layer, 0, 0)), mine, mine]
        given += [gp, m[name], v[name]]
        if name not in LATE:
            in_specs.append(pl.BlockSpec((count, 1, *block), lambda layer, s, start=start, step=step: (start + step * layer, s, 0, 0)))
            given.append(wp)
            full[name] = (pl.BlockSpec((1, height, width), lambda layer, s: (layer, s, 0)), jax.ShapeDtypeStruct((2, 8 * height, width), BF16))
        own_m.append((mine, jax.ShapeDtypeStruct(m[name].shape, F32)))
    outs = [*full.values(), *own_m, *own_m]
    got = pl.pallas_call(
        _unpack,
        grid=(2, 8),
        in_specs=in_specs,
        out_specs=[o[0] for o in outs],
        out_shape=[o[1] for o in outs],
        compiler_params=pltpu.CompilerParams(vmem_limit_bytes=VMEM),
        cost_estimate=pl.CostEstimate(flops=10**11, bytes_accessed=155 * 2**20, transcendentals=0),
        name="unpack",
    )(*given)
    n = len(full)
    return dict(zip(full, got)), got[n : n + len(NAMES)], got[n + len(NAMES) :]


def _finish(me_ref, *refs):
    came, packed, outs = refs[:8], refs[8:10], refs[10:]
    rows = P_BLOCK[0]
    for which, out in enumerate(outs):
        for j in range(P_BLOCK[1] // LANES):
            at, over = part_of(j, rows), part_of(j, LANES)
            for i in range(8):
                owner = (me_ref[0] + 8 - i) % 8
                out[0, pl.ds(pl.multiple_of(rows * owner, 16), rows), over] = came[i][which, at, :]
                out[1, part_of(i, rows), over] = packed[which][0, i, at, :]


def finish(last, wp, n_devices):
    me = lax.axis_index("dp")
    came = [last] + [lax.ppermute(last, "dp", [(s, (s + i) % n_devices) for s in range(n_devices)]) for i in range(1, n_devices)]
    block, (rows, cols) = (BLOCK, LANES), P_BLOCK
    whole = lambda *shape: pl.BlockSpec(shape, lambda i, _: (0,) * len(shape))
    layer_1 = [pl.BlockSpec((1, 8, *block), lambda i, _, at=at: (at, 0, 0, 0)) for at in (SPREAD, SPREAD + 1)]
    shape = (2, n_devices * rows, cols)
    return pl.pallas_call(
        _finish,
        grid_spec=pltpu.PrefetchScalarGridSpec(
            num_scalar_prefetch=1, grid=(1,), in_specs=[whole(2, *block)] * n_devices + layer_1, out_specs=[whole(*shape)] * 2
        ),
        out_shape=[jax.ShapeDtypeStruct(shape, BF16)] * 2,
        compiler_params=pltpu.CompilerParams(vmem_limit_bytes=VMEM // 2),
        name="finish",
    )(me.reshape(1).astype(jnp.int32), *came, wp, wp)


def solution(mesh):
    angle = np.arange(STRIDE)[:, None] * float(THETA) ** (-np.arange(HALF) / HALF)
    turns = np.stack([turn(angle * step) for step in (STRIDE, 1) for turn in (np.cos, np.sin)]).astype(np.float32)

    def step(x, dy, *arrays):
        w, m, v = (dict(zip(NAMES, some, strict=True)) for some in (arrays[:n], arrays[n : 2 * n], arrays[2 * n :]))
        wp, gp, last = update({"x": x[0], "dy": dy[0], "turns": jnp.asarray(turns)}, w.values(), m.values(), v.values())
        new, new_m, new_v = unpack(wp, gp, m, v)
        new |= dict(zip(LATE, finish(last, wp, mesh.shape["dp"])))
        return (*(new[name] for name in NAMES), *new_m, *new_v)

    n = len(NAMES)
    return jax.shard_map(
        step,
        mesh=mesh,
        in_specs=(P(("rep", "dp")),) * 2 + (P(),) * n + (P(None, "dp"),) * (2 * n),
        out_specs=(P("rep"),) * n + (P("rep", "dp"),) * (2 * n),
        check_vma=False,
    )
```

```python
import functools

import jax
import jax.numpy as jnp
import numpy as np
from jax import lax
from jax.experimental import pallas as pl
from jax.experimental.pallas import tpu as pltpu
from jax.sharding import PartitionSpec as P

LOG2E = 1.4426950408889634
HIDDEN = -2e30
VMEM = 56 * 2**20
F32, BF16 = jnp.float32, jnp.bfloat16
MESH = pl.DeviceIdType.MESH
T, D, FF, HEADS, KV, HEAD = 1024, 896, 3584, 4, 2, 256
THETA = 10000
STRIDE = 32
NAMES = ("wq", "wk", "wv", "wo", "w_gate", "w_up", "w_down")
ROWS = 256
TF = 512
PIECES = T // ROWS


def loop(count, body):
    lax.fori_loop(0, count, lambda i, _: body(i), None)


def dot(a, b):
    return jnp.dot(a, b, preferred_element_type=F32)


def dot_t(a, b):
    return lax.dot_general(a, b, (((1,), (1,)), ((), ())), preferred_element_type=F32)


def _scale(wide):
    return lax.rsqrt(jnp.mean(wide * wide, -1, keepdims=True) + 1e-6)


def _norm_back(h, by):
    s = _scale(h)
    return by * s - h * (s * s * s * jnp.mean(by * h, -1, keepdims=True))


E = HEAD**-0.5 * LOG2E
GROUP = HEADS // KV


def part_of(i, size):
    return slice(size * i, size * (i + 1))


def _piece(i):
    return part_of(i, ROWS)


def _visible():
    shape = (ROWS, GROUP * ROWS)
    return lax.broadcasted_iota(jnp.int32, shape, 0) <= lax.rem(lax.broadcasted_iota(jnp.int32, shape, 1), ROWS)


LANES = 128
BLOCK = 448
SLOTS = 4
SUMS = 5
EARLY = 1
LAG = 27
P_BLOCK, Q_BLOCK = (112, 512), (64, 896)
TILES = FF // TF
DOWN_AT, WO_AT, QKV_AT, PER_LAYER = 14, 21, 23, 27
CHUNKS = 2 * PER_LAYER
SPREAD = CHUNKS - 2
TICKS = CHUNKS + 6 + EARLY
CHIPS = 4
MATE_ORDER = (3, 0, 2, 1)
QKV_ORDER = (1, 3, 0, 2)
HALF, T_HALF = HEAD // 2, T // 2
N_Q, N_K = HEADS * HEAD, KV * HEAD
BEFORE, LEAVE, HEADS_AT, AFTER = 13, 14, 15, 18


def _is_q(r):
    return (r >= DOWN_AT) & (r < QKV_AT)


def _place(k):
    layer, r = 1 - k // PER_LAYER, k % PER_LAYER
    double, single = (r % 2) * DOWN_AT + layer * TILES + r // 2, 2 * DOWN_AT + layer * TILES + r - DOWN_AT
    return jnp.where(r < DOWN_AT, double, jnp.where(r < WO_AT, single, 3 * DOWN_AT + layer * (PER_LAYER - WO_AT) + r - WO_AT))


def _owners(layer, r):
    mlp_chunk = r < DOWN_AT
    return (
        ("w_gate", mlp_chunk & (r % 2 == 0), r // 2), ("w_up", mlp_chunk & (r % 2 == 1), r // 2),
        ("w_down", (r >= DOWN_AT) & (r < WO_AT), r - DOWN_AT), ("wo", (r >= WO_AT) & (r < QKV_AT), r - WO_AT),
        ("wq", (r >= QKV_AT) & (r < QKV_AT + 2), r - QKV_AT), ("wk", r == QKV_AT + 2, 0 * r), ("wv", r == QKV_AT + 3, 0 * r),
    )


INPUTS = ("x", "dy", "turns")
OUTPUTS = ("wp", "gp", "last", "hidt", "d1", "dqkv", "at", "ot", "bt", "b", "h1", "o", "qkv", "lse", "h", "by1")
SCRATCH = ("ab", "db", "chip", "ps", "pr", "su", "ru", "sd", "rd", "wn", "gn", "mb", "vb", "wb", "x1", "x2", "oo", "wg", "wu", "wd", "acc", "dg", "du", "ht",
           "qq", "kk", "vv", "dq", "st", "cosb", "sinb", "lseb", "delta", "tb",
           "ab_sem", "db_sem", "opt_sem", "out_sem", "tile_sem", "x_sem", "o_sem", "qkv_sem", "lse_sem", "write_sem", "save_sem",
           "ps_s", "ps_r", "su_s", "su_r", "sd_s", "sd_r", "am_s", "am_r", "au_s", "au_r", "ad_s", "ad_r", "free_m", "free_u", "free_d")


def _update(*refs):
    count = len(NAMES)
    w_in, m_in, v_in = (dict(zip(NAMES, some)) for some in (refs[:count], refs[count : 2 * count], refs[2 * count :]))
    r_ = dict(zip((*INPUTS, *OUTPUTS, *SCRATCH), refs[3 * count :], strict=True))
    (ab, db, chip, ps, pr, su, ru, sd, rd, wn, gn, mb, vb, wb, x1, x2, oo, wg, wu, wd, acc, dg, du, ht, qq, kk, vv, dq, st, cosb, sinb, lseb, delta, tb,
     ab_sem, db_sem, opt_sem, out_sem, tile_sem, x_sem, o_sem, qkv_sem, lse_sem, write_sem, save_sem,
     ps_s, ps_r, su_s, su_r, sd_s, sd_r, am_s, am_r, au_s, au_r, ad_s, ad_r, free_m, free_u, free_d) = (r_[name] for name in SCRATCH)
    wp, gp = r_["wp"], r_["gp"]
    any_block = wp.at[0, 0]
    rep, me = lax.axis_index("rep"), lax.axis_index("dp")
    z, core = me // 2, me % 2
    mate, above, below = me + 1 - 2 * core, me + 2, me - 2
    has_above, has_below = z < CHIPS - 1, z > 0

    def remote(src, dst, send, recv, to):
        return pltpu.make_async_remote_copy(src_ref=src, dst_ref=dst, send_sem=send, recv_sem=recv, device_id=(rep, to), device_id_type=MESH)

    def tell(sem, to):
        pl.semaphore_signal(sem, inc=1, device_id=(rep, to), device_id_type=MESH)

    def local(src, dst, sem):
        return pltpu.make_async_copy(src, dst, sem)

    def ok(k):
        return (k >= 0) & (k < CHUNKS)

    def spread_here(k):
        return (k >= 0) & (k < SPREAD)

    def for_mate(k, s):
        return spread_here(k) | (ok(k) & (s == z))

    def wait_of(s):
        return 3 + ((s == 0) | (s == CHIPS - 1)).astype(jnp.int32)

    mine = wait_of(z)

    def tokens(start, count):
        return pl.ds(pl.multiple_of(start, ROWS), count)


    def tile_copies(half, j, buf):
        layer, over = 1 - half, pl.ds(pl.multiple_of(TF * j, TF), TF)
        return [
            local(w_in["w_gate"].at[layer, :, over], wg.at[buf], tile_sem.at[buf, 0]),
            local(w_in["w_up"].at[layer, :, over], wu.at[buf], tile_sem.at[buf, 1]),
            local(w_in["w_down"].at[layer, over, :], wd.at[buf], tile_sem.at[buf, 2]),
        ]

    def wo_copies(half):
        return [local(w_in["wo"].at[1 - half, pl.ds(TF * n, TF), :], wd.at[n], tile_sem.at[n, 2]) for n in range(2)]

    def qkv_weight_copies(half):
        layer = 1 - half
        return [
            *(local(w_in["wq"].at[layer, :, pl.ds(TF * n, TF)], wg.at[n], tile_sem.at[n, 0]) for n in range(2)),
            local(w_in["wk"].at[layer], wu.at[0], tile_sem.at[0, 1]), local(w_in["wv"].at[layer], wu.at[1], tile_sem.at[1, 1]),
        ]

    def column(at):
        return pl.ds(pl.multiple_of(at, HEAD), HEAD)

    def head_copies(half, head):
        pair = pl.ds(pl.multiple_of(GROUP * HEAD * head, GROUP * HEAD), GROUP * HEAD)
        return [
            local(r_["qkv"].at[half, :, over], to, qkv_sem.at[n])
            for n, (over, to) in enumerate(((pair, qq), (column(N_Q + HEAD * head), kk), (column(N_Q + N_K + HEAD * head), vv)))
        ]

    def load_x2(ref):
        return local(ref, x2, x_sem.at[1])

    def unit_of(n):
        half = (n >= AFTER + 2 + EARLY).astype(jnp.int32)
        return half, n - EARLY - LAG * half

    def start(copies):
        for copy in copies:
            copy.start()

    def wait(copies):
        for copy in copies:
            copy.wait()

    def writes(half, tau):
        u = tau + EARLY
        j, first = u // 2, tokens(T_HALF * (u % 2), T_HALF)
        over = pl.ds(pl.multiple_of(TF * j, TF), TF)
        part = tokens(T_HALF * (tau - AFTER), T_HALF)
        after_at = (tau >= AFTER) & (tau < AFTER + 2)
        return (
            ((u >= 0) & (u < 2 * TILES), lambda: [local(ht, r_["hidt"].at[half, over, first], write_sem.at[0])]),
            (tau == LEAVE, lambda: [local(x1, r_["d1"].at[half], write_sem.at[0])]),
            (after_at, lambda: [local(dq.at[part, :], r_["dqkv"].at[half, part, :], write_sem.at[0])]),
            (after_at & (half == 0), lambda: [local(x1.at[part, :], r_["by1"].at[part, :], write_sem.at[1])]),
        )

    def fetch(n):
        half, tau = unit_of(n)
        u = tau + EARLY

        @pl.when((tau == -EARLY - 1) & (half == 1))
        def _():
            start([*tile_copies(half, 0, 0), load_x2(r_["b"].at[half])])

        @pl.when((u >= 0) & (u % 2 == 0) & (u < 2 * TILES - 2))
        def _():
            start(tile_copies(half, u // 2 + 1, (u // 2 + 1) % 2))

        @pl.when(tau == BEFORE)
        def _():
            start([*wo_copies(half), load_x2(r_["h1"].at[half]), local(r_["o"].at[half], oo, o_sem)])

        @pl.when(tau == LEAVE)
        def _():
            start([*head_copies(half, 0), local(r_["lse"].at[half], lseb, lse_sem)])

        @pl.when(tau == HEADS_AT + 1)
        def _():
            start(head_copies(half, 1))

        @pl.when((tau == BEFORE) & (half == 0))
        def _():
            start(tile_copies(0, 0, 0)[:2])

        @pl.when((tau == LEAVE) & (half == 0))
        def _():
            start(qkv_weight_copies(0))

        @pl.when((tau == HEADS_AT) & (half == 0))
        def _():
            start([load_x2(r_["h"])])

    def mlp_unit(u, buf, later):
        rows = tokens(T_HALF * (u % 2), T_HALF)
        gate, up = dot(x2[rows, :], wg[buf]), dot(x2[rows, :], wu[buf])
        sig = 1.0 / (1.0 + jnp.exp(-gate))
        silu = gate * sig
        by = dot_t(x1[rows, :], wd[buf]).astype(BF16).astype(F32)
        ht[...] = (silu * up).astype(BF16).T
        du[buf, rows, :] = (by * silu).astype(BF16)
        dg[buf, rows, :] = (by * up * (sig * (1.0 + gate * (1.0 - sig)))).astype(BF16)

        @pl.when(jnp.logical_not(later))
        def _():
            acc[rows, :] += dot_t(dg[buf, rows, :], wg[buf]) + dot_t(du[buf, rows, :], wu[buf])

    def late_unit(i):
        rows = tokens(ROWS * i, ROWS)
        acc[rows, :] += dot_t(st[rows, :TF], wg[0]) + dot_t(st[rows, TF:], wu[0])

    def leave_unit(i):
        rows = tokens(ROWS * i, ROWS)
        inner = _norm_back(x2[rows, :].astype(F32), acc[rows, :].astype(BF16).astype(F32)).astype(BF16)
        d1 = (x1[rows, :].astype(F32) + inner.astype(F32)).astype(BF16)
        x1[rows, :] = d1
        for n in range(HEADS):
            low, over = HEAD * (n % 2), _piece(n)
            do = dot_t(d1, wd[n // 2, low : low + HEAD, :]).astype(BF16)
            both = do.astype(F32) * oo[rows, over].astype(F32)
            oo[rows, over] = do
            delta[n // GROUP, n % GROUP : n % GROUP + 1, rows] = both.T.sum(0, keepdims=True)

    def side(ref, i, head):
        return jnp.concatenate([ref[_piece(i), column(HEAD * (GROUP * head + n))] for n in range(GROUP)], axis=0)

    def turn_back(part, rows):
        cos, sin = cosb[rows, :], sinb[rows, :]
        x, y = part[:, :HALF].astype(F32), part[:, HALF:].astype(F32)
        return jnp.concatenate([x * cos + y * sin, y * cos - x * sin], -1).astype(BF16)

    def head_unit(head):
        seen = _visible()
        turned = kk[...].T
        line = lambda ref, i: jnp.concatenate([ref[head, n : n + 1, _piece(i)] for n in range(GROUP)], axis=1)
        dk_at, dv_at = slice(0, HEAD), slice(HEAD, 2 * HEAD)
        for i in range(PIECES):
            lse, dl = line(lseb, i), line(delta, i)
            q = jnp.concatenate([qq[_piece(i), _piece(n)] for n in range(GROUP)], axis=0)
            do = side(oo, i, head)
            by_q = 0.0
            for j in range(i + 1):
                at = _piece(j)
                p = jnp.exp2(dot_t(kk[at, :], q) * E - lse)
                if j == i:
                    p = jnp.where(seen, p, 0.0)
                ds = (p * (dot_t(vv[at, :], do) - dl)).astype(BF16)
                by_v, by_k = dot(p.astype(BF16), do), dot(ds, q)
                acc[at, dv_at] = by_v if j == i else acc[at, dv_at] + by_v
                acc[at, dk_at] = by_k if j == i else acc[at, dk_at] + by_k
                by_q = by_q + dot(turned[:, at], ds)
            by_q = (by_q * HEAD**-0.5).astype(BF16)
            for n in range(GROUP):
                dq[_piece(i), column(HEAD * (GROUP * head + n))] = turn_back(by_q[:, _piece(n)].T, _piece(i))
        for i in range(PIECES):
            dq[_piece(i), column(N_Q + HEAD * head)] = turn_back((acc[_piece(i), dk_at] * HEAD**-0.5).astype(BF16), _piece(i))
            dq[_piece(i), column(N_Q + N_K + HEAD * head)] = acc[_piece(i), dv_at].astype(BF16)

    def after_unit(rows):
        by = sum(dot_t(dq[rows, part_of(n, TF)], (wg, wu)[n // 2][n % 2]) for n in range(4)).astype(BF16).astype(F32)
        inner = _norm_back(x2[rows, :].astype(F32), by).astype(BF16)
        x1[rows, :] = (x1[rows, :].astype(F32) + inner.astype(F32)).astype(BF16)

    def work(n):
        half, tau = unit_of(n)
        u = tau + EARLY

        @pl.when((u >= 0) & (u < 2 * TILES))
        def _():
            buf = u // 2 % 2

            @pl.when(u % 2 == 0)
            def _():
                wait(tile_copies(half, u // 2, buf))

            @pl.when(u == 0)
            def _():
                acc[...] = jnp.zeros((T, D), F32)

                @pl.when(half == 1)
                def _():
                    load_x2(r_["h"]).wait()

            mlp_unit(u, buf, (half == 0) & (u < 2))

            @pl.when((half == 0) & (u == 1))
            def _():
                st[:, :TF] = dg[0]
                st[:, TF:] = du[0]

        @pl.when((tau == BEFORE) & (half == 0))
        def _():
            wait(tile_copies(0, 0, 0)[:2])
            loop(PIECES, late_unit)

        @pl.when(tau == LEAVE)
        def _():
            wait([load_x2(r_["h"]), local(r_["o"].at[0], oo, o_sem), *wo_copies(half)])
            loop(PIECES, leave_unit)

        @pl.when((tau == HEADS_AT) | (tau == HEADS_AT + 2))
        def _():
            @pl.when(tau == HEADS_AT)
            def _():
                local(r_["lse"].at[0], lseb, lse_sem).wait()

            wait(head_copies(0, 0))
            head_unit((tau - HEADS_AT) // 2)

        @pl.when((tau >= AFTER) & (tau < AFTER + 2) & (half == 0))
        def _():
            @pl.when(tau == AFTER)
            def _():
                wait([load_x2(r_["h"]), *qkv_weight_copies(0)])

            loop(PIECES // 2, lambda i: after_unit(tokens(T_HALF * (tau - AFTER) + ROWS * i, ROWS)))

        for test, copies in writes(half, tau):
            pl.when(test)(lambda: start(copies()))


    def load_operands(k):
        half, r = k // PER_LAYER, k % PER_LAYER

        def from_rows(ref, block, down):
            rows, whole = block[0], ref.shape[0] // 8
            for e in range(8):
                owner = 2 * (e % 4) + (1 - core if e < 4 else core)
                at = pl.multiple_of(whole * owner + down, 16)
                local(ref.at[pl.ds(at, rows), :], ab.at[pl.ds(rows * e, rows), :], ab_sem).start()

        @pl.when(r < DOWN_AT)
        def _():
            from_rows(r_["bt"].at[half], P_BLOCK, 0)

        @pl.when((r >= DOWN_AT) & (r < WO_AT))
        def _():
            from_rows(r_["hidt"].at[half], Q_BLOCK, Q_BLOCK[0] * (r - DOWN_AT))

            @pl.when(half == 0)
            def _():
                local(r_["dy"], db, db_sem).start()

            @pl.when(half == 1)
            def _():
                local(r_["by1"], db, db_sem).start()

        @pl.when((r >= WO_AT) & (r < QKV_AT))
        def _():
            from_rows(r_["ot"].at[half], Q_BLOCK, Q_BLOCK[0] * (r - WO_AT))
            local(r_["d1"].at[half], db, db_sem).start()

        @pl.when(r >= QKV_AT)
        def _():
            from_rows(r_["at"].at[half], P_BLOCK, 0)
            local(r_["dqkv"].at[half, :, pl.ds(pl.multiple_of(TF * (r - QKV_AT), TF), TF)], db.at[:, pl.ds(0, TF)], db_sem).start()

    def wait_operands(block, r):
        rows, cols = block
        local(r_["hidt"].at[0, pl.ds(0, 8 * rows), :], ab.at[pl.ds(0, 8 * rows), :], ab_sem).wait()

        @pl.when(r >= DOWN_AT)
        def _():
            local(r_["dqkv"].at[0, :, pl.ds(0, cols)], db.at[:, pl.ds(0, cols)], db_sem).wait()

        for which, ref in enumerate((dg, du)):
            @pl.when((r < DOWN_AT) & (r % 2 == which))
            def _():
                db[:, :TF] = ref[r // 2 % 2]

    def optimizer_copies(k, buf, do):
        layer, r = 1 - k // PER_LAYER, k % PER_LAYER
        for name, test, j in _owners(layer, r):
            rows, cols = block = Q_BLOCK if name in ("w_down", "wo") else P_BLOCK

            @pl.when(test)
            def _():
                whole = w_in[name].shape[1] // 8
                down = pl.multiple_of(rows * j if block == Q_BLOCK else 0 * j, 16)
                right = pl.ds(0, cols) if block == Q_BLOCK else pl.ds(pl.multiple_of(cols * j, cols), cols)
                for n, (ref, at, to) in enumerate(((m_in[name], down, mb), (v_in[name], down, vb), (w_in[name], pl.multiple_of(whole * me + down, 16), wb))):
                    do(local(ref.at[layer, pl.ds(at, rows), right], to.at[buf, pl.ds(0, rows), pl.ds(0, cols)], opt_sem.at[buf, n]))


    def save(n, source, to):
        return local(source, to, save_sem.at[n])

    def attend_head(head):
        seen = _visible()
        k_at, turned = column(N_Q + HEAD * head), dq[:, column(N_Q + N_K + HEAD * head)].T

        def scores_of(i):
            q = side(dq, i, head)
            scores = [dot_t(dq[_piece(j), k_at], q) for j in range(i + 1)]
            return [*scores[:i], jnp.where(seen, scores[i], HIDDEN)]

        coming = scores_of(0)
        for i in range(PIECES):
            scores, coming = coming, scores_of(i + 1) if i + 1 < PIECES else None
            top = functools.reduce(jnp.maximum, [s.max(axis=0, keepdims=True) for s in scores])
            total, mix = 0.0, 0.0
            for j, s in enumerate(scores):
                p = jnp.exp2((s - top) * E)
                total = total + p.sum(axis=0, keepdims=True)
                mix = mix + dot(turned[:, _piece(j)], p.astype(BF16))
            out = (mix * (1.0 / total)).astype(BF16)
            lse = top * E + jnp.log(total) * LOG2E
            for n in range(GROUP):
                over = column(HEAD * (GROUP * head + n))
                st[over, _piece(i)] = out[:, _piece(n)]
                oo[_piece(i), over] = out[:, _piece(n)].T
                lseb[head, n : n + 1, _piece(i)] = lse[:, _piece(n)]

    def saves(half):
        kept = lambda name: r_[name].at[half]
        return [
            save(0, ab, kept("bt")), save(1, dq.at[:, pl.ds(0, D)], kept("h1")), save(2, x2, kept("b")),
            save(3, st, kept("ot")), save(4, oo, kept("o")), save(5, lseb, kept("lse")),
        ]

    by_y, by_h = local(r_["dy"], x1, x_sem.at[0]), save(6, x1, r_["h"])

    def forward(layer):
        half = 1 - layer
        weights = qkv_weight_copies(half)
        early = [save(0, ab, r_["at"].at[half]), save(1, dq, r_["qkv"].at[half])]
        for i in range(PIECES):
            wide = x1[_piece(i), :].astype(F32)
            a = (wide * _scale(wide)).astype(BF16)
            ab[:, _piece(i)] = a.T
            cos, sin = cosb[_piece(i), :], sinb[_piece(i), :]
            for c in QKV_ORDER:
                if i == 0:
                    weights[c].wait()
                t = dot(a, (wg, wu)[c // 2][c % 2]).astype(BF16)
                for n in range(2):
                    part = t[:, _piece(n)]
                    if c < 3:
                        p, q = part[:, :HALF].astype(F32), part[:, HALF:].astype(F32)
                        part = jnp.concatenate([p * cos - q * sin, q * cos + p * sin], -1).astype(BF16)
                    dq[_piece(i), TF * c + HEAD * n : TF * c + HEAD * (n + 1)] = part
        wo = local(w_in["wo"].at[layer], db, db_sem)
        start([*early, wo, *tile_copies(half, 0, 0)])
        loop(KV, attend_head)
        wait([*early, wo])
        start(saves(half)[3:])

        @pl.when(layer == 1)
        def _():
            by_h.wait()

        projected = lambda i: dot(oo[_piece(i), :], db[...])
        coming = projected(0)
        for i in range(PIECES):
            rows = _piece(i)
            total, coming = coming, projected(i + 1) if i + 1 < PIECES else None
            h1 = (x1[rows, :].astype(F32) + total.astype(BF16).astype(F32)).astype(BF16)
            dq[rows, :D] = h1
            wide = h1.astype(F32)
            b = (wide * _scale(wide)).astype(BF16)
            x2[rows, :] = b
            ab[:, rows] = b.T
        start(saves(half)[:3])

        @pl.when(layer == 1)
        def _():
            by_y.start()

        @pl.when(layer == 0)
        def _():
            acc[...] = jnp.zeros((T, D), F32)
            coming = qkv_weight_copies(0)

            def one(j):
                buf = j % 2

                @pl.when(j < TILES - 1)
                def _():
                    start(tile_copies(half, j + 1, 1 - buf))

                @pl.when(j == TILES - 1)
                def _():
                    start([coming[c] for c in QKV_ORDER[:2]])

                wait(tile_copies(half, j, buf))
                for i in range(2):
                    rows = part_of(i, T_HALF)
                    gate, up = dot(x2[rows, :], wg[buf]), dot(x2[rows, :], wu[buf])
                    hidden = (gate * (1.0 / (1.0 + jnp.exp(-gate))) * up).astype(BF16)
                    acc[rows, :] += dot(hidden, wd[buf])

            loop(TILES, one)
            start([coming[c] for c in QKV_ORDER[2:]])
            wait(saves(half))
            for i in range(PIECES):
                x1[_piece(i), :] = (dq[_piece(i), :D].astype(F32) + acc[_piece(i), :].astype(BF16).astype(F32)).astype(BF16)
            by_h.start()

    first = [local(r_["x"], x1, x_sem.at[0]), local(r_["turns"], tb, o_sem)]
    start([*first, *(qkv_weight_copies(1)[c] for c in QKV_ORDER)])


    barrier = pltpu.get_barrier_semaphore()
    tell(barrier, mate)

    @pl.when(has_above)
    def _():
        tell(barrier, above)

    @pl.when(has_below)
    def _():
        tell(barrier, below)

    wait(first)

    def spin(a):
        rows = pl.ds(pl.multiple_of(STRIDE * a, STRIDE), STRIDE)
        cos_a, sin_a, cos_b, sin_b = tb[0, pl.ds(a, 1), :], tb[1, pl.ds(a, 1), :], tb[2], tb[3]
        cosb[rows, :] = cos_a * cos_b - sin_a * sin_b
        sinb[rows, :] = sin_a * cos_b + cos_a * sin_b

    loop(T // STRIDE, spin)
    loop(2, forward)
    @pl.when(has_above & has_below)
    def _():
        pl.semaphore_wait(barrier, 3)

    @pl.when(jnp.logical_not(has_above & has_below))
    def _():
        pl.semaphore_wait(barrier, 2)

    by_y.wait()

    def sent(n):
        t, late = n - 3 - EARLY, (n + 1) % SLOTS

        @pl.when(ok(t))
        def _():
            for s in range(CHIPS):
                remote(ps.at[late, s], pr.at[late, s], ps_s.at[late, s], ps_r.at[late, s], mate).wait_send()

        @pl.when(ok(t - 1 - z))
        def _():
            for s in range(1, CHIPS):
                @pl.when(s > z)
                def _():
                    remote(su.at[late, s], ru.at[late, s], su_s.at[late, s], su_r.at[late, s], mate).wait_send()

        @pl.when(ok(t - 1 - (CHIPS - 1 - z)))
        def _():
            for s in range(CHIPS - 1):
                @pl.when(s < z)
                def _():
                    remote(sd.at[late, s], rd.at[late, s], sd_s.at[late, s], sd_r.at[late, s], mate).wait_send()

        def gone(s):
            k = t - wait_of(s) - jnp.abs(z - s)
            there = any_block

            @pl.when(for_mate(k, s))
            def _():
                remote(there, there, am_s.at[late, s], am_r.at[late, s], mate).wait_send()

            @pl.when(spread_here(k) & (s <= z) & has_above)
            def _():
                remote(there, there, au_s.at[late, s], au_r.at[late, s], mate).wait_send()

            @pl.when(spread_here(k) & (s >= z) & has_below)
            def _():
                remote(there, there, ad_s.at[late, s], ad_r.at[late, s], mate).wait_send()

        loop(CHIPS, gone)

        @pl.when(ok(t - mine))
        def _():
            local(wn.at[late], any_block, out_sem.at[late, 0]).wait()
            local(gn.at[late], gp.at[0], out_sem.at[late, 1]).wait()

    def tick(n):
        t = n - EARLY
        slot, prev = n % SLOTS, (n + SLOTS - 1) % SLOTS
        two = n % 2


        @pl.when(n >= 3)
        def _():
            pl.semaphore_wait(free_m, 1)

            @pl.when(has_above)
            def _():
                pl.semaphore_wait(free_u, 1)

            @pl.when(has_below)
            def _():
                pl.semaphore_wait(free_d, 1)

            sent(n)


        @pl.when(n == EARLY)
        def _():
            wait(saves(0))
            load_operands(0)

        for test, copies in writes(*unit_of(n - 1)):
            pl.when(test & (n > 0))(lambda: wait(copies()))
        fetch(n)

        @pl.when(ok(t + 1 - mine))
        def _():
            optimizer_copies(t + 1 - mine, 1 - two, lambda copy: copy.start())


        @pl.when(ok(t - 1))
        def _():
            for s in MATE_ORDER:
                remote(ps.at[prev, s], pr.at[prev, s], ps_s.at[prev, s], ps_r.at[prev, s], mate).wait_recv()
                value = chip[(t - 1) % SUMS, s] + pr[prev, s].astype(F32)
                chip[(t - 1) % SUMS, s] = value
                if s > 0:
                    @pl.when(z == 0)
                    def _():
                        su[slot, s] = value.astype(BF16)
                        remote(su.at[slot, s], ru.at[slot, s], su_s.at[slot, s], su_r.at[slot, s], above).start()
                if s < CHIPS - 1:
                    @pl.when(z == CHIPS - 1)
                    def _():
                        sd[slot, s] = value.astype(BF16)
                        remote(sd.at[slot, s], rd.at[slot, s], sd_s.at[slot, s], sd_r.at[slot, s], below).start()


        def pass_on(s, k, from_above):
            got, send, here, there, to = (rd, sd, sd_s, sd_r, below) if from_above else (ru, su, su_s, su_r, above)
            remote(send.at[prev, s], got.at[prev, s], here.at[prev, s], there.at[prev, s], mate).wait_recv()
            value = chip[k % SUMS, s] + got[prev, s].astype(F32)
            chip[k % SUMS, s] = value
            send[slot, s] = value.astype(BF16)

            @pl.when((s < z) if from_above else (s > z))
            def _():
                remote(send.at[slot, s], got.at[slot, s], here.at[slot, s], there.at[slot, s], to).start()

        up_k, down_k = t - 1 - z, t - 1 - (CHIPS - 1 - z)
        for i in range(CHIPS - 1):
            @pl.when(has_below & ok(up_k) & (CHIPS - 1 - i >= z))
            def _():
                pass_on(CHIPS - 1 - i, up_k, False)

            @pl.when(has_above & ok(down_k) & (i <= z))
            def _():
                pass_on(i, down_k, True)


        @pl.when(ok(t - mine))
        def _():
            k = t - mine
            optimizer_copies(k, two, lambda copy: copy.wait())
            is_q = _is_q(k % PER_LAYER)
            for (rows, cols), test in ((Q_BLOCK, is_q), (P_BLOCK, jnp.logical_not(is_q))):
                @pl.when(test)
                def _():
                    for j in range(cols // LANES):
                        at, over = part_of(j, rows), part_of(j, LANES)
                        low = chip[k % SUMS, z, at, :].astype(BF16)
                        m, v = _moments(mb[two, :rows, over], vb[two, :rows, over], low.astype(F32))
                        w = wb[two, :rows, over].astype(F32)
                        wn[slot, at, :] = (w - 0.02 * (m * lax.rsqrt(v + 1e-8) + 0.1 * w)).astype(BF16)
                        gn[slot, at, :] = low

            local(gn.at[slot], gp.at[_place(k)], out_sem.at[slot, 1]).start()

            @pl.when(k < SPREAD)
            def _():
                local(wn.at[slot], wp.at[_place(k), me], out_sem.at[slot, 0]).start()

            @pl.when(k >= SPREAD)
            def _():
                there = r_["last"].at[core, k - SPREAD]
                local(wn.at[slot], there, out_sem.at[slot, 0]).start()
                remote(wn.at[slot], there, am_s.at[slot, z], am_r.at[slot, z], mate).start()


        def sends(s, source, there):
            @pl.when((s <= z) & has_above)
            def _():
                remote(source, there, au_s.at[slot, s], au_r.at[slot, s], above).start()

            @pl.when((s >= z) & has_below)
            def _():
                remote(source, there, ad_s.at[slot, s], ad_r.at[slot, s], below).start()

            remote(source, there, am_s.at[slot, s], am_r.at[slot, s], mate).start()

        @pl.when(spread_here(t - mine))
        def _():
            sends(z, wn.at[slot], wp.at[_place(t - mine), me])

        work(n)


        @pl.when(ok(t))
        def _():
            r = t % PER_LAYER
            is_q = _is_q(r)
            for (rows, cols), test in ((Q_BLOCK, is_q), (P_BLOCK, jnp.logical_not(is_q))):
                @pl.when(test)
                def _():
                    wait_operands((rows, cols), r)
                    for own in range(2):
                        got = dot(ab[4 * rows * own : 4 * rows * (own + 1), :], db[:, :cols])
                        for s in range(CHIPS):
                            for j in range(cols // LANES):
                                piece = got[part_of(s, rows), part_of(j, LANES)]
                                if own:
                                    chip[t % SUMS, s, part_of(j, rows), :] = piece
                                else:
                                    ps[slot, s, part_of(j, rows), :] = piece.astype(BF16)
                        if not own:
                            for s in MATE_ORDER:
                                remote(ps.at[slot, s], pr.at[slot, s], ps_s.at[slot, s], ps_r.at[slot, s], mate).start()

        @pl.when((t >= 0) & ok(t + 1))
        def _():
            load_operands(t + 1)


        def spread(s):
            k = t - wait_of(s) - jnp.abs(z - s)

            @pl.when(spread_here(k) & (s != z))
            def _():
                there = wp.at[_place(k), 2 * s + core]

                @pl.when(s < z)
                def _():
                    remote(there, there, au_s.at[prev, s], au_r.at[prev, s], mate).wait_recv()

                @pl.when(s > z)
                def _():
                    remote(there, there, ad_s.at[prev, s], ad_r.at[prev, s], mate).wait_recv()

                sends(s, there, there)

        loop(CHIPS, spread)


        def arrived(s):
            @pl.when(for_mate(t - 1 - wait_of(s) - jnp.abs(z - s), s))
            def _():
                there = any_block
                remote(there, there, am_s.at[prev, s], am_r.at[prev, s], mate).wait_recv()

        loop(CHIPS, arrived)

        @pl.when(n < TICKS - 3)
        def _():
            tell(free_m, mate)

            @pl.when(has_above)
            def _():
                tell(free_d, above)

            @pl.when(has_below)
            def _():
                tell(free_u, below)

    loop(TICKS, tick)
    loop(3, lambda i: sent(TICKS + i))


def update(given, w, m, v):
    vm, sem = pltpu.VMEM, pltpu.SemaphoreType
    block, wide = (BLOCK, LANES), N_Q + 2 * N_K
    scratch = [
        vm((D, T), BF16), vm((T, D), BF16), vm((SUMS, CHIPS, *block), F32),
        *(vm((SLOTS, CHIPS, *block), BF16) for _ in range(6)),
        vm((SLOTS, *block), BF16), vm((SLOTS, *block), BF16),
        *(vm((2, P_BLOCK[0], D), dtype) for dtype in (F32, F32, BF16)),
        vm((T, D), BF16), vm((T, D), BF16), vm((T, N_Q), BF16),
        vm((2, D, TF), BF16), vm((2, D, TF), BF16), vm((2, TF, D), BF16), vm((T, D), F32),
        vm((2, T, TF), BF16), vm((2, T, TF), BF16), vm((TF, TF), BF16),
        vm((T, GROUP * HEAD), BF16), vm((T, HEAD), BF16), vm((T, HEAD), BF16), vm((T, wide), BF16), vm((N_Q, T), BF16),
        vm((T, HALF), F32), vm((T, HALF), F32), vm((KV, GROUP, T), F32), vm((KV, GROUP, T), F32), vm((4, STRIDE, HALF), F32),
        sem.DMA, sem.DMA, *(sem.DMA(shape) for shape in ((2, 3), (SLOTS, 2), (2, 3), (2,))), sem.DMA, sem.DMA((3,)), sem.DMA, sem.DMA((2,)), sem.DMA((7,)),
        *(sem.DMA((SLOTS, CHIPS)) for _ in range(12)),
        sem.REGULAR, sem.REGULAR, sem.REGULAR,
    ]
    refs = [*w, *m, *v, *(given[name] for name in INPUTS)]
    pair = [(FF, T), (T, D), (T, wide), (D, T), (N_Q, T), (D, T), (T, D), (T, D), (T, N_Q), (T, wide)]
    shapes = [(CHUNKS, 8, *block), (CHUNKS, *block), (2, 2, *block), *((2, *shape) for shape in pair)]
    outs = [*((shape, BF16) for shape in shapes), ((2, KV, GROUP, T), F32), ((T, D), BF16), ((T, D), BF16)]
    return pl.pallas_call(
        _update,
        in_specs=[pl.BlockSpec(memory_space=pl.ANY)] * len(refs),
        out_specs=[pl.BlockSpec(memory_space=pl.ANY)] * len(outs),
        out_shape=[jax.ShapeDtypeStruct(*out) for out in outs],
        scratch_shapes=scratch,
        compiler_params=pltpu.CompilerParams(collective_id=0, has_side_effects=True, vmem_limit_bytes=63 * 2**20),
        name="update",
    )(*refs)[:3]


def _moments(m, v, g):
    return 0.9 * m + 0.1 * g, 0.95 * v + 0.05 * g * g


LATE = ("wk", "wv")


def _unpack(*refs):
    s = pl.program_id(1)
    refs = list(refs)
    ins = [[refs.pop(0) for _ in range(3 if name in LATE else 4)] for name in NAMES]
    for i, name in enumerate(NAMES):
        gp_ref, m_ref, v_ref = ins[i][:3]
        w_out = None if name in LATE else refs.pop(0)
        m_out, v_out = refs[i - 2 * len(NAMES)], refs[i - len(NAMES)]
        tall = name in ("w_down", "wo")
        rows, cols = Q_BLOCK if tall else P_BLOCK
        some = m_ref.shape[1]
        for j in range(cols // LANES):
            for n in range(gp_ref.shape[0]):
                over = part_of(j, LANES) if tall else slice(cols * n + LANES * j, cols * n + LANES * (j + 1))
                down = part_of(n, rows) if tall else slice(0, rows)
                if w_out is not None:
                    w_out[0, down, over] = ins[i][3][n, 0, part_of(j, rows), :]
                if tall and n:
                    continue
                if tall:
                    per = rows // some
                    g = gp_ref[s // per if name == "wo" else jnp.minimum(s, 6), pl.ds(pl.multiple_of(rows * j + some * (s % per), 16), some), :]
                else:
                    g = gp_ref[n, pl.ds(pl.multiple_of(rows * j + some * jnp.minimum(s, 6), 16), some), :]
                m_out[0, :, over], v_out[0, :, over] = _moments(m_ref[0, :, over], v_ref[0, :, over], g.astype(F32))


def unpack(wp, gp, m, v):
    block = (BLOCK, LANES)
    where = {name: (TILES, 2 * i, 1) for i, name in enumerate(("w_gate", "w_up", "w_down"))}
    at = 3 * DOWN_AT
    for name, count in (("wo", 2), ("wq", 2), ("wk", 1), ("wv", 1)):
        where[name] = (count, at // count, (PER_LAYER - WO_AT) // count)
        at += count
    in_specs, given, full, own_m, own_v = [], [], {}, [], []
    for name in NAMES:
        count, start, step = where[name]
        _, height, width = m[name].shape
        some = Q_BLOCK[0] if name == "w_down" else 16
        last = height // some - 1
        mine = pl.BlockSpec((1, some, width), lambda layer, s, last=last: (layer, jnp.minimum(s, last), 0))
        in_specs += [pl.BlockSpec((count, *block), lambda layer, s, start=start, step=step: (start + step * layer, 0, 0)), mine, mine]
        given += [gp, m[name], v[name]]
        if name not in LATE:
            in_specs.append(pl.BlockSpec((count, 1, *block), lambda layer, s, start=start, step=step: (start + step * layer, s, 0, 0)))
            given.append(wp)
            full[name] = (pl.BlockSpec((1, height, width), lambda layer, s: (layer, s, 0)), jax.ShapeDtypeStruct((2, 8 * height, width), BF16))
        own_m.append((mine, jax.ShapeDtypeStruct(m[name].shape, F32)))
    outs = [*full.values(), *own_m, *own_m]
    got = pl.pallas_call(
        _unpack,
        grid=(2, 8),
        in_specs=in_specs,
        out_specs=[o[0] for o in outs],
        out_shape=[o[1] for o in outs],
        compiler_params=pltpu.CompilerParams(vmem_limit_bytes=VMEM),
        cost_estimate=pl.CostEstimate(flops=10**11, bytes_accessed=155 * 2**20, transcendentals=0),
        name="unpack",
    )(*given)
    n = len(full)
    return dict(zip(full, got)), got[n : n + len(NAMES)], got[n + len(NAMES) :]


def _finish(me_ref, *refs):
    came, packed, outs = refs[:CHIPS], refs[CHIPS : CHIPS + 2], refs[CHIPS + 2 :]
    rows, cols = P_BLOCK
    for which, out in enumerate(outs):
        for j in range(cols // LANES):
            at, over = part_of(j, rows), part_of(j, LANES)
            for n in range(2 * CHIPS):
                i, core = n // 2, n % 2
                owner = (me_ref[0] // 2 + CHIPS - i) % CHIPS * 2 + core
                out[0, pl.ds(pl.multiple_of(rows * owner, 16), rows), over] = came[i][core, which, at, :]
                out[1, part_of(n, rows), over] = packed[which][0, n, at, :]


def finish(last, wp):
    me, n = lax.axis_index("dp"), 2 * CHIPS
    came = [last] + [lax.ppermute(last, "dp", [(s, (s + 2 * i) % n) for s in range(n)]) for i in range(1, CHIPS)]
    block, (rows, cols) = (BLOCK, LANES), P_BLOCK
    whole = lambda *shape: pl.BlockSpec(shape, lambda i, _: (0,) * len(shape))
    layer_1 = [pl.BlockSpec((1, n, *block), lambda i, _, at=at: (at, 0, 0, 0)) for at in (SPREAD, SPREAD + 1)]
    shape = (2, n * rows, cols)
    return pl.pallas_call(
        _finish,
        grid_spec=pltpu.PrefetchScalarGridSpec(
            num_scalar_prefetch=1, grid=(1,), in_specs=[whole(*last.shape)] * CHIPS + layer_1, out_specs=[whole(*shape)] * 2
        ),
        out_shape=[jax.ShapeDtypeStruct(shape, BF16)] * 2,
        compiler_params=pltpu.CompilerParams(vmem_limit_bytes=VMEM // 2),
        name="finish",
    )(me.reshape(1).astype(jnp.int32), *came, wp, wp)


def solution(mesh):
    angle = np.arange(STRIDE)[:, None] * float(THETA) ** (-np.arange(HALF) / HALF)
    turns = np.stack([turn(angle * step) for step in (STRIDE, 1) for turn in (np.cos, np.sin)]).astype(np.float32)

    def step(x, dy, *arrays):
        w, m, v = (dict(zip(NAMES, some, strict=True)) for some in (arrays[:n], arrays[n : 2 * n], arrays[2 * n :]))
        wp, gp, last = update({"x": x[0], "dy": dy[0], "turns": jnp.asarray(turns)}, w.values(), m.values(), v.values())
        new, new_m, new_v = unpack(wp, gp, m, v)
        new |= dict(zip(LATE, finish(last, wp)))
        return (*(new[name] for name in NAMES), *new_m, *new_v)

    n = len(NAMES)
    return jax.shard_map(
        step,
        mesh=mesh,
        in_specs=(P(("rep", "dp")),) * 2 + (P(),) * n + (P(None, "dp"),) * (2 * n),
        out_specs=(P("rep"),) * n + (P("rep", "dp"),) * (2 * n),
        check_vma=False,
    )
```

```python
import functools

import jax
import jax.numpy as jnp
import numpy as np
from jax import lax
from jax.experimental import pallas as pl
from jax.experimental.pallas import tpu as pltpu
from jax.sharding import PartitionSpec as P

LOG2E = 1.4426950408889634
HIDDEN = float("-inf")
VMEM = 56 * 2**20
F32, BF16 = jnp.float32, jnp.bfloat16
MESH = pl.DeviceIdType.MESH
T, D, FF, HEADS, KV, HEAD = 1024, 896, 3584, 4, 2, 256
THETA = 10000
STRIDE = 32
NAMES = ("wq", "wk", "wv", "wo", "w_gate", "w_up", "w_down")
ROWS = 256
TF = 512
PIECES = T // ROWS


def loop(count, body):
    lax.fori_loop(0, count, lambda i, _: body(i), None)


def dot(a, b):
    return jnp.dot(a, b, preferred_element_type=F32)


def dot_t(a, b):
    return lax.dot_general(a, b, (((1,), (1,)), ((), ())), preferred_element_type=F32)


def _scale(wide):
    return lax.rsqrt(jnp.mean(wide * wide, -1, keepdims=True) + 1e-6)


def _norm_back(h, by):
    s = _scale(h)
    return by * s - h * (s * s * s * jnp.mean(by * h, -1, keepdims=True))


E = HEAD**-0.5 * LOG2E
GROUP = HEADS // KV


def part_of(i, size):
    return slice(size * i, size * (i + 1))


def _piece(i):
    return part_of(i, ROWS)


def _visible():
    shape = (ROWS, GROUP * ROWS)
    return lax.broadcasted_iota(jnp.int32, shape, 0) <= lax.rem(lax.broadcasted_iota(jnp.int32, shape, 1), ROWS)


LANES = 128
BLOCK = 448
SLOTS = 4
SUMS = 5
EARLY = 1
LAG = 27
P_BLOCK, Q_BLOCK = (112, 512), (64, 896)
TILES = FF // TF
DOWN_AT, WO_AT, QKV_AT, PER_LAYER = 14, 21, 23, 27
CHUNKS = 2 * PER_LAYER
SPREAD = CHUNKS - 2
TICKS = CHUNKS + 6 + EARLY
CHIPS = 4
MATE_ORDER = (3, 0, 2, 1)
QKV_ORDER = (1, 3, 0, 2)
HALF, T_HALF = HEAD // 2, T // 2
N_Q, N_K = HEADS * HEAD, KV * HEAD
BEFORE, LEAVE, HEADS_AT, AFTER = 13, 14, 15, 18


def _is_q(r):
    return (r >= DOWN_AT) & (r < QKV_AT)


def _place(k):
    layer, r = 1 - k // PER_LAYER, k % PER_LAYER
    double, single = (r % 2) * DOWN_AT + layer * TILES + r // 2, 2 * DOWN_AT + layer * TILES + r - DOWN_AT
    return jnp.where(r < DOWN_AT, double, jnp.where(r < WO_AT, single, 3 * DOWN_AT + layer * (PER_LAYER - WO_AT) + r - WO_AT))


def _owners(layer, r):
    mlp_chunk = r < DOWN_AT
    return (
        ("w_gate", mlp_chunk & (r % 2 == 0), r // 2), ("w_up", mlp_chunk & (r % 2 == 1), r // 2),
        ("w_down", (r >= DOWN_AT) & (r < WO_AT), r - DOWN_AT), ("wo", (r >= WO_AT) & (r < QKV_AT), r - WO_AT),
        ("wq", (r >= QKV_AT) & (r < QKV_AT + 2), r - QKV_AT), ("wk", r == QKV_AT + 2, 0 * r), ("wv", r == QKV_AT + 3, 0 * r),
    )


INPUTS = ("x", "dy", "turns")
OUTPUTS = ("wp", "gp", "last", "hidt", "d1", "dqkv", "at", "ot", "bt", "b", "h1", "o", "qkv", "lse", "h", "by1")
SCRATCH = ("ab", "db", "chip", "ps", "pr", "su", "ru", "sd", "rd", "wn", "gn", "mb", "vb", "wb", "x1", "x2", "oo", "wg", "wu", "wd", "acc", "dg", "du", "ht",
           "qq", "kk", "vv", "dq", "st", "cosb", "sinb", "lseb", "delta", "tb",
           "ab_sem", "db_sem", "opt_sem", "out_sem", "tile_sem", "x_sem", "o_sem", "qkv_sem", "lse_sem", "write_sem", "save_sem",
           "ps_s", "ps_r", "su_s", "su_r", "sd_s", "sd_r", "am_s", "am_r", "au_s", "au_r", "ad_s", "ad_r", "free_m", "free_u", "free_d")


def _update(*refs):
    count = len(NAMES)
    w_in, m_in, v_in = (dict(zip(NAMES, some)) for some in (refs[:count], refs[count : 2 * count], refs[2 * count :]))
    r_ = dict(zip((*INPUTS, *OUTPUTS, *SCRATCH), refs[3 * count :], strict=True))
    (ab, db, chip, ps, pr, su, ru, sd, rd, wn, gn, mb, vb, wb, x1, x2, oo, wg, wu, wd, acc, dg, du, ht, qq, kk, vv, dq, st, cosb, sinb, lseb, delta, tb,
     ab_sem, db_sem, opt_sem, out_sem, tile_sem, x_sem, o_sem, qkv_sem, lse_sem, write_sem, save_sem,
     ps_s, ps_r, su_s, su_r, sd_s, sd_r, am_s, am_r, au_s, au_r, ad_s, ad_r, free_m, free_u, free_d) = (r_[name] for name in SCRATCH)
    wp, gp = r_["wp"], r_["gp"]
    any_block = wp.at[0, 0]
    rep, me = lax.axis_index("rep"), lax.axis_index("dp")
    z, core = me // 2, me % 2
    mate, above, below = me + 1 - 2 * core, me + 2, me - 2
    has_above, has_below = z < CHIPS - 1, z > 0

    def remote(src, dst, send, recv, to):
        return pltpu.make_async_remote_copy(src_ref=src, dst_ref=dst, send_sem=send, recv_sem=recv, device_id=(rep, to), device_id_type=MESH)

    def tell(sem, to):
        pl.semaphore_signal(sem, inc=1, device_id=(rep, to), device_id_type=MESH)

    def local(src, dst, sem):
        return pltpu.make_async_copy(src, dst, sem)

    def ok(k):
        return (k >= 0) & (k < CHUNKS)

    def spread_here(k):
        return (k >= 0) & (k < SPREAD)

    def for_mate(k, s):
        return spread_here(k) | (ok(k) & (s == z))

    def wait_of(s):
        return 3 + ((s == 0) | (s == CHIPS - 1)).astype(jnp.int32)

    mine = wait_of(z)

    def tokens(start, count):
        return pl.ds(pl.multiple_of(start, ROWS), count)


    def tile_copies(half, j, buf):
        layer, over = 1 - half, pl.ds(pl.multiple_of(TF * j, TF), TF)
        return [
            local(w_in["w_gate"].at[layer, :, over], wg.at[buf], tile_sem.at[buf, 0]),
            local(w_in["w_up"].at[layer, :, over], wu.at[buf], tile_sem.at[buf, 1]),
            local(w_in["w_down"].at[layer, over, :], wd.at[buf], tile_sem.at[buf, 2]),
        ]

    def wo_copies(half):
        return [local(w_in["wo"].at[1 - half, pl.ds(TF * n, TF), :], wd.at[n], tile_sem.at[n, 2]) for n in range(2)]

    def qkv_weight_copies(half):
        layer = 1 - half
        return [
            *(local(w_in["wq"].at[layer, :, pl.ds(TF * n, TF)], wg.at[n], tile_sem.at[n, 0]) for n in range(2)),
            local(w_in["wk"].at[layer], wu.at[0], tile_sem.at[0, 1]), local(w_in["wv"].at[layer], wu.at[1], tile_sem.at[1, 1]),
        ]

    def column(at):
        return pl.ds(pl.multiple_of(at, HEAD), HEAD)

    def head_copies(half, head):
        pair = pl.ds(pl.multiple_of(GROUP * HEAD * head, GROUP * HEAD), GROUP * HEAD)
        return [
            local(r_["qkv"].at[half, :, over], to, qkv_sem.at[n])
            for n, (over, to) in enumerate(((pair, qq), (column(N_Q + HEAD * head), kk), (column(N_Q + N_K + HEAD * head), vv)))
        ]

    def load_x2(ref):
        return local(ref, x2, x_sem.at[1])

    def unit_of(n):
        half = (n >= AFTER + 2 + EARLY).astype(jnp.int32)
        return half, n - EARLY - LAG * half

    def start(copies):
        for copy in copies:
            copy.start()

    def wait(copies):
        for copy in copies:
            copy.wait()

    def writes(half, tau):
        u = tau + EARLY
        j, first = u // 2, tokens(T_HALF * (u % 2), T_HALF)
        over = pl.ds(pl.multiple_of(TF * j, TF), TF)
        part = tokens(T_HALF * (tau - AFTER), T_HALF)
        after_at = (tau >= AFTER) & (tau < AFTER + 2)
        return (
            ((u >= 0) & (u < 2 * TILES), lambda: [local(ht, r_["hidt"].at[half, over, first], write_sem.at[0])]),
            (tau == LEAVE, lambda: [local(x1, r_["d1"].at[half], write_sem.at[0])]),
            (after_at, lambda: [local(dq.at[part, :], r_["dqkv"].at[half, part, :], write_sem.at[0])]),
            (after_at & (half == 0), lambda: [local(x1.at[part, :], r_["by1"].at[part, :], write_sem.at[1])]),
        )

    def fetch(n):
        half, tau = unit_of(n)
        u = tau + EARLY

        @pl.when((tau == -EARLY - 1) & (half == 1))
        def _():
            start([*tile_copies(half, 0, 0), load_x2(r_["b"].at[half])])

        @pl.when((u >= 0) & (u % 2 == 0) & (u < 2 * TILES - 2))
        def _():
            start(tile_copies(half, u // 2 + 1, (u // 2 + 1) % 2))

        @pl.when(tau == BEFORE)
        def _():
            start([*wo_copies(half), load_x2(r_["h1"].at[half]), local(r_["o"].at[half], oo, o_sem)])

        @pl.when(tau == LEAVE)
        def _():
            start([*head_copies(half, 0), local(r_["lse"].at[half], lseb, lse_sem)])

        @pl.when(tau == HEADS_AT + 1)
        def _():
            start(head_copies(half, 1))

        @pl.when((tau == BEFORE) & (half == 0))
        def _():
            start(tile_copies(0, 0, 0)[:2])

        @pl.when((tau == LEAVE) & (half == 0))
        def _():
            start(qkv_weight_copies(0))

        @pl.when((tau == HEADS_AT) & (half == 0))
        def _():
            start([load_x2(r_["h"])])

    def mlp_unit(u, buf, later):
        rows = tokens(T_HALF * (u % 2), T_HALF)
        gate, up = dot(x2[rows, :], wg[buf]), dot(x2[rows, :], wu[buf])
        sig = 1.0 / (1.0 + jnp.exp(-gate))
        silu = gate * sig
        by = dot_t(x1[rows, :], wd[buf]).astype(BF16).astype(F32)
        ht[...] = (silu * up).astype(BF16).T
        du[buf, rows, :] = (by * silu).astype(BF16)
        dg[buf, rows, :] = (by * up * (sig * (1.0 + gate * (1.0 - sig)))).astype(BF16)

        @pl.when(jnp.logical_not(later))
        def _():
            acc[rows, :] += dot_t(dg[buf, rows, :], wg[buf]) + dot_t(du[buf, rows, :], wu[buf])

    def late_unit(i):
        rows = tokens(ROWS * i, ROWS)
        acc[rows, :] += dot_t(st[rows, :TF], wg[0]) + dot_t(st[rows, TF:], wu[0])

    def leave_unit(i):
        rows = tokens(ROWS * i, ROWS)
        inner = _norm_back(x2[rows, :].astype(F32), acc[rows, :].astype(BF16).astype(F32)).astype(BF16)
        d1 = (x1[rows, :].astype(F32) + inner.astype(F32)).astype(BF16)
        x1[rows, :] = d1
        for n in range(HEADS):
            low, over = HEAD * (n % 2), _piece(n)
            do = dot_t(d1, wd[n // 2, low : low + HEAD, :]).astype(BF16)
            both = do.astype(F32) * oo[rows, over].astype(F32)
            oo[rows, over] = do
            delta[n // GROUP, n % GROUP : n % GROUP + 1, rows] = both.T.sum(0, keepdims=True)

    def side(ref, i, head):
        return jnp.concatenate([ref[_piece(i), column(HEAD * (GROUP * head + n))] for n in range(GROUP)], axis=0)

    def turn_back(part, rows):
        cos, sin = cosb[rows, :], sinb[rows, :]
        x, y = part[:, :HALF].astype(F32), part[:, HALF:].astype(F32)
        return jnp.concatenate([x * cos + y * sin, y * cos - x * sin], -1).astype(BF16)

    def head_unit(head):
        seen = _visible()
        turned = kk[...].T
        line = lambda ref, i: jnp.concatenate([ref[head, n : n + 1, _piece(i)] for n in range(GROUP)], axis=1)
        dk_at, dv_at = slice(0, HEAD), slice(HEAD, 2 * HEAD)
        for i in range(PIECES):
            lse, dl = line(lseb, i), line(delta, i)
            q = jnp.concatenate([qq[_piece(i), _piece(n)] for n in range(GROUP)], axis=0)
            do = side(oo, i, head)
            by_q = 0.0
            for j in range(i + 1):
                at = _piece(j)
                p = jnp.exp2(dot_t(kk[at, :], q) * E - lse)
                if j == i:
                    p = jnp.where(seen, p, 0.0)
                ds = (p * (dot_t(vv[at, :], do) - dl)).astype(BF16)
                by_v, by_k = dot(p.astype(BF16), do), dot(ds, q)
                acc[at, dv_at] = by_v if j == i else acc[at, dv_at] + by_v
                acc[at, dk_at] = by_k if j == i else acc[at, dk_at] + by_k
                by_q = by_q + dot(turned[:, at], ds)
            by_q = (by_q * HEAD**-0.5).astype(BF16)
            for n in range(GROUP):
                dq[_piece(i), column(HEAD * (GROUP * head + n))] = turn_back(by_q[:, _piece(n)].T, _piece(i))
        for i in range(PIECES):
            dq[_piece(i), column(N_Q + HEAD * head)] = turn_back((acc[_piece(i), dk_at] * HEAD**-0.5).astype(BF16), _piece(i))
            dq[_piece(i), column(N_Q + N_K + HEAD * head)] = acc[_piece(i), dv_at].astype(BF16)

    def after_unit(rows):
        by = sum(dot_t(dq[rows, part_of(n, TF)], (wg, wu)[n // 2][n % 2]) for n in range(4)).astype(BF16).astype(F32)
        inner = _norm_back(x2[rows, :].astype(F32), by).astype(BF16)
        x1[rows, :] = (x1[rows, :].astype(F32) + inner.astype(F32)).astype(BF16)

    def work(n):
        half, tau = unit_of(n)
        u = tau + EARLY

        @pl.when((u >= 0) & (u < 2 * TILES))
        def _():
            buf = u // 2 % 2

            @pl.when(u % 2 == 0)
            def _():
                wait(tile_copies(half, u // 2, buf))

            @pl.when((u == 0) & (half == 1))
            def _():
                acc[...] = jnp.zeros((T, D), F32)
                load_x2(r_["h"]).wait()

            mlp_unit(u, buf, (half == 0) & (u < 2))

            @pl.when((half == 0) & (u == 1))
            def _():
                st[:, :TF] = dg[0]
                st[:, TF:] = du[0]

        @pl.when((tau == BEFORE) & (half == 0))
        def _():
            wait(tile_copies(0, 0, 0)[:2])
            loop(PIECES, late_unit)

        @pl.when(tau == LEAVE)
        def _():
            wait([load_x2(r_["h"]), local(r_["o"].at[0], oo, o_sem), *wo_copies(half)])
            loop(PIECES, leave_unit)

        @pl.when((tau == HEADS_AT) | (tau == HEADS_AT + 2))
        def _():
            @pl.when(tau == HEADS_AT)
            def _():
                local(r_["lse"].at[0], lseb, lse_sem).wait()

            wait(head_copies(0, 0))
            head_unit((tau - HEADS_AT) // 2)

        @pl.when((tau >= AFTER) & (tau < AFTER + 2) & (half == 0))
        def _():
            @pl.when(tau == AFTER)
            def _():
                wait([load_x2(r_["h"]), *qkv_weight_copies(0)])

            loop(PIECES // 2, lambda i: after_unit(tokens(T_HALF * (tau - AFTER) + ROWS * i, ROWS)))

        for test, copies in writes(half, tau):
            pl.when(test)(lambda: start(copies()))


    def load_operands(k):
        half, r = k // PER_LAYER, k % PER_LAYER

        def from_rows(ref, block, down):
            rows, whole = block[0], ref.shape[0] // 8
            for e in range(8):
                owner = 2 * (e % 4) + (1 - core if e < 4 else core)
                at = pl.multiple_of(whole * owner + down, 16)
                local(ref.at[pl.ds(at, rows), :], ab.at[pl.ds(rows * e, rows), :], ab_sem).start()

        @pl.when(r < DOWN_AT)
        def _():
            from_rows(r_["bt"].at[half], P_BLOCK, 0)

        @pl.when((r >= DOWN_AT) & (r < WO_AT))
        def _():
            from_rows(r_["hidt"].at[half], Q_BLOCK, Q_BLOCK[0] * (r - DOWN_AT))

            @pl.when(half == 0)
            def _():
                local(r_["dy"], db, db_sem).start()

            @pl.when(half == 1)
            def _():
                local(r_["by1"], db, db_sem).start()

        @pl.when((r >= WO_AT) & (r < QKV_AT))
        def _():
            from_rows(r_["ot"].at[half], Q_BLOCK, Q_BLOCK[0] * (r - WO_AT))
            local(r_["d1"].at[half], db, db_sem).start()

        @pl.when(r >= QKV_AT)
        def _():
            from_rows(r_["at"].at[half], P_BLOCK, 0)
            local(r_["dqkv"].at[half, :, pl.ds(pl.multiple_of(TF * (r - QKV_AT), TF), TF)], db.at[:, pl.ds(0, TF)], db_sem).start()

    def wait_operands(block, r):
        rows, cols = block
        local(r_["hidt"].at[0, pl.ds(0, 8 * rows), :], ab.at[pl.ds(0, 8 * rows), :], ab_sem).wait()

        @pl.when(r >= DOWN_AT)
        def _():
            local(r_["dqkv"].at[0, :, pl.ds(0, cols)], db.at[:, pl.ds(0, cols)], db_sem).wait()

        for which, ref in enumerate((dg, du)):
            @pl.when((r < DOWN_AT) & (r % 2 == which))
            def _():
                db[:, :TF] = ref[r // 2 % 2]

    def optimizer_copies(k, buf, do):
        layer, r = 1 - k // PER_LAYER, k % PER_LAYER
        for name, test, j in _owners(layer, r):
            rows, cols = block = Q_BLOCK if name in ("w_down", "wo") else P_BLOCK

            @pl.when(test)
            def _():
                whole = w_in[name].shape[1] // 8
                down = pl.multiple_of(rows * j if block == Q_BLOCK else 0 * j, 16)
                right = pl.ds(0, cols) if block == Q_BLOCK else pl.ds(pl.multiple_of(cols * j, cols), cols)
                for n, (ref, at, to) in enumerate(((m_in[name], down, mb), (v_in[name], down, vb), (w_in[name], pl.multiple_of(whole * me + down, 16), wb))):
                    do(local(ref.at[layer, pl.ds(at, rows), right], to.at[buf, pl.ds(0, rows), pl.ds(0, cols)], opt_sem.at[buf, n]))


    def save(n, source, to):
        return local(source, to, save_sem.at[n])

    def attend_head(head):
        seen = _visible()
        k_at, turned = column(N_Q + HEAD * head), dq[:, column(N_Q + N_K + HEAD * head)].T

        def scores_of(i):
            q = side(dq, i, head)
            scores = [dot_t(dq[_piece(j), k_at], q) for j in range(i + 1)]
            return [*scores[:i], jnp.where(seen, scores[i], HIDDEN)]

        coming = scores_of(0)
        for i in range(PIECES):
            scores, coming = coming, scores_of(i + 1) if i + 1 < PIECES else None
            top = functools.reduce(jnp.maximum, [s.max(axis=0, keepdims=True) for s in scores])
            total, mix = 0.0, 0.0
            for j, s in enumerate(scores):
                p = jnp.exp2((s - top) * E)
                total = total + p.sum(axis=0, keepdims=True)
                mix = mix + dot(turned[:, _piece(j)], p.astype(BF16))
            out = (mix * (1.0 / total)).astype(BF16)
            lse = top * E + jnp.log(total) * LOG2E
            for n in range(GROUP):
                over = column(HEAD * (GROUP * head + n))
                st[over, _piece(i)] = out[:, _piece(n)]
                oo[_piece(i), over] = out[:, _piece(n)].T
                lseb[head, n : n + 1, _piece(i)] = lse[:, _piece(n)]

    def saves(half):
        kept = lambda name: r_[name].at[half]
        return [
            save(0, ab, kept("bt")), save(1, dq.at[:, pl.ds(0, D)], kept("h1")), save(2, x2, kept("b")),
            save(3, st, kept("ot")), save(4, oo, kept("o")), save(5, lseb, kept("lse")),
        ]

    by_y, by_h = local(r_["dy"], x1, x_sem.at[0]), save(6, x1, r_["h"])

    def forward(layer):
        half = 1 - layer
        weights = qkv_weight_copies(half)
        early = [save(0, ab, r_["at"].at[half]), save(1, dq, r_["qkv"].at[half])]
        for i in range(PIECES):
            x2[_piece(i), :] = x1[_piece(i), :]
            wide = x1[_piece(i), :].astype(F32)
            a = (wide * _scale(wide)).astype(BF16)
            ab[:, _piece(i)] = a.T
            cos, sin = cosb[_piece(i), :], sinb[_piece(i), :]
            for c in QKV_ORDER:
                if i == 0:
                    weights[c].wait()
                t = dot(a, (wg, wu)[c // 2][c % 2]).astype(BF16)
                for n in range(2):
                    part = t[:, _piece(n)]
                    if c < 3:
                        p, q = part[:, :HALF].astype(F32), part[:, HALF:].astype(F32)
                        part = jnp.concatenate([p * cos - q * sin, q * cos + p * sin], -1).astype(BF16)
                    dq[_piece(i), TF * c + HEAD * n : TF * c + HEAD * (n + 1)] = part
        wo = local(w_in["wo"].at[layer], db, db_sem)
        start([*early, wo, *tile_copies(half, 0, 0)])

        @pl.when(layer == 1)
        def _():
            by_h.wait()
            by_y.start()

        loop(KV, attend_head)
        wait([*early, wo])
        start(saves(half)[3:])

        projected = lambda i: dot(oo[_piece(i), :], db[...])
        coming = projected(0)
        for i in range(PIECES):
            rows = _piece(i)
            total, coming = coming, projected(i + 1) if i + 1 < PIECES else None
            h1 = (x2[rows, :].astype(F32) + total.astype(BF16).astype(F32)).astype(BF16)
            dq[rows, :D] = h1
            wide = h1.astype(F32)
            b = (wide * _scale(wide)).astype(BF16)
            x2[rows, :] = b
            ab[:, rows] = b.T
        start(saves(half)[:3])

        @pl.when(layer == 0)
        def _():
            acc[...] = jnp.zeros((T, D), F32)
            coming = qkv_weight_copies(0)

            def one(j):
                buf = j % 2

                @pl.when(j < TILES - 1)
                def _():
                    start(tile_copies(half, j + 1, 1 - buf))

                @pl.when(j == TILES - 1)
                def _():
                    start([coming[c] for c in QKV_ORDER[:2]])

                wait(tile_copies(half, j, buf))
                for i in range(2):
                    rows = part_of(i, T_HALF)
                    gate, up = dot(x2[rows, :], wg[buf]), dot(x2[rows, :], wu[buf])
                    hidden = (gate * (1.0 / (1.0 + jnp.exp(-gate))) * up).astype(BF16)
                    acc[rows, :] += dot(hidden, wd[buf])

            loop(TILES, one)
            start([coming[c] for c in QKV_ORDER[2:]])
            wait(saves(half))
            for i in range(PIECES):
                x1[_piece(i), :] = (dq[_piece(i), :D].astype(F32) + acc[_piece(i), :].astype(BF16).astype(F32)).astype(BF16)
                acc[_piece(i), :] = jnp.zeros((ROWS, D), F32)
            by_h.start()

    first = [local(r_["x"], x1, x_sem.at[0]), local(r_["turns"], tb, o_sem)]
    start([*first, *(qkv_weight_copies(1)[c] for c in QKV_ORDER)])


    barrier = pltpu.get_barrier_semaphore()
    tell(barrier, mate)

    @pl.when(has_above)
    def _():
        tell(barrier, above)

    @pl.when(has_below)
    def _():
        tell(barrier, below)

    wait(first)

    def spin(a):
        rows = pl.ds(pl.multiple_of(STRIDE * a, STRIDE), STRIDE)
        cos_a, sin_a, cos_b, sin_b = tb[0, pl.ds(a, 1), :], tb[1, pl.ds(a, 1), :], tb[2], tb[3]
        cosb[rows, :] = cos_a * cos_b - sin_a * sin_b
        sinb[rows, :] = sin_a * cos_b + cos_a * sin_b

    loop(T // STRIDE, spin)
    loop(2, forward)
    @pl.when(has_above & has_below)
    def _():
        pl.semaphore_wait(barrier, 3)

    @pl.when(jnp.logical_not(has_above & has_below))
    def _():
        pl.semaphore_wait(barrier, 2)

    by_y.wait()

    def sent(n):
        t, late = n - 3 - EARLY, (n + 1) % SLOTS

        @pl.when(ok(t))
        def _():
            for s in range(CHIPS):
                remote(ps.at[late, s], pr.at[late, s], ps_s.at[late, s], ps_r.at[late, s], mate).wait_send()

        @pl.when(ok(t - 1 - z))
        def _():
            for s in range(1, CHIPS):
                @pl.when(s > z)
                def _():
                    remote(su.at[late, s], ru.at[late, s], su_s.at[late, s], su_r.at[late, s], mate).wait_send()

        @pl.when(ok(t - 1 - (CHIPS - 1 - z)))
        def _():
            for s in range(CHIPS - 1):
                @pl.when(s < z)
                def _():
                    remote(sd.at[late, s], rd.at[late, s], sd_s.at[late, s], sd_r.at[late, s], mate).wait_send()

        def gone(s):
            k = t - wait_of(s) - jnp.abs(z - s)
            there = any_block

            @pl.when(for_mate(k, s))
            def _():
                remote(there, there, am_s.at[late, s], am_r.at[late, s], mate).wait_send()

            @pl.when(spread_here(k) & (s <= z) & has_above)
            def _():
                remote(there, there, au_s.at[late, s], au_r.at[late, s], mate).wait_send()

            @pl.when(spread_here(k) & (s >= z) & has_below)
            def _():
                remote(there, there, ad_s.at[late, s], ad_r.at[late, s], mate).wait_send()

        loop(CHIPS, gone)

        @pl.when(ok(t - mine))
        def _():
            local(wn.at[late], any_block, out_sem.at[late, 0]).wait()
            local(gn.at[late], gp.at[0], out_sem.at[late, 1]).wait()

    def tick(n):
        t = n - EARLY
        slot, prev = n % SLOTS, (n + SLOTS - 1) % SLOTS
        two = n % 2


        @pl.when(n >= 3)
        def _():
            pl.semaphore_wait(free_m, 1)

            @pl.when(has_above)
            def _():
                pl.semaphore_wait(free_u, 1)

            @pl.when(has_below)
            def _():
                pl.semaphore_wait(free_d, 1)

            sent(n)


        @pl.when(n == EARLY)
        def _():
            wait(saves(0))
            load_operands(0)

        for test, copies in writes(*unit_of(n - 1)):
            pl.when(test & (n > 0))(lambda: wait(copies()))
        fetch(n)

        @pl.when(ok(t + 1 - mine))
        def _():
            optimizer_copies(t + 1 - mine, 1 - two, lambda copy: copy.start())


        @pl.when(ok(t - 1))
        def _():
            for s in MATE_ORDER:
                remote(ps.at[prev, s], pr.at[prev, s], ps_s.at[prev, s], ps_r.at[prev, s], mate).wait_recv()
                value = chip[(t - 1) % SUMS, s] + pr[prev, s].astype(F32)
                chip[(t - 1) % SUMS, s] = value
                if s > 0:
                    @pl.when(z == 0)
                    def _():
                        su[slot, s] = value.astype(BF16)
                        remote(su.at[slot, s], ru.at[slot, s], su_s.at[slot, s], su_r.at[slot, s], above).start()
                if s < CHIPS - 1:
                    @pl.when(z == CHIPS - 1)
                    def _():
                        sd[slot, s] = value.astype(BF16)
                        remote(sd.at[slot, s], rd.at[slot, s], sd_s.at[slot, s], sd_r.at[slot, s], below).start()


        def pass_on(s, k, from_above):
            got, send, here, there, to = (rd, sd, sd_s, sd_r, below) if from_above else (ru, su, su_s, su_r, above)
            remote(send.at[prev, s], got.at[prev, s], here.at[prev, s], there.at[prev, s], mate).wait_recv()
            value = chip[k % SUMS, s] + got[prev, s].astype(F32)
            chip[k % SUMS, s] = value
            send[slot, s] = value.astype(BF16)

            @pl.when((s < z) if from_above else (s > z))
            def _():
                remote(send.at[slot, s], got.at[slot, s], here.at[slot, s], there.at[slot, s], to).start()

        up_k, down_k = t - 1 - z, t - 1 - (CHIPS - 1 - z)
        for i in range(CHIPS - 1):
            @pl.when(has_below & ok(up_k) & (CHIPS - 1 - i >= z))
            def _():
                pass_on(CHIPS - 1 - i, up_k, False)

            @pl.when(has_above & ok(down_k) & (i <= z))
            def _():
                pass_on(i, down_k, True)


        @pl.when(ok(t - mine))
        def _():
            k = t - mine
            optimizer_copies(k, two, lambda copy: copy.wait())
            is_q = _is_q(k % PER_LAYER)
            for (rows, cols), test in ((Q_BLOCK, is_q), (P_BLOCK, jnp.logical_not(is_q))):
                @pl.when(test)
                def _():
                    for j in range(cols // LANES):
                        at, over = part_of(j, rows), part_of(j, LANES)
                        low = chip[k % SUMS, z, at, :].astype(BF16)
                        m, v = _moments(mb[two, :rows, over], vb[two, :rows, over], low.astype(F32))
                        w = wb[two, :rows, over].astype(F32)
                        wn[slot, at, :] = (w - 0.02 * (m * lax.rsqrt(v + 1e-8) + 0.1 * w)).astype(BF16)
                        gn[slot, at, :] = low

            local(gn.at[slot], gp.at[_place(k)], out_sem.at[slot, 1]).start()

            @pl.when(k < SPREAD)
            def _():
                local(wn.at[slot], wp.at[_place(k), me], out_sem.at[slot, 0]).start()

            @pl.when(k >= SPREAD)
            def _():
                there = r_["last"].at[core, k - SPREAD]
                local(wn.at[slot], there, out_sem.at[slot, 0]).start()
                remote(wn.at[slot], there, am_s.at[slot, z], am_r.at[slot, z], mate).start()


        def sends(s, source, there):
            @pl.when((s <= z) & has_above)
            def _():
                remote(source, there, au_s.at[slot, s], au_r.at[slot, s], above).start()

            @pl.when((s >= z) & has_below)
            def _():
                remote(source, there, ad_s.at[slot, s], ad_r.at[slot, s], below).start()

            remote(source, there, am_s.at[slot, s], am_r.at[slot, s], mate).start()

        @pl.when(spread_here(t - mine))
        def _():
            sends(z, wn.at[slot], wp.at[_place(t - mine), me])

        work(n)


        @pl.when(ok(t))
        def _():
            r = t % PER_LAYER
            is_q = _is_q(r)
            for (rows, cols), test in ((Q_BLOCK, is_q), (P_BLOCK, jnp.logical_not(is_q))):
                @pl.when(test)
                def _():
                    wait_operands((rows, cols), r)
                    for own in range(2):
                        got = dot(ab[4 * rows * own : 4 * rows * (own + 1), :], db[:, :cols])
                        for s in range(CHIPS):
                            for j in range(cols // LANES):
                                piece = got[part_of(s, rows), part_of(j, LANES)]
                                if own:
                                    chip[t % SUMS, s, part_of(j, rows), :] = piece
                                else:
                                    ps[slot, s, part_of(j, rows), :] = piece.astype(BF16)
                        if not own:
                            for s in MATE_ORDER:
                                remote(ps.at[slot, s], pr.at[slot, s], ps_s.at[slot, s], ps_r.at[slot, s], mate).start()

        @pl.when((t >= 0) & ok(t + 1))
        def _():
            load_operands(t + 1)


        def spread(s):
            k = t - wait_of(s) - jnp.abs(z - s)

            @pl.when(spread_here(k) & (s != z))
            def _():
                there = wp.at[_place(k), 2 * s + core]

                @pl.when(s < z)
                def _():
                    remote(there, there, au_s.at[prev, s], au_r.at[prev, s], mate).wait_recv()

                @pl.when(s > z)
                def _():
                    remote(there, there, ad_s.at[prev, s], ad_r.at[prev, s], mate).wait_recv()

                sends(s, there, there)

        loop(CHIPS, spread)


        def arrived(s):
            @pl.when(for_mate(t - 1 - wait_of(s) - jnp.abs(z - s), s))
            def _():
                there = any_block
                remote(there, there, am_s.at[prev, s], am_r.at[prev, s], mate).wait_recv()

        loop(CHIPS, arrived)

        @pl.when(n < TICKS - 3)
        def _():
            tell(free_m, mate)

            @pl.when(has_above)
            def _():
                tell(free_d, above)

            @pl.when(has_below)
            def _():
                tell(free_u, below)

    loop(TICKS, tick)
    loop(3, lambda i: sent(TICKS + i))


def update(given, w, m, v):
    vm, sem = pltpu.VMEM, pltpu.SemaphoreType
    block, wide = (BLOCK, LANES), N_Q + 2 * N_K
    scratch = [
        vm((D, T), BF16), vm((T, D), BF16), vm((SUMS, CHIPS, *block), F32),
        *(vm((SLOTS, CHIPS, *block), BF16) for _ in range(6)),
        vm((SLOTS, *block), BF16), vm((SLOTS, *block), BF16),
        *(vm((2, P_BLOCK[0], D), dtype) for dtype in (F32, F32, BF16)),
        vm((T, D), BF16), vm((T, D), BF16), vm((T, N_Q), BF16),
        vm((2, D, TF), BF16), vm((2, D, TF), BF16), vm((2, TF, D), BF16), vm((T, D), F32),
        vm((2, T, TF), BF16), vm((2, T, TF), BF16), vm((TF, TF), BF16),
        vm((T, GROUP * HEAD), BF16), vm((T, HEAD), BF16), vm((T, HEAD), BF16), vm((T, wide), BF16), vm((N_Q, T), BF16),
        vm((T, HALF), F32), vm((T, HALF), F32), vm((KV, GROUP, T), F32), vm((KV, GROUP, T), F32), vm((4, STRIDE, HALF), F32),
        sem.DMA, sem.DMA, *(sem.DMA(shape) for shape in ((2, 3), (SLOTS, 2), (2, 3), (2,))), sem.DMA, sem.DMA((3,)), sem.DMA, sem.DMA((2,)), sem.DMA((7,)),
        *(sem.DMA((SLOTS, CHIPS)) for _ in range(12)),
        sem.REGULAR, sem.REGULAR, sem.REGULAR,
    ]
    refs = [*w, *m, *v, *(given[name] for name in INPUTS)]
    pair = [(FF, T), (T, D), (T, wide), (D, T), (N_Q, T), (D, T), (T, D), (T, D), (T, N_Q), (T, wide)]
    shapes = [(CHUNKS, 8, *block), (CHUNKS, *block), (2, 2, *block), *((2, *shape) for shape in pair)]
    outs = [*((shape, BF16) for shape in shapes), ((2, KV, GROUP, T), F32), ((T, D), BF16), ((T, D), BF16)]
    return pl.pallas_call(
        _update,
        in_specs=[pl.BlockSpec(memory_space=pl.ANY)] * len(refs),
        out_specs=[pl.BlockSpec(memory_space=pl.ANY)] * len(outs),
        out_shape=[jax.ShapeDtypeStruct(*out) for out in outs],
        scratch_shapes=scratch,
        compiler_params=pltpu.CompilerParams(collective_id=0, has_side_effects=True, vmem_limit_bytes=63 * 2**20),
        name="update",
    )(*refs)[:3]


def _moments(m, v, g):
    return 0.9 * m + 0.1 * g, 0.95 * v + 0.05 * g * g


LATE = ("wk", "wv")


def _unpack(*refs):
    s = pl.program_id(1)
    refs = list(refs)
    ins = [[refs.pop(0) for _ in range(3 if name in LATE else 4)] for name in NAMES]
    for i, name in enumerate(NAMES):
        gp_ref, m_ref, v_ref = ins[i][:3]
        w_out = None if name in LATE else refs.pop(0)
        m_out, v_out = refs[i - 2 * len(NAMES)], refs[i - len(NAMES)]
        tall = name in ("w_down", "wo")
        rows, cols = Q_BLOCK if tall else P_BLOCK
        some = m_ref.shape[1]
        for j in range(cols // LANES):
            for n in range(gp_ref.shape[0]):
                over = part_of(j, LANES) if tall else slice(cols * n + LANES * j, cols * n + LANES * (j + 1))
                down = part_of(n, rows) if tall else slice(0, rows)
                if w_out is not None:
                    w_out[0, down, over] = ins[i][3][n, 0, part_of(j, rows), :]
                if tall and n:
                    continue
                if tall:
                    per = rows // some
                    g = gp_ref[s // per if name == "wo" else jnp.minimum(s, 6), pl.ds(pl.multiple_of(rows * j + some * (s % per), 16), some), :]
                else:
                    g = gp_ref[n, pl.ds(pl.multiple_of(rows * j + some * jnp.minimum(s, 6), 16), some), :]
                m_out[0, :, over], v_out[0, :, over] = _moments(m_ref[0, :, over], v_ref[0, :, over], g.astype(F32))


def unpack(wp, gp, m, v):
    block = (BLOCK, LANES)
    where = {name: (TILES, 2 * i, 1) for i, name in enumerate(("w_gate", "w_up", "w_down"))}
    at = 3 * DOWN_AT
    for name, count in (("wo", 2), ("wq", 2), ("wk", 1), ("wv", 1)):
        where[name] = (count, at // count, (PER_LAYER - WO_AT) // count)
        at += count
    in_specs, given, full, own_m, own_v = [], [], {}, [], []
    for name in NAMES:
        count, start, step = where[name]
        _, height, width = m[name].shape
        some = Q_BLOCK[0] if name == "w_down" else 16
        last = height // some - 1
        mine = pl.BlockSpec((1, some, width), lambda layer, s, last=last: (layer, jnp.minimum(s, last), 0))
        in_specs += [pl.BlockSpec((count, *block), lambda layer, s, start=start, step=step: (start + step * layer, 0, 0)), mine, mine]
        given += [gp, m[name], v[name]]
        if name not in LATE:
            in_specs.append(pl.BlockSpec((count, 1, *block), lambda layer, s, start=start, step=step: (start + step * layer, s, 0, 0)))
            given.append(wp)
            full[name] = (pl.BlockSpec((1, height, width), lambda layer, s: (layer, s, 0)), jax.ShapeDtypeStruct((2, 8 * height, width), BF16))
        own_m.append((mine, jax.ShapeDtypeStruct(m[name].shape, F32)))
    outs = [*full.values(), *own_m, *own_m]
    got = pl.pallas_call(
        _unpack,
        grid=(2, 8),
        in_specs=in_specs,
        out_specs=[o[0] for o in outs],
        out_shape=[o[1] for o in outs],
        compiler_params=pltpu.CompilerParams(vmem_limit_bytes=VMEM),
        cost_estimate=pl.CostEstimate(flops=10**11, bytes_accessed=155 * 2**20, transcendentals=0),
        name="unpack",
    )(*given)
    n = len(full)
    return dict(zip(full, got)), got[n : n + len(NAMES)], got[n + len(NAMES) :]


def _finish(me_ref, *refs):
    came, packed, outs = refs[:CHIPS], refs[CHIPS : CHIPS + 2], refs[CHIPS + 2 :]
    rows, cols = P_BLOCK
    for step in range(2):
        @pl.when(pl.program_id(0) == step)
        def _():
            for which, out in enumerate(outs):
                for j in range(cols // LANES):
                    at, over = part_of(j, rows), part_of(j, LANES)
                    for n in range(2 * CHIPS):
                        i, core = n // 2, n % 2
                        owner = (me_ref[0] // 2 + CHIPS - i) % CHIPS * 2 + core
                        if step:
                            out[0, pl.ds(pl.multiple_of(rows * owner, 16), rows), over] = came[i][core, which, at, :]
                        else:
                            out[0, part_of(n, rows), over] = packed[which][0, n, at, :]


def finish(last, wp):
    me, n = lax.axis_index("dp"), 2 * CHIPS
    came = [last] + [lax.ppermute(last, "dp", [(s, (s + 2 * i) % n) for s in range(n)]) for i in range(1, CHIPS)]
    block, (rows, cols) = (BLOCK, LANES), P_BLOCK
    whole = lambda *shape: pl.BlockSpec(shape, lambda i, _: (0,) * len(shape))
    layer_1 = [pl.BlockSpec((1, n, *block), lambda i, _, at=at: (at, 0, 0, 0)) for at in (SPREAD, SPREAD + 1)]
    shape = (2, n * rows, cols)
    return pl.pallas_call(
        _finish,
        grid_spec=pltpu.PrefetchScalarGridSpec(
            num_scalar_prefetch=1, grid=(2,), in_specs=[whole(*last.shape)] * CHIPS + layer_1,
            out_specs=[pl.BlockSpec((1, n * rows, cols), lambda i, _: (1 - i, 0, 0))] * 2,
        ),
        out_shape=[jax.ShapeDtypeStruct(shape, BF16)] * 2,
        compiler_params=pltpu.CompilerParams(vmem_limit_bytes=VMEM // 2),
        name="finish",
    )(me.reshape(1).astype(jnp.int32), *came, wp, wp)


def solution(mesh):
    angle = np.arange(STRIDE)[:, None] * float(THETA) ** (-np.arange(HALF) / HALF)
    turns = np.stack([turn(angle * step) for step in (STRIDE, 1) for turn in (np.cos, np.sin)]).astype(np.float32)

    def step(x, dy, *arrays):
        w, m, v = (dict(zip(NAMES, some, strict=True)) for some in (arrays[:n], arrays[n : 2 * n], arrays[2 * n :]))
        wp, gp, last = update({"x": x[0], "dy": dy[0], "turns": jnp.asarray(turns)}, w.values(), m.values(), v.values())
        new, new_m, new_v = unpack(wp, gp, m, v)
        new |= dict(zip(LATE, finish(last, wp)))
        return (*(new[name] for name in NAMES), *new_m, *new_v)

    n = len(NAMES)
    return jax.shard_map(
        step,
        mesh=mesh,
        in_specs=(P(("rep", "dp")),) * 2 + (P(),) * n + (P(None, "dp"),) * (2 * n),
        out_specs=(P("rep"),) * n + (P("rep", "dp"),) * (2 * n),
        check_vma=False,
    )
```

```python
import functools

import jax
import jax.numpy as jnp
import numpy as np
from jax import lax
from jax.experimental import pallas as pl
from jax.experimental.pallas import tpu as pltpu
from jax.sharding import PartitionSpec as P

LOG2E = 1.4426950408889634
HIDDEN = float("-inf")
VMEM = 56 * 2**20
F32, BF16 = jnp.float32, jnp.bfloat16
MESH = pl.DeviceIdType.MESH
T, D, FF, HEADS, KV, HEAD = 1024, 896, 3584, 4, 2, 256
THETA = 10000
STRIDE = 32
NAMES = ("wq", "wk", "wv", "wo", "w_gate", "w_up", "w_down")
ROWS = 256
TF = 512
PIECES = T // ROWS


def loop(count, body):
    lax.fori_loop(0, count, lambda i, _: body(i), None)


def dot(a, b):
    return jnp.dot(a, b, preferred_element_type=F32)


def dot_t(a, b):
    return lax.dot_general(a, b, (((1,), (1,)), ((), ())), preferred_element_type=F32)


def _scale(wide):
    return lax.rsqrt(jnp.mean(wide * wide, -1, keepdims=True) + 1e-6)


def _norm_back(h, by):
    s = _scale(h)
    return by * s - h * (s * s * s * jnp.mean(by * h, -1, keepdims=True))


E = HEAD**-0.5 * LOG2E
GROUP = HEADS // KV


def part_of(i, size):
    return slice(size * i, size * (i + 1))


def _piece(i):
    return part_of(i, ROWS)


def _visible():
    shape = (ROWS, GROUP * ROWS)
    return lax.broadcasted_iota(jnp.int32, shape, 0) <= lax.rem(lax.broadcasted_iota(jnp.int32, shape, 1), ROWS)


LANES = 128
BLOCK = 448
SLOTS = 4
SUMS = 5
EARLY = 1
LAG = 27
P_BLOCK, Q_BLOCK = (112, 512), (64, 896)
TILES = FF // TF
DOWN_AT, WO_AT, QKV_AT, PER_LAYER = 14, 21, 23, 27
CHUNKS = 2 * PER_LAYER
SPREAD = CHUNKS - 2
TICKS = CHUNKS + 6 + EARLY
CHIPS = 4
MATE_ORDER = (3, 0, 2, 1)
QKV_ORDER = (1, 3, 0, 2)
HALF, T_HALF = HEAD // 2, T // 2
N_Q, N_K = HEADS * HEAD, KV * HEAD
BEFORE, LEAVE, HEADS_AT, AFTER = 13, 14, 15, 18


def _is_q(r):
    return (r >= DOWN_AT) & (r < QKV_AT)


def _place(k):
    layer, r = 1 - k // PER_LAYER, k % PER_LAYER
    double, single = (r % 2) * DOWN_AT + layer * TILES + r // 2, 2 * DOWN_AT + layer * TILES + r - DOWN_AT
    return jnp.where(r < DOWN_AT, double, jnp.where(r < WO_AT, single, 3 * DOWN_AT + layer * (PER_LAYER - WO_AT) + r - WO_AT))


def _owners(layer, r):
    mlp_chunk = r < DOWN_AT
    return (
        ("w_gate", mlp_chunk & (r % 2 == 0), r // 2), ("w_up", mlp_chunk & (r % 2 == 1), r // 2),
        ("w_down", (r >= DOWN_AT) & (r < WO_AT), r - DOWN_AT), ("wo", (r >= WO_AT) & (r < QKV_AT), r - WO_AT),
        ("wq", (r >= QKV_AT) & (r < QKV_AT + 2), r - QKV_AT), ("wk", r == QKV_AT + 2, 0 * r), ("wv", r == QKV_AT + 3, 0 * r),
    )


INPUTS = ("x", "dy", "turns")
OUTPUTS = ("wp", "gp", "last", "hidt", "d1", "dqkv", "at", "ot", "bt", "b", "h1", "o", "qkv", "lse", "h", "by1")
SCRATCH = ("ab", "db", "chip", "ps", "pr", "su", "ru", "sd", "rd", "wn", "gn", "mb", "vb", "wb", "x1", "x2", "oo", "wg", "wu", "wd", "acc", "dg", "du", "ht",
           "qq", "kk", "vv", "dq", "st", "cosb", "sinb", "lseb", "delta", "tb",
           "ab_sem", "db_sem", "opt_sem", "out_sem", "tile_sem", "x_sem", "o_sem", "qkv_sem", "lse_sem", "write_sem", "save_sem",
           "ps_s", "ps_r", "su_s", "su_r", "sd_s", "sd_r", "am_s", "am_r", "au_s", "au_r", "ad_s", "ad_r", "free_m", "free_u", "free_d")


def _update(*refs):
    count = len(NAMES)
    w_in, m_in, v_in = (dict(zip(NAMES, some)) for some in (refs[:count], refs[count : 2 * count], refs[2 * count :]))
    r_ = dict(zip((*INPUTS, *OUTPUTS, *SCRATCH), refs[3 * count :], strict=True))
    (ab, db, chip, ps, pr, su, ru, sd, rd, wn, gn, mb, vb, wb, x1, x2, oo, wg, wu, wd, acc, dg, du, ht, qq, kk, vv, dq, st, cosb, sinb, lseb, delta, tb,
     ab_sem, db_sem, opt_sem, out_sem, tile_sem, x_sem, o_sem, qkv_sem, lse_sem, write_sem, save_sem,
     ps_s, ps_r, su_s, su_r, sd_s, sd_r, am_s, am_r, au_s, au_r, ad_s, ad_r, free_m, free_u, free_d) = (r_[name] for name in SCRATCH)
    wp, gp = r_["wp"], r_["gp"]
    any_block = wp.at[0, 0]
    rep, me = lax.axis_index("rep"), lax.axis_index("dp")
    z, core = me // 2, me % 2
    mate, above, below = me + 1 - 2 * core, me + 2, me - 2
    has_above, has_below = z < CHIPS - 1, z > 0

    def remote(src, dst, send, recv, to):
        return pltpu.make_async_remote_copy(src_ref=src, dst_ref=dst, send_sem=send, recv_sem=recv, device_id=(rep, to), device_id_type=MESH)

    def tell(sem, to):
        pl.semaphore_signal(sem, inc=1, device_id=(rep, to), device_id_type=MESH)

    def local(src, dst, sem):
        return pltpu.make_async_copy(src, dst, sem)

    def ok(k):
        return (k >= 0) & (k < CHUNKS)

    def spread_here(k):
        return (k >= 0) & (k < SPREAD)

    def for_mate(k, s):
        return spread_here(k) | (ok(k) & (s == z))

    def wait_of(s):
        return 3 + ((s == 0) | (s == CHIPS - 1)).astype(jnp.int32)

    mine = wait_of(z)

    def tokens(start, count):
        return pl.ds(pl.multiple_of(start, ROWS), count)


    def tile_copies(half, j, buf):
        layer, over = 1 - half, pl.ds(pl.multiple_of(TF * j, TF), TF)
        return [
            local(w_in["w_gate"].at[layer, :, over], wg.at[buf], tile_sem.at[buf, 0]),
            local(w_in["w_up"].at[layer, :, over], wu.at[buf], tile_sem.at[buf, 1]),
            local(w_in["w_down"].at[layer, over, :], wd.at[buf], tile_sem.at[buf, 2]),
        ]

    def wo_copies(half):
        return [local(w_in["wo"].at[1 - half, pl.ds(TF * n, TF), :], wd.at[n], tile_sem.at[n, 2]) for n in range(2)]

    def qkv_weight_copies(half):
        layer = 1 - half
        return [
            *(local(w_in["wq"].at[layer, :, pl.ds(TF * n, TF)], wg.at[n], tile_sem.at[n, 0]) for n in range(2)),
            local(w_in["wk"].at[layer], wu.at[0], tile_sem.at[0, 1]), local(w_in["wv"].at[layer], wu.at[1], tile_sem.at[1, 1]),
        ]

    def column(at):
        return pl.ds(pl.multiple_of(at, HEAD), HEAD)

    def head_copies(half, head):
        pair = pl.ds(pl.multiple_of(GROUP * HEAD * head, GROUP * HEAD), GROUP * HEAD)
        return [
            local(r_["qkv"].at[half, :, over], to, qkv_sem.at[n])
            for n, (over, to) in enumerate(((pair, qq), (column(N_Q + HEAD * head), kk), (column(N_Q + N_K + HEAD * head), vv)))
        ]

    def load_x2(ref):
        return local(ref, x2, x_sem.at[1])

    def unit_of(n):
        half = (n >= AFTER + 2 + EARLY).astype(jnp.int32)
        return half, n - EARLY - LAG * half

    def start(copies):
        for copy in copies:
            copy.start()

    def wait(copies):
        for copy in copies:
            copy.wait()

    def writes(half, tau):
        u = tau + EARLY
        j, first = u // 2, tokens(T_HALF * (u % 2), T_HALF)
        over = pl.ds(pl.multiple_of(TF * j, TF), TF)
        part = tokens(T_HALF * (tau - AFTER), T_HALF)
        after_at = (tau >= AFTER) & (tau < AFTER + 2)
        return (
            ((u >= 0) & (u < 2 * TILES), lambda: [local(ht, r_["hidt"].at[half, over, first], write_sem.at[0])]),
            (tau == LEAVE, lambda: [local(x1, r_["d1"].at[half], write_sem.at[0])]),
            (after_at, lambda: [local(dq.at[part, :], r_["dqkv"].at[half, part, :], write_sem.at[0])]),
            (after_at & (half == 0), lambda: [local(x1.at[part, :], r_["by1"].at[part, :], write_sem.at[1])]),
        )

    def fetch(n):
        half, tau = unit_of(n)
        u = tau + EARLY

        @pl.when((tau == -EARLY - 1) & (half == 1))
        def _():
            start([*tile_copies(half, 0, 0), load_x2(r_["b"].at[half])])

        @pl.when((u >= 0) & (u % 2 == 0) & (u < 2 * TILES - 2))
        def _():
            start(tile_copies(half, u // 2 + 1, (u // 2 + 1) % 2))

        @pl.when(tau == BEFORE)
        def _():
            start([*wo_copies(half), load_x2(r_["h1"].at[half]), local(r_["o"].at[half], oo, o_sem)])

        @pl.when(tau == LEAVE)
        def _():
            start([*head_copies(half, 0), local(r_["lse"].at[half], lseb, lse_sem)])

        @pl.when(tau == HEADS_AT + 1)
        def _():
            start(head_copies(half, 1))

        @pl.when((tau == BEFORE) & (half == 0))
        def _():
            start(tile_copies(0, 0, 0)[:2])

        @pl.when((tau == LEAVE) & (half == 0))
        def _():
            start(qkv_weight_copies(0))

        @pl.when((tau == HEADS_AT) & (half == 0))
        def _():
            start([load_x2(r_["h"])])

    def mlp_unit(u, buf, later):
        rows = tokens(T_HALF * (u % 2), T_HALF)
        gate, up = dot(x2[rows, :], wg[buf]), dot(x2[rows, :], wu[buf])
        sig = 1.0 / (1.0 + jnp.exp(-gate))
        silu = gate * sig
        by = dot_t(x1[rows, :], wd[buf]).astype(BF16).astype(F32)
        ht[...] = (silu * up).astype(BF16).T
        du[buf, rows, :] = (by * silu).astype(BF16)
        dg[buf, rows, :] = (by * up * (sig * (1.0 + gate * (1.0 - sig)))).astype(BF16)

        @pl.when(jnp.logical_not(later))
        def _():
            acc[rows, :] += dot_t(dg[buf, rows, :], wg[buf]) + dot_t(du[buf, rows, :], wu[buf])

    def late_unit(i):
        rows = tokens(ROWS * i, ROWS)
        acc[rows, :] += dot_t(st[rows, :TF], wg[0]) + dot_t(st[rows, TF:], wu[0])

    def leave_unit(i):
        rows = tokens(ROWS * i, ROWS)
        inner = _norm_back(x2[rows, :].astype(F32), acc[rows, :].astype(BF16).astype(F32)).astype(BF16)
        d1 = (x1[rows, :].astype(F32) + inner.astype(F32)).astype(BF16)
        x1[rows, :] = d1
        for n in range(HEADS):
            low, over = HEAD * (n % 2), _piece(n)
            do = dot_t(d1, wd[n // 2, low : low + HEAD, :]).astype(BF16)
            both = do.astype(F32) * oo[rows, over].astype(F32)
            oo[rows, over] = do
            delta[n // GROUP, n % GROUP : n % GROUP + 1, rows] = both.T.sum(0, keepdims=True)

    def side(ref, i, head):
        return jnp.concatenate([ref[_piece(i), column(HEAD * (GROUP * head + n))] for n in range(GROUP)], axis=0)

    def turn_back(part, rows):
        cos, sin = cosb[rows, :], sinb[rows, :]
        x, y = part[:, :HALF].astype(F32), part[:, HALF:].astype(F32)
        return jnp.concatenate([x * cos + y * sin, y * cos - x * sin], -1).astype(BF16)

    def head_unit(head):
        seen = _visible()
        turned = kk[...].T
        line = lambda ref, i: jnp.concatenate([ref[head, n : n + 1, _piece(i)] for n in range(GROUP)], axis=1)
        dk_at, dv_at = slice(0, HEAD), slice(HEAD, 2 * HEAD)
        for i in range(PIECES):
            lse, dl = line(lseb, i), line(delta, i)
            q = jnp.concatenate([qq[_piece(i), _piece(n)] for n in range(GROUP)], axis=0)
            do = side(oo, i, head)
            by_q = 0.0
            for j in range(i + 1):
                at = _piece(j)
                p = jnp.exp2(dot_t(kk[at, :], q) * E - lse)
                if j == i:
                    p = jnp.where(seen, p, 0.0)
                ds = (p * (dot_t(vv[at, :], do) - dl)).astype(BF16)
                by_v, by_k = dot(p.astype(BF16), do), dot(ds, q)
                acc[at, dv_at] = by_v if j == i else acc[at, dv_at] + by_v
                acc[at, dk_at] = by_k if j == i else acc[at, dk_at] + by_k
                by_q = by_q + dot(turned[:, at], ds)
            by_q = (by_q * HEAD**-0.5).astype(BF16)
            for n in range(GROUP):
                dq[_piece(i), column(HEAD * (GROUP * head + n))] = turn_back(by_q[:, _piece(n)].T, _piece(i))
        for i in range(PIECES):
            dq[_piece(i), column(N_Q + HEAD * head)] = turn_back((acc[_piece(i), dk_at] * HEAD**-0.5).astype(BF16), _piece(i))
            dq[_piece(i), column(N_Q + N_K + HEAD * head)] = acc[_piece(i), dv_at].astype(BF16)

    def after_unit(rows):
        by = sum(dot_t(dq[rows, part_of(n, TF)], (wg, wu)[n // 2][n % 2]) for n in range(4)).astype(BF16).astype(F32)
        inner = _norm_back(x2[rows, :].astype(F32), by).astype(BF16)
        x1[rows, :] = (x1[rows, :].astype(F32) + inner.astype(F32)).astype(BF16)

    def work(n):
        half, tau = unit_of(n)
        u = tau + EARLY

        @pl.when((u >= 0) & (u < 2 * TILES))
        def _():
            buf = u // 2 % 2

            @pl.when(u % 2 == 0)
            def _():
                wait(tile_copies(half, u // 2, buf))

            @pl.when((u == 0) & (half == 1))
            def _():
                acc[...] = jnp.zeros((T, D), F32)
                load_x2(r_["h"]).wait()

            mlp_unit(u, buf, (half == 0) & (u < 2))

            @pl.when((half == 0) & (u == 1))
            def _():
                st[:, :TF] = dg[0]
                st[:, TF:] = du[0]

        @pl.when((tau == BEFORE) & (half == 0))
        def _():
            wait(tile_copies(0, 0, 0)[:2])
            loop(PIECES, late_unit)

        @pl.when(tau == LEAVE)
        def _():
            wait([load_x2(r_["h"]), local(r_["o"].at[0], oo, o_sem), *wo_copies(half)])
            loop(PIECES, leave_unit)

        @pl.when((tau == HEADS_AT) | (tau == HEADS_AT + 2))
        def _():
            @pl.when(tau == HEADS_AT)
            def _():
                local(r_["lse"].at[0], lseb, lse_sem).wait()

            wait(head_copies(0, 0))
            head_unit((tau - HEADS_AT) // 2)

        @pl.when((tau >= AFTER) & (tau < AFTER + 2) & (half == 0))
        def _():
            @pl.when(tau == AFTER)
            def _():
                wait([load_x2(r_["h"]), *qkv_weight_copies(0)])

            loop(PIECES // 2, lambda i: after_unit(tokens(T_HALF * (tau - AFTER) + ROWS * i, ROWS)))

        for test, copies in writes(half, tau):
            pl.when(test)(lambda: start(copies()))


    def load_operands(k):
        half, r = k // PER_LAYER, k % PER_LAYER

        def from_rows(ref, block, down):
            rows, whole = block[0], ref.shape[0] // 8
            for e in range(8):
                owner = 2 * (e % 4) + (1 - core if e < 4 else core)
                at = pl.multiple_of(whole * owner + down, 16)
                local(ref.at[pl.ds(at, rows), :], ab.at[pl.ds(rows * e, rows), :], ab_sem).start()

        @pl.when(r < DOWN_AT)
        def _():
            from_rows(r_["bt"].at[half], P_BLOCK, 0)

        @pl.when((r >= DOWN_AT) & (r < WO_AT))
        def _():
            from_rows(r_["hidt"].at[half], Q_BLOCK, Q_BLOCK[0] * (r - DOWN_AT))

            @pl.when(half == 0)
            def _():
                local(r_["dy"], db, db_sem).start()

            @pl.when(half == 1)
            def _():
                local(r_["by1"], db, db_sem).start()

        @pl.when((r >= WO_AT) & (r < QKV_AT))
        def _():
            from_rows(r_["ot"].at[half], Q_BLOCK, Q_BLOCK[0] * (r - WO_AT))
            local(r_["d1"].at[half], db, db_sem).start()

        @pl.when(r >= QKV_AT)
        def _():
            from_rows(r_["at"].at[half], P_BLOCK, 0)
            local(r_["dqkv"].at[half, :, pl.ds(pl.multiple_of(TF * (r - QKV_AT), TF), TF)], db.at[:, pl.ds(0, TF)], db_sem).start()

    def wait_operands(block, r):
        rows, cols = block
        local(r_["hidt"].at[0, pl.ds(0, 8 * rows), :], ab.at[pl.ds(0, 8 * rows), :], ab_sem).wait()

        @pl.when(r >= DOWN_AT)
        def _():
            local(r_["dqkv"].at[0, :, pl.ds(0, cols)], db.at[:, pl.ds(0, cols)], db_sem).wait()

        for which, ref in enumerate((dg, du)):
            @pl.when((r < DOWN_AT) & (r % 2 == which))
            def _():
                db[:, :TF] = ref[r // 2 % 2]

    def optimizer_copies(k, buf, do):
        layer, r = 1 - k // PER_LAYER, k % PER_LAYER
        for name, test, j in _owners(layer, r):
            rows, cols = block = Q_BLOCK if name in ("w_down", "wo") else P_BLOCK

            @pl.when(test)
            def _():
                whole = w_in[name].shape[1] // 8
                down = pl.multiple_of(rows * j if block == Q_BLOCK else 0 * j, 16)
                right = pl.ds(0, cols) if block == Q_BLOCK else pl.ds(pl.multiple_of(cols * j, cols), cols)
                for n, (ref, at, to) in enumerate(((m_in[name], down, mb), (v_in[name], down, vb), (w_in[name], pl.multiple_of(whole * me + down, 16), wb))):
                    do(local(ref.at[layer, pl.ds(at, rows), right], to.at[buf, pl.ds(0, rows), pl.ds(0, cols)], opt_sem.at[buf, n]))


    def save(n, source, to):
        return local(source, to, save_sem.at[n])

    def attend_head(head):
        seen = _visible()
        k_at, turned = column(N_Q + HEAD * head), dq[:, column(N_Q + N_K + HEAD * head)].T

        def scores_of(i):
            q = side(dq, i, head)
            scores = [dot_t(dq[_piece(j), k_at], q) for j in range(i + 1)]
            return [*scores[:i], jnp.where(seen, scores[i], HIDDEN)]

        coming = scores_of(0)
        for i in range(PIECES):
            scores, coming = coming, scores_of(i + 1) if i + 1 < PIECES else None
            top = functools.reduce(jnp.maximum, [s.max(axis=0, keepdims=True) for s in scores])
            total, mix = 0.0, 0.0
            for j, s in enumerate(scores):
                p = jnp.exp2((s - top) * E)
                total = total + p.sum(axis=0, keepdims=True)
                mix = mix + dot(turned[:, _piece(j)], p.astype(BF16))
            out = (mix * (1.0 / total)).astype(BF16)
            lse = top * E + jnp.log(total) * LOG2E
            for n in range(GROUP):
                over = column(HEAD * (GROUP * head + n))
                st[over, _piece(i)] = out[:, _piece(n)]
                oo[_piece(i), over] = out[:, _piece(n)].T
                lseb[head, n : n + 1, _piece(i)] = lse[:, _piece(n)]

    def saves(half):
        kept = lambda name: r_[name].at[half]
        return [
            save(0, ab, kept("bt")), save(1, dq.at[:, pl.ds(0, D)], kept("h1")), save(2, x2, kept("b")),
            save(3, st, kept("ot")), save(4, oo, kept("o")), save(5, lseb, kept("lse")),
        ]

    by_y, by_h = local(r_["dy"], x1, x_sem.at[0]), save(6, x1, r_["h"])

    def forward(layer):
        half = 1 - layer
        weights = qkv_weight_copies(half)
        early = [save(0, ab, r_["at"].at[half]), save(1, dq, r_["qkv"].at[half])]
        for i in range(PIECES):
            x2[_piece(i), :] = x1[_piece(i), :]
            wide = x1[_piece(i), :].astype(F32)
            a = (wide * _scale(wide)).astype(BF16)
            ab[:, _piece(i)] = a.T
            cos, sin = cosb[_piece(i), :], sinb[_piece(i), :]
            for c in QKV_ORDER:
                if i == 0:
                    weights[c].wait()
                t = dot(a, (wg, wu)[c // 2][c % 2]).astype(BF16)
                for n in range(2):
                    part = t[:, _piece(n)]
                    if c < 3:
                        p, q = part[:, :HALF].astype(F32), part[:, HALF:].astype(F32)
                        part = jnp.concatenate([p * cos - q * sin, q * cos + p * sin], -1).astype(BF16)
                    dq[_piece(i), TF * c + HEAD * n : TF * c + HEAD * (n + 1)] = part
        wo = local(w_in["wo"].at[layer], db, db_sem)
        start([*early, wo, *tile_copies(half, 0, 0)])

        @pl.when(layer == 1)
        def _():
            by_h.wait()
            by_y.start()

        loop(KV, attend_head)
        wait([*early, wo])
        start(saves(half)[3:])

        projected = lambda i: dot(oo[_piece(i), :], db[...])
        coming = projected(0)
        for i in range(PIECES):
            rows = _piece(i)
            total, coming = coming, projected(i + 1) if i + 1 < PIECES else None
            h1 = (x2[rows, :].astype(F32) + total.astype(BF16).astype(F32)).astype(BF16)
            dq[rows, :D] = h1
            wide = h1.astype(F32)
            b = (wide * _scale(wide)).astype(BF16)
            x2[rows, :] = b
            ab[:, rows] = b.T
        start(saves(half)[:3])

        @pl.when(layer == 0)
        def _():
            acc[...] = jnp.zeros((T, D), F32)
            coming = qkv_weight_copies(0)

            def one(j):
                buf = j % 2

                @pl.when(j < TILES - 1)
                def _():
                    start(tile_copies(half, j + 1, 1 - buf))

                @pl.when(j == TILES - 1)
                def _():
                    start([coming[c] for c in QKV_ORDER[:2]])

                wait(tile_copies(half, j, buf))
                for i in range(2):
                    rows = part_of(i, T_HALF)
                    gate, up = dot(x2[rows, :], wg[buf]), dot(x2[rows, :], wu[buf])
                    hidden = (gate * (1.0 / (1.0 + jnp.exp(-gate))) * up).astype(BF16)
                    acc[rows, :] += dot(hidden, wd[buf])

            loop(TILES, one)
            start([coming[c] for c in QKV_ORDER[2:]])
            wait(saves(half))
            for i in range(PIECES):
                x1[_piece(i), :] = (dq[_piece(i), :D].astype(F32) + acc[_piece(i), :].astype(BF16).astype(F32)).astype(BF16)
                acc[_piece(i), :] = jnp.zeros((ROWS, D), F32)
            by_h.start()

    first = [local(r_["x"], x1, x_sem.at[0]), local(r_["turns"], tb, o_sem)]
    start([*first, *(qkv_weight_copies(1)[c] for c in QKV_ORDER)])


    barrier = pltpu.get_barrier_semaphore()
    tell(barrier, mate)

    @pl.when(has_above)
    def _():
        tell(barrier, above)

    @pl.when(has_below)
    def _():
        tell(barrier, below)

    wait(first)

    def spin(a):
        rows = pl.ds(pl.multiple_of(STRIDE * a, STRIDE), STRIDE)
        cos_a, sin_a, cos_b, sin_b = tb[0, pl.ds(a, 1), :], tb[1, pl.ds(a, 1), :], tb[2], tb[3]
        cosb[rows, :] = cos_a * cos_b - sin_a * sin_b
        sinb[rows, :] = sin_a * cos_b + cos_a * sin_b

    loop(T // STRIDE, spin)
    loop(2, forward)
    @pl.when(has_above & has_below)
    def _():
        pl.semaphore_wait(barrier, 3)

    @pl.when(jnp.logical_not(has_above & has_below))
    def _():
        pl.semaphore_wait(barrier, 2)

    by_y.wait()

    def sent(n):
        t, late = n - 3 - EARLY, (n + 1) % SLOTS

        @pl.when(ok(t))
        def _():
            for s in range(CHIPS):
                remote(ps.at[late, s], pr.at[late, s], ps_s.at[late, s], ps_r.at[late, s], mate).wait_send()

        @pl.when(ok(t - 1 - z))
        def _():
            for s in range(1, CHIPS):
                @pl.when(s > z)
                def _():
                    remote(su.at[late, s], ru.at[late, s], su_s.at[late, s], su_r.at[late, s], mate).wait_send()

        @pl.when(ok(t - 1 - (CHIPS - 1 - z)))
        def _():
            for s in range(CHIPS - 1):
                @pl.when(s < z)
                def _():
                    remote(sd.at[late, s], rd.at[late, s], sd_s.at[late, s], sd_r.at[late, s], mate).wait_send()

        def gone(s):
            k = t - wait_of(s) - jnp.abs(z - s)
            there = any_block

            @pl.when(for_mate(k, s))
            def _():
                remote(there, there, am_s.at[late, s], am_r.at[late, s], mate).wait_send()

            @pl.when(spread_here(k) & (s <= z) & has_above)
            def _():
                remote(there, there, au_s.at[late, s], au_r.at[late, s], mate).wait_send()

            @pl.when(spread_here(k) & (s >= z) & has_below)
            def _():
                remote(there, there, ad_s.at[late, s], ad_r.at[late, s], mate).wait_send()

        loop(CHIPS, gone)

        @pl.when(ok(t - mine))
        def _():
            local(wn.at[late], any_block, out_sem.at[late, 0]).wait()
            local(gn.at[late], gp.at[0], out_sem.at[late, 1]).wait()

    def tick(n):
        t = n - EARLY
        slot, prev = n % SLOTS, (n + SLOTS - 1) % SLOTS
        two = n % 2


        @pl.when(n >= 3)
        def _():
            pl.semaphore_wait(free_m, 1)

            @pl.when(has_above)
            def _():
                pl.semaphore_wait(free_u, 1)

            @pl.when(has_below)
            def _():
                pl.semaphore_wait(free_d, 1)

            sent(n)


        @pl.when(n == EARLY)
        def _():
            wait(saves(0))
            load_operands(0)

        for test, copies in writes(*unit_of(n - 1)):
            pl.when(test & (n > 0))(lambda: wait(copies()))
        fetch(n)

        @pl.when(ok(t + 1 - mine))
        def _():
            optimizer_copies(t + 1 - mine, 1 - two, lambda copy: copy.start())


        @pl.when(ok(t - 1))
        def _():
            for s in MATE_ORDER:
                remote(ps.at[prev, s], pr.at[prev, s], ps_s.at[prev, s], ps_r.at[prev, s], mate).wait_recv()
                value = chip[(t - 1) % SUMS, s] + pr[prev, s].astype(F32)
                chip[(t - 1) % SUMS, s] = value
                if s > 0:
                    @pl.when(z == 0)
                    def _():
                        su[slot, s] = value.astype(BF16)
                        remote(su.at[slot, s], ru.at[slot, s], su_s.at[slot, s], su_r.at[slot, s], above).start()
                if s < CHIPS - 1:
                    @pl.when(z == CHIPS - 1)
                    def _():
                        sd[slot, s] = value.astype(BF16)
                        remote(sd.at[slot, s], rd.at[slot, s], sd_s.at[slot, s], sd_r.at[slot, s], below).start()


        def pass_on(s, k, from_above):
            got, send, here, there, to = (rd, sd, sd_s, sd_r, below) if from_above else (ru, su, su_s, su_r, above)
            remote(send.at[prev, s], got.at[prev, s], here.at[prev, s], there.at[prev, s], mate).wait_recv()
            value = chip[k % SUMS, s] + got[prev, s].astype(F32)
            chip[k % SUMS, s] = value
            send[slot, s] = value.astype(BF16)

            @pl.when((s < z) if from_above else (s > z))
            def _():
                remote(send.at[slot, s], got.at[slot, s], here.at[slot, s], there.at[slot, s], to).start()

        up_k, down_k = t - 1 - z, t - 1 - (CHIPS - 1 - z)
        for i in range(CHIPS - 1):
            @pl.when(has_below & ok(up_k) & (CHIPS - 1 - i >= z))
            def _():
                pass_on(CHIPS - 1 - i, up_k, False)

            @pl.when(has_above & ok(down_k) & (i <= z))
            def _():
                pass_on(i, down_k, True)


        @pl.when(ok(t - mine))
        def _():
            k = t - mine
            optimizer_copies(k, two, lambda copy: copy.wait())
            is_q = _is_q(k % PER_LAYER)
            for (rows, cols), test in ((Q_BLOCK, is_q), (P_BLOCK, jnp.logical_not(is_q))):
                @pl.when(test)
                def _():
                    for j in range(cols // LANES):
                        at, over = part_of(j, rows), part_of(j, LANES)
                        low = chip[k % SUMS, z, at, :].astype(BF16)
                        m, v = _moments(mb[two, :rows, over], vb[two, :rows, over], low.astype(F32))
                        w = wb[two, :rows, over].astype(F32)
                        wn[slot, at, :] = (w - 0.02 * (m * lax.rsqrt(v + 1e-8) + 0.1 * w)).astype(BF16)
                        gn[slot, at, :] = low

            local(gn.at[slot], gp.at[_place(k)], out_sem.at[slot, 1]).start()

            @pl.when(k < SPREAD)
            def _():
                local(wn.at[slot], wp.at[_place(k), me], out_sem.at[slot, 0]).start()

            @pl.when(k >= SPREAD)
            def _():
                there = r_["last"].at[core, k - SPREAD]
                local(wn.at[slot], there, out_sem.at[slot, 0]).start()
                remote(wn.at[slot], there, am_s.at[slot, z], am_r.at[slot, z], mate).start()


        def sends(s, source, there):
            @pl.when((s <= z) & has_above)
            def _():
                remote(source, there, au_s.at[slot, s], au_r.at[slot, s], above).start()

            @pl.when((s >= z) & has_below)
            def _():
                remote(source, there, ad_s.at[slot, s], ad_r.at[slot, s], below).start()

            remote(source, there, am_s.at[slot, s], am_r.at[slot, s], mate).start()

        @pl.when(spread_here(t - mine))
        def _():
            sends(z, wn.at[slot], wp.at[_place(t - mine), me])

        work(n)


        @pl.when(ok(t))
        def _():
            r = t % PER_LAYER
            is_q = _is_q(r)
            for (rows, cols), test in ((Q_BLOCK, is_q), (P_BLOCK, jnp.logical_not(is_q))):
                @pl.when(test)
                def _():
                    wait_operands((rows, cols), r)
                    for own in range(2):
                        got = dot(ab[4 * rows * own : 4 * rows * (own + 1), :], db[:, :cols])
                        for s in range(CHIPS):
                            for j in range(cols // LANES):
                                piece = got[part_of(s, rows), part_of(j, LANES)]
                                if own:
                                    chip[t % SUMS, s, part_of(j, rows), :] = piece
                                else:
                                    ps[slot, s, part_of(j, rows), :] = piece.astype(BF16)
                        if not own:
                            for s in MATE_ORDER:
                                remote(ps.at[slot, s], pr.at[slot, s], ps_s.at[slot, s], ps_r.at[slot, s], mate).start()

        @pl.when((t >= 0) & ok(t + 1))
        def _():
            load_operands(t + 1)


        def spread(s):
            k = t - wait_of(s) - jnp.abs(z - s)

            @pl.when(spread_here(k) & (s != z))
            def _():
                there = wp.at[_place(k), 2 * s + core]

                @pl.when(s < z)
                def _():
                    remote(there, there, au_s.at[prev, s], au_r.at[prev, s], mate).wait_recv()

                @pl.when(s > z)
                def _():
                    remote(there, there, ad_s.at[prev, s], ad_r.at[prev, s], mate).wait_recv()

                sends(s, there, there)

        loop(CHIPS, spread)


        def arrived(s):
            @pl.when(for_mate(t - 1 - wait_of(s) - jnp.abs(z - s), s))
            def _():
                there = any_block
                remote(there, there, am_s.at[prev, s], am_r.at[prev, s], mate).wait_recv()

        loop(CHIPS, arrived)

        @pl.when(n < TICKS - 3)
        def _():
            tell(free_m, mate)

            @pl.when(has_above)
            def _():
                tell(free_d, above)

            @pl.when(has_below)
            def _():
                tell(free_u, below)

    loop(TICKS, tick)
    loop(3, lambda i: sent(TICKS + i))


def update(given, w, m, v):
    vm, sem = pltpu.VMEM, pltpu.SemaphoreType
    block, wide = (BLOCK, LANES), N_Q + 2 * N_K
    scratch = [
        vm((D, T), BF16), vm((T, D), BF16), vm((SUMS, CHIPS, *block), F32),
        *(vm((SLOTS, CHIPS, *block), BF16) for _ in range(6)),
        vm((SLOTS, *block), BF16), vm((SLOTS, *block), BF16),
        *(vm((2, P_BLOCK[0], D), dtype) for dtype in (F32, F32, BF16)),
        vm((T, D), BF16), vm((T, D), BF16), vm((T, N_Q), BF16),
        vm((2, D, TF), BF16), vm((2, D, TF), BF16), vm((2, TF, D), BF16), vm((T, D), F32),
        vm((2, T, TF), BF16), vm((2, T, TF), BF16), vm((TF, TF), BF16),
        vm((T, GROUP * HEAD), BF16), vm((T, HEAD), BF16), vm((T, HEAD), BF16), vm((T, wide), BF16), vm((N_Q, T), BF16),
        vm((T, HALF), F32), vm((T, HALF), F32), vm((KV, GROUP, T), F32), vm((KV, GROUP, T), F32), vm((4, STRIDE, HALF), F32),
        sem.DMA, sem.DMA, *(sem.DMA(shape) for shape in ((2, 3), (SLOTS, 2), (2, 3), (2,))), sem.DMA, sem.DMA((3,)), sem.DMA, sem.DMA((2,)), sem.DMA((7,)),
        *(sem.DMA((SLOTS, CHIPS)) for _ in range(12)),
        sem.REGULAR, sem.REGULAR, sem.REGULAR,
    ]
    refs = [*w, *m, *v, *(given[name] for name in INPUTS)]
    pair = [(FF, T), (T, D), (T, wide), (D, T), (N_Q, T), (D, T), (T, D), (T, D), (T, N_Q), (T, wide)]
    shapes = [(CHUNKS, 8, *block), (CHUNKS, *block), (2, 2, *block), *((2, *shape) for shape in pair)]
    outs = [*((shape, BF16) for shape in shapes), ((2, KV, GROUP, T), F32), ((T, D), BF16), ((T, D), BF16)]
    return pl.pallas_call(
        _update,
        in_specs=[pl.BlockSpec(memory_space=pl.ANY)] * len(refs),
        out_specs=[pl.BlockSpec(memory_space=pl.ANY)] * len(outs),
        out_shape=[jax.ShapeDtypeStruct(*out) for out in outs],
        scratch_shapes=scratch,
        compiler_params=pltpu.CompilerParams(collective_id=0, has_side_effects=True, vmem_limit_bytes=63 * 2**20),
        name="update",
    )(*refs)[:3]


def _moments(m, v, g):
    return 0.9 * m + 0.1 * g, 0.95 * v + 0.05 * g * g


LATE = ("wk", "wv")


def _unpack(*refs):
    s = pl.program_id(1)
    refs = list(refs)
    ins = [[refs.pop(0) for _ in range(3 if name in LATE else 4)] for name in NAMES]
    for i, name in enumerate(NAMES):
        gp_ref, m_ref, v_ref = ins[i][:3]
        w_out = None if name in LATE else refs.pop(0)
        m_out, v_out = refs[i - 2 * len(NAMES)], refs[i - len(NAMES)]
        tall = name in ("w_down", "wo")
        rows, cols = Q_BLOCK if tall else P_BLOCK
        some = m_ref.shape[1]
        for j in range(cols // LANES):
            for n in range(gp_ref.shape[0]):
                over = part_of(j, LANES) if tall else slice(cols * n + LANES * j, cols * n + LANES * (j + 1))
                down = part_of(n, rows) if tall else slice(0, rows)
                if w_out is not None:
                    w_out[0, down, over] = ins[i][3][n, 0, part_of(j, rows), :]
                if tall and n:
                    continue
                if tall:
                    per = rows // some
                    g = gp_ref[s // per if name == "wo" else jnp.minimum(s, 6), pl.ds(pl.multiple_of(rows * j + some * (s % per), 16), some), :]
                else:
                    g = gp_ref[n, pl.ds(pl.multiple_of(rows * j + some * jnp.minimum(s, 6), 16), some), :]
                m_out[0, :, over], v_out[0, :, over] = _moments(m_ref[0, :, over], v_ref[0, :, over], g.astype(F32))


def unpack(wp, gp, m, v):
    block = (BLOCK, LANES)
    where = {name: (TILES, 2 * i, 1) for i, name in enumerate(("w_gate", "w_up", "w_down"))}
    at = 3 * DOWN_AT
    for name, count in (("wo", 2), ("wq", 2), ("wk", 1), ("wv", 1)):
        where[name] = (count, at // count, (PER_LAYER - WO_AT) // count)
        at += count
    deep = pl.Buffered(3)
    in_specs, given, full, own_m = [], [], {}, []
    for name in NAMES:
        count, start, step = where[name]
        _, height, width = m[name].shape
        some = Q_BLOCK[0] if name == "w_down" else 16
        last = height // some - 1
        place = lambda layer, s, last=last: (layer, jnp.minimum(s, last), 0)
        mine, ahead = pl.BlockSpec((1, some, width), place), pl.BlockSpec((1, some, width), place, pipeline_mode=deep)
        in_specs += [pl.BlockSpec((count, *block), lambda layer, s, start=start, step=step: (start + step * layer, 0, 0)), ahead, ahead]
        given += [gp, m[name], v[name]]
        if name not in LATE:
            in_specs.append(pl.BlockSpec((count, 1, *block), lambda layer, s, start=start, step=step: (start + step * layer, s, 0, 0), pipeline_mode=deep))
            given.append(wp)
            full[name] = (pl.BlockSpec((1, height, width), lambda layer, s: (layer, s, 0)), jax.ShapeDtypeStruct((2, 8 * height, width), BF16))
        own_m.append((mine, jax.ShapeDtypeStruct(m[name].shape, F32)))
    outs = [*full.values(), *own_m, *own_m]
    got = pl.pallas_call(
        pltpu.emit_pipeline(_unpack, grid=(2, 8), in_specs=in_specs, out_specs=[o[0] for o in outs]),
        in_specs=[pl.BlockSpec(memory_space=pl.ANY)] * len(given),
        out_specs=[pl.BlockSpec(memory_space=pl.ANY)] * len(outs),
        out_shape=[o[1] for o in outs],
        compiler_params=pltpu.CompilerParams(vmem_limit_bytes=VMEM),
        cost_estimate=pl.CostEstimate(flops=10**11, bytes_accessed=155 * 2**20, transcendentals=0),
        name="unpack",
    )(*given)
    n = len(full)
    return dict(zip(full, got)), got[n : n + len(NAMES)], got[n + len(NAMES) :]


def _finish(me_ref, *refs):
    came, packed, outs = refs[:CHIPS], refs[CHIPS : CHIPS + 2], refs[CHIPS + 2 :]
    rows, cols = P_BLOCK
    for step in range(2):
        @pl.when(pl.program_id(0) == step)
        def _():
            for which, out in enumerate(outs):
                for j in range(cols // LANES):
                    at, over = part_of(j, rows), part_of(j, LANES)
                    for n in range(2 * CHIPS):
                        i, core = n // 2, n % 2
                        owner = (me_ref[0] // 2 + CHIPS - i) % CHIPS * 2 + core
                        if step:
                            out[0, pl.ds(pl.multiple_of(rows * owner, 16), rows), over] = came[i][core, which, at, :]
                        else:
                            out[0, part_of(n, rows), over] = packed[which][0, n, at, :]


def finish(last, wp):
    me, n = lax.axis_index("dp"), 2 * CHIPS
    came = [last] + [lax.ppermute(last, "dp", [(s, (s + 2 * i) % n) for s in range(n)]) for i in range(1, CHIPS)]
    block, (rows, cols) = (BLOCK, LANES), P_BLOCK
    whole = lambda *shape: pl.BlockSpec(shape, lambda i, _: (0,) * len(shape))
    layer_1 = [pl.BlockSpec((1, n, *block), lambda i, _, at=at: (at, 0, 0, 0)) for at in (SPREAD, SPREAD + 1)]
    shape = (2, n * rows, cols)
    return pl.pallas_call(
        _finish,
        grid_spec=pltpu.PrefetchScalarGridSpec(
            num_scalar_prefetch=1, grid=(2,), in_specs=[whole(*last.shape)] * CHIPS + layer_1,
            out_specs=[pl.BlockSpec((1, n * rows, cols), lambda i, _: (1 - i, 0, 0))] * 2,
        ),
        out_shape=[jax.ShapeDtypeStruct(shape, BF16)] * 2,
        compiler_params=pltpu.CompilerParams(vmem_limit_bytes=VMEM // 2),
        name="finish",
    )(me.reshape(1).astype(jnp.int32), *came, wp, wp)


def solution(mesh):
    angle = np.arange(STRIDE)[:, None] * float(THETA) ** (-np.arange(HALF) / HALF)
    turns = np.stack([turn(angle * step) for step in (STRIDE, 1) for turn in (np.cos, np.sin)]).astype(np.float32)

    def step(x, dy, *arrays):
        w, m, v = (dict(zip(NAMES, some, strict=True)) for some in (arrays[:n], arrays[n : 2 * n], arrays[2 * n :]))
        wp, gp, last = update({"x": x[0], "dy": dy[0], "turns": jnp.asarray(turns)}, w.values(), m.values(), v.values())
        new, new_m, new_v = unpack(wp, gp, m, v)
        new |= dict(zip(LATE, finish(last, wp)))
        return (*(new[name] for name in NAMES), *new_m, *new_v)

    n = len(NAMES)
    return jax.shard_map(
        step,
        mesh=mesh,
        in_specs=(P(("rep", "dp")),) * 2 + (P(),) * n + (P(None, "dp"),) * (2 * n),
        out_specs=(P("rep"),) * n + (P("rep", "dp"),) * (2 * n),
        check_vma=False,
    )
```
